32 devices in a mesh: dp: 8 (over z, x), seq: 4 (over y, core).
Axes of the slice: x: 2, y: 2, z: 4, core: 2. Of those that a mesh axis runs over, the one named last changes fastest.
Arguments:
- hidden_in: bfloat16 [16, 2048, 768], P('dp', 'seq'), may hold values from -6 to 6
- w_query: bfloat16 [768, 768], P('seq', 'dp'), may hold values from -0.21875 to 0.21875
- w_key: bfloat16 [768, 768], P('seq', 'dp'), may hold values from -0.21875 to 0.21875
- w_value: bfloat16 [768, 768], P('seq', 'dp'), may hold values from -0.21875 to 0.21875
- w_output: bfloat16 [768, 768], P('seq', 'dp'), may hold values from -2.5 to 2.5
- w_inner: bfloat16 [768, 3072], P('seq', 'dp'), may hold values from -0.21875 to 0.21875
- w_outer: bfloat16 [3072, 768], P('dp', 'seq'), may hold values from -0.109375 to 0.109375
- pool_weight: float32 [2, 4, 768], P(None, None, ('dp', 'seq')), may hold values from -3 to 3
- ln_gain: float32 [2, 768], P(None, ('dp', 'seq')), may hold values from 0.25 to 1.75
- ln_bias: float32 [2, 768], P(None, ('dp', 'seq')), may hold values from -1.75 to 1.75
- branch_blocks: int32 [16, 8], P('dp'), may hold values from 64 to 256
- grad_out: bfloat16 [16, 2048, 768], P('dp', 'seq'), may hold values from -8 to 8
Outputs:
- hidden_out: bfloat16 [16, 2048, 768], P('dp', 'seq')
- grad_in: bfloat16 [16, 2048, 768], P('dp', 'seq')
- grad_query: float32 [768, 768], P('seq', 'dp')
- grad_key: float32 [768, 768], P('seq', 'dp')
- grad_value: float32 [768, 768], P('seq', 'dp')
- grad_output: float32 [768, 768], P('seq', 'dp')
- grad_inner: float32 [768, 3072], P('seq', 'dp')
- grad_outer: float32 [3072, 768], P('dp', 'seq')
- grad_pool: float32 [2, 4, 768], P(None, None, ('dp', 'seq'))
- grad_gain: float32 [2, 768], P(None, ('dp', 'seq'))
- grad_bias: float32 [2, 768], P(None, ('dp', 'seq'))
The draws below stay inside these ranges and needn't reach their ends.
Inputs may be any that keep to these rules, and one draw needn't show every extreme that they name: Continuation c of group g follows the first 4 * branch_blocks[g, c] tokens of the group's prompt.
All inputs are finite; a program needn't handle non-finite values.
Results may differ from the reference program's by a relative error of at most 0.017.
Values may be sent and summed in bfloat16 or wider, within the bound.
A program may use at most 256 MiB of HBM per device.

```python
import jax
import jax.numpy as jnp
from jax import lax

D = 768
HEADS = 12
HEAD_DIM = 64
FF = 3072
PROMPT = 1024
CONT = 8
CLEN = 128
WINDOW = 128
POOL_SPAN = 512
STRIDE = 4
GLEN = 2048
GROUPS = 16


def set_ends(entries, key, low, high):
    shape = entries.shape
    index_at = [jax.random.randint(jax.random.fold_in(key, axis), (), 0, shape[axis]) for axis in range(len(shape))]
    entries = entries.at[tuple(index_at)].set(low)
    longest = shape.index(max(shape))
    index_at[longest] = (index_at[longest] + 1) % shape[longest]
    return entries.at[tuple(index_at)].set(high)


def raised(array, stream_key, source, target, parts, factor):
    def block_of(axis_at):
        return (jnp.arange(array.shape[axis_at]) // (array.shape[axis_at] // parts)).reshape((-1,) + (1,) * (array.ndim - 1 - axis_at))

    near = jax.random.permutation(stream_key, parts)[block_of(target)]
    second = (block_of(target) + parts // 2) % parts
    return jnp.where((block_of(source) == near) | (block_of(source) == second), factor * array, array)


def steps_of(key, shape, cuts, least, high):
    factor_of, own = 1.0, jax.random.fold_in(key, 6)
    for dim, parts in cuts:
        steps = jnp.exp(jax.random.uniform(jax.random.fold_in(own, dim), (parts,), jnp.float32, least / len(cuts), high / len(cuts)))
        factor_of = factor_of * jnp.repeat(steps, shape[dim] // parts).reshape([-1 if axis == dim else 1 for axis in range(len(shape))])
    return factor_of


def noise(key, extent, width, bound, split=(), kind=jnp.bfloat16):
    entries = width * jax.random.normal(key, extent, jnp.float32)
    if split:
        entries = entries * steps_of(key, extent, split, -0.22, 0.18)
    return jnp.clip(entries, -bound, bound).astype(kind)


def heavy_noise(stream_key, shape, scale, limit, shards, heavy, kind=jnp.bfloat16):
    result = scale * jax.random.normal(stream_key, shape, jnp.float32)
    if shards:
        result = result * steps_of(stream_key, shape, shards, -0.22, 0.18)
    return jnp.clip(raised(result, jax.random.fold_in(stream_key, 3), *heavy), -limit, limit).astype(kind)


def setup_inputs(seed: int = 0) -> dict:
    seeds = jax.random.split(jax.random.key(seed), 13)
    hidden_in = noise(seeds[0], (GROUPS, GLEN, D), 1.0, 6.0, ((0, 8), (1, 4)))
    w_query = noise(seeds[1], (D, D), D ** -0.5, 0.21875, ((0, 4), (1, 8)))
    w_key = noise(seeds[2], (D, D), D ** -0.5, 0.21875, ((0, 4), (1, 8)))
    w_value = noise(seeds[3], (D, D), D ** -0.5, 0.21875, ((0, 4), (1, 8)))
    w_output = noise(seeds[4], (D, D), (D // 128) ** -0.5, 2.5, ((0, 4), (1, 8)))
    w_inner = noise(seeds[5], (D, FF), D ** -0.5, 0.21875, ((0, 4), (1, 8)))
    w_outer = noise(seeds[6], (FF, D), FF ** -0.5, 0.109375, ((0, 8), (1, 4)))
    pool_weight = noise(seeds[7], (2, STRIDE, D), STRIDE ** -0.5, 3.0, ((2, 32),), jnp.float32)
    ln_gain = jnp.clip(1.0 + 0.15 * jax.random.normal(seeds[8], (2, D), jnp.float32), 0.25, 1.75)
    ln_bias = noise(seeds[9], (2, D), 0.3, 1.75, ((1, 32),), jnp.float32)
    branch_blocks = set_ends(jax.random.randint(seeds[10], (GROUPS, CONT), PROMPT // 16, PROMPT // 4 + 1), jax.random.fold_in(seeds[10], 1), PROMPT // 16, (PROMPT // 4 + 1) - 1).astype(jnp.int32)
    grad_out = heavy_noise(seeds[11], (GROUPS, GLEN, D), 1.0, 8.0, ((0, 8), (1, 4)), (0, 2, 8, 2.0))
    return dict(hidden_in=hidden_in, w_query=w_query, w_key=w_key, w_value=w_value, w_output=w_output, w_inner=w_inner, w_outer=w_outer, pool_weight=pool_weight, ln_gain=ln_gain, ln_bias=ln_bias, branch_blocks=branch_blocks, grad_out=grad_out)


@jax.custom_vjp
def low(v):
    return lax.optimization_barrier(v.astype(jnp.bfloat16)).astype(jnp.float32)

@jax.custom_vjp
def low_back(v):
    return v

def low_keep(v):
    return (low(v), None)

def low_pass(kept, grad):
    return (grad,)

def back_keep(v):
    return (v, None)

def back_low(kept, grad):
    return (low(grad),)
low.defvjp(low_keep, low_pass)
low_back.defvjp(back_keep, back_low)
eps_norm = 1e-05

def round_both(value):
    return low_back(low(value))

def matmul(left, right):
    return jnp.dot(left, right, precision=lax.Precision.HIGHEST)

def token_layout(positions_in, offsets):
    in_prompt = positions_in < PROMPT
    segment = jnp.where(in_prompt, -1, (positions_in - PROMPT) // CLEN)
    within = positions_in - PROMPT - segment * CLEN
    choose = (segment[:, None] == jnp.arange(CONT, dtype=jnp.int32)[None, :]).astype(jnp.int32)
    cont_start = lax.optimization_barrier(jnp.sum(choose * offsets[None, :], axis=1))
    position = jnp.where(in_prompt, positions_in, cont_start + within)
    prompt_limit = jnp.where(in_prompt, PROMPT, cont_start)
    return (segment, position, prompt_limit)

def visible_keys(query_rows, key_index, offsets, reach):
    query_seg, query_pos, query_limit = token_layout(query_rows, offsets)
    key_seg, key_pos, key_limit = token_layout(key_index, offsets)
    prompt_key = (key_seg[None, :] < 0) & (key_pos[None, :] < query_limit[:, None])
    own_key = (key_seg[None, :] == query_seg[:, None]) & (query_seg[:, None] >= 0)
    distance = key_pos[None, :] - query_pos[:, None]
    return (prompt_key | own_key) & (distance >= -(reach // 2)) & (distance < reach // 2)

def key_mask(query_rows, offsets):
    group_len = PROMPT + CONT * CLEN
    full_keys = jnp.arange(group_len, dtype=jnp.int32)
    pooled_keys = jnp.arange(group_len // STRIDE, dtype=jnp.int32) * STRIDE
    return jnp.concatenate([visible_keys(query_rows, full_keys, offsets, WINDOW), visible_keys(query_rows, pooled_keys, offsets, POOL_SPAN)], axis=1)

def pool_rows(source, weight):
    return lax.optimization_barrier(jnp.sum(source.reshape(source.shape[0] // STRIDE, STRIDE, source.shape[1]) * weight[None, :, :], axis=1))

def layer_norm(source, gain, bias):
    centre = lax.optimization_barrier(jnp.mean(source, axis=-1, keepdims=True))
    centred = source - centre
    spread = lax.optimization_barrier(jnp.mean(centred * centred, axis=-1, keepdims=True))
    return centred * lax.rsqrt(spread + eps_norm) * gain + bias

def block_forward(params, tokens_in, visible_mask):
    w_query, w_key, w_value, w_output, w_inner, w_outer, pool_weight, ln_gain, ln_bias = params
    queries = round_both(matmul(tokens_in, w_query))
    key_rows = round_both(matmul(tokens_in, w_key))
    value_rows = round_both(matmul(tokens_in, w_value))
    keys_all = jnp.concatenate([key_rows, low(pool_rows(key_rows, pool_weight[0]))], axis=0)
    values_all = jnp.concatenate([value_rows, low(pool_rows(value_rows, pool_weight[1]))], axis=0)
    score_scale = 1.0 / HEAD_DIM ** 0.5

    def one_head(head_index):
        head_query = lax.dynamic_slice_in_dim(queries, head_index * HEAD_DIM, HEAD_DIM, 1)
        head_keys = lax.dynamic_slice_in_dim(keys_all, head_index * HEAD_DIM, HEAD_DIM, 1)
        head_values = lax.dynamic_slice_in_dim(values_all, head_index * HEAD_DIM, HEAD_DIM, 1)
        scores = low_back(matmul(head_query, head_keys.T) * score_scale)
        scores = jnp.where(visible_mask, scores, -1000000000.0)
        attend_weights = jax.nn.softmax(scores, axis=1)
        return matmul(low(attend_weights), head_values)
    head_outputs = lax.map(jax.checkpoint(one_head), jnp.arange(HEADS, dtype=jnp.int32))
    attended = round_both(jnp.transpose(head_outputs, (1, 0, 2)).reshape(tokens_in.shape[0], -1))
    mixed_rows = tokens_in + low_back(matmul(attended, w_output))
    normed_first = layer_norm(mixed_rows, ln_gain[0], ln_bias[0])
    inner_act = low_back(matmul(low(normed_first), w_inner))
    active = low(jax.nn.gelu(inner_act, approximate=False))
    second = normed_first + low_back(matmul(active, w_outer))
    return layer_norm(second, ln_gain[1], ln_bias[1])

def add_pair(left_term, right_term):
    return left_term + right_term

def reference(hidden_in, w_query, w_key, w_value, w_output, w_inner, w_outer, pool_weight, ln_gain, ln_bias, branch_blocks, grad_out):
    params = (w_query.astype(jnp.float32), w_key.astype(jnp.float32), w_value.astype(jnp.float32), w_output.astype(jnp.float32), w_inner.astype(jnp.float32), w_outer.astype(jnp.float32), pool_weight.astype(jnp.float32), ln_gain.astype(jnp.float32), ln_bias.astype(jnp.float32))
    group_rows = jnp.arange(PROMPT + CONT * CLEN, dtype=jnp.int32)

    def one_group(accum, group_item):
        tokens_in, blocks, cotangent = group_item
        visible_mask = key_mask(group_rows, (STRIDE * blocks).astype(jnp.int32))

        def forward_only(weights_now, tokens_now):
            return block_forward(weights_now, tokens_now, visible_mask)
        output, pullback = jax.vjp(forward_only, params, tokens_in.astype(jnp.float32))
        weight_grads, grad_tokens = pullback(cotangent.astype(jnp.float32))
        accum = jax.tree.map(add_pair, accum, weight_grads)
        return (accum, (output.astype(jnp.bfloat16), grad_tokens.astype(jnp.bfloat16)))
    zeros_init = jax.tree.map(jnp.zeros_like, params)
    accum, (outputs, grads_in) = lax.scan(one_group, zeros_init, (hidden_in, branch_blocks, grad_out))
    return (outputs, grads_in, accum[0], accum[1], accum[2], accum[3], accum[4], accum[5], accum[6], accum[7], accum[8])
```

```python
from functools import partial

import jax
import jax.numpy as jnp
from jax import lax
from jax.sharding import PartitionSpec as P

HEADS = 12
HEAD_DIM = 64
PROMPT = 1024
CONT = 8
CLEN = 128
WINDOW = 128
POOL_SPAN = 512
STRIDE = 4


eps_norm = 1e-05


def token_layout(positions_in, offsets):
    in_prompt = positions_in < PROMPT
    segment = jnp.where(in_prompt, -1, (positions_in - PROMPT) // CLEN)
    within = positions_in - PROMPT - segment * CLEN
    choose = (segment[:, None] == jnp.arange(CONT, dtype=jnp.int32)[None, :]).astype(jnp.int32)
    cont_start = jnp.sum(choose * offsets[None, :], axis=1)
    position = jnp.where(in_prompt, positions_in, cont_start + within)
    prompt_limit = jnp.where(in_prompt, PROMPT, cont_start)
    return (segment, position, prompt_limit)


def visible_keys(query_rows, key_index, offsets, reach):
    query_seg, query_pos, query_limit = token_layout(query_rows, offsets)
    key_seg, key_pos, key_limit = token_layout(key_index, offsets)
    prompt_key = (key_seg[None, :] < 0) & (key_pos[None, :] < query_limit[:, None])
    own_key = (key_seg[None, :] == query_seg[:, None]) & (query_seg[:, None] >= 0)
    distance = key_pos[None, :] - query_pos[:, None]
    return (prompt_key | own_key) & (distance >= -(reach // 2)) & (distance < reach // 2)


def key_mask(query_rows, offsets):
    group_len = PROMPT + CONT * CLEN
    full_keys = jnp.arange(group_len, dtype=jnp.int32)
    pooled_keys = jnp.arange(group_len // STRIDE, dtype=jnp.int32) * STRIDE
    return jnp.concatenate(
        [
            visible_keys(query_rows, full_keys, offsets, WINDOW),
            visible_keys(query_rows, pooled_keys, offsets, POOL_SPAN),
        ],
        axis=1,
    )


def pool_rows(source, weight):
    return jnp.sum(
        source.reshape(source.shape[0] // STRIDE, STRIDE, source.shape[1]) * weight[None, :, :],
        axis=1,
    )


def unpool(pooled_grad, weight):
    return (pooled_grad[:, None, :] * weight[None, :, :]).reshape(-1, pooled_grad.shape[1])


def pool_grad(pooled_grad, source):
    blocks_view = source.astype(jnp.float32).reshape(-1, STRIDE, source.shape[1])
    return jnp.sum(pooled_grad[:, None, :] * blocks_view, axis=0)


def layer_norm(source, gain, bias):
    centre = jnp.mean(source, axis=-1, keepdims=True)
    centred = source - centre
    spread = jnp.mean(centred * centred, axis=-1, keepdims=True)
    return centred * lax.rsqrt(spread + eps_norm) * gain + bias


def product(left, right):
    return jnp.dot(left, right, preferred_element_type=jnp.float32)


def product_left(left, right):
    return lax.dot_general(
        left, right, (((0,), (0,)), ((), ())), preferred_element_type=jnp.float32
    )


def product_right(left, right):
    return lax.dot_general(
        left, right, (((1,), (1,)), ((), ())), preferred_element_type=jnp.float32
    )


def add_pair(left_term, right_term):
    return left_term + right_term


def gather_weights(w_query, w_key, w_value, w_output, w_inner, w_outer):
    partial_rows = (
        lax.all_gather(w_query, "seq", axis=0, tiled=True),
        lax.all_gather(w_key, "seq", axis=0, tiled=True),
        lax.all_gather(w_value, "seq", axis=0, tiled=True),
        lax.all_gather(w_output, "seq", axis=0, tiled=True),
        lax.all_gather(w_inner, "seq", axis=0, tiled=True),
        lax.all_gather(w_outer, "seq", axis=1, tiled=True),
    )
    return (
        lax.all_gather(partial_rows[0], "dp", axis=1, tiled=True),
        lax.all_gather(partial_rows[1], "dp", axis=1, tiled=True),
        lax.all_gather(partial_rows[2], "dp", axis=1, tiled=True),
        lax.all_gather(partial_rows[3], "dp", axis=1, tiled=True),
        lax.all_gather(partial_rows[4], "dp", axis=1, tiled=True),
        lax.all_gather(partial_rows[5], "dp", axis=0, tiled=True),
    )


def reduce_grads(weight_grads):
    partial_sums = (
        lax.psum_scatter(weight_grads[0], "dp", scatter_dimension=1, tiled=True),
        lax.psum_scatter(weight_grads[1], "dp", scatter_dimension=1, tiled=True),
        lax.psum_scatter(weight_grads[2], "dp", scatter_dimension=1, tiled=True),
        lax.psum_scatter(weight_grads[3], "dp", scatter_dimension=1, tiled=True),
        lax.psum_scatter(weight_grads[4], "dp", scatter_dimension=1, tiled=True),
        lax.psum_scatter(weight_grads[5], "dp", scatter_dimension=0, tiled=True),
    )
    return (
        lax.psum_scatter(
            partial_sums[0].astype(jnp.bfloat16), "seq", scatter_dimension=0, tiled=True
        ).astype(jnp.float32),
        lax.psum_scatter(
            partial_sums[1].astype(jnp.bfloat16), "seq", scatter_dimension=0, tiled=True
        ).astype(jnp.float32),
        lax.psum_scatter(
            partial_sums[2].astype(jnp.bfloat16), "seq", scatter_dimension=0, tiled=True
        ).astype(jnp.float32),
        lax.psum_scatter(
            partial_sums[3].astype(jnp.bfloat16), "seq", scatter_dimension=0, tiled=True
        ).astype(jnp.float32),
        lax.psum_scatter(
            partial_sums[4].astype(jnp.bfloat16), "seq", scatter_dimension=0, tiled=True
        ).astype(jnp.float32),
        lax.psum_scatter(
            partial_sums[5].astype(jnp.bfloat16), "seq", scatter_dimension=1, tiled=True
        ).astype(jnp.float32),
    )


HALF_FULL = WINDOW // 2
HALF_POOL = POOL_SPAN // 2 // STRIDE
BLOCK_POOL = CLEN // STRIDE


def layout_of(index, offsets):
    in_prompt = index < PROMPT
    segment = jnp.where(in_prompt, -1, (index - PROMPT) // CLEN)
    within = index - PROMPT - segment * CLEN
    chosen = jnp.clip(segment, 0, CONT - 1)
    flat = chosen.reshape(chosen.shape[0], -1)
    cont_start = jnp.take_along_axis(offsets, flat, axis=1).reshape(index.shape)
    position = jnp.where(in_prompt, index, cont_start + within)
    limit = jnp.where(in_prompt, PROMPT, cont_start)
    return segment, position, limit


def window_rows(source, starts, length):
    groups, blocks = starts.shape
    return jnp.stack(
        [
            jnp.stack(
                [lax.dynamic_slice_in_dim(source[g], starts[g, b], length, 0) for b in range(blocks)]
            )
            for g in range(groups)
        ]
    )


def window_add(target, updates, starts):
    groups, blocks = starts.shape
    length = updates.shape[2]
    rows = []
    for g in range(groups):
        row = target[g]
        for b in range(blocks):
            start = starts[g, b]
            current = lax.dynamic_slice_in_dim(row, start, length, 0)
            row = lax.dynamic_update_slice_in_dim(row, current + updates[g, b], start, 0)
        rows.append(row)
    return jnp.stack(rows)


def block_geometry(seq_index, groups, shard_rows, offsets):
    group_len = PROMPT + CONT * CLEN
    pooled_len = group_len // STRIDE
    blocks = shard_rows // CLEN
    block_start = (seq_index * blocks + jnp.arange(blocks, dtype=jnp.int32)) * CLEN
    prompt_block = block_start < PROMPT
    cont_index = jnp.clip((block_start - PROMPT) // CLEN, 0, CONT - 1)
    anchor = jnp.where(prompt_block[None, :], block_start[None, :], offsets[:, cont_index])
    pooled_start = block_start // STRIDE
    intended = (
        anchor - HALF_FULL,
        jnp.broadcast_to(block_start + CLEN, anchor.shape),
        anchor // STRIDE - HALF_POOL,
        jnp.broadcast_to(pooled_start + BLOCK_POOL, anchor.shape),
    )
    limits = (group_len, group_len, pooled_len, pooled_len)
    lengths = (HALF_FULL, HALF_FULL, HALF_POOL, HALF_POOL)
    clamped = tuple(
        jnp.clip(start, 0, limit - length) for start, limit, length in zip(intended, limits, lengths)
    )
    ramp = lambda n: jnp.arange(n, dtype=jnp.int32)

    def span(window):
        actual = clamped[window][:, :, None] + ramp(lengths[window])
        offset = actual - intended[window][:, :, None]
        return actual, (offset >= 0) & (offset < lengths[window])

    before_full, before_full_ok = span(0)
    after_full, after_full_ok = span(1)
    before_pool, before_pool_ok = span(2)
    after_pool, after_pool_ok = span(3)
    after_ok = prompt_block[None, :, None]
    own_full = jnp.broadcast_to(block_start[None, :, None] + ramp(CLEN), anchor.shape + (CLEN,))
    own_pool = jnp.broadcast_to(
        pooled_start[None, :, None] + ramp(BLOCK_POOL), anchor.shape + (BLOCK_POOL,)
    )
    full_index = jnp.concatenate([before_full, own_full, after_full], axis=2)
    pooled_index = jnp.concatenate([before_pool, own_pool, after_pool], axis=2)
    full_valid = jnp.concatenate(
        [before_full_ok, jnp.ones(own_full.shape, bool), after_ok & after_full_ok], axis=2
    )
    pooled_valid = jnp.concatenate(
        [before_pool_ok, jnp.ones(own_pool.shape, bool), after_ok & after_pool_ok], axis=2
    )
    query_index = block_start[None, :, None] + ramp(CLEN)
    query_index = jnp.broadcast_to(query_index, anchor.shape + (CLEN,))
    q_seg, q_pos, q_lim = layout_of(query_index, offsets)

    def visible(key_token, valid, reach):
        k_seg, k_pos, _ = layout_of(key_token, offsets)
        k_seg, k_pos, valid = k_seg[:, :, None, :], k_pos[:, :, None, :], valid[:, :, None, :]
        prompt_key = (k_seg < 0) & (k_pos < q_lim[..., None])
        own_key = (k_seg == q_seg[..., None]) & (q_seg[..., None] >= 0)
        distance = k_pos - q_pos[..., None]
        return valid & (prompt_key | own_key) & (distance >= -(reach // 2)) & (distance < reach // 2)

    mask = jnp.concatenate(
        [
            visible(full_index, full_valid, WINDOW),
            visible(pooled_index * STRIDE, pooled_valid, POOL_SPAN),
        ],
        axis=3,
    )
    return clamped, mask


def attention_fwd(queries, kv_local, pkv_local, kv_all, pkv_all, starts, mask):
    groups, shard_rows, width = queries.shape
    blocks = shard_rows // CLEN
    score_scale = 1.0 / HEAD_DIM**0.5
    keys_cat = jnp.concatenate(
        [
            window_rows(kv_all, starts[0], HALF_FULL),
            kv_local.reshape(groups, blocks, CLEN, 2 * width),
            window_rows(kv_all, starts[1], HALF_FULL),
            window_rows(pkv_all, starts[2], HALF_POOL),
            pkv_local.reshape(groups, blocks, BLOCK_POOL, 2 * width),
            window_rows(pkv_all, starts[3], HALF_POOL),
        ],
        axis=2,
    )
    span = keys_cat.shape[2]
    head_keys = keys_cat[..., :width].reshape(groups, blocks, span, HEADS, HEAD_DIM)
    head_values = keys_cat[..., width:].reshape(groups, blocks, span, HEADS, HEAD_DIM)
    head_query = queries.reshape(groups, blocks, CLEN, HEADS, HEAD_DIM)
    scores = jnp.einsum(
        "gbqhd,gbkhd->gbhqk", head_query, head_keys, preferred_element_type=jnp.float32
    )
    scores = jnp.where(mask[:, :, None], scores * score_scale, -1000000000.0)
    row_top = jnp.max(scores, axis=-1, keepdims=True)
    exponent = jnp.exp(scores - row_top)
    row_total = jnp.sum(exponent, axis=-1, keepdims=True)
    probs = exponent / row_total
    attended = jnp.einsum(
        "gbhqk,gbkhd->gbqhd",
        probs.astype(jnp.bfloat16),
        head_values,
        preferred_element_type=jnp.float32,
    )
    attended = attended.reshape(groups * shard_rows, width).astype(jnp.bfloat16)
    return attended, (head_query, head_keys, head_values, probs)


def attention_bwd(grad_attended, saved, starts, seq_index):
    head_query, head_keys, head_values, probs = saved
    groups, blocks = head_query.shape[:2]
    width = HEADS * HEAD_DIM
    score_scale = 1.0 / HEAD_DIM**0.5
    head_grad = grad_attended.reshape(groups, blocks, CLEN, HEADS, HEAD_DIM)
    grad_probs = jnp.einsum(
        "gbqhd,gbkhd->gbhqk", head_grad, head_values, preferred_element_type=jnp.float32
    )
    centre = jnp.sum(probs * grad_probs, axis=-1, keepdims=True)
    grad_scores = (probs * (grad_probs - centre)).astype(jnp.bfloat16)
    grad_queries = jnp.einsum(
        "gbhqk,gbkhd->gbqhd", grad_scores, head_keys, preferred_element_type=jnp.float32
    ) * score_scale
    grad_keys = jnp.einsum(
        "gbhqk,gbqhd->gbkhd", grad_scores, head_query, preferred_element_type=jnp.float32
    ) * score_scale
    grad_values = jnp.einsum(
        "gbhqk,gbqhd->gbkhd",
        probs.astype(jnp.bfloat16),
        head_grad,
        preferred_element_type=jnp.float32,
    )
    span = grad_keys.shape[2]
    grad_kv = jnp.concatenate(
        [grad_keys.reshape(groups, blocks, span, width), grad_values.reshape(groups, blocks, span, width)],
        axis=3,
    )
    shard_rows = blocks * CLEN
    group_len = PROMPT + CONT * CLEN
    cut = (0, HALF_FULL, HALF_FULL + CLEN, 2 * HALF_FULL + CLEN)
    pcut = tuple(cut[-1] + c for c in (0, HALF_POOL, HALF_POOL + BLOCK_POOL, 2 * HALF_POOL + BLOCK_POOL))
    own_full = grad_kv[:, :, cut[1] : cut[2]].reshape(groups, shard_rows, 2 * width)
    own_pooled = grad_kv[:, :, pcut[1] : pcut[2]].reshape(groups, shard_rows // STRIDE, 2 * width)
    full = jnp.zeros((groups, group_len, 2 * width), jnp.float32)
    full = lax.dynamic_update_slice_in_dim(full, own_full, seq_index * shard_rows, 1)
    full = window_add(full, grad_kv[:, :, cut[0] : cut[1]], starts[0])
    full = window_add(full, grad_kv[:, :, cut[2] : cut[3]], starts[1])
    pooled = jnp.zeros((groups, group_len // STRIDE, 2 * width), jnp.float32)
    pooled = lax.dynamic_update_slice_in_dim(pooled, own_pooled, seq_index * shard_rows // STRIDE, 1)
    pooled = window_add(pooled, grad_kv[:, :, pcut[0] : pcut[1]], starts[2])
    pooled = window_add(pooled, grad_kv[:, :, pcut[2] : pcut[3]], starts[3])
    full = lax.psum_scatter(full, "seq", scatter_dimension=1, tiled=True)
    pooled = lax.psum_scatter(pooled, "seq", scatter_dimension=1, tiled=True)
    grad_queries = grad_queries.reshape(groups * shard_rows, width).astype(jnp.bfloat16)
    return grad_queries, full, pooled


def pool_grouped(source, weight):
    groups, rows, width = source.shape
    return jnp.sum(
        source.reshape(groups, rows // STRIDE, STRIDE, width) * weight[None, None], axis=2
    )


def unpool_grouped(pooled_grad, weight):
    groups, rows, width = pooled_grad.shape
    return (pooled_grad[:, :, None, :] * weight[None, None]).reshape(groups, rows * STRIDE, width)


def pool_grad_grouped(pooled_grad, source):
    groups, rows, width = source.shape
    blocks_view = source.astype(jnp.float32).reshape(groups, rows // STRIDE, STRIDE, width)
    return jnp.sum(pooled_grad[:, :, None, :] * blocks_view, axis=(0, 1))


def local(
    hidden_in,
    w_query,
    w_key,
    w_value,
    w_output,
    w_inner,
    w_outer,
    pool_weight,
    ln_gain,
    ln_bias,
    branch_blocks,
    grad_out,
):
    pool_full = lax.all_gather(pool_weight, ("dp", "seq"), axis=2, tiled=True)
    gain_full = lax.all_gather(ln_gain, ("dp", "seq"), axis=1, tiled=True)
    bias_full = lax.all_gather(ln_bias, ("dp", "seq"), axis=1, tiled=True)
    weights = gather_weights(w_query, w_key, w_value, w_output, w_inner, w_outer)
    wq, wk, wv, wo, wi, wu = weights
    groups, shard_rows, width = hidden_in.shape
    seq_index = lax.axis_index("seq")
    offsets = STRIDE * branch_blocks
    starts, mask = block_geometry(seq_index, groups, shard_rows, offsets)

    tokens = hidden_in.reshape(groups * shard_rows, width)
    queries = product(tokens, wq).astype(jnp.bfloat16)
    key_rows = product(tokens, wk).astype(jnp.bfloat16)
    value_rows = product(tokens, wv).astype(jnp.bfloat16)
    key_g = key_rows.reshape(groups, shard_rows, width)
    value_g = value_rows.reshape(groups, shard_rows, width)
    pooled_keys = pool_grouped(key_g.astype(jnp.float32), pool_full[0]).astype(jnp.bfloat16)
    pooled_values = pool_grouped(value_g.astype(jnp.float32), pool_full[1]).astype(jnp.bfloat16)
    kv_local = jnp.concatenate([key_g, value_g], axis=2)
    pkv_local = jnp.concatenate([pooled_keys, pooled_values], axis=2)
    kv_all = lax.all_gather(kv_local, "seq", axis=1, tiled=True)
    pkv_all = lax.all_gather(pkv_local, "seq", axis=1, tiled=True)
    attended, att_saved = attention_fwd(
        queries.reshape(groups, shard_rows, width), kv_local, pkv_local, kv_all, pkv_all, starts, mask
    )
    mixed_rows = tokens.astype(jnp.float32) + product(attended, wo)
    normed_first = layer_norm(mixed_rows, gain_full[0], bias_full[0])
    first_low = normed_first.astype(jnp.bfloat16)
    inner_act = product(first_low, wi)
    active = jax.nn.gelu(inner_act, approximate=False).astype(jnp.bfloat16)
    second = normed_first + product(active, wu)
    norm_value, second_back = jax.vjp(layer_norm, second, gain_full[1], bias_full[1])
    output = norm_value.astype(jnp.bfloat16)

    cotangent = grad_out.reshape(groups * shard_rows, width).astype(jnp.float32)
    grad_second, gain_second, bias_second = second_back(cotangent)
    grad_ffn_out = grad_second.astype(jnp.bfloat16)
    grad_outer = product_left(active, grad_ffn_out)
    grad_active = product_right(grad_ffn_out, wu)
    gelu_value, gelu_back = jax.vjp(partial(jax.nn.gelu, approximate=False), inner_act)
    grad_inner_act = gelu_back(grad_active)[0].astype(jnp.bfloat16)
    grad_inner = product_left(first_low, grad_inner_act)
    grad_first = grad_second + product_right(grad_inner_act, wi)
    first_value, first_back = jax.vjp(layer_norm, mixed_rows, gain_full[0], bias_full[0])
    grad_mixed, gain_first, bias_first = first_back(grad_first)
    grad_branch = grad_mixed.astype(jnp.bfloat16)
    grad_output = product_left(attended, grad_branch)
    grad_attended = product_right(grad_branch, wo).astype(jnp.bfloat16)

    grad_queries, grad_full, grad_pooled = attention_bwd(grad_attended, att_saved, starts, seq_index)
    grad_keys = (
        grad_full[..., :width] + unpool_grouped(grad_pooled[..., :width], pool_full[0])
    ).astype(jnp.bfloat16).reshape(groups * shard_rows, width)
    grad_values = (
        grad_full[..., width:] + unpool_grouped(grad_pooled[..., width:], pool_full[1])
    ).astype(jnp.bfloat16).reshape(groups * shard_rows, width)
    grad_pooling = jnp.stack(
        [
            pool_grad_grouped(grad_pooled[..., :width], key_g),
            pool_grad_grouped(grad_pooled[..., width:], value_g),
        ]
    )
    grad_query_w = product_left(tokens, grad_queries)
    grad_key_w = product_left(tokens, grad_keys)
    grad_value_w = product_left(tokens, grad_values)
    grad_tokens = (
        grad_mixed
        + product_right(grad_queries, wq)
        + product_right(grad_keys, wk)
        + product_right(grad_values, wv)
    )
    accum = reduce_grads((grad_query_w, grad_key_w, grad_value_w, grad_output, grad_inner, grad_outer))
    small_sums = (
        lax.psum_scatter(grad_pooling, ("dp", "seq"), scatter_dimension=2, tiled=True),
        lax.psum_scatter(
            jnp.stack([gain_first, gain_second]), ("dp", "seq"), scatter_dimension=1, tiled=True
        ),
        lax.psum_scatter(
            jnp.stack([bias_first, bias_second]), ("dp", "seq"), scatter_dimension=1, tiled=True
        ),
    )
    return (
        output.reshape(groups, shard_rows, width),
        grad_tokens.astype(jnp.bfloat16).reshape(groups, shard_rows, width),
        accum[0],
        accum[1],
        accum[2],
        accum[3],
        accum[4],
        accum[5],
        small_sums[0],
        small_sums[1],
        small_sums[2],
    )


def solution(mesh):
    in_specs = (
        P("dp", "seq", None),
        P("seq", "dp"),
        P("seq", "dp"),
        P("seq", "dp"),
        P("seq", "dp"),
        P("seq", "dp"),
        P("dp", "seq"),
        P(None, None, ("dp", "seq")),
        P(None, ("dp", "seq")),
        P(None, ("dp", "seq")),
        P("dp", None),
        P("dp", "seq", None),
    )
    out_specs = (
        P("dp", "seq", None),
        P("dp", "seq", None),
        P("seq", "dp"),
        P("seq", "dp"),
        P("seq", "dp"),
        P("seq", "dp"),
        P("seq", "dp"),
        P("dp", "seq"),
        P(None, None, ("dp", "seq")),
        P(None, ("dp", "seq")),
        P(None, ("dp", "seq")),
    )
    return jax.shard_map(local, mesh=mesh, in_specs=in_specs, out_specs=out_specs, check_vma=False)
```

```python
from functools import partial

import jax
import jax.numpy as jnp
from jax import lax
from jax.sharding import PartitionSpec as P

HEADS = 12
HEAD_DIM = 64
PROMPT = 1024
CONT = 8
CLEN = 128
WINDOW = 128
POOL_SPAN = 512
STRIDE = 4


eps_norm = 1e-05


def token_layout(positions_in, offsets):
    in_prompt = positions_in < PROMPT
    segment = jnp.where(in_prompt, -1, (positions_in - PROMPT) // CLEN)
    within = positions_in - PROMPT - segment * CLEN
    choose = (segment[:, None] == jnp.arange(CONT, dtype=jnp.int32)[None, :]).astype(jnp.int32)
    cont_start = jnp.sum(choose * offsets[None, :], axis=1)
    position = jnp.where(in_prompt, positions_in, cont_start + within)
    prompt_limit = jnp.where(in_prompt, PROMPT, cont_start)
    return (segment, position, prompt_limit)


def visible_keys(query_rows, key_index, offsets, reach):
    query_seg, query_pos, query_limit = token_layout(query_rows, offsets)
    key_seg, key_pos, key_limit = token_layout(key_index, offsets)
    prompt_key = (key_seg[None, :] < 0) & (key_pos[None, :] < query_limit[:, None])
    own_key = (key_seg[None, :] == query_seg[:, None]) & (query_seg[:, None] >= 0)
    distance = key_pos[None, :] - query_pos[:, None]
    return (prompt_key | own_key) & (distance >= -(reach // 2)) & (distance < reach // 2)


def key_mask(query_rows, offsets):
    group_len = PROMPT + CONT * CLEN
    full_keys = jnp.arange(group_len, dtype=jnp.int32)
    pooled_keys = jnp.arange(group_len // STRIDE, dtype=jnp.int32) * STRIDE
    return jnp.concatenate(
        [
            visible_keys(query_rows, full_keys, offsets, WINDOW),
            visible_keys(query_rows, pooled_keys, offsets, POOL_SPAN),
        ],
        axis=1,
    )


def pool_rows(source, weight):
    return jnp.sum(
        source.reshape(source.shape[0] // STRIDE, STRIDE, source.shape[1]) * weight[None, :, :],
        axis=1,
    )


def unpool(pooled_grad, weight):
    return (pooled_grad[:, None, :] * weight[None, :, :]).reshape(-1, pooled_grad.shape[1])


def pool_grad(pooled_grad, source):
    blocks_view = source.astype(jnp.float32).reshape(-1, STRIDE, source.shape[1])
    return jnp.sum(pooled_grad[:, None, :] * blocks_view, axis=0)


def layer_norm(source, gain, bias):
    centre = jnp.mean(source, axis=-1, keepdims=True)
    centred = source - centre
    spread = jnp.mean(centred * centred, axis=-1, keepdims=True)
    return centred * lax.rsqrt(spread + eps_norm) * gain + bias


def product(left, right):
    return jnp.dot(left, right, preferred_element_type=jnp.float32)


def product_left(left, right):
    return lax.dot_general(
        left, right, (((0,), (0,)), ((), ())), preferred_element_type=jnp.float32
    )


def product_right(left, right):
    return lax.dot_general(
        left, right, (((1,), (1,)), ((), ())), preferred_element_type=jnp.float32
    )


def add_pair(left_term, right_term):
    return left_term + right_term


def gather_grouped(shards):
    local_block = jnp.concatenate(shards, axis=1)
    across = lax.all_gather(local_block, "dp", axis=1, tiled=False)
    return lax.all_gather(across, "seq", axis=0, tiled=True)


def split_grouped(gathered, widths):
    pieces, at = [], 0
    for width in widths:
        piece = gathered[:, :, at : at + width]
        pieces.append(piece.reshape(piece.shape[0], -1))
        at += width
    return pieces


def gather_weights(w_query, w_key, w_value, w_output, w_inner, w_outer):
    first = gather_grouped((w_query, w_key, w_value))
    second = gather_grouped((w_output, w_inner, w_outer.T))
    wq, wk, wv = split_grouped(first, (w_query.shape[1], w_key.shape[1], w_value.shape[1]))
    wo, wi, wu_t = split_grouped(second, (w_output.shape[1], w_inner.shape[1], w_outer.shape[0]))
    return (wq, wk, wv, wo, wi, wu_t.T)


def reduce_grouped(grads):
    dp_size = lax.psum(1, "dp")
    chunks = [grad.reshape(grad.shape[0], dp_size, grad.shape[1] // dp_size) for grad in grads]
    stacked = jnp.concatenate(chunks, axis=2)
    over_seq = lax.psum_scatter(stacked, "seq", scatter_dimension=0, tiled=True)
    over_dp = lax.psum_scatter(over_seq.astype(jnp.bfloat16), "dp", scatter_dimension=1, tiled=True)
    over_dp = over_dp[:, 0].astype(jnp.float32)
    pieces, at = [], 0
    for chunk in chunks:
        pieces.append(over_dp[:, at : at + chunk.shape[2]])
        at += chunk.shape[2]
    return pieces


HALF_FULL = WINDOW // 2
HALF_POOL = POOL_SPAN // 2 // STRIDE
BLOCK_POOL = CLEN // STRIDE


def layout_of(index, offsets):
    in_prompt = index < PROMPT
    segment = jnp.where(in_prompt, -1, (index - PROMPT) // CLEN)
    within = index - PROMPT - segment * CLEN
    chosen = jnp.clip(segment, 0, CONT - 1)
    flat = chosen.reshape(chosen.shape[0], -1)
    cont_start = jnp.take_along_axis(offsets, flat, axis=1).reshape(index.shape)
    position = jnp.where(in_prompt, index, cont_start + within)
    limit = jnp.where(in_prompt, PROMPT, cont_start)
    return segment, position, limit


def window_rows(source, starts, length):
    groups, blocks = starts.shape
    return jnp.stack(
        [
            jnp.stack(
                [lax.dynamic_slice_in_dim(source[g], starts[g, b], length, 0) for b in range(blocks)]
            )
            for g in range(groups)
        ]
    )


def window_add(target, updates, starts):
    groups, blocks = starts.shape
    length = updates.shape[2]
    rows = []
    for g in range(groups):
        row = target[g]
        for b in range(blocks):
            start = starts[g, b]
            current = lax.dynamic_slice_in_dim(row, start, length, 0)
            row = lax.dynamic_update_slice_in_dim(row, current + updates[g, b], start, 0)
        rows.append(row)
    return jnp.stack(rows)


def block_geometry(seq_index, groups, shard_rows, offsets):
    group_len = PROMPT + CONT * CLEN
    pooled_len = group_len // STRIDE
    blocks = shard_rows // CLEN
    block_start = (seq_index * blocks + jnp.arange(blocks, dtype=jnp.int32)) * CLEN
    prompt_block = block_start < PROMPT
    cont_index = jnp.clip((block_start - PROMPT) // CLEN, 0, CONT - 1)
    anchor = jnp.where(prompt_block[None, :], block_start[None, :], offsets[:, cont_index])
    pooled_start = block_start // STRIDE
    intended = (
        anchor - HALF_FULL,
        jnp.broadcast_to(block_start + CLEN, anchor.shape),
        anchor // STRIDE - HALF_POOL,
        jnp.broadcast_to(pooled_start + BLOCK_POOL, anchor.shape),
    )
    limits = (group_len, group_len, pooled_len, pooled_len)
    lengths = (HALF_FULL, HALF_FULL, HALF_POOL, HALF_POOL)
    clamped = tuple(
        jnp.clip(start, 0, limit - length) for start, limit, length in zip(intended, limits, lengths)
    )
    ramp = lambda n: jnp.arange(n, dtype=jnp.int32)

    def span(window):
        actual = clamped[window][:, :, None] + ramp(lengths[window])
        offset = actual - intended[window][:, :, None]
        return actual, (offset >= 0) & (offset < lengths[window])

    before_full, before_full_ok = span(0)
    after_full, after_full_ok = span(1)
    before_pool, before_pool_ok = span(2)
    after_pool, after_pool_ok = span(3)
    after_ok = prompt_block[None, :, None]
    own_full = jnp.broadcast_to(block_start[None, :, None] + ramp(CLEN), anchor.shape + (CLEN,))
    own_pool = jnp.broadcast_to(
        pooled_start[None, :, None] + ramp(BLOCK_POOL), anchor.shape + (BLOCK_POOL,)
    )
    full_index = jnp.concatenate([before_full, own_full, after_full], axis=2)
    pooled_index = jnp.concatenate([before_pool, own_pool, after_pool], axis=2)
    full_valid = jnp.concatenate(
        [before_full_ok, jnp.ones(own_full.shape, bool), after_ok & after_full_ok], axis=2
    )
    pooled_valid = jnp.concatenate(
        [before_pool_ok, jnp.ones(own_pool.shape, bool), after_ok & after_pool_ok], axis=2
    )
    query_index = block_start[None, :, None] + ramp(CLEN)
    query_index = jnp.broadcast_to(query_index, anchor.shape + (CLEN,))
    q_seg, q_pos, q_lim = layout_of(query_index, offsets)

    def visible(key_token, valid, reach):
        k_seg, k_pos, _ = layout_of(key_token, offsets)
        k_seg, k_pos, valid = k_seg[:, :, None, :], k_pos[:, :, None, :], valid[:, :, None, :]
        prompt_key = (k_seg < 0) & (k_pos < q_lim[..., None])
        own_key = (k_seg == q_seg[..., None]) & (q_seg[..., None] >= 0)
        distance = k_pos - q_pos[..., None]
        return valid & (prompt_key | own_key) & (distance >= -(reach // 2)) & (distance < reach // 2)

    mask = jnp.concatenate(
        [
            visible(full_index, full_valid, WINDOW),
            visible(pooled_index * STRIDE, pooled_valid, POOL_SPAN),
        ],
        axis=3,
    )
    return clamped, mask


def attention_fwd(queries, kv_local, pkv_local, kv_all, pkv_all, starts, mask):
    groups, shard_rows, width = queries.shape
    blocks = shard_rows // CLEN
    score_scale = 1.0 / HEAD_DIM**0.5
    keys_cat = jnp.concatenate(
        [
            window_rows(kv_all, starts[0], HALF_FULL),
            kv_local.reshape(groups, blocks, CLEN, 2 * width),
            window_rows(kv_all, starts[1], HALF_FULL),
            window_rows(pkv_all, starts[2], HALF_POOL),
            pkv_local.reshape(groups, blocks, BLOCK_POOL, 2 * width),
            window_rows(pkv_all, starts[3], HALF_POOL),
        ],
        axis=2,
    )
    span = keys_cat.shape[2]
    head_keys = keys_cat[..., :width].reshape(groups, blocks, span, HEADS, HEAD_DIM)
    head_values = keys_cat[..., width:].reshape(groups, blocks, span, HEADS, HEAD_DIM)
    head_query = queries.reshape(groups, blocks, CLEN, HEADS, HEAD_DIM)
    scores = jnp.einsum(
        "gbqhd,gbkhd->gbhqk", head_query, head_keys, preferred_element_type=jnp.float32
    )
    scores = jnp.where(mask[:, :, None], scores * score_scale, -1000000000.0)
    row_top = jnp.max(scores, axis=-1, keepdims=True)
    exponent = jnp.exp(scores - row_top)
    row_total = jnp.sum(exponent, axis=-1, keepdims=True)
    probs = exponent / row_total
    attended = jnp.einsum(
        "gbhqk,gbkhd->gbqhd",
        probs.astype(jnp.bfloat16),
        head_values,
        preferred_element_type=jnp.float32,
    )
    attended = attended.reshape(groups * shard_rows, width).astype(jnp.bfloat16)
    return attended, (head_query, head_keys, head_values, probs)


def attention_bwd(grad_attended, saved, starts, seq_index):
    head_query, head_keys, head_values, probs = saved
    groups, blocks = head_query.shape[:2]
    width = HEADS * HEAD_DIM
    score_scale = 1.0 / HEAD_DIM**0.5
    head_grad = grad_attended.reshape(groups, blocks, CLEN, HEADS, HEAD_DIM)
    grad_probs = jnp.einsum(
        "gbqhd,gbkhd->gbhqk", head_grad, head_values, preferred_element_type=jnp.float32
    )
    centre = jnp.sum(probs * grad_probs, axis=-1, keepdims=True)
    grad_scores = (probs * (grad_probs - centre)).astype(jnp.bfloat16)
    grad_queries = jnp.einsum(
        "gbhqk,gbkhd->gbqhd", grad_scores, head_keys, preferred_element_type=jnp.float32
    ) * score_scale
    grad_keys = jnp.einsum(
        "gbhqk,gbqhd->gbkhd", grad_scores, head_query, preferred_element_type=jnp.float32
    ) * score_scale
    grad_values = jnp.einsum(
        "gbhqk,gbqhd->gbkhd",
        probs.astype(jnp.bfloat16),
        head_grad,
        preferred_element_type=jnp.float32,
    )
    span = grad_keys.shape[2]
    grad_kv = jnp.concatenate(
        [grad_keys.reshape(groups, blocks, span, width), grad_values.reshape(groups, blocks, span, width)],
        axis=3,
    )
    shard_rows = blocks * CLEN
    group_len = PROMPT + CONT * CLEN
    cut = (0, HALF_FULL, HALF_FULL + CLEN, 2 * HALF_FULL + CLEN)
    pcut = tuple(cut[-1] + c for c in (0, HALF_POOL, HALF_POOL + BLOCK_POOL, 2 * HALF_POOL + BLOCK_POOL))
    own_full = grad_kv[:, :, cut[1] : cut[2]].reshape(groups, shard_rows, 2 * width)
    own_pooled = grad_kv[:, :, pcut[1] : pcut[2]].reshape(groups, shard_rows // STRIDE, 2 * width)
    full = jnp.zeros((groups, group_len, 2 * width), jnp.float32)
    full = lax.dynamic_update_slice_in_dim(full, own_full, seq_index * shard_rows, 1)
    full = window_add(full, grad_kv[:, :, cut[0] : cut[1]], starts[0])
    full = window_add(full, grad_kv[:, :, cut[2] : cut[3]], starts[1])
    pooled = jnp.zeros((groups, group_len // STRIDE, 2 * width), jnp.float32)
    pooled = lax.dynamic_update_slice_in_dim(pooled, own_pooled, seq_index * shard_rows // STRIDE, 1)
    pooled = window_add(pooled, grad_kv[:, :, pcut[0] : pcut[1]], starts[2])
    pooled = window_add(pooled, grad_kv[:, :, pcut[2] : pcut[3]], starts[3])
    full = lax.psum_scatter(full, "seq", scatter_dimension=1, tiled=True)
    pooled = lax.psum_scatter(pooled, "seq", scatter_dimension=1, tiled=True)
    grad_queries = grad_queries.reshape(groups * shard_rows, width).astype(jnp.bfloat16)
    return grad_queries, full, pooled


def pool_grouped(source, weight):
    groups, rows, width = source.shape
    return jnp.sum(
        source.reshape(groups, rows // STRIDE, STRIDE, width) * weight[None, None], axis=2
    )


def unpool_grouped(pooled_grad, weight):
    groups, rows, width = pooled_grad.shape
    return (pooled_grad[:, :, None, :] * weight[None, None]).reshape(groups, rows * STRIDE, width)


def pool_grad_grouped(pooled_grad, source):
    groups, rows, width = source.shape
    blocks_view = source.astype(jnp.float32).reshape(groups, rows // STRIDE, STRIDE, width)
    return jnp.sum(pooled_grad[:, :, None, :] * blocks_view, axis=(0, 1))


def local(
    hidden_in,
    w_query,
    w_key,
    w_value,
    w_output,
    w_inner,
    w_outer,
    pool_weight,
    ln_gain,
    ln_bias,
    branch_blocks,
    grad_out,
):
    pool_full = lax.all_gather(pool_weight, ("dp", "seq"), axis=2, tiled=True)
    gain_full = lax.all_gather(ln_gain, ("dp", "seq"), axis=1, tiled=True)
    bias_full = lax.all_gather(ln_bias, ("dp", "seq"), axis=1, tiled=True)
    weights = gather_weights(w_query, w_key, w_value, w_output, w_inner, w_outer)
    wq, wk, wv, wo, wi, wu = weights
    groups, shard_rows, width = hidden_in.shape
    seq_index = lax.axis_index("seq")
    offsets = STRIDE * branch_blocks
    starts, mask = block_geometry(seq_index, groups, shard_rows, offsets)

    tokens = hidden_in.reshape(groups * shard_rows, width)
    queries = product(tokens, wq).astype(jnp.bfloat16)
    key_rows = product(tokens, wk).astype(jnp.bfloat16)
    value_rows = product(tokens, wv).astype(jnp.bfloat16)
    key_g = key_rows.reshape(groups, shard_rows, width)
    value_g = value_rows.reshape(groups, shard_rows, width)
    pooled_keys = pool_grouped(key_g.astype(jnp.float32), pool_full[0]).astype(jnp.bfloat16)
    pooled_values = pool_grouped(value_g.astype(jnp.float32), pool_full[1]).astype(jnp.bfloat16)
    kv_local = jnp.concatenate([key_g, value_g], axis=2)
    pkv_local = jnp.concatenate([pooled_keys, pooled_values], axis=2)
    kv_all = lax.all_gather(kv_local, "seq", axis=1, tiled=True)
    pkv_all = lax.all_gather(pkv_local, "seq", axis=1, tiled=True)
    attended, att_saved = attention_fwd(
        queries.reshape(groups, shard_rows, width), kv_local, pkv_local, kv_all, pkv_all, starts, mask
    )
    mixed_rows = tokens.astype(jnp.float32) + product(attended, wo)
    normed_first = layer_norm(mixed_rows, gain_full[0], bias_full[0])
    first_low = normed_first.astype(jnp.bfloat16)
    inner_act = product(first_low, wi)
    active = jax.nn.gelu(inner_act, approximate=False).astype(jnp.bfloat16)
    second = normed_first + product(active, wu)
    norm_value, second_back = jax.vjp(layer_norm, second, gain_full[1], bias_full[1])
    output = norm_value.astype(jnp.bfloat16)

    cotangent = grad_out.reshape(groups * shard_rows, width).astype(jnp.float32)
    grad_second, gain_second, bias_second = second_back(cotangent)
    grad_ffn_out = grad_second.astype(jnp.bfloat16)
    grad_outer = product_left(active, grad_ffn_out)
    grad_active = product_right(grad_ffn_out, wu)
    gelu_value, gelu_back = jax.vjp(partial(jax.nn.gelu, approximate=False), inner_act)
    grad_inner_act = gelu_back(grad_active)[0].astype(jnp.bfloat16)
    grad_inner = product_left(first_low, grad_inner_act)
    grad_first = grad_second + product_right(grad_inner_act, wi)
    first_value, first_back = jax.vjp(layer_norm, mixed_rows, gain_full[0], bias_full[0])
    grad_mixed, gain_first, bias_first = first_back(grad_first)
    grad_branch = grad_mixed.astype(jnp.bfloat16)
    grad_output = product_left(attended, grad_branch)
    grad_attended = product_right(grad_branch, wo).astype(jnp.bfloat16)
    early = reduce_grouped((grad_output, grad_inner, grad_outer.T))

    grad_queries, grad_full, grad_pooled = attention_bwd(grad_attended, att_saved, starts, seq_index)
    grad_keys = (
        grad_full[..., :width] + unpool_grouped(grad_pooled[..., :width], pool_full[0])
    ).astype(jnp.bfloat16).reshape(groups * shard_rows, width)
    grad_values = (
        grad_full[..., width:] + unpool_grouped(grad_pooled[..., width:], pool_full[1])
    ).astype(jnp.bfloat16).reshape(groups * shard_rows, width)
    grad_pooling = jnp.stack(
        [
            pool_grad_grouped(grad_pooled[..., :width], key_g),
            pool_grad_grouped(grad_pooled[..., width:], value_g),
        ]
    )
    grad_query_w = product_left(tokens, grad_queries)
    grad_key_w = product_left(tokens, grad_keys)
    grad_value_w = product_left(tokens, grad_values)
    grad_tokens = (
        grad_mixed
        + product_right(grad_queries, wq)
        + product_right(grad_keys, wk)
        + product_right(grad_values, wv)
    )
    late = reduce_grouped((grad_query_w, grad_key_w, grad_value_w))
    accum = (late[0], late[1], late[2], early[0], early[1], early[2].T)
    small_sums = (
        lax.psum_scatter(grad_pooling, ("dp", "seq"), scatter_dimension=2, tiled=True),
        lax.psum_scatter(
            jnp.stack([gain_first, gain_second]), ("dp", "seq"), scatter_dimension=1, tiled=True
        ),
        lax.psum_scatter(
            jnp.stack([bias_first, bias_second]), ("dp", "seq"), scatter_dimension=1, tiled=True
        ),
    )
    return (
        output.reshape(groups, shard_rows, width),
        grad_tokens.astype(jnp.bfloat16).reshape(groups, shard_rows, width),
        accum[0],
        accum[1],
        accum[2],
        accum[3],
        accum[4],
        accum[5],
        small_sums[0],
        small_sums[1],
        small_sums[2],
    )


def solution(mesh):
    in_specs = (
        P("dp", "seq", None),
        P("seq", "dp"),
        P("seq", "dp"),
        P("seq", "dp"),
        P("seq", "dp"),
        P("seq", "dp"),
        P("dp", "seq"),
        P(None, None, ("dp", "seq")),
        P(None, ("dp", "seq")),
        P(None, ("dp", "seq")),
        P("dp", None),
        P("dp", "seq", None),
    )
    out_specs = (
        P("dp", "seq", None),
        P("dp", "seq", None),
        P("seq", "dp"),
        P("seq", "dp"),
        P("seq", "dp"),
        P("seq", "dp"),
        P("seq", "dp"),
        P("dp", "seq"),
        P(None, None, ("dp", "seq")),
        P(None, ("dp", "seq")),
        P(None, ("dp", "seq")),
    )
    return jax.shard_map(local, mesh=mesh, in_specs=in_specs, out_specs=out_specs, check_vma=False)
```

```python
from functools import partial

import jax
import jax.numpy as jnp
from jax import lax
from jax.sharding import PartitionSpec as P

HEADS = 12
HEAD_DIM = 64
PROMPT = 1024
CONT = 8
CLEN = 128
WINDOW = 128
POOL_SPAN = 512
STRIDE = 4


eps_norm = 1e-05


def token_layout(positions_in, offsets):
    in_prompt = positions_in < PROMPT
    segment = jnp.where(in_prompt, -1, (positions_in - PROMPT) // CLEN)
    within = positions_in - PROMPT - segment * CLEN
    choose = (segment[:, None] == jnp.arange(CONT, dtype=jnp.int32)[None, :]).astype(jnp.int32)
    cont_start = jnp.sum(choose * offsets[None, :], axis=1)
    position = jnp.where(in_prompt, positions_in, cont_start + within)
    prompt_limit = jnp.where(in_prompt, PROMPT, cont_start)
    return (segment, position, prompt_limit)


def visible_keys(query_rows, key_index, offsets, reach):
    query_seg, query_pos, query_limit = token_layout(query_rows, offsets)
    key_seg, key_pos, key_limit = token_layout(key_index, offsets)
    prompt_key = (key_seg[None, :] < 0) & (key_pos[None, :] < query_limit[:, None])
    own_key = (key_seg[None, :] == query_seg[:, None]) & (query_seg[:, None] >= 0)
    distance = key_pos[None, :] - query_pos[:, None]
    return (prompt_key | own_key) & (distance >= -(reach // 2)) & (distance < reach // 2)


def key_mask(query_rows, offsets):
    group_len = PROMPT + CONT * CLEN
    full_keys = jnp.arange(group_len, dtype=jnp.int32)
    pooled_keys = jnp.arange(group_len // STRIDE, dtype=jnp.int32) * STRIDE
    return jnp.concatenate(
        [
            visible_keys(query_rows, full_keys, offsets, WINDOW),
            visible_keys(query_rows, pooled_keys, offsets, POOL_SPAN),
        ],
        axis=1,
    )


def pool_rows(source, weight):
    return jnp.sum(
        source.reshape(source.shape[0] // STRIDE, STRIDE, source.shape[1]) * weight[None, :, :],
        axis=1,
    )


def unpool(pooled_grad, weight):
    return (pooled_grad[:, None, :] * weight[None, :, :]).reshape(-1, pooled_grad.shape[1])


def pool_grad(pooled_grad, source):
    blocks_view = source.astype(jnp.float32).reshape(-1, STRIDE, source.shape[1])
    return jnp.sum(pooled_grad[:, None, :] * blocks_view, axis=0)


def layer_norm(source, gain, bias):
    centre = jnp.mean(source, axis=-1, keepdims=True)
    centred = source - centre
    spread = jnp.mean(centred * centred, axis=-1, keepdims=True)
    return centred * lax.rsqrt(spread + eps_norm) * gain + bias


def product(left, right):
    return jnp.dot(left, right, preferred_element_type=jnp.float32)


def product_left(left, right):
    return lax.dot_general(
        left, right, (((0,), (0,)), ((), ())), preferred_element_type=jnp.float32
    )


def product_right(left, right):
    return lax.dot_general(
        left, right, (((1,), (1,)), ((), ())), preferred_element_type=jnp.float32
    )


def add_pair(left_term, right_term):
    return left_term + right_term


def gather_grouped(shards):
    local_block = jnp.concatenate(shards, axis=1)
    across = lax.all_gather(local_block, "dp", axis=1, tiled=False)
    return lax.all_gather(across, "seq", axis=0, tiled=True)


def split_grouped(gathered, widths):
    pieces, at = [], 0
    for width in widths:
        piece = gathered[:, :, at : at + width]
        pieces.append(piece.reshape(piece.shape[0], -1))
        at += width
    return pieces


def gather_weights(w_query, w_key, w_value, w_output, w_inner, w_outer):
    first = gather_grouped((w_query, w_key, w_value))
    second = gather_grouped((w_output, w_inner, w_outer.T))
    wq, wk, wv = split_grouped(first, (w_query.shape[1], w_key.shape[1], w_value.shape[1]))
    wo, wi, wu_t = split_grouped(second, (w_output.shape[1], w_inner.shape[1], w_outer.shape[0]))
    return (wq, wk, wv, wo, wi, wu_t.T)


def reduce_seq_stage(grads):
    dp_size = lax.psum(1, "dp")
    chunks = [grad.reshape(grad.shape[0], dp_size, grad.shape[1] // dp_size) for grad in grads]
    stacked = jnp.concatenate(chunks, axis=2).astype(jnp.bfloat16)
    return lax.psum_scatter(stacked, "seq", scatter_dimension=0, tiled=True), [c.shape[2] for c in chunks]


def reduce_dp_stage(stages):
    joined = jnp.concatenate([stage for stage, _ in stages], axis=2)
    over_dp = lax.psum_scatter(joined, "dp", scatter_dimension=1, tiled=True)[:, 0].astype(jnp.float32)
    pieces, at = [], 0
    for _, widths in stages:
        for width in widths:
            pieces.append(over_dp[:, at : at + width])
            at += width
    return pieces


HALF_FULL = WINDOW // 2
HALF_POOL = POOL_SPAN // 2 // STRIDE
BLOCK_POOL = CLEN // STRIDE


def layout_of(index, offsets):
    in_prompt = index < PROMPT
    segment = jnp.where(in_prompt, -1, (index - PROMPT) // CLEN)
    within = index - PROMPT - segment * CLEN
    chosen = jnp.clip(segment, 0, CONT - 1)
    flat = chosen.reshape(chosen.shape[0], -1)
    cont_start = jnp.take_along_axis(offsets, flat, axis=1).reshape(index.shape)
    position = jnp.where(in_prompt, index, cont_start + within)
    limit = jnp.where(in_prompt, PROMPT, cont_start)
    return segment, position, limit


def window_rows(source, starts, length):
    groups, blocks = starts.shape
    return jnp.stack(
        [
            jnp.stack(
                [lax.dynamic_slice_in_dim(source[g], starts[g, b], length, 0) for b in range(blocks)]
            )
            for g in range(groups)
        ]
    )


def window_add(target, updates, starts):
    groups, blocks = starts.shape
    length = updates.shape[2]
    rows = []
    for g in range(groups):
        row = target[g]
        for b in range(blocks):
            start = starts[g, b]
            current = lax.dynamic_slice_in_dim(row, start, length, 0)
            row = lax.dynamic_update_slice_in_dim(row, current + updates[g, b], start, 0)
        rows.append(row)
    return jnp.stack(rows)


def block_geometry(seq_index, groups, shard_rows, offsets):
    group_len = PROMPT + CONT * CLEN
    pooled_len = group_len // STRIDE
    blocks = shard_rows // CLEN
    block_start = (seq_index * blocks + jnp.arange(blocks, dtype=jnp.int32)) * CLEN
    prompt_block = block_start < PROMPT
    cont_index = jnp.clip((block_start - PROMPT) // CLEN, 0, CONT - 1)
    anchor = jnp.where(prompt_block[None, :], block_start[None, :], offsets[:, cont_index])
    pooled_start = block_start // STRIDE
    intended = (
        anchor - HALF_FULL,
        jnp.broadcast_to(block_start + CLEN, anchor.shape),
        anchor // STRIDE - HALF_POOL,
        jnp.broadcast_to(pooled_start + BLOCK_POOL, anchor.shape),
    )
    limits = (group_len, group_len, pooled_len, pooled_len)
    lengths = (HALF_FULL, HALF_FULL, HALF_POOL, HALF_POOL)
    clamped = tuple(
        jnp.clip(start, 0, limit - length) for start, limit, length in zip(intended, limits, lengths)
    )
    ramp = lambda n: jnp.arange(n, dtype=jnp.int32)

    def span(window):
        actual = clamped[window][:, :, None] + ramp(lengths[window])
        offset = actual - intended[window][:, :, None]
        return actual, (offset >= 0) & (offset < lengths[window])

    before_full, before_full_ok = span(0)
    after_full, after_full_ok = span(1)
    before_pool, before_pool_ok = span(2)
    after_pool, after_pool_ok = span(3)
    after_ok = prompt_block[None, :, None]
    own_full = jnp.broadcast_to(block_start[None, :, None] + ramp(CLEN), anchor.shape + (CLEN,))
    own_pool = jnp.broadcast_to(
        pooled_start[None, :, None] + ramp(BLOCK_POOL), anchor.shape + (BLOCK_POOL,)
    )
    full_index = jnp.concatenate([before_full, own_full, after_full], axis=2)
    pooled_index = jnp.concatenate([before_pool, own_pool, after_pool], axis=2)
    full_valid = jnp.concatenate(
        [before_full_ok, jnp.ones(own_full.shape, bool), after_ok & after_full_ok], axis=2
    )
    pooled_valid = jnp.concatenate(
        [before_pool_ok, jnp.ones(own_pool.shape, bool), after_ok & after_pool_ok], axis=2
    )
    query_index = block_start[None, :, None] + ramp(CLEN)
    query_index = jnp.broadcast_to(query_index, anchor.shape + (CLEN,))
    q_seg, q_pos, q_lim = layout_of(query_index, offsets)

    def visible(key_token, valid, reach):
        k_seg, k_pos, _ = layout_of(key_token, offsets)
        k_seg, k_pos, valid = k_seg[:, :, None, :], k_pos[:, :, None, :], valid[:, :, None, :]
        prompt_key = (k_seg < 0) & (k_pos < q_lim[..., None])
        own_key = (k_seg == q_seg[..., None]) & (q_seg[..., None] >= 0)
        distance = k_pos - q_pos[..., None]
        return valid & (prompt_key | own_key) & (distance >= -(reach // 2)) & (distance < reach // 2)

    mask = jnp.concatenate(
        [
            visible(full_index, full_valid, WINDOW),
            visible(pooled_index * STRIDE, pooled_valid, POOL_SPAN),
        ],
        axis=3,
    )
    return clamped, mask


def attention_fwd(queries, kv_local, pkv_local, kv_all, pkv_all, starts, mask):
    groups, shard_rows, width = queries.shape
    blocks = shard_rows // CLEN
    score_scale = 1.0 / HEAD_DIM**0.5
    keys_cat = jnp.concatenate(
        [
            window_rows(kv_all, starts[0], HALF_FULL),
            kv_local.reshape(groups, blocks, CLEN, 2 * width),
            window_rows(kv_all, starts[1], HALF_FULL),
            window_rows(pkv_all, starts[2], HALF_POOL),
            pkv_local.reshape(groups, blocks, BLOCK_POOL, 2 * width),
            window_rows(pkv_all, starts[3], HALF_POOL),
        ],
        axis=2,
    )
    span = keys_cat.shape[2]
    head_keys = keys_cat[..., :width].reshape(groups, blocks, span, HEADS, HEAD_DIM)
    head_values = keys_cat[..., width:].reshape(groups, blocks, span, HEADS, HEAD_DIM)
    head_query = queries.reshape(groups, blocks, CLEN, HEADS, HEAD_DIM)
    scores = jnp.einsum(
        "gbqhd,gbkhd->gbhqk", head_query, head_keys, preferred_element_type=jnp.float32
    )
    scores = jnp.where(mask[:, :, None], scores * score_scale, -1000000000.0)
    row_top = jnp.max(scores, axis=-1, keepdims=True)
    exponent = jnp.exp(scores - row_top)
    row_total = jnp.sum(exponent, axis=-1, keepdims=True)
    probs = exponent / row_total
    attended = jnp.einsum(
        "gbhqk,gbkhd->gbqhd",
        probs.astype(jnp.bfloat16),
        head_values,
        preferred_element_type=jnp.float32,
    )
    attended = attended.reshape(groups * shard_rows, width).astype(jnp.bfloat16)
    return attended, (head_query, head_keys, head_values, probs)


def attention_bwd(grad_attended, saved, starts, seq_index):
    head_query, head_keys, head_values, probs = saved
    groups, blocks = head_query.shape[:2]
    width = HEADS * HEAD_DIM
    score_scale = 1.0 / HEAD_DIM**0.5
    head_grad = grad_attended.reshape(groups, blocks, CLEN, HEADS, HEAD_DIM)
    grad_probs = jnp.einsum(
        "gbqhd,gbkhd->gbhqk", head_grad, head_values, preferred_element_type=jnp.float32
    )
    centre = jnp.sum(probs * grad_probs, axis=-1, keepdims=True)
    grad_scores = (probs * (grad_probs - centre)).astype(jnp.bfloat16)
    grad_queries = jnp.einsum(
        "gbhqk,gbkhd->gbqhd", grad_scores, head_keys, preferred_element_type=jnp.float32
    ) * score_scale
    grad_keys = jnp.einsum(
        "gbhqk,gbqhd->gbkhd", grad_scores, head_query, preferred_element_type=jnp.float32
    ) * score_scale
    grad_values = jnp.einsum(
        "gbhqk,gbqhd->gbkhd",
        probs.astype(jnp.bfloat16),
        head_grad,
        preferred_element_type=jnp.float32,
    )
    span = grad_keys.shape[2]
    grad_kv = jnp.concatenate(
        [grad_keys.reshape(groups, blocks, span, width), grad_values.reshape(groups, blocks, span, width)],
        axis=3,
    )
    shard_rows = blocks * CLEN
    group_len = PROMPT + CONT * CLEN
    cut = (0, HALF_FULL, HALF_FULL + CLEN, 2 * HALF_FULL + CLEN)
    pcut = tuple(cut[-1] + c for c in (0, HALF_POOL, HALF_POOL + BLOCK_POOL, 2 * HALF_POOL + BLOCK_POOL))
    own_full = grad_kv[:, :, cut[1] : cut[2]].reshape(groups, shard_rows, 2 * width)
    own_pooled = grad_kv[:, :, pcut[1] : pcut[2]].reshape(groups, shard_rows // STRIDE, 2 * width)
    full = jnp.zeros((groups, group_len, 2 * width), jnp.float32)
    full = lax.dynamic_update_slice_in_dim(full, own_full, seq_index * shard_rows, 1)
    full = window_add(full, grad_kv[:, :, cut[0] : cut[1]], starts[0])
    full = window_add(full, grad_kv[:, :, cut[2] : cut[3]], starts[1])
    pooled = jnp.zeros((groups, group_len // STRIDE, 2 * width), jnp.float32)
    pooled = lax.dynamic_update_slice_in_dim(pooled, own_pooled, seq_index * shard_rows // STRIDE, 1)
    pooled = window_add(pooled, grad_kv[:, :, pcut[0] : pcut[1]], starts[2])
    pooled = window_add(pooled, grad_kv[:, :, pcut[2] : pcut[3]], starts[3])
    full = lax.psum_scatter(full.astype(jnp.bfloat16), "seq", scatter_dimension=1, tiled=True)
    pooled = lax.psum_scatter(pooled.astype(jnp.bfloat16), "seq", scatter_dimension=1, tiled=True)
    full = full.astype(jnp.float32)
    pooled = pooled.astype(jnp.float32)
    grad_queries = grad_queries.reshape(groups * shard_rows, width).astype(jnp.bfloat16)
    return grad_queries, full, pooled


def pool_grouped(source, weight):
    groups, rows, width = source.shape
    return jnp.sum(
        source.reshape(groups, rows // STRIDE, STRIDE, width) * weight[None, None], axis=2
    )


def unpool_grouped(pooled_grad, weight):
    groups, rows, width = pooled_grad.shape
    return (pooled_grad[:, :, None, :] * weight[None, None]).reshape(groups, rows * STRIDE, width)


def pool_grad_grouped(pooled_grad, source):
    groups, rows, width = source.shape
    blocks_view = source.astype(jnp.float32).reshape(groups, rows // STRIDE, STRIDE, width)
    return jnp.sum(pooled_grad[:, :, None, :] * blocks_view, axis=(0, 1))


def local(
    hidden_in,
    w_query,
    w_key,
    w_value,
    w_output,
    w_inner,
    w_outer,
    pool_weight,
    ln_gain,
    ln_bias,
    branch_blocks,
    grad_out,
):
    pool_rows_count = pool_weight.shape[0] * pool_weight.shape[1]
    small_local = jnp.concatenate(
        [pool_weight.reshape(pool_rows_count, -1), ln_gain, ln_bias], axis=0
    )
    small_full = lax.all_gather(small_local, ("dp", "seq"), axis=1, tiled=True)
    pool_full = small_full[:pool_rows_count].reshape(pool_weight.shape[0], pool_weight.shape[1], -1)
    gain_full = small_full[pool_rows_count : pool_rows_count + ln_gain.shape[0]]
    bias_full = small_full[pool_rows_count + ln_gain.shape[0] :]
    weights = gather_weights(w_query, w_key, w_value, w_output, w_inner, w_outer)
    wq, wk, wv, wo, wi, wu = weights
    groups, shard_rows, width = hidden_in.shape
    seq_index = lax.axis_index("seq")
    offsets = STRIDE * branch_blocks
    starts, mask = block_geometry(seq_index, groups, shard_rows, offsets)

    tokens = hidden_in.reshape(groups * shard_rows, width)
    queries = product(tokens, wq).astype(jnp.bfloat16)
    key_rows = product(tokens, wk).astype(jnp.bfloat16)
    value_rows = product(tokens, wv).astype(jnp.bfloat16)
    key_g = key_rows.reshape(groups, shard_rows, width)
    value_g = value_rows.reshape(groups, shard_rows, width)
    pooled_keys = pool_grouped(key_g.astype(jnp.float32), pool_full[0]).astype(jnp.bfloat16)
    pooled_values = pool_grouped(value_g.astype(jnp.float32), pool_full[1]).astype(jnp.bfloat16)
    kv_local = jnp.concatenate([key_g, value_g], axis=2)
    pkv_local = jnp.concatenate([pooled_keys, pooled_values], axis=2)
    kv_all = lax.all_gather(kv_local, "seq", axis=1, tiled=True)
    pkv_all = lax.all_gather(pkv_local, "seq", axis=1, tiled=True)
    attended, att_saved = attention_fwd(
        queries.reshape(groups, shard_rows, width), kv_local, pkv_local, kv_all, pkv_all, starts, mask
    )
    mixed_rows = tokens.astype(jnp.float32) + product(attended, wo)
    normed_first = layer_norm(mixed_rows, gain_full[0], bias_full[0])
    first_low = normed_first.astype(jnp.bfloat16)
    inner_act = product(first_low, wi)
    active = jax.nn.gelu(inner_act, approximate=False).astype(jnp.bfloat16)
    second = normed_first + product(active, wu)
    norm_value, second_back = jax.vjp(layer_norm, second, gain_full[1], bias_full[1])
    output = norm_value.astype(jnp.bfloat16)

    cotangent = grad_out.reshape(groups * shard_rows, width).astype(jnp.float32)
    grad_second, gain_second, bias_second = second_back(cotangent)
    grad_ffn_out = grad_second.astype(jnp.bfloat16)
    grad_outer = product_left(active, grad_ffn_out)
    grad_active = product_right(grad_ffn_out, wu)
    gelu_value, gelu_back = jax.vjp(partial(jax.nn.gelu, approximate=False), inner_act)
    grad_inner_act = gelu_back(grad_active)[0].astype(jnp.bfloat16)
    grad_inner = product_left(first_low, grad_inner_act)
    grad_first = grad_second + product_right(grad_inner_act, wi)
    first_value, first_back = jax.vjp(layer_norm, mixed_rows, gain_full[0], bias_full[0])
    grad_mixed, gain_first, bias_first = first_back(grad_first)
    grad_branch = grad_mixed.astype(jnp.bfloat16)
    grad_output = product_left(attended, grad_branch)
    grad_attended = product_right(grad_branch, wo).astype(jnp.bfloat16)
    early = reduce_seq_stage((grad_output, grad_inner, grad_outer.T))

    grad_queries, grad_full, grad_pooled = attention_bwd(grad_attended, att_saved, starts, seq_index)
    grad_keys = (
        grad_full[..., :width] + unpool_grouped(grad_pooled[..., :width], pool_full[0])
    ).astype(jnp.bfloat16).reshape(groups * shard_rows, width)
    grad_values = (
        grad_full[..., width:] + unpool_grouped(grad_pooled[..., width:], pool_full[1])
    ).astype(jnp.bfloat16).reshape(groups * shard_rows, width)
    grad_pooling = jnp.stack(
        [
            pool_grad_grouped(grad_pooled[..., :width], key_g),
            pool_grad_grouped(grad_pooled[..., width:], value_g),
        ]
    )
    grad_query_w = product_left(tokens, grad_queries)
    grad_key_w = product_left(tokens, grad_keys)
    grad_value_w = product_left(tokens, grad_values)
    grad_tokens = (
        grad_mixed
        + product_right(grad_queries, wq)
        + product_right(grad_keys, wk)
        + product_right(grad_values, wv)
    )
    late = reduce_seq_stage((grad_query_w, grad_key_w, grad_value_w))
    pieces = reduce_dp_stage((early, late))
    accum = (pieces[3], pieces[4], pieces[5], pieces[0], pieces[1], pieces[2].T)
    small_sums = (
        lax.psum_scatter(grad_pooling, ("dp", "seq"), scatter_dimension=2, tiled=True),
        lax.psum_scatter(
            jnp.stack([gain_first, gain_second]), ("dp", "seq"), scatter_dimension=1, tiled=True
        ),
        lax.psum_scatter(
            jnp.stack([bias_first, bias_second]), ("dp", "seq"), scatter_dimension=1, tiled=True
        ),
    )
    return (
        output.reshape(groups, shard_rows, width),
        grad_tokens.astype(jnp.bfloat16).reshape(groups, shard_rows, width),
        accum[0],
        accum[1],
        accum[2],
        accum[3],
        accum[4],
        accum[5],
        small_sums[0],
        small_sums[1],
        small_sums[2],
    )


def solution(mesh):
    in_specs = (
        P("dp", "seq", None),
        P("seq", "dp"),
        P("seq", "dp"),
        P("seq", "dp"),
        P("seq", "dp"),
        P("seq", "dp"),
        P("dp", "seq"),
        P(None, None, ("dp", "seq")),
        P(None, ("dp", "seq")),
        P(None, ("dp", "seq")),
        P("dp", None),
        P("dp", "seq", None),
    )
    out_specs = (
        P("dp", "seq", None),
        P("dp", "seq", None),
        P("seq", "dp"),
        P("seq", "dp"),
        P("seq", "dp"),
        P("seq", "dp"),
        P("seq", "dp"),
        P("dp", "seq"),
        P(None, None, ("dp", "seq")),
        P(None, ("dp", "seq")),
        P(None, ("dp", "seq")),
    )
    return jax.shard_map(local, mesh=mesh, in_specs=in_specs, out_specs=out_specs, check_vma=False)
```

```python
from functools import partial

import jax
import jax.numpy as jnp
from jax import lax
from jax.sharding import PartitionSpec as P

HEADS = 12
HEAD_DIM = 64
PROMPT = 1024
CONT = 8
CLEN = 128
WINDOW = 128
POOL_SPAN = 512
STRIDE = 4


eps_norm = 1e-05


def token_layout(positions_in, offsets):
    in_prompt = positions_in < PROMPT
    segment = jnp.where(in_prompt, -1, (positions_in - PROMPT) // CLEN)
    within = positions_in - PROMPT - segment * CLEN
    choose = (segment[:, None] == jnp.arange(CONT, dtype=jnp.int32)[None, :]).astype(jnp.int32)
    cont_start = jnp.sum(choose * offsets[None, :], axis=1)
    position = jnp.where(in_prompt, positions_in, cont_start + within)
    prompt_limit = jnp.where(in_prompt, PROMPT, cont_start)
    return (segment, position, prompt_limit)


def visible_keys(query_rows, key_index, offsets, reach):
    query_seg, query_pos, query_limit = token_layout(query_rows, offsets)
    key_seg, key_pos, key_limit = token_layout(key_index, offsets)
    prompt_key = (key_seg[None, :] < 0) & (key_pos[None, :] < query_limit[:, None])
    own_key = (key_seg[None, :] == query_seg[:, None]) & (query_seg[:, None] >= 0)
    distance = key_pos[None, :] - query_pos[:, None]
    return (prompt_key | own_key) & (distance >= -(reach // 2)) & (distance < reach // 2)


def key_mask(query_rows, offsets):
    group_len = PROMPT + CONT * CLEN
    full_keys = jnp.arange(group_len, dtype=jnp.int32)
    pooled_keys = jnp.arange(group_len // STRIDE, dtype=jnp.int32) * STRIDE
    return jnp.concatenate(
        [
            visible_keys(query_rows, full_keys, offsets, WINDOW),
            visible_keys(query_rows, pooled_keys, offsets, POOL_SPAN),
        ],
        axis=1,
    )


def pool_rows(source, weight):
    return jnp.sum(
        source.reshape(source.shape[0] // STRIDE, STRIDE, source.shape[1]) * weight[None, :, :],
        axis=1,
    )


def unpool(pooled_grad, weight):
    return (pooled_grad[:, None, :] * weight[None, :, :]).reshape(-1, pooled_grad.shape[1])


def pool_grad(pooled_grad, source):
    blocks_view = source.astype(jnp.float32).reshape(-1, STRIDE, source.shape[1])
    return jnp.sum(pooled_grad[:, None, :] * blocks_view, axis=0)


def layer_norm(source, gain, bias):
    centre = jnp.mean(source, axis=-1, keepdims=True)
    centred = source - centre
    spread = jnp.mean(centred * centred, axis=-1, keepdims=True)
    return centred * lax.rsqrt(spread + eps_norm) * gain + bias


def product(left, right):
    return jnp.dot(left, right, preferred_element_type=jnp.float32)


def product_left(left, right):
    return lax.dot_general(
        left, right, (((0,), (0,)), ((), ())), preferred_element_type=jnp.float32
    )


def product_right(left, right):
    return lax.dot_general(
        left, right, (((1,), (1,)), ((), ())), preferred_element_type=jnp.float32
    )


def add_pair(left_term, right_term):
    return left_term + right_term


def gather_grouped(shards):
    local_block = jnp.concatenate(shards, axis=1)
    across = lax.all_gather(local_block, "dp", axis=1, tiled=False)
    return lax.all_gather(across, "seq", axis=0, tiled=True)


def split_grouped(gathered, widths):
    pieces, at = [], 0
    for width in widths:
        piece = gathered[:, :, at : at + width]
        pieces.append(piece.reshape(piece.shape[0], -1))
        at += width
    return pieces


def gather_first(w_query, w_key, w_value):
    first = gather_grouped((w_query, w_key, w_value))
    return split_grouped(first, (w_query.shape[1], w_key.shape[1], w_value.shape[1]))


def gather_second(w_output, w_inner, w_outer):
    second = gather_grouped((w_output, w_inner, w_outer.T))
    wo, wi, wu_t = split_grouped(second, (w_output.shape[1], w_inner.shape[1], w_outer.shape[0]))
    return (wo, wi, wu_t.T)


def reduce_seq_stage(grads):
    dp_size = lax.psum(1, "dp")
    chunks = [grad.reshape(grad.shape[0], dp_size, grad.shape[1] // dp_size) for grad in grads]
    stacked = jnp.concatenate(chunks, axis=2).astype(jnp.bfloat16)
    return lax.psum_scatter(stacked, "seq", scatter_dimension=0, tiled=True), [c.shape[2] for c in chunks]


def reduce_dp_stage(stages):
    joined = jnp.concatenate([stage for stage, _ in stages], axis=2)
    over_dp = lax.psum_scatter(joined, "dp", scatter_dimension=1, tiled=True)[:, 0].astype(jnp.float32)
    pieces, at = [], 0
    for _, widths in stages:
        for width in widths:
            pieces.append(over_dp[:, at : at + width])
            at += width
    return pieces


HALF_FULL = WINDOW // 2
HALF_POOL = POOL_SPAN // 2 // STRIDE
BLOCK_POOL = CLEN // STRIDE


def layout_of(index, offsets):
    in_prompt = index < PROMPT
    segment = jnp.where(in_prompt, -1, (index - PROMPT) // CLEN)
    within = index - PROMPT - segment * CLEN
    choose = segment[..., None] == jnp.arange(CONT, dtype=jnp.int32)
    spread = offsets.reshape(offsets.shape[:1] + (1,) * (index.ndim - 1) + offsets.shape[1:])
    cont_start = jnp.sum(jnp.where(choose, spread, 0), axis=-1)
    position = jnp.where(in_prompt, index, cont_start + within)
    limit = jnp.where(in_prompt, PROMPT, cont_start)
    return segment, position, limit


def window_rows(source, starts, length):
    groups, blocks = starts.shape
    return jnp.stack(
        [
            jnp.stack(
                [lax.dynamic_slice_in_dim(source[g], starts[g, b], length, 0) for b in range(blocks)]
            )
            for g in range(groups)
        ]
    )


def window_add(target, updates, starts):
    groups, blocks = starts.shape
    length = updates.shape[2]
    rows = []
    for g in range(groups):
        row = target[g]
        for b in range(blocks):
            start = starts[g, b]
            current = lax.dynamic_slice_in_dim(row, start, length, 0)
            row = lax.dynamic_update_slice_in_dim(row, current + updates[g, b], start, 0)
        rows.append(row)
    return jnp.stack(rows)


def block_geometry(seq_index, groups, shard_rows, offsets):
    group_len = PROMPT + CONT * CLEN
    pooled_len = group_len // STRIDE
    blocks = shard_rows // CLEN
    block_start = (seq_index * blocks + jnp.arange(blocks, dtype=jnp.int32)) * CLEN
    prompt_block = block_start < PROMPT
    cont_index = jnp.clip((block_start - PROMPT) // CLEN, 0, CONT - 1)
    anchor = jnp.where(prompt_block[None, :], block_start[None, :], offsets[:, cont_index])
    pooled_start = block_start // STRIDE
    intended = (
        anchor - HALF_FULL,
        jnp.broadcast_to(block_start + CLEN, anchor.shape),
        anchor // STRIDE - HALF_POOL,
        jnp.broadcast_to(pooled_start + BLOCK_POOL, anchor.shape),
    )
    limits = (group_len, group_len, pooled_len, pooled_len)
    lengths = (HALF_FULL, HALF_FULL, HALF_POOL, HALF_POOL)
    clamped = tuple(
        jnp.clip(start, 0, limit - length) for start, limit, length in zip(intended, limits, lengths)
    )
    ramp = lambda n: jnp.arange(n, dtype=jnp.int32)

    def span(window):
        actual = clamped[window][:, :, None] + ramp(lengths[window])
        offset = actual - intended[window][:, :, None]
        return actual, (offset >= 0) & (offset < lengths[window])

    before_full, before_full_ok = span(0)
    after_full, after_full_ok = span(1)
    before_pool, before_pool_ok = span(2)
    after_pool, after_pool_ok = span(3)
    after_ok = prompt_block[None, :, None]
    own_full = jnp.broadcast_to(block_start[None, :, None] + ramp(CLEN), anchor.shape + (CLEN,))
    own_pool = jnp.broadcast_to(
        pooled_start[None, :, None] + ramp(BLOCK_POOL), anchor.shape + (BLOCK_POOL,)
    )
    full_index = jnp.concatenate([before_full, own_full, after_full], axis=2)
    pooled_index = jnp.concatenate([before_pool, own_pool, after_pool], axis=2)
    full_valid = jnp.concatenate(
        [before_full_ok, jnp.ones(own_full.shape, bool), after_ok & after_full_ok], axis=2
    )
    pooled_valid = jnp.concatenate(
        [before_pool_ok, jnp.ones(own_pool.shape, bool), after_ok & after_pool_ok], axis=2
    )
    query_index = block_start[None, :, None] + ramp(CLEN)
    query_index = jnp.broadcast_to(query_index, anchor.shape + (CLEN,))
    q_seg, q_pos, q_lim = layout_of(query_index, offsets)

    def visible(key_token, valid, reach):
        k_seg, k_pos, _ = layout_of(key_token, offsets)
        k_seg, k_pos, valid = k_seg[:, :, None, :], k_pos[:, :, None, :], valid[:, :, None, :]
        prompt_key = (k_seg < 0) & (k_pos < q_lim[..., None])
        own_key = (k_seg == q_seg[..., None]) & (q_seg[..., None] >= 0)
        distance = k_pos - q_pos[..., None]
        return valid & (prompt_key | own_key) & (distance >= -(reach // 2)) & (distance < reach // 2)

    mask = jnp.concatenate(
        [
            visible(full_index, full_valid, WINDOW),
            visible(pooled_index * STRIDE, pooled_valid, POOL_SPAN),
        ],
        axis=3,
    )
    return clamped, mask


def attention_fwd(queries, kv_local, pkv_local, kv_all, pkv_all, starts, mask):
    groups, shard_rows, width = queries.shape
    blocks = shard_rows // CLEN
    score_scale = 1.0 / HEAD_DIM**0.5
    keys_cat = jnp.concatenate(
        [
            window_rows(kv_all, starts[0], HALF_FULL),
            kv_local.reshape(groups, blocks, CLEN, 2 * width),
            window_rows(kv_all, starts[1], HALF_FULL),
            window_rows(pkv_all, starts[2], HALF_POOL),
            pkv_local.reshape(groups, blocks, BLOCK_POOL, 2 * width),
            window_rows(pkv_all, starts[3], HALF_POOL),
        ],
        axis=2,
    )
    span = keys_cat.shape[2]
    head_keys = keys_cat[..., :width].reshape(groups, blocks, span, HEADS, HEAD_DIM)
    head_values = keys_cat[..., width:].reshape(groups, blocks, span, HEADS, HEAD_DIM)
    head_query = queries.reshape(groups, blocks, CLEN, HEADS, HEAD_DIM)
    scores = jnp.einsum(
        "gbqhd,gbkhd->gbhqk", head_query, head_keys, preferred_element_type=jnp.float32
    )
    scores = jnp.where(mask[:, :, None], scores * score_scale, -1000000000.0)
    row_top = jnp.max(scores, axis=-1, keepdims=True)
    exponent = jnp.exp(scores - row_top)
    row_total = jnp.sum(exponent, axis=-1, keepdims=True)
    probs = exponent / row_total
    attended = jnp.einsum(
        "gbhqk,gbkhd->gbqhd",
        probs.astype(jnp.bfloat16),
        head_values,
        preferred_element_type=jnp.float32,
    )
    attended = attended.reshape(groups * shard_rows, width).astype(jnp.bfloat16)
    return attended, (head_query, head_keys, head_values, probs)


def attention_bwd(grad_attended, saved, starts, seq_index):
    head_query, head_keys, head_values, probs = saved
    groups, blocks = head_query.shape[:2]
    width = HEADS * HEAD_DIM
    score_scale = 1.0 / HEAD_DIM**0.5
    head_grad = grad_attended.reshape(groups, blocks, CLEN, HEADS, HEAD_DIM)
    grad_probs = jnp.einsum(
        "gbqhd,gbkhd->gbhqk", head_grad, head_values, preferred_element_type=jnp.float32
    )
    centre = jnp.sum(probs * grad_probs, axis=-1, keepdims=True)
    grad_scores = (probs * (grad_probs - centre)).astype(jnp.bfloat16)
    grad_queries = jnp.einsum(
        "gbhqk,gbkhd->gbqhd", grad_scores, head_keys, preferred_element_type=jnp.float32
    ) * score_scale
    grad_keys = jnp.einsum(
        "gbhqk,gbqhd->gbkhd", grad_scores, head_query, preferred_element_type=jnp.float32
    ) * score_scale
    grad_values = jnp.einsum(
        "gbhqk,gbqhd->gbkhd",
        probs.astype(jnp.bfloat16),
        head_grad,
        preferred_element_type=jnp.float32,
    )
    span = grad_keys.shape[2]
    grad_kv = jnp.concatenate(
        [grad_keys.reshape(groups, blocks, span, width), grad_values.reshape(groups, blocks, span, width)],
        axis=3,
    )
    shard_rows = blocks * CLEN
    group_len = PROMPT + CONT * CLEN
    cut = (0, HALF_FULL, HALF_FULL + CLEN, 2 * HALF_FULL + CLEN)
    pcut = tuple(cut[-1] + c for c in (0, HALF_POOL, HALF_POOL + BLOCK_POOL, 2 * HALF_POOL + BLOCK_POOL))
    own_full = grad_kv[:, :, cut[1] : cut[2]].reshape(groups, shard_rows, 2 * width)
    own_pooled = grad_kv[:, :, pcut[1] : pcut[2]].reshape(groups, shard_rows // STRIDE, 2 * width)
    full = jnp.zeros((groups, group_len, 2 * width), jnp.float32)
    full = lax.dynamic_update_slice_in_dim(full, own_full, seq_index * shard_rows, 1)
    full = window_add(full, grad_kv[:, :, cut[0] : cut[1]], starts[0])
    full = window_add(full, grad_kv[:, :, cut[2] : cut[3]], starts[1])
    pooled = jnp.zeros((groups, group_len // STRIDE, 2 * width), jnp.float32)
    pooled = lax.dynamic_update_slice_in_dim(pooled, own_pooled, seq_index * shard_rows // STRIDE, 1)
    pooled = window_add(pooled, grad_kv[:, :, pcut[0] : pcut[1]], starts[2])
    pooled = window_add(pooled, grad_kv[:, :, pcut[2] : pcut[3]], starts[3])
    full = lax.psum_scatter(full.astype(jnp.bfloat16), "seq", scatter_dimension=1, tiled=True)
    pooled = lax.psum_scatter(pooled.astype(jnp.bfloat16), "seq", scatter_dimension=1, tiled=True)
    full = full.astype(jnp.float32)
    pooled = pooled.astype(jnp.float32)
    grad_queries = grad_queries.reshape(groups * shard_rows, width).astype(jnp.bfloat16)
    return grad_queries, full, pooled


def pool_grouped(source, weight):
    groups, rows, width = source.shape
    return jnp.sum(
        source.reshape(groups, rows // STRIDE, STRIDE, width) * weight[None, None], axis=2
    )


def unpool_grouped(pooled_grad, weight):
    groups, rows, width = pooled_grad.shape
    return (pooled_grad[:, :, None, :] * weight[None, None]).reshape(groups, rows * STRIDE, width)


def pool_grad_grouped(pooled_grad, source):
    groups, rows, width = source.shape
    blocks_view = source.astype(jnp.float32).reshape(groups, rows // STRIDE, STRIDE, width)
    return jnp.sum(pooled_grad[:, :, None, :] * blocks_view, axis=(0, 1))


def local(
    hidden_in,
    w_query,
    w_key,
    w_value,
    w_output,
    w_inner,
    w_outer,
    pool_weight,
    ln_gain,
    ln_bias,
    branch_blocks,
    grad_out,
):
    pool_rows_count = pool_weight.shape[0] * pool_weight.shape[1]
    small_local = jnp.concatenate(
        [pool_weight.reshape(pool_rows_count, -1), ln_gain, ln_bias], axis=0
    )
    small_full = lax.all_gather(small_local, ("dp", "seq"), axis=1, tiled=True)
    pool_full = small_full[:pool_rows_count].reshape(pool_weight.shape[0], pool_weight.shape[1], -1)
    gain_full = small_full[pool_rows_count : pool_rows_count + ln_gain.shape[0]]
    bias_full = small_full[pool_rows_count + ln_gain.shape[0] :]
    wq, wk, wv = gather_first(w_query, w_key, w_value)
    groups, shard_rows, width = hidden_in.shape
    seq_index = lax.axis_index("seq")
    offsets = STRIDE * branch_blocks
    starts, mask = block_geometry(seq_index, groups, shard_rows, offsets)

    tokens = hidden_in.reshape(groups * shard_rows, width)
    queries = product(tokens, wq).astype(jnp.bfloat16)
    key_rows = product(tokens, wk).astype(jnp.bfloat16)
    value_rows = product(tokens, wv).astype(jnp.bfloat16)
    key_g = key_rows.reshape(groups, shard_rows, width)
    value_g = value_rows.reshape(groups, shard_rows, width)
    pooled_keys = pool_grouped(key_g.astype(jnp.float32), pool_full[0]).astype(jnp.bfloat16)
    pooled_values = pool_grouped(value_g.astype(jnp.float32), pool_full[1]).astype(jnp.bfloat16)
    kv_local = jnp.concatenate([key_g, value_g], axis=2)
    pkv_local = jnp.concatenate([pooled_keys, pooled_values], axis=2)
    kv_all = lax.all_gather(kv_local, "seq", axis=1, tiled=True)
    pkv_all = lax.all_gather(pkv_local, "seq", axis=1, tiled=True)
    kv_all, pkv_all, w_output, w_inner, w_outer = lax.optimization_barrier(
        (kv_all, pkv_all, w_output, w_inner, w_outer)
    )
    wo, wi, wu = gather_second(w_output, w_inner, w_outer)
    attended, att_saved = attention_fwd(
        queries.reshape(groups, shard_rows, width), kv_local, pkv_local, kv_all, pkv_all, starts, mask
    )
    mixed_rows = tokens.astype(jnp.float32) + product(attended, wo)
    normed_first = layer_norm(mixed_rows, gain_full[0], bias_full[0])
    first_low = normed_first.astype(jnp.bfloat16)
    inner_act = product(first_low, wi)
    active = jax.nn.gelu(inner_act, approximate=False).astype(jnp.bfloat16)
    second = normed_first + product(active, wu)
    norm_value, second_back = jax.vjp(layer_norm, second, gain_full[1], bias_full[1])
    output = norm_value.astype(jnp.bfloat16)

    cotangent = grad_out.reshape(groups * shard_rows, width).astype(jnp.float32)
    grad_second, gain_second, bias_second = second_back(cotangent)
    grad_ffn_out = grad_second.astype(jnp.bfloat16)
    grad_outer = product_left(active, grad_ffn_out)
    grad_active = product_right(grad_ffn_out, wu)
    gelu_value, gelu_back = jax.vjp(partial(jax.nn.gelu, approximate=False), inner_act)
    grad_inner_act = gelu_back(grad_active)[0].astype(jnp.bfloat16)
    grad_inner = product_left(first_low, grad_inner_act)
    grad_first = grad_second + product_right(grad_inner_act, wi)
    first_value, first_back = jax.vjp(layer_norm, mixed_rows, gain_full[0], bias_full[0])
    grad_mixed, gain_first, bias_first = first_back(grad_first)
    grad_branch = grad_mixed.astype(jnp.bfloat16)
    grad_output = product_left(attended, grad_branch)
    grad_attended = product_right(grad_branch, wo).astype(jnp.bfloat16)
    early = reduce_seq_stage((grad_output, grad_inner, grad_outer.T))

    grad_queries, grad_full, grad_pooled = attention_bwd(grad_attended, att_saved, starts, seq_index)
    grad_keys = (
        grad_full[..., :width] + unpool_grouped(grad_pooled[..., :width], pool_full[0])
    ).astype(jnp.bfloat16).reshape(groups * shard_rows, width)
    grad_values = (
        grad_full[..., width:] + unpool_grouped(grad_pooled[..., width:], pool_full[1])
    ).astype(jnp.bfloat16).reshape(groups * shard_rows, width)
    grad_pooling = jnp.stack(
        [
            pool_grad_grouped(grad_pooled[..., :width], key_g),
            pool_grad_grouped(grad_pooled[..., width:], value_g),
        ]
    )
    grad_query_w = product_left(tokens, grad_queries)
    grad_key_w = product_left(tokens, grad_keys)
    grad_value_w = product_left(tokens, grad_values)
    grad_tokens = (
        grad_mixed
        + product_right(grad_queries, wq)
        + product_right(grad_keys, wk)
        + product_right(grad_values, wv)
    )
    late = reduce_seq_stage((grad_query_w, grad_key_w, grad_value_w))
    pieces = reduce_dp_stage((early, late))
    accum = (pieces[3], pieces[4], pieces[5], pieces[0], pieces[1], pieces[2].T)
    small_sums = (
        lax.psum_scatter(grad_pooling, ("dp", "seq"), scatter_dimension=2, tiled=True),
        lax.psum_scatter(
            jnp.stack([gain_first, gain_second]), ("dp", "seq"), scatter_dimension=1, tiled=True
        ),
        lax.psum_scatter(
            jnp.stack([bias_first, bias_second]), ("dp", "seq"), scatter_dimension=1, tiled=True
        ),
    )
    return (
        output.reshape(groups, shard_rows, width),
        grad_tokens.astype(jnp.bfloat16).reshape(groups, shard_rows, width),
        accum[0],
        accum[1],
        accum[2],
        accum[3],
        accum[4],
        accum[5],
        small_sums[0],
        small_sums[1],
        small_sums[2],
    )


def solution(mesh):
    in_specs = (
        P("dp", "seq", None),
        P("seq", "dp"),
        P("seq", "dp"),
        P("seq", "dp"),
        P("seq", "dp"),
        P("seq", "dp"),
        P("dp", "seq"),
        P(None, None, ("dp", "seq")),
        P(None, ("dp", "seq")),
        P(None, ("dp", "seq")),
        P("dp", None),
        P("dp", "seq", None),
    )
    out_specs = (
        P("dp", "seq", None),
        P("dp", "seq", None),
        P("seq", "dp"),
        P("seq", "dp"),
        P("seq", "dp"),
        P("seq", "dp"),
        P("seq", "dp"),
        P("dp", "seq"),
        P(None, None, ("dp", "seq")),
        P(None, ("dp", "seq")),
        P(None, ("dp", "seq")),
    )
    return jax.shard_map(local, mesh=mesh, in_specs=in_specs, out_specs=out_specs, check_vma=False)
```

```python
from functools import partial

import jax
import jax.numpy as jnp
from jax import lax
from jax.sharding import PartitionSpec as P

HEADS = 12
HEAD_DIM = 64
PROMPT = 1024
CONT = 8
CLEN = 128
WINDOW = 128
POOL_SPAN = 512
STRIDE = 4


eps_norm = 1e-05


def token_layout(positions_in, offsets):
    in_prompt = positions_in < PROMPT
    segment = jnp.where(in_prompt, -1, (positions_in - PROMPT) // CLEN)
    within = positions_in - PROMPT - segment * CLEN
    choose = (segment[:, None] == jnp.arange(CONT, dtype=jnp.int32)[None, :]).astype(jnp.int32)
    cont_start = jnp.sum(choose * offsets[None, :], axis=1)
    position = jnp.where(in_prompt, positions_in, cont_start + within)
    prompt_limit = jnp.where(in_prompt, PROMPT, cont_start)
    return (segment, position, prompt_limit)


def visible_keys(query_rows, key_index, offsets, reach):
    query_seg, query_pos, query_limit = token_layout(query_rows, offsets)
    key_seg, key_pos, key_limit = token_layout(key_index, offsets)
    prompt_key = (key_seg[None, :] < 0) & (key_pos[None, :] < query_limit[:, None])
    own_key = (key_seg[None, :] == query_seg[:, None]) & (query_seg[:, None] >= 0)
    distance = key_pos[None, :] - query_pos[:, None]
    return (prompt_key | own_key) & (distance >= -(reach // 2)) & (distance < reach // 2)


def key_mask(query_rows, offsets):
    group_len = PROMPT + CONT * CLEN
    full_keys = jnp.arange(group_len, dtype=jnp.int32)
    pooled_keys = jnp.arange(group_len // STRIDE, dtype=jnp.int32) * STRIDE
    return jnp.concatenate(
        [
            visible_keys(query_rows, full_keys, offsets, WINDOW),
            visible_keys(query_rows, pooled_keys, offsets, POOL_SPAN),
        ],
        axis=1,
    )


def pool_rows(source, weight):
    return jnp.sum(
        source.reshape(source.shape[0] // STRIDE, STRIDE, source.shape[1]) * weight[None, :, :],
        axis=1,
    )


def unpool(pooled_grad, weight):
    return (pooled_grad[:, None, :] * weight[None, :, :]).reshape(-1, pooled_grad.shape[1])


def pool_grad(pooled_grad, source):
    blocks_view = source.astype(jnp.float32).reshape(-1, STRIDE, source.shape[1])
    return jnp.sum(pooled_grad[:, None, :] * blocks_view, axis=0)


def layer_norm(source, gain, bias):
    centre = jnp.mean(source, axis=-1, keepdims=True)
    centred = source - centre
    spread = jnp.mean(centred * centred, axis=-1, keepdims=True)
    return centred * lax.rsqrt(spread + eps_norm) * gain + bias


def product(left, right):
    return jnp.dot(left, right, preferred_element_type=jnp.float32)


def product_left(left, right):
    return lax.dot_general(
        left, right, (((0,), (0,)), ((), ())), preferred_element_type=jnp.float32
    )


def product_right(left, right):
    return lax.dot_general(
        left, right, (((1,), (1,)), ((), ())), preferred_element_type=jnp.float32
    )


def add_pair(left_term, right_term):
    return left_term + right_term


def gather_grouped(shards):
    local_block = jnp.concatenate(shards, axis=1)
    across = lax.all_gather(local_block, "dp", axis=1, tiled=False)
    return lax.all_gather(across, "seq", axis=0, tiled=True)


def split_grouped(gathered, widths):
    pieces, at = [], 0
    for width in widths:
        piece = gathered[:, :, at : at + width]
        pieces.append(piece.reshape(piece.shape[0], -1))
        at += width
    return pieces


def gather_first(w_query, w_key, w_value):
    first = gather_grouped((w_query, w_key, w_value))
    return split_grouped(first, (w_query.shape[1], w_key.shape[1], w_value.shape[1]))


def gather_second(w_output, w_inner, w_outer):
    second = gather_grouped((w_output, w_inner, w_outer.T))
    wo, wi, wu_t = split_grouped(second, (w_output.shape[1], w_inner.shape[1], w_outer.shape[0]))
    return (wo, wi, wu_t.T)


def reduce_seq_stage(grads):
    dp_size = lax.psum(1, "dp")
    chunks = [grad.reshape(grad.shape[0], dp_size, grad.shape[1] // dp_size) for grad in grads]
    stacked = jnp.concatenate(chunks, axis=2).astype(jnp.bfloat16)
    return lax.psum_scatter(stacked, "seq", scatter_dimension=0, tiled=True), [c.shape[2] for c in chunks]


def reduce_dp_stage(stages):
    joined = jnp.concatenate([stage for stage, _ in stages], axis=2)
    over_dp = lax.psum_scatter(joined, "dp", scatter_dimension=1, tiled=True)[:, 0].astype(jnp.float32)
    pieces, at = [], 0
    for _, widths in stages:
        for width in widths:
            pieces.append(over_dp[:, at : at + width])
            at += width
    return pieces


HALF_FULL = WINDOW // 2
HALF_POOL = POOL_SPAN // 2 // STRIDE
BLOCK_POOL = CLEN // STRIDE


def layout_of(index, offsets):
    in_prompt = index < PROMPT
    segment = jnp.where(in_prompt, -1, (index - PROMPT) // CLEN)
    within = index - PROMPT - segment * CLEN
    choose = segment[..., None] == jnp.arange(CONT, dtype=jnp.int32)
    spread = offsets.reshape(offsets.shape[:1] + (1,) * (index.ndim - 1) + offsets.shape[1:])
    cont_start = jnp.sum(jnp.where(choose, spread, 0), axis=-1)
    position = jnp.where(in_prompt, index, cont_start + within)
    limit = jnp.where(in_prompt, PROMPT, cont_start)
    return segment, position, limit


def window_rows(source, starts, length):
    groups, blocks = starts.shape
    return jnp.stack(
        [
            jnp.stack(
                [lax.dynamic_slice_in_dim(source[g], starts[g, b], length, 0) for b in range(blocks)]
            )
            for g in range(groups)
        ]
    )


def window_add(target, updates, starts):
    groups, blocks = starts.shape
    length = updates.shape[2]
    rows = []
    for g in range(groups):
        row = target[g]
        for b in range(blocks):
            start = starts[g, b]
            current = lax.dynamic_slice_in_dim(row, start, length, 0)
            row = lax.dynamic_update_slice_in_dim(row, current + updates[g, b], start, 0)
        rows.append(row)
    return jnp.stack(rows)


def block_geometry(seq_index, groups, shard_rows, offsets):
    group_len = PROMPT + CONT * CLEN
    pooled_len = group_len // STRIDE
    blocks = shard_rows // CLEN
    block_start = (seq_index * blocks + jnp.arange(blocks, dtype=jnp.int32)) * CLEN
    prompt_block = block_start < PROMPT
    cont_index = jnp.clip((block_start - PROMPT) // CLEN, 0, CONT - 1)
    anchor = jnp.where(prompt_block[None, :], block_start[None, :], offsets[:, cont_index])
    pooled_start = block_start // STRIDE
    intended = (
        anchor - HALF_FULL,
        jnp.broadcast_to(block_start + CLEN, anchor.shape),
        anchor // STRIDE - HALF_POOL,
        jnp.broadcast_to(pooled_start + BLOCK_POOL, anchor.shape),
    )
    limits = (group_len, group_len, pooled_len, pooled_len)
    lengths = (HALF_FULL, HALF_FULL, HALF_POOL, HALF_POOL)
    clamped = tuple(
        jnp.clip(start, 0, limit - length) for start, limit, length in zip(intended, limits, lengths)
    )
    ramp = lambda n: jnp.arange(n, dtype=jnp.int32)

    def span(window):
        actual = clamped[window][:, :, None] + ramp(lengths[window])
        offset = actual - intended[window][:, :, None]
        return actual, (offset >= 0) & (offset < lengths[window])

    before_full, before_full_ok = span(0)
    after_full, after_full_ok = span(1)
    before_pool, before_pool_ok = span(2)
    after_pool, after_pool_ok = span(3)
    after_ok = prompt_block[None, :, None]
    own_full = jnp.broadcast_to(block_start[None, :, None] + ramp(CLEN), anchor.shape + (CLEN,))
    own_pool = jnp.broadcast_to(
        pooled_start[None, :, None] + ramp(BLOCK_POOL), anchor.shape + (BLOCK_POOL,)
    )
    full_index = jnp.concatenate([before_full, own_full, after_full], axis=2)
    pooled_index = jnp.concatenate([before_pool, own_pool, after_pool], axis=2)
    full_valid = jnp.concatenate(
        [before_full_ok, jnp.ones(own_full.shape, bool), after_ok & after_full_ok], axis=2
    )
    pooled_valid = jnp.concatenate(
        [before_pool_ok, jnp.ones(own_pool.shape, bool), after_ok & after_pool_ok], axis=2
    )
    query_index = block_start[None, :, None] + ramp(CLEN)
    query_index = jnp.broadcast_to(query_index, anchor.shape + (CLEN,))
    q_seg, q_pos, q_lim = layout_of(query_index, offsets)

    def visible(key_token, valid, reach):
        k_seg, k_pos, _ = layout_of(key_token, offsets)
        k_seg, k_pos, valid = k_seg[:, :, None, :], k_pos[:, :, None, :], valid[:, :, None, :]
        prompt_key = (k_seg < 0) & (k_pos < q_lim[..., None])
        own_key = (k_seg == q_seg[..., None]) & (q_seg[..., None] >= 0)
        distance = k_pos - q_pos[..., None]
        return valid & (prompt_key | own_key) & (distance >= -(reach // 2)) & (distance < reach // 2)

    mask = jnp.concatenate(
        [
            visible(full_index, full_valid, WINDOW),
            visible(pooled_index * STRIDE, pooled_valid, POOL_SPAN),
        ],
        axis=3,
    )
    return clamped, mask


def attention_fwd(queries, kv_local, pkv_local, kv_all, pkv_all, starts, mask):
    groups, shard_rows, width = queries.shape
    blocks = shard_rows // CLEN
    score_scale = 1.0 / HEAD_DIM**0.5
    keys_cat = jnp.concatenate(
        [
            window_rows(kv_all, starts[0], HALF_FULL),
            kv_local.reshape(groups, blocks, CLEN, 2 * width),
            window_rows(kv_all, starts[1], HALF_FULL),
            window_rows(pkv_all, starts[2], HALF_POOL),
            pkv_local.reshape(groups, blocks, BLOCK_POOL, 2 * width),
            window_rows(pkv_all, starts[3], HALF_POOL),
        ],
        axis=2,
    )
    span = keys_cat.shape[2]
    head_keys = keys_cat[..., :width].reshape(groups, blocks, span, HEADS, HEAD_DIM)
    head_values = keys_cat[..., width:].reshape(groups, blocks, span, HEADS, HEAD_DIM)
    head_query = queries.reshape(groups, blocks, CLEN, HEADS, HEAD_DIM)
    scores = jnp.einsum(
        "gbqhd,gbkhd->gbhqk", head_query, head_keys, preferred_element_type=jnp.float32
    )
    scores = jnp.where(mask[:, :, None], scores * score_scale, -1000000000.0)
    row_top = jnp.max(scores, axis=-1, keepdims=True)
    exponent = jnp.exp(scores - row_top)
    row_total = jnp.sum(exponent, axis=-1, keepdims=True)
    probs = exponent / row_total
    attended = jnp.einsum(
        "gbhqk,gbkhd->gbqhd",
        probs.astype(jnp.bfloat16),
        head_values,
        preferred_element_type=jnp.float32,
    )
    attended = attended.reshape(groups * shard_rows, width).astype(jnp.bfloat16)
    return attended, (head_query, head_keys, head_values, probs)


def attention_bwd(grad_attended, saved, starts, seq_index):
    head_query, head_keys, head_values, probs = saved
    groups, blocks = head_query.shape[:2]
    width = HEADS * HEAD_DIM
    score_scale = 1.0 / HEAD_DIM**0.5
    head_grad = grad_attended.reshape(groups, blocks, CLEN, HEADS, HEAD_DIM)
    grad_probs = jnp.einsum(
        "gbqhd,gbkhd->gbhqk", head_grad, head_values, preferred_element_type=jnp.float32
    )
    centre = jnp.sum(probs * grad_probs, axis=-1, keepdims=True)
    grad_scores = (probs * (grad_probs - centre)).astype(jnp.bfloat16)
    grad_queries = jnp.einsum(
        "gbhqk,gbkhd->gbqhd", grad_scores, head_keys, preferred_element_type=jnp.float32
    ) * score_scale
    grad_keys = jnp.einsum(
        "gbhqk,gbqhd->gbkhd", grad_scores, head_query, preferred_element_type=jnp.float32
    ) * score_scale
    grad_values = jnp.einsum(
        "gbhqk,gbqhd->gbkhd",
        probs.astype(jnp.bfloat16),
        head_grad,
        preferred_element_type=jnp.float32,
    )
    span = grad_keys.shape[2]
    grad_kv = jnp.concatenate(
        [grad_keys.reshape(groups, blocks, span, width), grad_values.reshape(groups, blocks, span, width)],
        axis=3,
    )
    shard_rows = blocks * CLEN
    group_len = PROMPT + CONT * CLEN
    cut = (0, HALF_FULL, HALF_FULL + CLEN, 2 * HALF_FULL + CLEN)
    pcut = tuple(cut[-1] + c for c in (0, HALF_POOL, HALF_POOL + BLOCK_POOL, 2 * HALF_POOL + BLOCK_POOL))
    own_full = grad_kv[:, :, cut[1] : cut[2]].reshape(groups, shard_rows, 2 * width)
    own_pooled = grad_kv[:, :, pcut[1] : pcut[2]].reshape(groups, shard_rows // STRIDE, 2 * width)
    full = jnp.zeros((groups, group_len, 2 * width), jnp.float32)
    full = lax.dynamic_update_slice_in_dim(full, own_full, seq_index * shard_rows, 1)
    full = window_add(full, grad_kv[:, :, cut[0] : cut[1]], starts[0])
    full = window_add(full, grad_kv[:, :, cut[2] : cut[3]], starts[1])
    pooled = jnp.zeros((groups, group_len // STRIDE, 2 * width), jnp.float32)
    pooled = lax.dynamic_update_slice_in_dim(pooled, own_pooled, seq_index * shard_rows // STRIDE, 1)
    pooled = window_add(pooled, grad_kv[:, :, pcut[0] : pcut[1]], starts[2])
    pooled = window_add(pooled, grad_kv[:, :, pcut[2] : pcut[3]], starts[3])
    grad_queries = grad_queries.reshape(groups * shard_rows, width).astype(jnp.bfloat16)
    return grad_queries, full, pooled


def pool_grouped(source, weight):
    groups, rows, width = source.shape
    return jnp.sum(
        source.reshape(groups, rows // STRIDE, STRIDE, width) * weight[None, None], axis=2
    )


def unpool_grouped(pooled_grad, weight):
    groups, rows, width = pooled_grad.shape
    return (pooled_grad[:, :, None, :] * weight[None, None]).reshape(groups, rows * STRIDE, width)


def pool_grad_grouped(pooled_grad, source):
    groups, rows, width = source.shape
    blocks_view = source.astype(jnp.float32).reshape(groups, rows // STRIDE, STRIDE, width)
    return jnp.sum(pooled_grad[:, :, None, :] * blocks_view, axis=(0, 1))


def local(
    hidden_in,
    w_query,
    w_key,
    w_value,
    w_output,
    w_inner,
    w_outer,
    pool_weight,
    ln_gain,
    ln_bias,
    branch_blocks,
    grad_out,
):
    pool_rows_count = pool_weight.shape[0] * pool_weight.shape[1]
    small_local = jnp.concatenate(
        [pool_weight.reshape(pool_rows_count, -1), ln_gain, ln_bias], axis=0
    )
    small_full = lax.all_gather(small_local, ("dp", "seq"), axis=1, tiled=True)
    pool_full = small_full[:pool_rows_count].reshape(pool_weight.shape[0], pool_weight.shape[1], -1)
    gain_full = small_full[pool_rows_count : pool_rows_count + ln_gain.shape[0]]
    bias_full = small_full[pool_rows_count + ln_gain.shape[0] :]
    wq, wk, wv = gather_first(w_query, w_key, w_value)
    groups, shard_rows, width = hidden_in.shape
    seq_index = lax.axis_index("seq")
    offsets = STRIDE * branch_blocks
    starts, mask = block_geometry(seq_index, groups, shard_rows, offsets)

    hidden_all = lax.all_gather(hidden_in, "seq", axis=1, tiled=True)
    group_len = hidden_all.shape[1]
    tokens = hidden_in.reshape(groups * shard_rows, width)
    all_tokens = hidden_all.reshape(groups * group_len, width)
    queries = product(tokens, wq).astype(jnp.bfloat16)
    key_g = product(all_tokens, wk).astype(jnp.bfloat16).reshape(groups, group_len, width)
    value_g = product(all_tokens, wv).astype(jnp.bfloat16).reshape(groups, group_len, width)
    pooled_keys = pool_grouped(key_g.astype(jnp.float32), pool_full[0]).astype(jnp.bfloat16)
    pooled_values = pool_grouped(value_g.astype(jnp.float32), pool_full[1]).astype(jnp.bfloat16)
    kv_all = jnp.concatenate([key_g, value_g], axis=2)
    pkv_all = jnp.concatenate([pooled_keys, pooled_values], axis=2)
    kv_local = lax.dynamic_slice_in_dim(kv_all, seq_index * shard_rows, shard_rows, 1)
    pkv_local = lax.dynamic_slice_in_dim(
        pkv_all, seq_index * (shard_rows // STRIDE), shard_rows // STRIDE, 1
    )
    wq, wk, wv, w_output, w_inner, w_outer = lax.optimization_barrier(
        (wq, wk, wv, w_output, w_inner, w_outer)
    )
    wo, wi, wu = gather_second(w_output, w_inner, w_outer)
    attended, att_saved = attention_fwd(
        queries.reshape(groups, shard_rows, width), kv_local, pkv_local, kv_all, pkv_all, starts, mask
    )
    mixed_rows = tokens.astype(jnp.float32) + product(attended, wo)
    normed_first = layer_norm(mixed_rows, gain_full[0], bias_full[0])
    first_low = normed_first.astype(jnp.bfloat16)
    inner_act = product(first_low, wi)
    active = jax.nn.gelu(inner_act, approximate=False).astype(jnp.bfloat16)
    second = normed_first + product(active, wu)
    norm_value, second_back = jax.vjp(layer_norm, second, gain_full[1], bias_full[1])
    output = norm_value.astype(jnp.bfloat16)

    cotangent = grad_out.reshape(groups * shard_rows, width).astype(jnp.float32)
    grad_second, gain_second, bias_second = second_back(cotangent)
    grad_ffn_out = grad_second.astype(jnp.bfloat16)
    grad_outer = product_left(active, grad_ffn_out)
    grad_active = product_right(grad_ffn_out, wu)
    gelu_value, gelu_back = jax.vjp(partial(jax.nn.gelu, approximate=False), inner_act)
    grad_inner_act = gelu_back(grad_active)[0].astype(jnp.bfloat16)
    grad_inner = product_left(first_low, grad_inner_act)
    grad_first = grad_second + product_right(grad_inner_act, wi)
    first_value, first_back = jax.vjp(layer_norm, mixed_rows, gain_full[0], bias_full[0])
    grad_mixed, gain_first, bias_first = first_back(grad_first)
    grad_branch = grad_mixed.astype(jnp.bfloat16)
    grad_output = product_left(attended, grad_branch)
    grad_attended = product_right(grad_branch, wo).astype(jnp.bfloat16)
    early = reduce_seq_stage((grad_output, grad_inner, grad_outer.T))

    grad_queries, grad_full, grad_pooled = attention_bwd(grad_attended, att_saved, starts, seq_index)
    key_partial = (
        grad_full[..., :width] + unpool_grouped(grad_pooled[..., :width], pool_full[0])
    ).astype(jnp.bfloat16).reshape(groups * group_len, width)
    value_partial = (
        grad_full[..., width:] + unpool_grouped(grad_pooled[..., width:], pool_full[1])
    ).astype(jnp.bfloat16).reshape(groups * group_len, width)
    grad_pooling = jnp.stack(
        [
            pool_grad_grouped(grad_pooled[..., :width], key_g),
            pool_grad_grouped(grad_pooled[..., width:], value_g),
        ]
    )
    grad_query_w = product_left(tokens, grad_queries)
    grad_key_w = product_left(all_tokens, key_partial)
    grad_value_w = product_left(all_tokens, value_partial)
    back_rows = product_right(key_partial, wk) + product_right(value_partial, wv)
    back_rows = back_rows.reshape(groups, group_len, width).astype(jnp.bfloat16)
    back_own = lax.psum_scatter(back_rows, "seq", scatter_dimension=1, tiled=True)
    grad_tokens = (
        grad_mixed
        + product_right(grad_queries, wq)
        + back_own.reshape(groups * shard_rows, width).astype(jnp.float32)
    )
    late = reduce_seq_stage((grad_query_w, grad_key_w, grad_value_w))
    pieces = reduce_dp_stage((early, late))
    accum = (pieces[3], pieces[4], pieces[5], pieces[0], pieces[1], pieces[2].T)
    small_sums = (
        lax.psum_scatter(grad_pooling, ("dp", "seq"), scatter_dimension=2, tiled=True),
        lax.psum_scatter(
            jnp.stack([gain_first, gain_second]), ("dp", "seq"), scatter_dimension=1, tiled=True
        ),
        lax.psum_scatter(
            jnp.stack([bias_first, bias_second]), ("dp", "seq"), scatter_dimension=1, tiled=True
        ),
    )
    return (
        output.reshape(groups, shard_rows, width),
        grad_tokens.astype(jnp.bfloat16).reshape(groups, shard_rows, width),
        accum[0],
        accum[1],
        accum[2],
        accum[3],
        accum[4],
        accum[5],
        small_sums[0],
        small_sums[1],
        small_sums[2],
    )


def solution(mesh):
    in_specs = (
        P("dp", "seq", None),
        P("seq", "dp"),
        P("seq", "dp"),
        P("seq", "dp"),
        P("seq", "dp"),
        P("seq", "dp"),
        P("dp", "seq"),
        P(None, None, ("dp", "seq")),
        P(None, ("dp", "seq")),
        P(None, ("dp", "seq")),
        P("dp", None),
        P("dp", "seq", None),
    )
    out_specs = (
        P("dp", "seq", None),
        P("dp", "seq", None),
        P("seq", "dp"),
        P("seq", "dp"),
        P("seq", "dp"),
        P("seq", "dp"),
        P("seq", "dp"),
        P("dp", "seq"),
        P(None, None, ("dp", "seq")),
        P(None, ("dp", "seq")),
        P(None, ("dp", "seq")),
    )
    return jax.shard_map(local, mesh=mesh, in_specs=in_specs, out_specs=out_specs, check_vma=False)
```

```python
from functools import partial

import jax
import jax.numpy as jnp
from jax import lax
from jax.sharding import PartitionSpec as P

HEADS = 12
HEAD_DIM = 64
PROMPT = 1024
CONT = 8
CLEN = 128
WINDOW = 128
POOL_SPAN = 512
STRIDE = 4


eps_norm = 1e-05


def token_layout(positions_in, offsets):
    in_prompt = positions_in < PROMPT
    segment = jnp.where(in_prompt, -1, (positions_in - PROMPT) // CLEN)
    within = positions_in - PROMPT - segment * CLEN
    choose = (segment[:, None] == jnp.arange(CONT, dtype=jnp.int32)[None, :]).astype(jnp.int32)
    cont_start = jnp.sum(choose * offsets[None, :], axis=1)
    position = jnp.where(in_prompt, positions_in, cont_start + within)
    prompt_limit = jnp.where(in_prompt, PROMPT, cont_start)
    return (segment, position, prompt_limit)


def visible_keys(query_rows, key_index, offsets, reach):
    query_seg, query_pos, query_limit = token_layout(query_rows, offsets)
    key_seg, key_pos, key_limit = token_layout(key_index, offsets)
    prompt_key = (key_seg[None, :] < 0) & (key_pos[None, :] < query_limit[:, None])
    own_key = (key_seg[None, :] == query_seg[:, None]) & (query_seg[:, None] >= 0)
    distance = key_pos[None, :] - query_pos[:, None]
    return (prompt_key | own_key) & (distance >= -(reach // 2)) & (distance < reach // 2)


def key_mask(query_rows, offsets):
    group_len = PROMPT + CONT * CLEN
    full_keys = jnp.arange(group_len, dtype=jnp.int32)
    pooled_keys = jnp.arange(group_len // STRIDE, dtype=jnp.int32) * STRIDE
    return jnp.concatenate(
        [
            visible_keys(query_rows, full_keys, offsets, WINDOW),
            visible_keys(query_rows, pooled_keys, offsets, POOL_SPAN),
        ],
        axis=1,
    )


def pool_rows(source, weight):
    return jnp.sum(
        source.reshape(source.shape[0] // STRIDE, STRIDE, source.shape[1]) * weight[None, :, :],
        axis=1,
    )


def unpool(pooled_grad, weight):
    return (pooled_grad[:, None, :] * weight[None, :, :]).reshape(-1, pooled_grad.shape[1])


def pool_grad(pooled_grad, source):
    blocks_view = source.astype(jnp.float32).reshape(-1, STRIDE, source.shape[1])
    return jnp.sum(pooled_grad[:, None, :] * blocks_view, axis=0)


def layer_norm(source, gain, bias):
    centre = jnp.mean(source, axis=-1, keepdims=True)
    centred = source - centre
    spread = jnp.mean(centred * centred, axis=-1, keepdims=True)
    return centred * lax.rsqrt(spread + eps_norm) * gain + bias


def product(left, right):
    return jnp.dot(left, right, preferred_element_type=jnp.float32)


def product_left(left, right):
    return lax.dot_general(
        left, right, (((0,), (0,)), ((), ())), preferred_element_type=jnp.float32
    )


def product_right(left, right):
    return lax.dot_general(
        left, right, (((1,), (1,)), ((), ())), preferred_element_type=jnp.float32
    )


def add_pair(left_term, right_term):
    return left_term + right_term


def gather_grouped(shards):
    local_block = jnp.concatenate(shards, axis=1)
    across = lax.all_gather(local_block, "dp", axis=1, tiled=False)
    return lax.all_gather(across, "seq", axis=0, tiled=True)


def split_grouped(gathered, widths):
    pieces, at = [], 0
    for width in widths:
        piece = gathered[:, :, at : at + width]
        pieces.append(piece.reshape(piece.shape[0], -1))
        at += width
    return pieces


def gather_first(w_query, w_key, w_value):
    first = gather_grouped((w_query, w_key, w_value))
    return split_grouped(first, (w_query.shape[1], w_key.shape[1], w_value.shape[1]))


def gather_second(w_output, w_inner, w_outer):
    second = gather_grouped((w_output, w_inner, w_outer.T))
    wo, wi, wu_t = split_grouped(second, (w_output.shape[1], w_inner.shape[1], w_outer.shape[0]))
    return (wo, wi, wu_t.T)


def reduce_seq_stage(grads, tie=None):
    dp_size = lax.psum(1, "dp")
    chunks = [grad.reshape(grad.shape[0], dp_size, grad.shape[1] // dp_size) for grad in grads]
    stacked = jnp.concatenate(chunks, axis=2).astype(jnp.bfloat16)
    stacked, tie = lax.optimization_barrier((stacked, tie))
    reduced = lax.psum_scatter(stacked, "seq", scatter_dimension=0, tiled=True)
    return (reduced, [c.shape[2] for c in chunks]), tie


def reduce_dp_stage(stages):
    joined = jnp.concatenate([stage for stage, _ in stages], axis=2)
    over_dp = lax.psum_scatter(joined, "dp", scatter_dimension=1, tiled=True)[:, 0].astype(jnp.float32)
    pieces, at = [], 0
    for _, widths in stages:
        for width in widths:
            pieces.append(over_dp[:, at : at + width])
            at += width
    return pieces


HALF_FULL = WINDOW // 2
HALF_POOL = POOL_SPAN // 2 // STRIDE
BLOCK_POOL = CLEN // STRIDE


def layout_of(index, offsets):
    in_prompt = index < PROMPT
    segment = jnp.where(in_prompt, -1, (index - PROMPT) // CLEN)
    within = index - PROMPT - segment * CLEN
    choose = segment[..., None] == jnp.arange(CONT, dtype=jnp.int32)
    spread = offsets.reshape(offsets.shape[:1] + (1,) * (index.ndim - 1) + offsets.shape[1:])
    cont_start = jnp.sum(jnp.where(choose, spread, 0), axis=-1)
    position = jnp.where(in_prompt, index, cont_start + within)
    limit = jnp.where(in_prompt, PROMPT, cont_start)
    return segment, position, limit


def window_rows(source, starts, length):
    groups, blocks = starts.shape
    return jnp.stack(
        [
            jnp.stack(
                [lax.dynamic_slice_in_dim(source[g], starts[g, b], length, 0) for b in range(blocks)]
            )
            for g in range(groups)
        ]
    )


def window_add(target, updates, starts):
    groups, blocks = starts.shape
    length = updates.shape[2]
    rows = []
    for g in range(groups):
        row = target[g]
        for b in range(blocks):
            start = starts[g, b]
            current = lax.dynamic_slice_in_dim(row, start, length, 0)
            row = lax.dynamic_update_slice_in_dim(row, current + updates[g, b], start, 0)
        rows.append(row)
    return jnp.stack(rows)


def block_geometry(seq_index, groups, shard_rows, offsets):
    group_len = PROMPT + CONT * CLEN
    pooled_len = group_len // STRIDE
    blocks = shard_rows // CLEN
    block_start = (seq_index * blocks + jnp.arange(blocks, dtype=jnp.int32)) * CLEN
    prompt_block = block_start < PROMPT
    cont_index = jnp.clip((block_start - PROMPT) // CLEN, 0, CONT - 1)
    anchor = jnp.where(prompt_block[None, :], block_start[None, :], offsets[:, cont_index])
    pooled_start = block_start // STRIDE
    intended = (
        anchor - HALF_FULL,
        jnp.broadcast_to(block_start + CLEN, anchor.shape),
        anchor // STRIDE - HALF_POOL,
        jnp.broadcast_to(pooled_start + BLOCK_POOL, anchor.shape),
    )
    limits = (group_len, group_len, pooled_len, pooled_len)
    lengths = (HALF_FULL, HALF_FULL, HALF_POOL, HALF_POOL)
    clamped = tuple(
        jnp.clip(start, 0, limit - length) for start, limit, length in zip(intended, limits, lengths)
    )
    ramp = lambda n: jnp.arange(n, dtype=jnp.int32)

    def span(window):
        actual = clamped[window][:, :, None] + ramp(lengths[window])
        offset = actual - intended[window][:, :, None]
        return actual, (offset >= 0) & (offset < lengths[window])

    before_full, before_full_ok = span(0)
    after_full, after_full_ok = span(1)
    before_pool, before_pool_ok = span(2)
    after_pool, after_pool_ok = span(3)
    after_ok = prompt_block[None, :, None]
    own_full = jnp.broadcast_to(block_start[None, :, None] + ramp(CLEN), anchor.shape + (CLEN,))
    own_pool = jnp.broadcast_to(
        pooled_start[None, :, None] + ramp(BLOCK_POOL), anchor.shape + (BLOCK_POOL,)
    )
    full_index = jnp.concatenate([before_full, own_full, after_full], axis=2)
    pooled_index = jnp.concatenate([before_pool, own_pool, after_pool], axis=2)
    full_valid = jnp.concatenate(
        [before_full_ok, jnp.ones(own_full.shape, bool), after_ok & after_full_ok], axis=2
    )
    pooled_valid = jnp.concatenate(
        [before_pool_ok, jnp.ones(own_pool.shape, bool), after_ok & after_pool_ok], axis=2
    )
    query_index = block_start[None, :, None] + ramp(CLEN)
    query_index = jnp.broadcast_to(query_index, anchor.shape + (CLEN,))
    q_seg, q_pos, q_lim = layout_of(query_index, offsets)

    def visible(key_token, valid, reach):
        k_seg, k_pos, _ = layout_of(key_token, offsets)
        k_seg, k_pos, valid = k_seg[:, :, None, :], k_pos[:, :, None, :], valid[:, :, None, :]
        prompt_key = (k_seg < 0) & (k_pos < q_lim[..., None])
        own_key = (k_seg == q_seg[..., None]) & (q_seg[..., None] >= 0)
        distance = k_pos - q_pos[..., None]
        return valid & (prompt_key | own_key) & (distance >= -(reach // 2)) & (distance < reach // 2)

    mask = jnp.concatenate(
        [
            visible(full_index, full_valid, WINDOW),
            visible(pooled_index * STRIDE, pooled_valid, POOL_SPAN),
        ],
        axis=3,
    )
    return clamped, mask


def attention_fwd(queries, kv_local, pkv_local, kv_all, pkv_all, starts, mask):
    groups, shard_rows, width = queries.shape
    blocks = shard_rows // CLEN
    score_scale = 1.0 / HEAD_DIM**0.5
    keys_cat = jnp.concatenate(
        [
            window_rows(kv_all, starts[0], HALF_FULL),
            kv_local.reshape(groups, blocks, CLEN, 2 * width),
            window_rows(kv_all, starts[1], HALF_FULL),
            window_rows(pkv_all, starts[2], HALF_POOL),
            pkv_local.reshape(groups, blocks, BLOCK_POOL, 2 * width),
            window_rows(pkv_all, starts[3], HALF_POOL),
        ],
        axis=2,
    )
    span = keys_cat.shape[2]
    head_keys = keys_cat[..., :width].reshape(groups, blocks, span, HEADS, HEAD_DIM)
    head_values = keys_cat[..., width:].reshape(groups, blocks, span, HEADS, HEAD_DIM)
    head_query = queries.reshape(groups, blocks, CLEN, HEADS, HEAD_DIM)
    scores = jnp.einsum(
        "gbqhd,gbkhd->gbhqk", head_query, head_keys, preferred_element_type=jnp.float32
    )
    scores = jnp.where(mask[:, :, None], scores * score_scale, -1000000000.0)
    row_top = jnp.max(scores, axis=-1, keepdims=True)
    exponent = jnp.exp(scores - row_top)
    row_total = jnp.sum(exponent, axis=-1, keepdims=True)
    probs = exponent / row_total
    attended = jnp.einsum(
        "gbhqk,gbkhd->gbqhd",
        probs.astype(jnp.bfloat16),
        head_values,
        preferred_element_type=jnp.float32,
    )
    attended = attended.reshape(groups * shard_rows, width).astype(jnp.bfloat16)
    return attended, (head_query, head_keys, head_values, probs)


def attention_bwd(grad_attended, saved, starts, seq_index):
    head_query, head_keys, head_values, probs = saved
    groups, blocks = head_query.shape[:2]
    width = HEADS * HEAD_DIM
    score_scale = 1.0 / HEAD_DIM**0.5
    head_grad = grad_attended.reshape(groups, blocks, CLEN, HEADS, HEAD_DIM)
    grad_probs = jnp.einsum(
        "gbqhd,gbkhd->gbhqk", head_grad, head_values, preferred_element_type=jnp.float32
    )
    centre = jnp.sum(probs * grad_probs, axis=-1, keepdims=True)
    grad_scores = (probs * (grad_probs - centre)).astype(jnp.bfloat16)
    grad_queries = jnp.einsum(
        "gbhqk,gbkhd->gbqhd", grad_scores, head_keys, preferred_element_type=jnp.float32
    ) * score_scale
    grad_keys = jnp.einsum(
        "gbhqk,gbqhd->gbkhd", grad_scores, head_query, preferred_element_type=jnp.float32
    ) * score_scale
    grad_values = jnp.einsum(
        "gbhqk,gbqhd->gbkhd",
        probs.astype(jnp.bfloat16),
        head_grad,
        preferred_element_type=jnp.float32,
    )
    span = grad_keys.shape[2]
    grad_kv = jnp.concatenate(
        [grad_keys.reshape(groups, blocks, span, width), grad_values.reshape(groups, blocks, span, width)],
        axis=3,
    )
    shard_rows = blocks * CLEN
    group_len = PROMPT + CONT * CLEN
    cut = (0, HALF_FULL, HALF_FULL + CLEN, 2 * HALF_FULL + CLEN)
    pcut = tuple(cut[-1] + c for c in (0, HALF_POOL, HALF_POOL + BLOCK_POOL, 2 * HALF_POOL + BLOCK_POOL))
    own_full = grad_kv[:, :, cut[1] : cut[2]].reshape(groups, shard_rows, 2 * width)
    own_pooled = grad_kv[:, :, pcut[1] : pcut[2]].reshape(groups, shard_rows // STRIDE, 2 * width)
    full = jnp.zeros((groups, group_len, 2 * width), jnp.float32)
    full = lax.dynamic_update_slice_in_dim(full, own_full, seq_index * shard_rows, 1)
    full = window_add(full, grad_kv[:, :, cut[0] : cut[1]], starts[0])
    full = window_add(full, grad_kv[:, :, cut[2] : cut[3]], starts[1])
    pooled = jnp.zeros((groups, group_len // STRIDE, 2 * width), jnp.float32)
    pooled = lax.dynamic_update_slice_in_dim(pooled, own_pooled, seq_index * shard_rows // STRIDE, 1)
    pooled = window_add(pooled, grad_kv[:, :, pcut[0] : pcut[1]], starts[2])
    pooled = window_add(pooled, grad_kv[:, :, pcut[2] : pcut[3]], starts[3])
    grad_queries = grad_queries.reshape(groups * shard_rows, width).astype(jnp.bfloat16)
    return grad_queries, full, pooled


def pool_grouped(source, weight):
    groups, rows, width = source.shape
    return jnp.sum(
        source.reshape(groups, rows // STRIDE, STRIDE, width) * weight[None, None], axis=2
    )


def unpool_grouped(pooled_grad, weight):
    groups, rows, width = pooled_grad.shape
    return (pooled_grad[:, :, None, :] * weight[None, None]).reshape(groups, rows * STRIDE, width)


def pool_grad_grouped(pooled_grad, source):
    groups, rows, width = source.shape
    blocks_view = source.astype(jnp.float32).reshape(groups, rows // STRIDE, STRIDE, width)
    return jnp.sum(pooled_grad[:, :, None, :] * blocks_view, axis=(0, 1))


def local(
    hidden_in,
    w_query,
    w_key,
    w_value,
    w_output,
    w_inner,
    w_outer,
    pool_weight,
    ln_gain,
    ln_bias,
    branch_blocks,
    grad_out,
):
    pool_rows_count = pool_weight.shape[0] * pool_weight.shape[1]
    small_local = jnp.concatenate(
        [pool_weight.reshape(pool_rows_count, -1), ln_gain, ln_bias], axis=0
    )
    small_full = lax.all_gather(small_local, ("dp", "seq"), axis=1, tiled=True)
    small_full, w_query, w_key, w_value = lax.optimization_barrier(
        (small_full, w_query, w_key, w_value)
    )
    wq, wk, wv = gather_first(w_query, w_key, w_value)
    pool_full = small_full[:pool_rows_count].reshape(pool_weight.shape[0], pool_weight.shape[1], -1)
    gain_full = small_full[pool_rows_count : pool_rows_count + ln_gain.shape[0]]
    bias_full = small_full[pool_rows_count + ln_gain.shape[0] :]
    groups, shard_rows, width = hidden_in.shape
    seq_index = lax.axis_index("seq")
    offsets = STRIDE * branch_blocks
    starts, mask = block_geometry(seq_index, groups, shard_rows, offsets)

    hidden_all = lax.all_gather(hidden_in, "seq", axis=1, tiled=True)
    group_len = hidden_all.shape[1]
    tokens = hidden_in.reshape(groups * shard_rows, width)
    all_tokens = hidden_all.reshape(groups * group_len, width)
    queries = product(tokens, wq).astype(jnp.bfloat16)
    key_g = product(all_tokens, wk).astype(jnp.bfloat16).reshape(groups, group_len, width)
    value_g = product(all_tokens, wv).astype(jnp.bfloat16).reshape(groups, group_len, width)
    pooled_keys = pool_grouped(key_g.astype(jnp.float32), pool_full[0]).astype(jnp.bfloat16)
    pooled_values = pool_grouped(value_g.astype(jnp.float32), pool_full[1]).astype(jnp.bfloat16)
    kv_all = jnp.concatenate([key_g, value_g], axis=2)
    pkv_all = jnp.concatenate([pooled_keys, pooled_values], axis=2)
    kv_local = lax.dynamic_slice_in_dim(kv_all, seq_index * shard_rows, shard_rows, 1)
    pkv_local = lax.dynamic_slice_in_dim(
        pkv_all, seq_index * (shard_rows // STRIDE), shard_rows // STRIDE, 1
    )
    wq, wk, wv, hidden_all, w_output, w_inner, w_outer = lax.optimization_barrier(
        (wq, wk, wv, hidden_all, w_output, w_inner, w_outer)
    )
    wo, wi, wu = gather_second(w_output, w_inner, w_outer)
    attended, att_saved = attention_fwd(
        queries.reshape(groups, shard_rows, width), kv_local, pkv_local, kv_all, pkv_all, starts, mask
    )
    mixed_rows = tokens.astype(jnp.float32) + product(attended, wo)
    normed_first = layer_norm(mixed_rows, gain_full[0], bias_full[0])
    first_low = normed_first.astype(jnp.bfloat16)
    inner_act = product(first_low, wi)
    active = jax.nn.gelu(inner_act, approximate=False).astype(jnp.bfloat16)
    second = normed_first + product(active, wu)
    norm_value, second_back = jax.vjp(layer_norm, second, gain_full[1], bias_full[1])
    output = norm_value.astype(jnp.bfloat16)

    cotangent = grad_out.reshape(groups * shard_rows, width).astype(jnp.float32)
    grad_second, gain_second, bias_second = second_back(cotangent)
    grad_ffn_out = grad_second.astype(jnp.bfloat16)
    grad_outer = product_left(active, grad_ffn_out)
    grad_active = product_right(grad_ffn_out, wu)
    gelu_value, gelu_back = jax.vjp(partial(jax.nn.gelu, approximate=False), inner_act)
    grad_inner_act = gelu_back(grad_active)[0].astype(jnp.bfloat16)
    grad_inner = product_left(first_low, grad_inner_act)
    grad_first = grad_second + product_right(grad_inner_act, wi)
    first_value, first_back = jax.vjp(layer_norm, mixed_rows, gain_full[0], bias_full[0])
    grad_mixed, gain_first, bias_first = first_back(grad_first)
    grad_branch = grad_mixed.astype(jnp.bfloat16)
    grad_output = product_left(attended, grad_branch)
    grad_attended = product_right(grad_branch, wo).astype(jnp.bfloat16)
    early, grad_attended = reduce_seq_stage((grad_output, grad_inner, grad_outer.T), grad_attended)
    early_reduced, early_widths = early

    grad_rows = grad_attended.reshape(groups, shard_rows, width)
    pieces_back = []
    for g in range(groups):
        saved_g = tuple(item[g : g + 1] for item in att_saved)
        starts_g = tuple(item[g : g + 1] for item in starts)
        grad_g = grad_rows[g].reshape(shard_rows, width)
        if g == 1:
            grad_g, early_reduced = lax.optimization_barrier((grad_g, early_reduced))
        pieces_back.append(attention_bwd(grad_g, saved_g, starts_g, seq_index))
    grad_queries = jnp.concatenate([piece[0] for piece in pieces_back], axis=0)
    grad_full = jnp.concatenate([piece[1] for piece in pieces_back], axis=0)
    grad_pooled = jnp.concatenate([piece[2] for piece in pieces_back], axis=0)
    early = (early_reduced, early_widths)
    key_partial = (
        grad_full[..., :width] + unpool_grouped(grad_pooled[..., :width], pool_full[0])
    ).astype(jnp.bfloat16).reshape(groups * group_len, width)
    value_partial = (
        grad_full[..., width:] + unpool_grouped(grad_pooled[..., width:], pool_full[1])
    ).astype(jnp.bfloat16).reshape(groups * group_len, width)
    grad_pooling = jnp.stack(
        [
            pool_grad_grouped(grad_pooled[..., :width], key_g),
            pool_grad_grouped(grad_pooled[..., width:], value_g),
        ]
    )
    grad_query_w = product_left(tokens, grad_queries)
    grad_key_w = product_left(all_tokens, key_partial)
    grad_value_w = product_left(all_tokens, value_partial)
    back_rows = product_right(key_partial, wk) + product_right(value_partial, wv)
    back_rows = back_rows.reshape(groups, group_len, width).astype(jnp.bfloat16)
    back_own = lax.psum_scatter(back_rows, "seq", scatter_dimension=1, tiled=True)
    grad_tokens = (
        grad_mixed
        + product_right(grad_queries, wq)
        + back_own.reshape(groups * shard_rows, width).astype(jnp.float32)
    )
    late, _ = reduce_seq_stage((grad_query_w, grad_key_w, grad_value_w))
    pieces = reduce_dp_stage((early, late))
    accum = (pieces[3], pieces[4], pieces[5], pieces[0], pieces[1], pieces[2].T)
    small_sums = (
        lax.psum_scatter(grad_pooling, ("dp", "seq"), scatter_dimension=2, tiled=True),
        lax.psum_scatter(
            jnp.stack([gain_first, gain_second]), ("dp", "seq"), scatter_dimension=1, tiled=True
        ),
        lax.psum_scatter(
            jnp.stack([bias_first, bias_second]), ("dp", "seq"), scatter_dimension=1, tiled=True
        ),
    )
    return (
        output.reshape(groups, shard_rows, width),
        grad_tokens.astype(jnp.bfloat16).reshape(groups, shard_rows, width),
        accum[0],
        accum[1],
        accum[2],
        accum[3],
        accum[4],
        accum[5],
        small_sums[0],
        small_sums[1],
        small_sums[2],
    )


def solution(mesh):
    in_specs = (
        P("dp", "seq", None),
        P("seq", "dp"),
        P("seq", "dp"),
        P("seq", "dp"),
        P("seq", "dp"),
        P("seq", "dp"),
        P("dp", "seq"),
        P(None, None, ("dp", "seq")),
        P(None, ("dp", "seq")),
        P(None, ("dp", "seq")),
        P("dp", None),
        P("dp", "seq", None),
    )
    out_specs = (
        P("dp", "seq", None),
        P("dp", "seq", None),
        P("seq", "dp"),
        P("seq", "dp"),
        P("seq", "dp"),
        P("seq", "dp"),
        P("seq", "dp"),
        P("dp", "seq"),
        P(None, None, ("dp", "seq")),
        P(None, ("dp", "seq")),
        P(None, ("dp", "seq")),
    )
    return jax.shard_map(local, mesh=mesh, in_specs=in_specs, out_specs=out_specs, check_vma=False)
```

```python
from functools import partial

import jax
import jax.numpy as jnp
from jax import lax
from jax.sharding import PartitionSpec as P

HEADS = 12
HEAD_DIM = 64
PROMPT = 1024
CONT = 8
CLEN = 128
WINDOW = 128
POOL_SPAN = 512
STRIDE = 4


eps_norm = 1e-05


def token_layout(positions_in, offsets):
    in_prompt = positions_in < PROMPT
    segment = jnp.where(in_prompt, -1, (positions_in - PROMPT) // CLEN)
    within = positions_in - PROMPT - segment * CLEN
    choose = (segment[:, None] == jnp.arange(CONT, dtype=jnp.int32)[None, :]).astype(jnp.int32)
    cont_start = jnp.sum(choose * offsets[None, :], axis=1)
    position = jnp.where(in_prompt, positions_in, cont_start + within)
    prompt_limit = jnp.where(in_prompt, PROMPT, cont_start)
    return (segment, position, prompt_limit)


def visible_keys(query_rows, key_index, offsets, reach):
    query_seg, query_pos, query_limit = token_layout(query_rows, offsets)
    key_seg, key_pos, key_limit = token_layout(key_index, offsets)
    prompt_key = (key_seg[None, :] < 0) & (key_pos[None, :] < query_limit[:, None])
    own_key = (key_seg[None, :] == query_seg[:, None]) & (query_seg[:, None] >= 0)
    distance = key_pos[None, :] - query_pos[:, None]
    return (prompt_key | own_key) & (distance >= -(reach // 2)) & (distance < reach // 2)


def key_mask(query_rows, offsets):
    group_len = PROMPT + CONT * CLEN
    full_keys = jnp.arange(group_len, dtype=jnp.int32)
    pooled_keys = jnp.arange(group_len // STRIDE, dtype=jnp.int32) * STRIDE
    return jnp.concatenate(
        [
            visible_keys(query_rows, full_keys, offsets, WINDOW),
            visible_keys(query_rows, pooled_keys, offsets, POOL_SPAN),
        ],
        axis=1,
    )


def pool_rows(source, weight):
    return jnp.sum(
        source.reshape(source.shape[0] // STRIDE, STRIDE, source.shape[1]) * weight[None, :, :],
        axis=1,
    )


def unpool(pooled_grad, weight):
    return (pooled_grad[:, None, :] * weight[None, :, :]).reshape(-1, pooled_grad.shape[1])


def pool_grad(pooled_grad, source):
    blocks_view = source.astype(jnp.float32).reshape(-1, STRIDE, source.shape[1])
    return jnp.sum(pooled_grad[:, None, :] * blocks_view, axis=0)


def layer_norm(source, gain, bias):
    centre = jnp.mean(source, axis=-1, keepdims=True)
    centred = source - centre
    spread = jnp.mean(centred * centred, axis=-1, keepdims=True)
    return centred * lax.rsqrt(spread + eps_norm) * gain + bias


def product(left, right):
    return jnp.dot(left, right, preferred_element_type=jnp.float32)


def product_left(left, right):
    return lax.dot_general(
        left, right, (((0,), (0,)), ((), ())), preferred_element_type=jnp.float32
    )


def product_right(left, right):
    return lax.dot_general(
        left, right, (((1,), (1,)), ((), ())), preferred_element_type=jnp.float32
    )


def add_pair(left_term, right_term):
    return left_term + right_term


def gather_grouped(shards, tie=None):
    local_block = jnp.concatenate(shards, axis=1)
    across = lax.all_gather(local_block, "dp", axis=1, tiled=False)
    across, tie = lax.optimization_barrier((across, tie))
    return lax.all_gather(across, "seq", axis=0, tiled=True), tie


def split_grouped(gathered, widths):
    pieces, at = [], 0
    for width in widths:
        piece = gathered[:, :, at : at + width]
        pieces.append(piece.reshape(piece.shape[0], -1))
        at += width
    return pieces


def gather_first(w_query, w_key, w_value, tie):
    first, tie = gather_grouped((w_query, w_key, w_value), tie)
    return split_grouped(first, (w_query.shape[1], w_key.shape[1], w_value.shape[1])), tie


def gather_second(w_output, w_inner, w_outer):
    second, _ = gather_grouped((w_output, w_inner, w_outer.T))
    wo, wi, wu_t = split_grouped(second, (w_output.shape[1], w_inner.shape[1], w_outer.shape[0]))
    return (wo, wi, wu_t.T)


def reduce_seq_stage(grads, tie=None):
    dp_size = lax.psum(1, "dp")
    chunks = [grad.reshape(grad.shape[0], dp_size, grad.shape[1] // dp_size) for grad in grads]
    stacked = jnp.concatenate(chunks, axis=2).astype(jnp.bfloat16)
    stacked, tie = lax.optimization_barrier((stacked, tie))
    reduced = lax.psum_scatter(stacked, "seq", scatter_dimension=0, tiled=True)
    return (reduced, [c.shape[2] for c in chunks]), tie


def reduce_dp_stage(stages):
    joined = jnp.concatenate([stage for stage, _ in stages], axis=2)
    over_dp = lax.psum_scatter(joined, "dp", scatter_dimension=1, tiled=True)[:, 0].astype(jnp.float32)
    pieces, at = [], 0
    for _, widths in stages:
        for width in widths:
            pieces.append(over_dp[:, at : at + width])
            at += width
    return pieces


HALF_FULL = WINDOW // 2
HALF_POOL = POOL_SPAN // 2 // STRIDE
BLOCK_POOL = CLEN // STRIDE


def layout_of(index, offsets):
    in_prompt = index < PROMPT
    segment = jnp.where(in_prompt, -1, (index - PROMPT) // CLEN)
    within = index - PROMPT - segment * CLEN
    choose = segment[..., None] == jnp.arange(CONT, dtype=jnp.int32)
    spread = offsets.reshape(offsets.shape[:1] + (1,) * (index.ndim - 1) + offsets.shape[1:])
    cont_start = jnp.sum(jnp.where(choose, spread, 0), axis=-1)
    position = jnp.where(in_prompt, index, cont_start + within)
    limit = jnp.where(in_prompt, PROMPT, cont_start)
    return segment, position, limit


def window_rows(source, starts, length):
    groups, blocks = starts.shape
    return jnp.stack(
        [
            jnp.stack(
                [lax.dynamic_slice_in_dim(source[g], starts[g, b], length, 0) for b in range(blocks)]
            )
            for g in range(groups)
        ]
    )


def window_add(target, updates, starts):
    groups, blocks = starts.shape
    length = updates.shape[2]
    rows = []
    for g in range(groups):
        row = target[g]
        for b in range(blocks):
            start = starts[g, b]
            current = lax.dynamic_slice_in_dim(row, start, length, 0)
            row = lax.dynamic_update_slice_in_dim(row, current + updates[g, b], start, 0)
        rows.append(row)
    return jnp.stack(rows)


def block_geometry(seq_index, groups, shard_rows, offsets):
    group_len = PROMPT + CONT * CLEN
    pooled_len = group_len // STRIDE
    blocks = shard_rows // CLEN
    block_start = (seq_index * blocks + jnp.arange(blocks, dtype=jnp.int32)) * CLEN
    prompt_block = block_start < PROMPT
    cont_index = jnp.clip((block_start - PROMPT) // CLEN, 0, CONT - 1)
    anchor = jnp.where(prompt_block[None, :], block_start[None, :], offsets[:, cont_index])
    pooled_start = block_start // STRIDE
    intended = (
        anchor - HALF_FULL,
        jnp.broadcast_to(block_start + CLEN, anchor.shape),
        anchor // STRIDE - HALF_POOL,
        jnp.broadcast_to(pooled_start + BLOCK_POOL, anchor.shape),
    )
    limits = (group_len, group_len, pooled_len, pooled_len)
    lengths = (HALF_FULL, HALF_FULL, HALF_POOL, HALF_POOL)
    clamped = tuple(
        jnp.clip(start, 0, limit - length) for start, limit, length in zip(intended, limits, lengths)
    )
    ramp = lambda n: jnp.arange(n, dtype=jnp.int32)

    def span(window):
        actual = clamped[window][:, :, None] + ramp(lengths[window])
        offset = actual - intended[window][:, :, None]
        return actual, (offset >= 0) & (offset < lengths[window])

    before_full, before_full_ok = span(0)
    after_full, after_full_ok = span(1)
    before_pool, before_pool_ok = span(2)
    after_pool, after_pool_ok = span(3)
    after_ok = prompt_block[None, :, None]
    own_full = jnp.broadcast_to(block_start[None, :, None] + ramp(CLEN), anchor.shape + (CLEN,))
    own_pool = jnp.broadcast_to(
        pooled_start[None, :, None] + ramp(BLOCK_POOL), anchor.shape + (BLOCK_POOL,)
    )
    full_index = jnp.concatenate([before_full, own_full, after_full], axis=2)
    pooled_index = jnp.concatenate([before_pool, own_pool, after_pool], axis=2)
    full_valid = jnp.concatenate(
        [before_full_ok, jnp.ones(own_full.shape, bool), after_ok & after_full_ok], axis=2
    )
    pooled_valid = jnp.concatenate(
        [before_pool_ok, jnp.ones(own_pool.shape, bool), after_ok & after_pool_ok], axis=2
    )
    query_index = block_start[None, :, None] + ramp(CLEN)
    query_index = jnp.broadcast_to(query_index, anchor.shape + (CLEN,))
    q_seg, q_pos, q_lim = layout_of(query_index, offsets)

    def visible(key_token, valid, reach):
        k_seg, k_pos, _ = layout_of(key_token, offsets)
        k_seg, k_pos, valid = k_seg[:, :, None, :], k_pos[:, :, None, :], valid[:, :, None, :]
        prompt_key = (k_seg < 0) & (k_pos < q_lim[..., None])
        own_key = (k_seg == q_seg[..., None]) & (q_seg[..., None] >= 0)
        distance = k_pos - q_pos[..., None]
        return valid & (prompt_key | own_key) & (distance >= -(reach // 2)) & (distance < reach // 2)

    mask = jnp.concatenate(
        [
            visible(full_index, full_valid, WINDOW),
            visible(pooled_index * STRIDE, pooled_valid, POOL_SPAN),
        ],
        axis=3,
    )
    return clamped, mask


def attention_fwd(queries, kv_local, pkv_local, kv_all, pkv_all, starts, mask):
    groups, shard_rows, width = queries.shape
    blocks = shard_rows // CLEN
    score_scale = 1.0 / HEAD_DIM**0.5
    keys_cat = jnp.concatenate(
        [
            window_rows(kv_all, starts[0], HALF_FULL),
            kv_local.reshape(groups, blocks, CLEN, 2 * width),
            window_rows(kv_all, starts[1], HALF_FULL),
            window_rows(pkv_all, starts[2], HALF_POOL),
            pkv_local.reshape(groups, blocks, BLOCK_POOL, 2 * width),
            window_rows(pkv_all, starts[3], HALF_POOL),
        ],
        axis=2,
    )
    span = keys_cat.shape[2]
    head_keys = keys_cat[..., :width].reshape(groups, blocks, span, HEADS, HEAD_DIM)
    head_values = keys_cat[..., width:].reshape(groups, blocks, span, HEADS, HEAD_DIM)
    head_query = queries.reshape(groups, blocks, CLEN, HEADS, HEAD_DIM)
    scores = jnp.einsum(
        "gbqhd,gbkhd->gbhqk", head_query, head_keys, preferred_element_type=jnp.float32
    )
    scores = jnp.where(mask[:, :, None], scores * score_scale, -1000000000.0)
    row_top = jnp.max(scores, axis=-1, keepdims=True)
    exponent = jnp.exp(scores - row_top)
    row_total = jnp.sum(exponent, axis=-1, keepdims=True)
    probs = exponent / row_total
    attended = jnp.einsum(
        "gbhqk,gbkhd->gbqhd",
        probs.astype(jnp.bfloat16),
        head_values,
        preferred_element_type=jnp.float32,
    )
    attended = attended.reshape(groups * shard_rows, width).astype(jnp.bfloat16)
    return attended, (head_query, head_keys, head_values, probs)


def attention_bwd(grad_attended, saved, starts, seq_index):
    head_query, head_keys, head_values, probs = saved
    groups, blocks = head_query.shape[:2]
    width = HEADS * HEAD_DIM
    score_scale = 1.0 / HEAD_DIM**0.5
    head_grad = grad_attended.reshape(groups, blocks, CLEN, HEADS, HEAD_DIM)
    grad_probs = jnp.einsum(
        "gbqhd,gbkhd->gbhqk", head_grad, head_values, preferred_element_type=jnp.float32
    )
    centre = jnp.sum(probs * grad_probs, axis=-1, keepdims=True)
    grad_scores = (probs * (grad_probs - centre)).astype(jnp.bfloat16)
    grad_queries = jnp.einsum(
        "gbhqk,gbkhd->gbqhd", grad_scores, head_keys, preferred_element_type=jnp.float32
    ) * score_scale
    grad_keys = jnp.einsum(
        "gbhqk,gbqhd->gbkhd", grad_scores, head_query, preferred_element_type=jnp.float32
    ) * score_scale
    grad_values = jnp.einsum(
        "gbhqk,gbqhd->gbkhd",
        probs.astype(jnp.bfloat16),
        head_grad,
        preferred_element_type=jnp.float32,
    )
    span = grad_keys.shape[2]
    grad_kv = jnp.concatenate(
        [grad_keys.reshape(groups, blocks, span, width), grad_values.reshape(groups, blocks, span, width)],
        axis=3,
    )
    shard_rows = blocks * CLEN
    group_len = PROMPT + CONT * CLEN
    cut = (0, HALF_FULL, HALF_FULL + CLEN, 2 * HALF_FULL + CLEN)
    pcut = tuple(cut[-1] + c for c in (0, HALF_POOL, HALF_POOL + BLOCK_POOL, 2 * HALF_POOL + BLOCK_POOL))
    own_full = grad_kv[:, :, cut[1] : cut[2]].reshape(groups, shard_rows, 2 * width)
    own_pooled = grad_kv[:, :, pcut[1] : pcut[2]].reshape(groups, shard_rows // STRIDE, 2 * width)
    full = jnp.zeros((groups, group_len, 2 * width), jnp.float32)
    full = lax.dynamic_update_slice_in_dim(full, own_full, seq_index * shard_rows, 1)
    full = window_add(full, grad_kv[:, :, cut[0] : cut[1]], starts[0])
    full = window_add(full, grad_kv[:, :, cut[2] : cut[3]], starts[1])
    pooled = jnp.zeros((groups, group_len // STRIDE, 2 * width), jnp.float32)
    pooled = lax.dynamic_update_slice_in_dim(pooled, own_pooled, seq_index * shard_rows // STRIDE, 1)
    pooled = window_add(pooled, grad_kv[:, :, pcut[0] : pcut[1]], starts[2])
    pooled = window_add(pooled, grad_kv[:, :, pcut[2] : pcut[3]], starts[3])
    grad_queries = grad_queries.reshape(groups * shard_rows, width).astype(jnp.bfloat16)
    return grad_queries, full, pooled


def pool_grouped(source, weight):
    groups, rows, width = source.shape
    return jnp.sum(
        source.reshape(groups, rows // STRIDE, STRIDE, width) * weight[None, None], axis=2
    )


def unpool_grouped(pooled_grad, weight):
    groups, rows, width = pooled_grad.shape
    return (pooled_grad[:, :, None, :] * weight[None, None]).reshape(groups, rows * STRIDE, width)


def pool_grad_grouped(pooled_grad, source):
    groups, rows, width = source.shape
    blocks_view = source.astype(jnp.float32).reshape(groups, rows // STRIDE, STRIDE, width)
    return jnp.sum(pooled_grad[:, :, None, :] * blocks_view, axis=(0, 1))


def local(
    hidden_in,
    w_query,
    w_key,
    w_value,
    w_output,
    w_inner,
    w_outer,
    pool_weight,
    ln_gain,
    ln_bias,
    branch_blocks,
    grad_out,
):
    pool_rows_count = pool_weight.shape[0] * pool_weight.shape[1]
    small_local = jnp.concatenate(
        [pool_weight.reshape(pool_rows_count, -1), ln_gain, ln_bias], axis=0
    )
    small_full = lax.all_gather(small_local, ("dp", "seq"), axis=1, tiled=True)
    hidden_all = lax.all_gather(hidden_in, "seq", axis=1, tiled=True)
    (wq, wk, wv), hidden_all = gather_first(w_query, w_key, w_value, hidden_all)
    pool_full = small_full[:pool_rows_count].reshape(pool_weight.shape[0], pool_weight.shape[1], -1)
    gain_full = small_full[pool_rows_count : pool_rows_count + ln_gain.shape[0]]
    bias_full = small_full[pool_rows_count + ln_gain.shape[0] :]
    groups, shard_rows, width = hidden_in.shape
    seq_index = lax.axis_index("seq")
    offsets = STRIDE * branch_blocks
    starts, mask = block_geometry(seq_index, groups, shard_rows, offsets)

    group_len = hidden_all.shape[1]
    tokens = hidden_in.reshape(groups * shard_rows, width)
    all_tokens = hidden_all.reshape(groups * group_len, width)
    queries = product(tokens, wq).astype(jnp.bfloat16)
    key_g = product(all_tokens, wk).astype(jnp.bfloat16).reshape(groups, group_len, width)
    value_g = product(all_tokens, wv).astype(jnp.bfloat16).reshape(groups, group_len, width)
    pooled_keys = pool_grouped(key_g.astype(jnp.float32), pool_full[0]).astype(jnp.bfloat16)
    pooled_values = pool_grouped(value_g.astype(jnp.float32), pool_full[1]).astype(jnp.bfloat16)
    kv_all = jnp.concatenate([key_g, value_g], axis=2)
    pkv_all = jnp.concatenate([pooled_keys, pooled_values], axis=2)
    kv_local = lax.dynamic_slice_in_dim(kv_all, seq_index * shard_rows, shard_rows, 1)
    pkv_local = lax.dynamic_slice_in_dim(
        pkv_all, seq_index * (shard_rows // STRIDE), shard_rows // STRIDE, 1
    )
    wq, wk, wv, w_output, w_inner, w_outer = lax.optimization_barrier(
        (wq, wk, wv, w_output, w_inner, w_outer)
    )
    wo, wi, wu = gather_second(w_output, w_inner, w_outer)
    attended, att_saved = attention_fwd(
        queries.reshape(groups, shard_rows, width), kv_local, pkv_local, kv_all, pkv_all, starts, mask
    )
    mixed_rows = tokens.astype(jnp.float32) + product(attended, wo)
    normed_first = layer_norm(mixed_rows, gain_full[0], bias_full[0])
    first_low = normed_first.astype(jnp.bfloat16)
    inner_act = product(first_low, wi)
    active = jax.nn.gelu(inner_act, approximate=False).astype(jnp.bfloat16)
    second = normed_first + product(active, wu)
    norm_value, second_back = jax.vjp(layer_norm, second, gain_full[1], bias_full[1])
    output = norm_value.astype(jnp.bfloat16)

    cotangent = grad_out.reshape(groups * shard_rows, width).astype(jnp.float32)
    grad_second, gain_second, bias_second = second_back(cotangent)
    grad_ffn_out = grad_second.astype(jnp.bfloat16)
    grad_outer = product_left(active, grad_ffn_out)
    grad_active = product_right(grad_ffn_out, wu)
    gelu_value, gelu_back = jax.vjp(partial(jax.nn.gelu, approximate=False), inner_act)
    grad_inner_act = gelu_back(grad_active)[0].astype(jnp.bfloat16)
    grad_inner = product_left(first_low, grad_inner_act)
    grad_first = grad_second + product_right(grad_inner_act, wi)
    first_value, first_back = jax.vjp(layer_norm, mixed_rows, gain_full[0], bias_full[0])
    grad_mixed, gain_first, bias_first = first_back(grad_first)
    grad_branch = grad_mixed.astype(jnp.bfloat16)
    grad_output = product_left(attended, grad_branch)
    grad_attended = product_right(grad_branch, wo).astype(jnp.bfloat16)
    early, grad_attended = reduce_seq_stage((grad_output, grad_inner, grad_outer.T), grad_attended)
    early_reduced, early_widths = early

    grad_rows = grad_attended.reshape(groups, shard_rows, width)
    pieces_back = []
    for g in range(groups):
        saved_g = tuple(item[g : g + 1] for item in att_saved)
        starts_g = tuple(item[g : g + 1] for item in starts)
        grad_g = grad_rows[g].reshape(shard_rows, width)
        if g == 1:
            grad_g, early_reduced = lax.optimization_barrier((grad_g, early_reduced))
        grad_queries_g, full_g, pooled_g = attention_bwd(grad_g, saved_g, starts_g, seq_index)
        if g == 1:
            full_g, pooled_g, earlier_back = lax.optimization_barrier(
                (full_g, pooled_g, pieces_back[0][4])
            )
            pieces_back[0] = pieces_back[0][:4] + (earlier_back,)
        key_partial_g = (
            full_g[..., :width] + unpool_grouped(pooled_g[..., :width], pool_full[0])
        ).astype(jnp.bfloat16).reshape(group_len, width)
        value_partial_g = (
            full_g[..., width:] + unpool_grouped(pooled_g[..., width:], pool_full[1])
        ).astype(jnp.bfloat16).reshape(group_len, width)
        back_g = product_right(key_partial_g, wk) + product_right(value_partial_g, wv)
        back_g = back_g.reshape(1, group_len, width).astype(jnp.bfloat16)
        back_own_g = lax.psum_scatter(back_g, "seq", scatter_dimension=1, tiled=True)
        pieces_back.append((grad_queries_g, pooled_g, key_partial_g, value_partial_g, back_own_g))
    grad_queries = jnp.concatenate([piece[0] for piece in pieces_back], axis=0)
    grad_pooled = jnp.concatenate([piece[1] for piece in pieces_back], axis=0)
    key_partial = jnp.concatenate([piece[2] for piece in pieces_back], axis=0)
    value_partial = jnp.concatenate([piece[3] for piece in pieces_back], axis=0)
    back_own = jnp.concatenate([piece[4] for piece in pieces_back], axis=0)
    early = (early_reduced, early_widths)
    grad_pooling = jnp.stack(
        [
            pool_grad_grouped(grad_pooled[..., :width], key_g),
            pool_grad_grouped(grad_pooled[..., width:], value_g),
        ]
    )
    grad_query_w = product_left(tokens, grad_queries)
    grad_key_w = product_left(all_tokens, key_partial)
    grad_value_w = product_left(all_tokens, value_partial)
    grad_tokens = (
        grad_mixed
        + product_right(grad_queries, wq)
        + back_own.reshape(groups * shard_rows, width).astype(jnp.float32)
    )
    late, _ = reduce_seq_stage((grad_query_w, grad_key_w, grad_value_w))
    pieces = reduce_dp_stage((early, late))
    accum = (pieces[3], pieces[4], pieces[5], pieces[0], pieces[1], pieces[2].T)
    small_sums = (
        lax.psum_scatter(grad_pooling, ("dp", "seq"), scatter_dimension=2, tiled=True),
        lax.psum_scatter(
            jnp.stack([gain_first, gain_second]), ("dp", "seq"), scatter_dimension=1, tiled=True
        ),
        lax.psum_scatter(
            jnp.stack([bias_first, bias_second]), ("dp", "seq"), scatter_dimension=1, tiled=True
        ),
    )
    return (
        output.reshape(groups, shard_rows, width),
        grad_tokens.astype(jnp.bfloat16).reshape(groups, shard_rows, width),
        accum[0],
        accum[1],
        accum[2],
        accum[3],
        accum[4],
        accum[5],
        small_sums[0],
        small_sums[1],
        small_sums[2],
    )


def solution(mesh):
    in_specs = (
        P("dp", "seq", None),
        P("seq", "dp"),
        P("seq", "dp"),
        P("seq", "dp"),
        P("seq", "dp"),
        P("seq", "dp"),
        P("dp", "seq"),
        P(None, None, ("dp", "seq")),
        P(None, ("dp", "seq")),
        P(None, ("dp", "seq")),
        P("dp", None),
        P("dp", "seq", None),
    )
    out_specs = (
        P("dp", "seq", None),
        P("dp", "seq", None),
        P("seq", "dp"),
        P("seq", "dp"),
        P("seq", "dp"),
        P("seq", "dp"),
        P("seq", "dp"),
        P("dp", "seq"),
        P(None, None, ("dp", "seq")),
        P(None, ("dp", "seq")),
        P(None, ("dp", "seq")),
    )
    return jax.shard_map(local, mesh=mesh, in_specs=in_specs, out_specs=out_specs, check_vma=False)
```

```python
from functools import partial

import jax
import jax.numpy as jnp
from jax import lax
from jax.sharding import PartitionSpec as P

HEADS = 12
HEAD_DIM = 64
PROMPT = 1024
CONT = 8
CLEN = 128
WINDOW = 128
POOL_SPAN = 512
STRIDE = 4


eps_norm = 1e-05


def token_layout(positions_in, offsets):
    in_prompt = positions_in < PROMPT
    segment = jnp.where(in_prompt, -1, (positions_in - PROMPT) // CLEN)
    within = positions_in - PROMPT - segment * CLEN
    choose = (segment[:, None] == jnp.arange(CONT, dtype=jnp.int32)[None, :]).astype(jnp.int32)
    cont_start = jnp.sum(choose * offsets[None, :], axis=1)
    position = jnp.where(in_prompt, positions_in, cont_start + within)
    prompt_limit = jnp.where(in_prompt, PROMPT, cont_start)
    return (segment, position, prompt_limit)


def visible_keys(query_rows, key_index, offsets, reach):
    query_seg, query_pos, query_limit = token_layout(query_rows, offsets)
    key_seg, key_pos, key_limit = token_layout(key_index, offsets)
    prompt_key = (key_seg[None, :] < 0) & (key_pos[None, :] < query_limit[:, None])
    own_key = (key_seg[None, :] == query_seg[:, None]) & (query_seg[:, None] >= 0)
    distance = key_pos[None, :] - query_pos[:, None]
    return (prompt_key | own_key) & (distance >= -(reach // 2)) & (distance < reach // 2)


def key_mask(query_rows, offsets):
    group_len = PROMPT + CONT * CLEN
    full_keys = jnp.arange(group_len, dtype=jnp.int32)
    pooled_keys = jnp.arange(group_len // STRIDE, dtype=jnp.int32) * STRIDE
    return jnp.concatenate(
        [
            visible_keys(query_rows, full_keys, offsets, WINDOW),
            visible_keys(query_rows, pooled_keys, offsets, POOL_SPAN),
        ],
        axis=1,
    )


def pool_rows(source, weight):
    return jnp.sum(
        source.reshape(source.shape[0] // STRIDE, STRIDE, source.shape[1]) * weight[None, :, :],
        axis=1,
    )


def unpool(pooled_grad, weight):
    return (pooled_grad[:, None, :] * weight[None, :, :]).reshape(-1, pooled_grad.shape[1])


def pool_grad(pooled_grad, source):
    blocks_view = source.astype(jnp.float32).reshape(-1, STRIDE, source.shape[1])
    return jnp.sum(pooled_grad[:, None, :] * blocks_view, axis=0)


def layer_norm(source, gain, bias):
    centre = jnp.mean(source, axis=-1, keepdims=True)
    centred = source - centre
    spread = jnp.mean(centred * centred, axis=-1, keepdims=True)
    return centred * lax.rsqrt(spread + eps_norm) * gain + bias


def product(left, right):
    return jnp.dot(left, right, preferred_element_type=jnp.float32)


def product_left(left, right):
    return lax.dot_general(
        left, right, (((0,), (0,)), ((), ())), preferred_element_type=jnp.float32
    )


def product_right(left, right):
    return lax.dot_general(
        left, right, (((1,), (1,)), ((), ())), preferred_element_type=jnp.float32
    )


def add_pair(left_term, right_term):
    return left_term + right_term


def gather_grouped(shards, tie=None):
    local_block = jnp.concatenate(shards, axis=1)
    across = lax.all_gather(local_block, "dp", axis=1, tiled=False)
    across, tie = lax.optimization_barrier((across, tie))
    return lax.all_gather(across, "seq", axis=0, tiled=True), tie


def split_grouped(gathered, widths):
    pieces, at = [], 0
    for width in widths:
        piece = gathered[:, :, at : at + width]
        pieces.append(piece.reshape(piece.shape[0], -1))
        at += width
    return pieces


def gather_first(w_query, w_key, w_value, tie):
    first, tie = gather_grouped((w_query, w_key, w_value), tie)
    return split_grouped(first, (w_query.shape[1], w_key.shape[1], w_value.shape[1])), tie


def gather_second(w_output, w_inner, w_outer):
    second, _ = gather_grouped((w_output, w_inner, w_outer.T))
    wo, wi, wu_t = split_grouped(second, (w_output.shape[1], w_inner.shape[1], w_outer.shape[0]))
    return (wo, wi, wu_t.T)


def reduce_seq_stage(grads, tie=None):
    dp_size = lax.psum(1, "dp")
    chunks = [grad.reshape(grad.shape[0], dp_size, grad.shape[1] // dp_size) for grad in grads]
    stacked = jnp.concatenate(chunks, axis=2).astype(jnp.bfloat16)
    stacked, tie = lax.optimization_barrier((stacked, tie))
    reduced = lax.psum_scatter(stacked, "seq", scatter_dimension=0, tiled=True)
    return (reduced, [c.shape[2] for c in chunks]), tie


def reduce_dp_stage(stages):
    joined = jnp.concatenate([stage for stage, _ in stages], axis=2)
    over_dp = lax.psum_scatter(joined, "dp", scatter_dimension=1, tiled=True)[:, 0].astype(jnp.float32)
    pieces, at = [], 0
    for _, widths in stages:
        for width in widths:
            pieces.append(over_dp[:, at : at + width])
            at += width
    return pieces


HALF_FULL = WINDOW // 2
HALF_POOL = POOL_SPAN // 2 // STRIDE
BLOCK_POOL = CLEN // STRIDE


def layout_of(index, offsets):
    in_prompt = index < PROMPT
    segment = jnp.where(in_prompt, -1, (index - PROMPT) // CLEN)
    within = index - PROMPT - segment * CLEN
    choose = segment[..., None] == jnp.arange(CONT, dtype=jnp.int32)
    spread = offsets.reshape(offsets.shape[:1] + (1,) * (index.ndim - 1) + offsets.shape[1:])
    cont_start = jnp.sum(jnp.where(choose, spread, 0), axis=-1)
    position = jnp.where(in_prompt, index, cont_start + within)
    limit = jnp.where(in_prompt, PROMPT, cont_start)
    return segment, position, limit


def window_rows(source, starts, length):
    groups, blocks = starts.shape
    return jnp.stack(
        [
            jnp.stack(
                [lax.dynamic_slice_in_dim(source[g], starts[g, b], length, 0) for b in range(blocks)]
            )
            for g in range(groups)
        ]
    )


def window_add(target, updates, starts):
    groups, blocks = starts.shape
    length = updates.shape[2]
    rows = []
    for g in range(groups):
        row = target[g]
        for b in range(blocks):
            start = starts[g, b]
            current = lax.dynamic_slice_in_dim(row, start, length, 0)
            row = lax.dynamic_update_slice_in_dim(row, current + updates[g, b], start, 0)
        rows.append(row)
    return jnp.stack(rows)


def block_geometry(seq_index, groups, shard_rows, offsets):
    group_len = PROMPT + CONT * CLEN
    pooled_len = group_len // STRIDE
    blocks = shard_rows // CLEN
    block_start = (seq_index * blocks + jnp.arange(blocks, dtype=jnp.int32)) * CLEN
    prompt_block = block_start < PROMPT
    cont_index = jnp.clip((block_start - PROMPT) // CLEN, 0, CONT - 1)
    anchor = jnp.where(prompt_block[None, :], block_start[None, :], offsets[:, cont_index])
    pooled_start = block_start // STRIDE
    intended = (
        anchor - HALF_FULL,
        jnp.broadcast_to(block_start + CLEN, anchor.shape),
        anchor // STRIDE - HALF_POOL,
        jnp.broadcast_to(pooled_start + BLOCK_POOL, anchor.shape),
    )
    limits = (group_len, group_len, pooled_len, pooled_len)
    lengths = (HALF_FULL, HALF_FULL, HALF_POOL, HALF_POOL)
    clamped = tuple(
        jnp.clip(start, 0, limit - length) for start, limit, length in zip(intended, limits, lengths)
    )
    ramp = lambda n: jnp.arange(n, dtype=jnp.int32)

    def span(window):
        actual = clamped[window][:, :, None] + ramp(lengths[window])
        offset = actual - intended[window][:, :, None]
        return actual, (offset >= 0) & (offset < lengths[window])

    before_full, before_full_ok = span(0)
    after_full, after_full_ok = span(1)
    before_pool, before_pool_ok = span(2)
    after_pool, after_pool_ok = span(3)
    after_ok = prompt_block[None, :, None]
    own_full = jnp.broadcast_to(block_start[None, :, None] + ramp(CLEN), anchor.shape + (CLEN,))
    own_pool = jnp.broadcast_to(
        pooled_start[None, :, None] + ramp(BLOCK_POOL), anchor.shape + (BLOCK_POOL,)
    )
    full_index = jnp.concatenate([before_full, own_full, after_full], axis=2)
    pooled_index = jnp.concatenate([before_pool, own_pool, after_pool], axis=2)
    full_valid = jnp.concatenate(
        [before_full_ok, jnp.ones(own_full.shape, bool), after_ok & after_full_ok], axis=2
    )
    pooled_valid = jnp.concatenate(
        [before_pool_ok, jnp.ones(own_pool.shape, bool), after_ok & after_pool_ok], axis=2
    )
    query_index = block_start[None, :, None] + ramp(CLEN)
    query_index = jnp.broadcast_to(query_index, anchor.shape + (CLEN,))
    q_seg, q_pos, q_lim = layout_of(query_index, offsets)

    def visible(key_token, valid, reach):
        k_seg, k_pos, _ = layout_of(key_token, offsets)
        k_seg, k_pos, valid = k_seg[:, :, None, :], k_pos[:, :, None, :], valid[:, :, None, :]
        prompt_key = (k_seg < 0) & (k_pos < q_lim[..., None])
        own_key = (k_seg == q_seg[..., None]) & (q_seg[..., None] >= 0)
        distance = k_pos - q_pos[..., None]
        return valid & (prompt_key | own_key) & (distance >= -(reach // 2)) & (distance < reach // 2)

    mask = jnp.concatenate(
        [
            visible(full_index, full_valid, WINDOW),
            visible(pooled_index * STRIDE, pooled_valid, POOL_SPAN),
        ],
        axis=3,
    )
    return clamped, mask


def attention_fwd(queries, kv_local, pkv_local, kv_all, pkv_all, starts, mask):
    groups, shard_rows, width = queries.shape
    blocks = shard_rows // CLEN
    score_scale = 1.0 / HEAD_DIM**0.5
    keys_cat = jnp.concatenate(
        [
            window_rows(kv_all, starts[0], HALF_FULL),
            kv_local.reshape(groups, blocks, CLEN, 2 * width),
            window_rows(kv_all, starts[1], HALF_FULL),
            window_rows(pkv_all, starts[2], HALF_POOL),
            pkv_local.reshape(groups, blocks, BLOCK_POOL, 2 * width),
            window_rows(pkv_all, starts[3], HALF_POOL),
        ],
        axis=2,
    )
    span = keys_cat.shape[2]
    head_keys = keys_cat[..., :width].reshape(groups, blocks, span, HEADS, HEAD_DIM)
    head_values = keys_cat[..., width:].reshape(groups, blocks, span, HEADS, HEAD_DIM)
    head_query = queries.reshape(groups, blocks, CLEN, HEADS, HEAD_DIM)
    scores = jnp.einsum(
        "gbqhd,gbkhd->gbhqk", head_query, head_keys, preferred_element_type=jnp.float32
    )
    scores = jnp.where(mask[:, :, None], scores * score_scale, -1000000000.0)
    row_top = jnp.max(scores, axis=-1, keepdims=True)
    exponent = jnp.exp(scores - row_top)
    row_total = jnp.sum(exponent, axis=-1, keepdims=True)
    probs = exponent / row_total
    attended = jnp.einsum(
        "gbhqk,gbkhd->gbqhd",
        probs.astype(jnp.bfloat16),
        head_values,
        preferred_element_type=jnp.float32,
    )
    attended = attended.reshape(groups * shard_rows, width).astype(jnp.bfloat16)
    return attended, (head_query, head_keys, head_values, probs)


def attention_bwd(grad_attended, saved, starts, seq_index):
    head_query, head_keys, head_values, probs = saved
    groups, blocks = head_query.shape[:2]
    width = HEADS * HEAD_DIM
    score_scale = 1.0 / HEAD_DIM**0.5
    head_grad = grad_attended.reshape(groups, blocks, CLEN, HEADS, HEAD_DIM)
    grad_probs = jnp.einsum(
        "gbqhd,gbkhd->gbhqk", head_grad, head_values, preferred_element_type=jnp.float32
    )
    centre = jnp.sum(probs * grad_probs, axis=-1, keepdims=True)
    grad_scores = (probs * (grad_probs - centre)).astype(jnp.bfloat16)
    grad_queries = jnp.einsum(
        "gbhqk,gbkhd->gbqhd", grad_scores, head_keys, preferred_element_type=jnp.float32
    ) * score_scale
    grad_keys = jnp.einsum(
        "gbhqk,gbqhd->gbkhd", grad_scores, head_query, preferred_element_type=jnp.float32
    ) * score_scale
    grad_values = jnp.einsum(
        "gbhqk,gbqhd->gbkhd",
        probs.astype(jnp.bfloat16),
        head_grad,
        preferred_element_type=jnp.float32,
    )
    span = grad_keys.shape[2]
    grad_kv = jnp.concatenate(
        [grad_keys.reshape(groups, blocks, span, width), grad_values.reshape(groups, blocks, span, width)],
        axis=3,
    )
    shard_rows = blocks * CLEN
    group_len = PROMPT + CONT * CLEN
    cut = (0, HALF_FULL, HALF_FULL + CLEN, 2 * HALF_FULL + CLEN)
    pcut = tuple(cut[-1] + c for c in (0, HALF_POOL, HALF_POOL + BLOCK_POOL, 2 * HALF_POOL + BLOCK_POOL))
    own_full = grad_kv[:, :, cut[1] : cut[2]].reshape(groups, shard_rows, 2 * width)
    own_pooled = grad_kv[:, :, pcut[1] : pcut[2]].reshape(groups, shard_rows // STRIDE, 2 * width)
    full = jnp.zeros((groups, group_len, 2 * width), jnp.float32)
    full = lax.dynamic_update_slice_in_dim(full, own_full, seq_index * shard_rows, 1)
    full = window_add(full, grad_kv[:, :, cut[0] : cut[1]], starts[0])
    full = window_add(full, grad_kv[:, :, cut[2] : cut[3]], starts[1])
    pooled = jnp.zeros((groups, group_len // STRIDE, 2 * width), jnp.float32)
    pooled = lax.dynamic_update_slice_in_dim(pooled, own_pooled, seq_index * shard_rows // STRIDE, 1)
    pooled = window_add(pooled, grad_kv[:, :, pcut[0] : pcut[1]], starts[2])
    pooled = window_add(pooled, grad_kv[:, :, pcut[2] : pcut[3]], starts[3])
    grad_queries = grad_queries.reshape(groups * shard_rows, width).astype(jnp.bfloat16)
    return grad_queries, full, pooled


def pool_grouped(source, weight):
    groups, rows, width = source.shape
    return jnp.sum(
        source.reshape(groups, rows // STRIDE, STRIDE, width) * weight[None, None], axis=2
    )


def unpool_grouped(pooled_grad, weight):
    groups, rows, width = pooled_grad.shape
    return (pooled_grad[:, :, None, :] * weight[None, None]).reshape(groups, rows * STRIDE, width)


def pool_grad_grouped(pooled_grad, source):
    groups, rows, width = source.shape
    blocks_view = source.astype(jnp.float32).reshape(groups, rows // STRIDE, STRIDE, width)
    return jnp.sum(pooled_grad[:, :, None, :] * blocks_view, axis=(0, 1))


def local(
    hidden_in,
    w_query,
    w_key,
    w_value,
    w_output,
    w_inner,
    w_outer,
    pool_weight,
    ln_gain,
    ln_bias,
    branch_blocks,
    grad_out,
):
    pool_rows_count = pool_weight.shape[0] * pool_weight.shape[1]
    small_local = jnp.concatenate(
        [pool_weight.reshape(pool_rows_count, -1), ln_gain, ln_bias], axis=0
    )
    small_full = lax.all_gather(small_local, ("dp", "seq"), axis=1, tiled=True)
    hidden_all = lax.all_gather(hidden_in, "seq", axis=1, tiled=True)
    (wq, wk, wv), (hidden_all, small_full) = gather_first(
        w_query, w_key, w_value, (hidden_all, small_full)
    )
    pool_full = small_full[:pool_rows_count].reshape(pool_weight.shape[0], pool_weight.shape[1], -1)
    gain_full = small_full[pool_rows_count : pool_rows_count + ln_gain.shape[0]]
    bias_full = small_full[pool_rows_count + ln_gain.shape[0] :]
    groups, shard_rows, width = hidden_in.shape
    seq_index = lax.axis_index("seq")
    offsets = STRIDE * branch_blocks
    starts, mask = block_geometry(seq_index, groups, shard_rows, offsets)

    group_len = hidden_all.shape[1]
    tokens = hidden_in.reshape(groups * shard_rows, width)
    all_tokens = hidden_all.reshape(groups * group_len, width)
    queries = product(tokens, wq).astype(jnp.bfloat16)
    key_g = product(all_tokens, wk).astype(jnp.bfloat16).reshape(groups, group_len, width)
    value_g = product(all_tokens, wv).astype(jnp.bfloat16).reshape(groups, group_len, width)
    pooled_keys = pool_grouped(key_g.astype(jnp.float32), pool_full[0]).astype(jnp.bfloat16)
    pooled_values = pool_grouped(value_g.astype(jnp.float32), pool_full[1]).astype(jnp.bfloat16)
    kv_all = jnp.concatenate([key_g, value_g], axis=2)
    pkv_all = jnp.concatenate([pooled_keys, pooled_values], axis=2)
    kv_local = lax.dynamic_slice_in_dim(kv_all, seq_index * shard_rows, shard_rows, 1)
    pkv_local = lax.dynamic_slice_in_dim(
        pkv_all, seq_index * (shard_rows // STRIDE), shard_rows // STRIDE, 1
    )
    wq, wk, wv, w_output, w_inner, w_outer = lax.optimization_barrier(
        (wq, wk, wv, w_output, w_inner, w_outer)
    )
    wo, wi, wu = gather_second(w_output, w_inner, w_outer)
    attended, att_saved = attention_fwd(
        queries.reshape(groups, shard_rows, width), kv_local, pkv_local, kv_all, pkv_all, starts, mask
    )
    mixed_rows = tokens.astype(jnp.float32) + product(attended, wo)
    normed_first = layer_norm(mixed_rows, gain_full[0], bias_full[0])
    first_low = normed_first.astype(jnp.bfloat16)
    inner_act = product(first_low, wi)
    active = jax.nn.gelu(inner_act, approximate=False).astype(jnp.bfloat16)
    second = normed_first + product(active, wu)
    norm_value, second_back = jax.vjp(layer_norm, second, gain_full[1], bias_full[1])
    output = norm_value.astype(jnp.bfloat16)

    cotangent = grad_out.reshape(groups * shard_rows, width).astype(jnp.float32)
    grad_second, gain_second, bias_second = second_back(cotangent)
    grad_ffn_out = grad_second.astype(jnp.bfloat16)
    grad_outer = product_left(active, grad_ffn_out)
    grad_active = product_right(grad_ffn_out, wu)
    gelu_value, gelu_back = jax.vjp(partial(jax.nn.gelu, approximate=False), inner_act)
    grad_inner_act = gelu_back(grad_active)[0].astype(jnp.bfloat16)
    grad_inner = product_left(first_low, grad_inner_act)
    grad_first = grad_second + product_right(grad_inner_act, wi)
    first_value, first_back = jax.vjp(layer_norm, mixed_rows, gain_full[0], bias_full[0])
    grad_mixed, gain_first, bias_first = first_back(grad_first)
    grad_branch = grad_mixed.astype(jnp.bfloat16)
    grad_output = product_left(attended, grad_branch)
    grad_attended = product_right(grad_branch, wo).astype(jnp.bfloat16)
    early, grad_attended = reduce_seq_stage((grad_output, grad_inner, grad_outer.T), grad_attended)
    early_reduced, early_widths = early

    grad_rows = grad_attended.reshape(groups, shard_rows, width)
    pieces_back = []
    for g in range(groups):
        saved_g = tuple(item[g : g + 1] for item in att_saved)
        starts_g = tuple(item[g : g + 1] for item in starts)
        grad_g = grad_rows[g].reshape(shard_rows, width)
        grad_queries_g, full_g, pooled_g = attention_bwd(grad_g, saved_g, starts_g, seq_index)
        if g == 1:
            full_g, pooled_g, earlier_back, early_reduced = lax.optimization_barrier(
                (full_g, pooled_g, pieces_back[0][4], early_reduced)
            )
            pieces_back[0] = pieces_back[0][:4] + (earlier_back,)
        key_partial_g = (
            full_g[..., :width] + unpool_grouped(pooled_g[..., :width], pool_full[0])
        ).astype(jnp.bfloat16).reshape(group_len, width)
        value_partial_g = (
            full_g[..., width:] + unpool_grouped(pooled_g[..., width:], pool_full[1])
        ).astype(jnp.bfloat16).reshape(group_len, width)
        back_g = product_right(key_partial_g, wk) + product_right(value_partial_g, wv)
        back_g = back_g.reshape(1, group_len, width).astype(jnp.bfloat16)
        back_own_g = lax.psum_scatter(back_g, "seq", scatter_dimension=1, tiled=True)
        pieces_back.append((grad_queries_g, pooled_g, key_partial_g, value_partial_g, back_own_g))
    grad_queries = jnp.concatenate([piece[0] for piece in pieces_back], axis=0)
    grad_pooled = jnp.concatenate([piece[1] for piece in pieces_back], axis=0)
    key_partial = jnp.concatenate([piece[2] for piece in pieces_back], axis=0)
    value_partial = jnp.concatenate([piece[3] for piece in pieces_back], axis=0)
    back_own = jnp.concatenate([piece[4] for piece in pieces_back], axis=0)
    early = (early_reduced, early_widths)
    grad_pooling = jnp.stack(
        [
            pool_grad_grouped(grad_pooled[..., :width], key_g),
            pool_grad_grouped(grad_pooled[..., width:], value_g),
        ]
    )
    grad_query_w = product_left(tokens, grad_queries)
    grad_key_w = product_left(all_tokens, key_partial)
    grad_value_w = product_left(all_tokens, value_partial)
    grad_tokens = (
        grad_mixed
        + product_right(grad_queries, wq)
        + back_own.reshape(groups * shard_rows, width).astype(jnp.float32)
    )
    late, _ = reduce_seq_stage((grad_query_w, grad_key_w, grad_value_w))
    pieces = reduce_dp_stage((early, late))
    accum = (pieces[3], pieces[4], pieces[5], pieces[0], pieces[1], pieces[2].T)
    small_sums = (
        lax.psum_scatter(grad_pooling, ("dp", "seq"), scatter_dimension=2, tiled=True),
        lax.psum_scatter(
            jnp.stack([gain_first, gain_second]), ("dp", "seq"), scatter_dimension=1, tiled=True
        ),
        lax.psum_scatter(
            jnp.stack([bias_first, bias_second]), ("dp", "seq"), scatter_dimension=1, tiled=True
        ),
    )
    return (
        output.reshape(groups, shard_rows, width),
        grad_tokens.astype(jnp.bfloat16).reshape(groups, shard_rows, width),
        accum[0],
        accum[1],
        accum[2],
        accum[3],
        accum[4],
        accum[5],
        small_sums[0],
        small_sums[1],
        small_sums[2],
    )


def solution(mesh):
    in_specs = (
        P("dp", "seq", None),
        P("seq", "dp"),
        P("seq", "dp"),
        P("seq", "dp"),
        P("seq", "dp"),
        P("seq", "dp"),
        P("dp", "seq"),
        P(None, None, ("dp", "seq")),
        P(None, ("dp", "seq")),
        P(None, ("dp", "seq")),
        P("dp", None),
        P("dp", "seq", None),
    )
    out_specs = (
        P("dp", "seq", None),
        P("dp", "seq", None),
        P("seq", "dp"),
        P("seq", "dp"),
        P("seq", "dp"),
        P("seq", "dp"),
        P("seq", "dp"),
        P("dp", "seq"),
        P(None, None, ("dp", "seq")),
        P(None, ("dp", "seq")),
        P(None, ("dp", "seq")),
    )
    return jax.shard_map(local, mesh=mesh, in_specs=in_specs, out_specs=out_specs, check_vma=False)
```

```python
from functools import partial

import jax
import jax.numpy as jnp
from jax import lax
from jax.sharding import PartitionSpec as P

HEADS = 12
HEAD_DIM = 64
PROMPT = 1024
CONT = 8
CLEN = 128
WINDOW = 128
POOL_SPAN = 512
STRIDE = 4


eps_norm = 1e-05


def token_layout(positions_in, offsets):
    in_prompt = positions_in < PROMPT
    segment = jnp.where(in_prompt, -1, (positions_in - PROMPT) // CLEN)
    within = positions_in - PROMPT - segment * CLEN
    choose = (segment[:, None] == jnp.arange(CONT, dtype=jnp.int32)[None, :]).astype(jnp.int32)
    cont_start = jnp.sum(choose * offsets[None, :], axis=1)
    position = jnp.where(in_prompt, positions_in, cont_start + within)
    prompt_limit = jnp.where(in_prompt, PROMPT, cont_start)
    return (segment, position, prompt_limit)


def visible_keys(query_rows, key_index, offsets, reach):
    query_seg, query_pos, query_limit = token_layout(query_rows, offsets)
    key_seg, key_pos, key_limit = token_layout(key_index, offsets)
    prompt_key = (key_seg[None, :] < 0) & (key_pos[None, :] < query_limit[:, None])
    own_key = (key_seg[None, :] == query_seg[:, None]) & (query_seg[:, None] >= 0)
    distance = key_pos[None, :] - query_pos[:, None]
    return (prompt_key | own_key) & (distance >= -(reach // 2)) & (distance < reach // 2)


def key_mask(query_rows, offsets):
    group_len = PROMPT + CONT * CLEN
    full_keys = jnp.arange(group_len, dtype=jnp.int32)
    pooled_keys = jnp.arange(group_len // STRIDE, dtype=jnp.int32) * STRIDE
    return jnp.concatenate(
        [
            visible_keys(query_rows, full_keys, offsets, WINDOW),
            visible_keys(query_rows, pooled_keys, offsets, POOL_SPAN),
        ],
        axis=1,
    )


def pool_rows(source, weight):
    return jnp.sum(
        source.reshape(source.shape[0] // STRIDE, STRIDE, source.shape[1]) * weight[None, :, :],
        axis=1,
    )


def unpool(pooled_grad, weight):
    return (pooled_grad[:, None, :] * weight[None, :, :]).reshape(-1, pooled_grad.shape[1])


def pool_grad(pooled_grad, source):
    blocks_view = source.astype(jnp.float32).reshape(-1, STRIDE, source.shape[1])
    return jnp.sum(pooled_grad[:, None, :] * blocks_view, axis=0)


def layer_norm(source, gain, bias):
    centre = jnp.mean(source, axis=-1, keepdims=True)
    centred = source - centre
    spread = jnp.mean(centred * centred, axis=-1, keepdims=True)
    return centred * lax.rsqrt(spread + eps_norm) * gain + bias


def product(left, right):
    return jnp.dot(left, right, preferred_element_type=jnp.float32)


def product_left(left, right):
    return lax.dot_general(
        left, right, (((0,), (0,)), ((), ())), preferred_element_type=jnp.float32
    )


def product_right(left, right):
    return lax.dot_general(
        left, right, (((1,), (1,)), ((), ())), preferred_element_type=jnp.float32
    )


def add_pair(left_term, right_term):
    return left_term + right_term


def gather_grouped(shards, tie=None):
    local_block = jnp.concatenate(shards, axis=1)
    across = lax.all_gather(local_block, "dp", axis=1, tiled=False)
    across, tie = lax.optimization_barrier((across, tie))
    return lax.all_gather(across, "seq", axis=0, tiled=True), tie


def split_grouped(gathered, widths):
    pieces, at = [], 0
    for width in widths:
        piece = gathered[:, :, at : at + width]
        pieces.append(piece.reshape(piece.shape[0], -1))
        at += width
    return pieces


def gather_first(w_query, w_key, w_value, tie):
    first, tie = gather_grouped((w_query, w_key, w_value), tie)
    return split_grouped(first, (w_query.shape[1], w_key.shape[1], w_value.shape[1])), tie


def gather_second(w_output, w_inner, w_outer):
    second, _ = gather_grouped((w_output, w_inner, w_outer.T))
    wo, wi, wu_t = split_grouped(second, (w_output.shape[1], w_inner.shape[1], w_outer.shape[0]))
    return (wo, wi, wu_t.T)


def reduce_seq_stage(grads, tie=None):
    dp_size = lax.psum(1, "dp")
    chunks = [grad.reshape(grad.shape[0], dp_size, grad.shape[1] // dp_size) for grad in grads]
    stacked = jnp.concatenate(chunks, axis=2).astype(jnp.bfloat16)
    stacked, tie = lax.optimization_barrier((stacked, tie))
    reduced = lax.psum_scatter(stacked, "seq", scatter_dimension=0, tiled=True)
    return (reduced, [c.shape[2] for c in chunks]), tie


def stack_for_seq(grads):
    dp_size = lax.psum(1, "dp")
    chunks = [grad.reshape(grad.shape[0], dp_size, grad.shape[1] // dp_size) for grad in grads]
    return jnp.concatenate(chunks, axis=2).astype(jnp.bfloat16), [c.shape[2] for c in chunks]


def reduce_dp_stage(stages):
    joined = jnp.concatenate([stage for stage, _ in stages], axis=2)
    over_dp = lax.psum_scatter(joined, "dp", scatter_dimension=1, tiled=True)[:, 0].astype(jnp.float32)
    pieces, at = [], 0
    for _, widths in stages:
        for width in widths:
            pieces.append(over_dp[:, at : at + width])
            at += width
    return pieces


HALF_FULL = WINDOW // 2
HALF_POOL = POOL_SPAN // 2 // STRIDE
BLOCK_POOL = CLEN // STRIDE


def layout_of(index, offsets):
    in_prompt = index < PROMPT
    segment = jnp.where(in_prompt, -1, (index - PROMPT) // CLEN)
    within = index - PROMPT - segment * CLEN
    choose = segment[..., None] == jnp.arange(CONT, dtype=jnp.int32)
    spread = offsets.reshape(offsets.shape[:1] + (1,) * (index.ndim - 1) + offsets.shape[1:])
    cont_start = jnp.sum(jnp.where(choose, spread, 0), axis=-1)
    position = jnp.where(in_prompt, index, cont_start + within)
    limit = jnp.where(in_prompt, PROMPT, cont_start)
    return segment, position, limit


def window_rows(source, starts, length):
    groups, blocks = starts.shape
    return jnp.stack(
        [
            jnp.stack(
                [lax.dynamic_slice_in_dim(source[g], starts[g, b], length, 0) for b in range(blocks)]
            )
            for g in range(groups)
        ]
    )


def window_add(target, updates, starts):
    groups, blocks = starts.shape
    length = updates.shape[2]
    rows = []
    for g in range(groups):
        row = target[g]
        for b in range(blocks):
            start = starts[g, b]
            current = lax.dynamic_slice_in_dim(row, start, length, 0)
            row = lax.dynamic_update_slice_in_dim(row, current + updates[g, b], start, 0)
        rows.append(row)
    return jnp.stack(rows)


def block_geometry(seq_index, groups, shard_rows, offsets):
    group_len = PROMPT + CONT * CLEN
    pooled_len = group_len // STRIDE
    blocks = shard_rows // CLEN
    block_start = (seq_index * blocks + jnp.arange(blocks, dtype=jnp.int32)) * CLEN
    prompt_block = block_start < PROMPT
    cont_index = jnp.clip((block_start - PROMPT) // CLEN, 0, CONT - 1)
    anchor = jnp.where(prompt_block[None, :], block_start[None, :], offsets[:, cont_index])
    pooled_start = block_start // STRIDE
    intended = (
        anchor - HALF_FULL,
        jnp.broadcast_to(block_start + CLEN, anchor.shape),
        anchor // STRIDE - HALF_POOL,
        jnp.broadcast_to(pooled_start + BLOCK_POOL, anchor.shape),
    )
    limits = (group_len, group_len, pooled_len, pooled_len)
    lengths = (HALF_FULL, HALF_FULL, HALF_POOL, HALF_POOL)
    clamped = tuple(
        jnp.clip(start, 0, limit - length) for start, limit, length in zip(intended, limits, lengths)
    )
    ramp = lambda n: jnp.arange(n, dtype=jnp.int32)

    def span(window):
        actual = clamped[window][:, :, None] + ramp(lengths[window])
        offset = actual - intended[window][:, :, None]
        return actual, (offset >= 0) & (offset < lengths[window])

    before_full, before_full_ok = span(0)
    after_full, after_full_ok = span(1)
    before_pool, before_pool_ok = span(2)
    after_pool, after_pool_ok = span(3)
    after_ok = prompt_block[None, :, None]
    own_full = jnp.broadcast_to(block_start[None, :, None] + ramp(CLEN), anchor.shape + (CLEN,))
    own_pool = jnp.broadcast_to(
        pooled_start[None, :, None] + ramp(BLOCK_POOL), anchor.shape + (BLOCK_POOL,)
    )
    full_index = jnp.concatenate([before_full, own_full, after_full], axis=2)
    pooled_index = jnp.concatenate([before_pool, own_pool, after_pool], axis=2)
    full_valid = jnp.concatenate(
        [before_full_ok, jnp.ones(own_full.shape, bool), after_ok & after_full_ok], axis=2
    )
    pooled_valid = jnp.concatenate(
        [before_pool_ok, jnp.ones(own_pool.shape, bool), after_ok & after_pool_ok], axis=2
    )
    query_index = block_start[None, :, None] + ramp(CLEN)
    query_index = jnp.broadcast_to(query_index, anchor.shape + (CLEN,))
    q_seg, q_pos, q_lim = layout_of(query_index, offsets)

    def visible(key_token, valid, reach):
        k_seg, k_pos, _ = layout_of(key_token, offsets)
        k_seg, k_pos, valid = k_seg[:, :, None, :], k_pos[:, :, None, :], valid[:, :, None, :]
        prompt_key = (k_seg < 0) & (k_pos < q_lim[..., None])
        own_key = (k_seg == q_seg[..., None]) & (q_seg[..., None] >= 0)
        distance = k_pos - q_pos[..., None]
        return valid & (prompt_key | own_key) & (distance >= -(reach // 2)) & (distance < reach // 2)

    mask = jnp.concatenate(
        [
            visible(full_index, full_valid, WINDOW),
            visible(pooled_index * STRIDE, pooled_valid, POOL_SPAN),
        ],
        axis=3,
    )
    return clamped, mask


def attention_fwd(queries, kv_local, pkv_local, kv_all, pkv_all, starts, mask):
    groups, shard_rows, width = queries.shape
    blocks = shard_rows // CLEN
    score_scale = 1.0 / HEAD_DIM**0.5
    keys_cat = jnp.concatenate(
        [
            window_rows(kv_all, starts[0], HALF_FULL),
            kv_local.reshape(groups, blocks, CLEN, 2 * width),
            window_rows(kv_all, starts[1], HALF_FULL),
            window_rows(pkv_all, starts[2], HALF_POOL),
            pkv_local.reshape(groups, blocks, BLOCK_POOL, 2 * width),
            window_rows(pkv_all, starts[3], HALF_POOL),
        ],
        axis=2,
    )
    span = keys_cat.shape[2]
    head_keys = keys_cat[..., :width].reshape(groups, blocks, span, HEADS, HEAD_DIM)
    head_values = keys_cat[..., width:].reshape(groups, blocks, span, HEADS, HEAD_DIM)
    head_query = queries.reshape(groups, blocks, CLEN, HEADS, HEAD_DIM)
    scores = jnp.einsum(
        "gbqhd,gbkhd->gbhqk", head_query, head_keys, preferred_element_type=jnp.float32
    )
    scores = jnp.where(mask[:, :, None], scores * score_scale, -1000000000.0)
    row_top = jnp.max(scores, axis=-1, keepdims=True)
    exponent = jnp.exp(scores - row_top)
    row_total = jnp.sum(exponent, axis=-1, keepdims=True)
    probs = exponent / row_total
    attended = jnp.einsum(
        "gbhqk,gbkhd->gbqhd",
        probs.astype(jnp.bfloat16),
        head_values,
        preferred_element_type=jnp.float32,
    )
    attended = attended.reshape(groups * shard_rows, width).astype(jnp.bfloat16)
    return attended, (head_query, head_keys, head_values, probs)


def attention_bwd(grad_attended, saved, starts, seq_index):
    head_query, head_keys, head_values, probs = saved
    groups, blocks = head_query.shape[:2]
    width = HEADS * HEAD_DIM
    score_scale = 1.0 / HEAD_DIM**0.5
    head_grad = grad_attended.reshape(groups, blocks, CLEN, HEADS, HEAD_DIM)
    grad_probs = jnp.einsum(
        "gbqhd,gbkhd->gbhqk", head_grad, head_values, preferred_element_type=jnp.float32
    )
    centre = jnp.sum(probs * grad_probs, axis=-1, keepdims=True)
    grad_scores = (probs * (grad_probs - centre)).astype(jnp.bfloat16)
    grad_queries = jnp.einsum(
        "gbhqk,gbkhd->gbqhd", grad_scores, head_keys, preferred_element_type=jnp.float32
    ) * score_scale
    grad_keys = jnp.einsum(
        "gbhqk,gbqhd->gbkhd", grad_scores, head_query, preferred_element_type=jnp.float32
    ) * score_scale
    grad_values = jnp.einsum(
        "gbhqk,gbqhd->gbkhd",
        probs.astype(jnp.bfloat16),
        head_grad,
        preferred_element_type=jnp.float32,
    )
    span = grad_keys.shape[2]
    grad_kv = jnp.concatenate(
        [grad_keys.reshape(groups, blocks, span, width), grad_values.reshape(groups, blocks, span, width)],
        axis=3,
    )
    shard_rows = blocks * CLEN
    group_len = PROMPT + CONT * CLEN
    cut = (0, HALF_FULL, HALF_FULL + CLEN, 2 * HALF_FULL + CLEN)
    pcut = tuple(cut[-1] + c for c in (0, HALF_POOL, HALF_POOL + BLOCK_POOL, 2 * HALF_POOL + BLOCK_POOL))
    own_full = grad_kv[:, :, cut[1] : cut[2]].reshape(groups, shard_rows, 2 * width)
    own_pooled = grad_kv[:, :, pcut[1] : pcut[2]].reshape(groups, shard_rows // STRIDE, 2 * width)
    full = jnp.zeros((groups, group_len, 2 * width), jnp.float32)
    full = lax.dynamic_update_slice_in_dim(full, own_full, seq_index * shard_rows, 1)
    full = window_add(full, grad_kv[:, :, cut[0] : cut[1]], starts[0])
    full = window_add(full, grad_kv[:, :, cut[2] : cut[3]], starts[1])
    pooled = jnp.zeros((groups, group_len // STRIDE, 2 * width), jnp.float32)
    pooled = lax.dynamic_update_slice_in_dim(pooled, own_pooled, seq_index * shard_rows // STRIDE, 1)
    pooled = window_add(pooled, grad_kv[:, :, pcut[0] : pcut[1]], starts[2])
    pooled = window_add(pooled, grad_kv[:, :, pcut[2] : pcut[3]], starts[3])
    grad_queries = grad_queries.reshape(groups * shard_rows, width).astype(jnp.bfloat16)
    return grad_queries, full, pooled


def pool_grouped(source, weight):
    groups, rows, width = source.shape
    return jnp.sum(
        source.reshape(groups, rows // STRIDE, STRIDE, width) * weight[None, None], axis=2
    )


def unpool_grouped(pooled_grad, weight):
    groups, rows, width = pooled_grad.shape
    return (pooled_grad[:, :, None, :] * weight[None, None]).reshape(groups, rows * STRIDE, width)


def pool_grad_grouped(pooled_grad, source):
    groups, rows, width = source.shape
    blocks_view = source.astype(jnp.float32).reshape(groups, rows // STRIDE, STRIDE, width)
    return jnp.sum(pooled_grad[:, :, None, :] * blocks_view, axis=(0, 1))


def local(
    hidden_in,
    w_query,
    w_key,
    w_value,
    w_output,
    w_inner,
    w_outer,
    pool_weight,
    ln_gain,
    ln_bias,
    branch_blocks,
    grad_out,
):
    pool_rows_count = pool_weight.shape[0] * pool_weight.shape[1]
    small_local = jnp.concatenate(
        [pool_weight.reshape(pool_rows_count, -1), ln_gain, ln_bias], axis=0
    )
    small_full = lax.all_gather(small_local, ("dp", "seq"), axis=1, tiled=True)
    hidden_all = lax.all_gather(hidden_in, "seq", axis=1, tiled=True)
    (wq, wk, wv), (hidden_all, small_full) = gather_first(
        w_query, w_key, w_value, (hidden_all, small_full)
    )
    pool_full = small_full[:pool_rows_count].reshape(pool_weight.shape[0], pool_weight.shape[1], -1)
    gain_full = small_full[pool_rows_count : pool_rows_count + ln_gain.shape[0]]
    bias_full = small_full[pool_rows_count + ln_gain.shape[0] :]
    groups, shard_rows, width = hidden_in.shape
    seq_index = lax.axis_index("seq")
    offsets = STRIDE * branch_blocks
    starts, mask = block_geometry(seq_index, groups, shard_rows, offsets)

    group_len = hidden_all.shape[1]
    tokens = hidden_in.reshape(groups * shard_rows, width)
    all_tokens = hidden_all.reshape(groups * group_len, width)
    queries = product(tokens, wq).astype(jnp.bfloat16)
    key_g = product(all_tokens, wk).astype(jnp.bfloat16).reshape(groups, group_len, width)
    value_g = product(all_tokens, wv).astype(jnp.bfloat16).reshape(groups, group_len, width)
    pooled_keys = pool_grouped(key_g.astype(jnp.float32), pool_full[0]).astype(jnp.bfloat16)
    pooled_values = pool_grouped(value_g.astype(jnp.float32), pool_full[1]).astype(jnp.bfloat16)
    kv_all = jnp.concatenate([key_g, value_g], axis=2)
    pkv_all = jnp.concatenate([pooled_keys, pooled_values], axis=2)
    kv_local = lax.dynamic_slice_in_dim(kv_all, seq_index * shard_rows, shard_rows, 1)
    pkv_local = lax.dynamic_slice_in_dim(
        pkv_all, seq_index * (shard_rows // STRIDE), shard_rows // STRIDE, 1
    )
    wq, wk, wv, w_output, w_inner, w_outer = lax.optimization_barrier(
        (wq, wk, wv, w_output, w_inner, w_outer)
    )
    wo, wi, wu = gather_second(w_output, w_inner, w_outer)
    attended, att_saved = attention_fwd(
        queries.reshape(groups, shard_rows, width), kv_local, pkv_local, kv_all, pkv_all, starts, mask
    )
    mixed_rows = tokens.astype(jnp.float32) + product(attended, wo)
    normed_first = layer_norm(mixed_rows, gain_full[0], bias_full[0])
    first_low = normed_first.astype(jnp.bfloat16)
    inner_act = product(first_low, wi)
    active = jax.nn.gelu(inner_act, approximate=False).astype(jnp.bfloat16)
    second = normed_first + product(active, wu)
    norm_value, second_back = jax.vjp(layer_norm, second, gain_full[1], bias_full[1])
    output = norm_value.astype(jnp.bfloat16)

    cotangent = grad_out.reshape(groups * shard_rows, width).astype(jnp.float32)
    grad_second, gain_second, bias_second = second_back(cotangent)
    grad_ffn_out = grad_second.astype(jnp.bfloat16)
    grad_outer = product_left(active, grad_ffn_out)
    grad_active = product_right(grad_ffn_out, wu)
    gelu_value, gelu_back = jax.vjp(partial(jax.nn.gelu, approximate=False), inner_act)
    grad_inner_act = gelu_back(grad_active)[0].astype(jnp.bfloat16)
    grad_inner = product_left(first_low, grad_inner_act)
    grad_first = grad_second + product_right(grad_inner_act, wi)
    first_value, first_back = jax.vjp(layer_norm, mixed_rows, gain_full[0], bias_full[0])
    grad_mixed, gain_first, bias_first = first_back(grad_first)
    grad_branch = grad_mixed.astype(jnp.bfloat16)
    grad_output = product_left(attended, grad_branch)
    grad_attended = product_right(grad_branch, wo).astype(jnp.bfloat16)
    early, grad_attended = reduce_seq_stage((grad_output, grad_inner, grad_outer.T), grad_attended)
    early_reduced, early_widths = early

    grad_rows = grad_attended.reshape(groups, shard_rows, width)
    pieces_back = []
    for g in range(groups):
        saved_g = tuple(item[g : g + 1] for item in att_saved)
        starts_g = tuple(item[g : g + 1] for item in starts)
        grad_g = grad_rows[g].reshape(shard_rows, width)
        grad_queries_g, full_g, pooled_g = attention_bwd(grad_g, saved_g, starts_g, seq_index)
        if g == 1:
            full_g, pooled_g, earlier_back, early_reduced = lax.optimization_barrier(
                (full_g, pooled_g, pieces_back[0][4], early_reduced)
            )
            pieces_back[0] = pieces_back[0][:4] + (earlier_back,)
        key_partial_g = (
            full_g[..., :width] + unpool_grouped(pooled_g[..., :width], pool_full[0])
        ).astype(jnp.bfloat16).reshape(group_len, width)
        value_partial_g = (
            full_g[..., width:] + unpool_grouped(pooled_g[..., width:], pool_full[1])
        ).astype(jnp.bfloat16).reshape(group_len, width)
        back_g = product_right(key_partial_g, wk) + product_right(value_partial_g, wv)
        back_g = back_g.reshape(1, group_len, width).astype(jnp.bfloat16)
        if g == groups - 1:
            back_own_g = back_g
        else:
            back_own_g = lax.psum_scatter(back_g, "seq", scatter_dimension=1, tiled=True)
        pieces_back.append((grad_queries_g, pooled_g, key_partial_g, value_partial_g, back_own_g))
    grad_queries = jnp.concatenate([piece[0] for piece in pieces_back], axis=0)
    grad_pooled = jnp.concatenate([piece[1] for piece in pieces_back], axis=0)
    key_partial = jnp.concatenate([piece[2] for piece in pieces_back], axis=0)
    value_partial = jnp.concatenate([piece[3] for piece in pieces_back], axis=0)
    last_back = pieces_back[-1][4]
    early_dp = reduce_dp_stage(((early_reduced, early_widths),))
    grad_pooling = jnp.stack(
        [
            pool_grad_grouped(grad_pooled[..., :width], key_g),
            pool_grad_grouped(grad_pooled[..., width:], value_g),
        ]
    )
    grad_query_w = product_left(tokens, grad_queries)
    grad_key_w = product_left(all_tokens, key_partial)
    grad_value_w = product_left(all_tokens, value_partial)
    late_stacked, late_widths = stack_for_seq((grad_query_w, grad_key_w, grad_value_w))
    late_stacked, early_dp = lax.optimization_barrier((late_stacked, early_dp))
    seq_size = lax.psum(1, "seq")
    late_flat = late_stacked.reshape(seq_size, -1, width)
    back_flat = last_back.reshape(seq_size, -1, width)
    joined = jnp.concatenate([late_flat, back_flat], axis=1)
    chunk_rows = joined.shape[1]
    joined = joined.reshape(seq_size * chunk_rows, width)
    joined = lax.psum_scatter(joined, "seq", scatter_dimension=0, tiled=True)
    late_reduced = joined[: late_flat.shape[1]].reshape(
        late_stacked.shape[0] // seq_size, late_stacked.shape[1], late_stacked.shape[2]
    )
    back_last = joined[late_flat.shape[1] :].reshape(1, shard_rows, width)
    back_own = jnp.concatenate([piece[4] for piece in pieces_back[:-1]] + [back_last], axis=0)
    grad_tokens = (
        grad_mixed
        + product_right(grad_queries, wq)
        + back_own.reshape(groups * shard_rows, width).astype(jnp.float32)
    )
    late_dp = reduce_dp_stage(((late_reduced, late_widths),))
    accum = (late_dp[0], late_dp[1], late_dp[2], early_dp[0], early_dp[1], early_dp[2].T)
    small_sums = (
        lax.psum_scatter(grad_pooling, ("dp", "seq"), scatter_dimension=2, tiled=True),
        lax.psum_scatter(
            jnp.stack([gain_first, gain_second]), ("dp", "seq"), scatter_dimension=1, tiled=True
        ),
        lax.psum_scatter(
            jnp.stack([bias_first, bias_second]), ("dp", "seq"), scatter_dimension=1, tiled=True
        ),
    )
    return (
        output.reshape(groups, shard_rows, width),
        grad_tokens.astype(jnp.bfloat16).reshape(groups, shard_rows, width),
        accum[0],
        accum[1],
        accum[2],
        accum[3],
        accum[4],
        accum[5],
        small_sums[0],
        small_sums[1],
        small_sums[2],
    )


def solution(mesh):
    in_specs = (
        P("dp", "seq", None),
        P("seq", "dp"),
        P("seq", "dp"),
        P("seq", "dp"),
        P("seq", "dp"),
        P("seq", "dp"),
        P("dp", "seq"),
        P(None, None, ("dp", "seq")),
        P(None, ("dp", "seq")),
        P(None, ("dp", "seq")),
        P("dp", None),
        P("dp", "seq", None),
    )
    out_specs = (
        P("dp", "seq", None),
        P("dp", "seq", None),
        P("seq", "dp"),
        P("seq", "dp"),
        P("seq", "dp"),
        P("seq", "dp"),
        P("seq", "dp"),
        P("dp", "seq"),
        P(None, None, ("dp", "seq")),
        P(None, ("dp", "seq")),
        P(None, ("dp", "seq")),
    )
    return jax.shard_map(local, mesh=mesh, in_specs=in_specs, out_specs=out_specs, check_vma=False)
```

```python
from functools import partial

import jax
import jax.numpy as jnp
from jax import lax
from jax.sharding import PartitionSpec as P

HEADS = 12
HEAD_DIM = 64
PROMPT = 1024
CONT = 8
CLEN = 128
WINDOW = 128
POOL_SPAN = 512
STRIDE = 4


eps_norm = 1e-05


def token_layout(positions_in, offsets):
    in_prompt = positions_in < PROMPT
    segment = jnp.where(in_prompt, -1, (positions_in - PROMPT) // CLEN)
    within = positions_in - PROMPT - segment * CLEN
    choose = (segment[:, None] == jnp.arange(CONT, dtype=jnp.int32)[None, :]).astype(jnp.int32)
    cont_start = jnp.sum(choose * offsets[None, :], axis=1)
    position = jnp.where(in_prompt, positions_in, cont_start + within)
    prompt_limit = jnp.where(in_prompt, PROMPT, cont_start)
    return (segment, position, prompt_limit)


def visible_keys(query_rows, key_index, offsets, reach):
    query_seg, query_pos, query_limit = token_layout(query_rows, offsets)
    key_seg, key_pos, key_limit = token_layout(key_index, offsets)
    prompt_key = (key_seg[None, :] < 0) & (key_pos[None, :] < query_limit[:, None])
    own_key = (key_seg[None, :] == query_seg[:, None]) & (query_seg[:, None] >= 0)
    distance = key_pos[None, :] - query_pos[:, None]
    return (prompt_key | own_key) & (distance >= -(reach // 2)) & (distance < reach // 2)


def key_mask(query_rows, offsets):
    group_len = PROMPT + CONT * CLEN
    full_keys = jnp.arange(group_len, dtype=jnp.int32)
    pooled_keys = jnp.arange(group_len // STRIDE, dtype=jnp.int32) * STRIDE
    return jnp.concatenate(
        [
            visible_keys(query_rows, full_keys, offsets, WINDOW),
            visible_keys(query_rows, pooled_keys, offsets, POOL_SPAN),
        ],
        axis=1,
    )


def pool_rows(source, weight):
    return jnp.sum(
        source.reshape(source.shape[0] // STRIDE, STRIDE, source.shape[1]) * weight[None, :, :],
        axis=1,
    )


def unpool(pooled_grad, weight):
    return (pooled_grad[:, None, :] * weight[None, :, :]).reshape(-1, pooled_grad.shape[1])


def pool_grad(pooled_grad, source):
    blocks_view = source.astype(jnp.float32).reshape(-1, STRIDE, source.shape[1])
    return jnp.sum(pooled_grad[:, None, :] * blocks_view, axis=0)


def layer_norm(source, gain, bias):
    centre = jnp.mean(source, axis=-1, keepdims=True)
    centred = source - centre
    spread = jnp.mean(centred * centred, axis=-1, keepdims=True)
    return centred * lax.rsqrt(spread + eps_norm) * gain + bias


def product(left, right):
    return jnp.dot(left, right, preferred_element_type=jnp.float32)


def product_left(left, right):
    return lax.dot_general(
        left, right, (((0,), (0,)), ((), ())), preferred_element_type=jnp.float32
    )


def product_right(left, right):
    return lax.dot_general(
        left, right, (((1,), (1,)), ((), ())), preferred_element_type=jnp.float32
    )


def add_pair(left_term, right_term):
    return left_term + right_term


def gather_grouped(shards, tie=None):
    local_block = jnp.concatenate(shards, axis=1)
    across = lax.all_gather(local_block, "dp", axis=1, tiled=False)
    across, tie = lax.optimization_barrier((across, tie))
    return lax.all_gather(across, "seq", axis=0, tiled=True), tie


def split_grouped(gathered, widths):
    pieces, at = [], 0
    for width in widths:
        piece = gathered[:, :, at : at + width]
        pieces.append(piece.reshape(piece.shape[0], -1))
        at += width
    return pieces


def gather_first(w_query, w_key, w_value, tie):
    first, tie = gather_grouped((w_query, w_key, w_value), tie)
    return split_grouped(first, (w_query.shape[1], w_key.shape[1], w_value.shape[1])), tie


def gather_second(w_output, w_inner, w_outer):
    second, _ = gather_grouped((w_output, w_inner, w_outer.T))
    wo, wi, wu_t = split_grouped(second, (w_output.shape[1], w_inner.shape[1], w_outer.shape[0]))
    return (wo, wi, wu_t.T)


def reduce_seq_stage(grads, tie=None):
    dp_size = lax.psum(1, "dp")
    chunks = [grad.reshape(grad.shape[0], dp_size, grad.shape[1] // dp_size) for grad in grads]
    stacked = jnp.concatenate(chunks, axis=2).astype(jnp.bfloat16)
    stacked, tie = lax.optimization_barrier((stacked, tie))
    reduced = lax.psum_scatter(stacked, "seq", scatter_dimension=0, tiled=True)
    return (reduced, [c.shape[2] for c in chunks]), tie


def stack_for_seq(grads):
    dp_size = lax.psum(1, "dp")
    chunks = [grad.reshape(grad.shape[0], dp_size, grad.shape[1] // dp_size) for grad in grads]
    return jnp.concatenate(chunks, axis=2).astype(jnp.bfloat16), [c.shape[2] for c in chunks]


def reduce_dp_stage(stages):
    joined = jnp.concatenate([stage for stage, _ in stages], axis=2)
    over_dp = lax.psum_scatter(joined, "dp", scatter_dimension=1, tiled=True)[:, 0].astype(jnp.float32)
    pieces, at = [], 0
    for _, widths in stages:
        for width in widths:
            pieces.append(over_dp[:, at : at + width])
            at += width
    return pieces


HALF_FULL = WINDOW // 2
HALF_POOL = POOL_SPAN // 2 // STRIDE
BLOCK_POOL = CLEN // STRIDE


def layout_of(index, offsets):
    in_prompt = index < PROMPT
    segment = jnp.where(in_prompt, -1, (index - PROMPT) // CLEN)
    within = index - PROMPT - segment * CLEN
    choose = segment[..., None] == jnp.arange(CONT, dtype=jnp.int32)
    spread = offsets.reshape(offsets.shape[:1] + (1,) * (index.ndim - 1) + offsets.shape[1:])
    cont_start = jnp.sum(jnp.where(choose, spread, 0), axis=-1)
    position = jnp.where(in_prompt, index, cont_start + within)
    limit = jnp.where(in_prompt, PROMPT, cont_start)
    return segment, position, limit


def window_rows(source, starts, length):
    groups, blocks = starts.shape
    return jnp.stack(
        [
            jnp.stack(
                [lax.dynamic_slice_in_dim(source[g], starts[g, b], length, 0) for b in range(blocks)]
            )
            for g in range(groups)
        ]
    )


def window_add(target, updates, starts):
    groups, blocks = starts.shape
    length = updates.shape[2]
    rows = []
    for g in range(groups):
        row = target[g]
        for b in range(blocks):
            start = starts[g, b]
            current = lax.dynamic_slice_in_dim(row, start, length, 0)
            row = lax.dynamic_update_slice_in_dim(row, current + updates[g, b], start, 0)
        rows.append(row)
    return jnp.stack(rows)


def block_geometry(seq_index, groups, shard_rows, offsets):
    group_len = PROMPT + CONT * CLEN
    pooled_len = group_len // STRIDE
    blocks = shard_rows // CLEN
    block_start = (seq_index * blocks + jnp.arange(blocks, dtype=jnp.int32)) * CLEN
    prompt_block = block_start < PROMPT
    cont_index = jnp.clip((block_start - PROMPT) // CLEN, 0, CONT - 1)
    anchor = jnp.where(prompt_block[None, :], block_start[None, :], offsets[:, cont_index])
    pooled_start = block_start // STRIDE
    intended = (
        anchor - HALF_FULL,
        jnp.broadcast_to(block_start + CLEN, anchor.shape),
        anchor // STRIDE - HALF_POOL,
        jnp.broadcast_to(pooled_start + BLOCK_POOL, anchor.shape),
    )
    limits = (group_len, group_len, pooled_len, pooled_len)
    lengths = (HALF_FULL, HALF_FULL, HALF_POOL, HALF_POOL)
    clamped = tuple(
        jnp.clip(start, 0, limit - length) for start, limit, length in zip(intended, limits, lengths)
    )
    ramp = lambda n: jnp.arange(n, dtype=jnp.int32)

    def span(window):
        actual = clamped[window][:, :, None] + ramp(lengths[window])
        offset = actual - intended[window][:, :, None]
        return actual, (offset >= 0) & (offset < lengths[window])

    before_full, before_full_ok = span(0)
    after_full, after_full_ok = span(1)
    before_pool, before_pool_ok = span(2)
    after_pool, after_pool_ok = span(3)
    after_ok = prompt_block[None, :, None]
    own_full = jnp.broadcast_to(block_start[None, :, None] + ramp(CLEN), anchor.shape + (CLEN,))
    own_pool = jnp.broadcast_to(
        pooled_start[None, :, None] + ramp(BLOCK_POOL), anchor.shape + (BLOCK_POOL,)
    )
    full_index = jnp.concatenate([before_full, own_full, after_full], axis=2)
    pooled_index = jnp.concatenate([before_pool, own_pool, after_pool], axis=2)
    full_valid = jnp.concatenate(
        [before_full_ok, jnp.ones(own_full.shape, bool), after_ok & after_full_ok], axis=2
    )
    pooled_valid = jnp.concatenate(
        [before_pool_ok, jnp.ones(own_pool.shape, bool), after_ok & after_pool_ok], axis=2
    )
    query_index = block_start[None, :, None] + ramp(CLEN)
    query_index = jnp.broadcast_to(query_index, anchor.shape + (CLEN,))
    q_seg, q_pos, q_lim = layout_of(query_index, offsets)

    def visible(key_token, valid, reach):
        k_seg, k_pos, _ = layout_of(key_token, offsets)
        k_seg, k_pos, valid = k_seg[:, :, None, :], k_pos[:, :, None, :], valid[:, :, None, :]
        prompt_key = (k_seg < 0) & (k_pos < q_lim[..., None])
        own_key = (k_seg == q_seg[..., None]) & (q_seg[..., None] >= 0)
        distance = k_pos - q_pos[..., None]
        return valid & (prompt_key | own_key) & (distance >= -(reach // 2)) & (distance < reach // 2)

    mask = jnp.concatenate(
        [
            visible(full_index, full_valid, WINDOW),
            visible(pooled_index * STRIDE, pooled_valid, POOL_SPAN),
        ],
        axis=3,
    )
    return clamped, mask


def attention_fwd(queries, kv_local, pkv_local, kv_all, pkv_all, starts, mask):
    groups, shard_rows, width = queries.shape
    blocks = shard_rows // CLEN
    score_scale = 1.0 / HEAD_DIM**0.5
    keys_cat = jnp.concatenate(
        [
            window_rows(kv_all, starts[0], HALF_FULL),
            kv_local.reshape(groups, blocks, CLEN, 2 * width),
            window_rows(kv_all, starts[1], HALF_FULL),
            window_rows(pkv_all, starts[2], HALF_POOL),
            pkv_local.reshape(groups, blocks, BLOCK_POOL, 2 * width),
            window_rows(pkv_all, starts[3], HALF_POOL),
        ],
        axis=2,
    )
    span = keys_cat.shape[2]
    head_keys = keys_cat[..., :width].reshape(groups, blocks, span, HEADS, HEAD_DIM)
    head_values = keys_cat[..., width:].reshape(groups, blocks, span, HEADS, HEAD_DIM)
    head_query = queries.reshape(groups, blocks, CLEN, HEADS, HEAD_DIM)
    scores = jnp.einsum(
        "gbqhd,gbkhd->gbhqk", head_query, head_keys, preferred_element_type=jnp.float32
    )
    scores = jnp.where(mask[:, :, None], scores * score_scale, -1000000000.0)
    row_top = jnp.max(scores, axis=-1, keepdims=True)
    exponent = jnp.exp(scores - row_top)
    row_total = jnp.sum(exponent, axis=-1, keepdims=True)
    probs = exponent / row_total
    attended = jnp.einsum(
        "gbhqk,gbkhd->gbqhd",
        probs.astype(jnp.bfloat16),
        head_values,
        preferred_element_type=jnp.float32,
    )
    attended = attended.reshape(groups * shard_rows, width).astype(jnp.bfloat16)
    return attended, (head_query, head_keys, head_values, probs)


def attention_bwd(grad_attended, saved, starts, seq_index):
    head_query, head_keys, head_values, probs = saved
    groups, blocks = head_query.shape[:2]
    width = HEADS * HEAD_DIM
    score_scale = 1.0 / HEAD_DIM**0.5
    head_grad = grad_attended.reshape(groups, blocks, CLEN, HEADS, HEAD_DIM)
    grad_probs = jnp.einsum(
        "gbqhd,gbkhd->gbhqk", head_grad, head_values, preferred_element_type=jnp.float32
    )
    centre = jnp.sum(probs * grad_probs, axis=-1, keepdims=True)
    grad_scores = (probs * (grad_probs - centre)).astype(jnp.bfloat16)
    grad_queries = jnp.einsum(
        "gbhqk,gbkhd->gbqhd", grad_scores, head_keys, preferred_element_type=jnp.float32
    ) * score_scale
    grad_keys = jnp.einsum(
        "gbhqk,gbqhd->gbkhd", grad_scores, head_query, preferred_element_type=jnp.float32
    ) * score_scale
    grad_values = jnp.einsum(
        "gbhqk,gbqhd->gbkhd",
        probs.astype(jnp.bfloat16),
        head_grad,
        preferred_element_type=jnp.float32,
    )
    span = grad_keys.shape[2]
    grad_kv = jnp.concatenate(
        [grad_keys.reshape(groups, blocks, span, width), grad_values.reshape(groups, blocks, span, width)],
        axis=3,
    )
    shard_rows = blocks * CLEN
    group_len = PROMPT + CONT * CLEN
    pooled_len = group_len // STRIDE
    cut = (0, HALF_FULL, HALF_FULL + CLEN, 2 * HALF_FULL + CLEN)
    pcut = tuple(cut[-1] + c for c in (0, HALF_POOL, HALF_POOL + BLOCK_POOL, 2 * HALF_POOL + BLOCK_POOL))
    ramp = lambda n: jnp.arange(n, dtype=jnp.int32)
    own_full = grad_kv[:, :, cut[1] : cut[2]].reshape(groups, shard_rows, 2 * width)
    full = jnp.zeros((groups, group_len, 2 * width), jnp.float32)
    full = lax.dynamic_update_slice_in_dim(full, own_full, seq_index * shard_rows, 1)
    side_values = jnp.concatenate(
        [grad_kv[:, :, cut[0] : cut[1]], grad_kv[:, :, cut[2] : cut[3]]], axis=2
    ).reshape(groups, -1, 2 * width)
    side_rows = jnp.concatenate(
        [starts[0][:, :, None] + ramp(HALF_FULL), starts[1][:, :, None] + ramp(HALF_FULL)], axis=2
    ).reshape(groups, -1)
    own_pool_rows = (seq_index * (shard_rows // STRIDE) + ramp(blocks)[:, None] * BLOCK_POOL + ramp(BLOCK_POOL))
    pool_values = grad_kv[:, :, pcut[0] : pcut[3]].reshape(groups, -1, 2 * width)
    pool_rows_index = jnp.concatenate(
        [
            starts[2][:, :, None] + ramp(HALF_POOL),
            jnp.broadcast_to(own_pool_rows[None], (groups, blocks, BLOCK_POOL)),
            starts[3][:, :, None] + ramp(HALF_POOL),
        ],
        axis=2,
    ).reshape(groups, -1)
    fulls, pooleds, unpooleds = [], [], []
    for g in range(groups):
        fulls.append(full[g] + select_sum(side_values[g], side_rows[g] == ramp(group_len)[:, None]))
        pooleds.append(select_sum(pool_values[g], pool_rows_index[g] == ramp(pooled_len)[:, None]))
        unpooleds.append(
            select_sum(pool_values[g], pool_rows_index[g] == (ramp(group_len) // STRIDE)[:, None])
        )
    full = jnp.stack(fulls)
    pooled = jnp.stack(pooleds)
    unpooled = jnp.stack(unpooleds)
    grad_queries = grad_queries.reshape(groups * shard_rows, width).astype(jnp.bfloat16)
    return grad_queries, full, pooled, unpooled


def select_sum(values, chosen):
    onehot = chosen.astype(jnp.bfloat16)
    high = values.astype(jnp.bfloat16)
    low = (values - high.astype(jnp.float32)).astype(jnp.bfloat16)
    return product(onehot, high) + product(onehot, low)


def phase_weights(weight, rows):
    phase = (jnp.arange(rows, dtype=jnp.int32) % STRIDE)[:, None]
    total = jnp.zeros((rows, weight.shape[1]), jnp.float32)
    for r in range(STRIDE):
        total = total + jnp.where(phase == r, weight[r][None, :], 0.0)
    return total


def pool_grouped(source, weight):
    groups, rows, width = source.shape
    return jnp.sum(
        source.reshape(groups, rows // STRIDE, STRIDE, width) * weight[None, None], axis=2
    )


def unpool_grouped(pooled_grad, weight):
    groups, rows, width = pooled_grad.shape
    return (pooled_grad[:, :, None, :] * weight[None, None]).reshape(groups, rows * STRIDE, width)


def pool_grad_grouped(pooled_grad, source):
    groups, rows, width = source.shape
    blocks_view = source.astype(jnp.float32).reshape(groups, rows // STRIDE, STRIDE, width)
    return jnp.sum(pooled_grad[:, :, None, :] * blocks_view, axis=(0, 1))


def local(
    hidden_in,
    w_query,
    w_key,
    w_value,
    w_output,
    w_inner,
    w_outer,
    pool_weight,
    ln_gain,
    ln_bias,
    branch_blocks,
    grad_out,
):
    pool_rows_count = pool_weight.shape[0] * pool_weight.shape[1]
    small_local = jnp.concatenate(
        [pool_weight.reshape(pool_rows_count, -1), ln_gain, ln_bias], axis=0
    )
    small_full = lax.all_gather(small_local, ("dp", "seq"), axis=1, tiled=True)
    hidden_all = lax.all_gather(hidden_in, "seq", axis=1, tiled=True)
    (wq, wk, wv), (hidden_all, small_full) = gather_first(
        w_query, w_key, w_value, (hidden_all, small_full)
    )
    pool_full = small_full[:pool_rows_count].reshape(pool_weight.shape[0], pool_weight.shape[1], -1)
    gain_full = small_full[pool_rows_count : pool_rows_count + ln_gain.shape[0]]
    bias_full = small_full[pool_rows_count + ln_gain.shape[0] :]
    groups, shard_rows, width = hidden_in.shape
    seq_index = lax.axis_index("seq")
    offsets = STRIDE * branch_blocks
    starts, mask = block_geometry(seq_index, groups, shard_rows, offsets)

    group_len = hidden_all.shape[1]
    tokens = hidden_in.reshape(groups * shard_rows, width)
    all_tokens = hidden_all.reshape(groups * group_len, width)
    queries = product(tokens, wq).astype(jnp.bfloat16)
    key_g = product(all_tokens, wk).astype(jnp.bfloat16).reshape(groups, group_len, width)
    value_g = product(all_tokens, wv).astype(jnp.bfloat16).reshape(groups, group_len, width)
    pooled_keys = pool_grouped(key_g.astype(jnp.float32), pool_full[0]).astype(jnp.bfloat16)
    pooled_values = pool_grouped(value_g.astype(jnp.float32), pool_full[1]).astype(jnp.bfloat16)
    kv_all = jnp.concatenate([key_g, value_g], axis=2)
    pkv_all = jnp.concatenate([pooled_keys, pooled_values], axis=2)
    kv_local = lax.dynamic_slice_in_dim(kv_all, seq_index * shard_rows, shard_rows, 1)
    pkv_local = lax.dynamic_slice_in_dim(
        pkv_all, seq_index * (shard_rows // STRIDE), shard_rows // STRIDE, 1
    )
    wq, wk, wv, w_output, w_inner, w_outer = lax.optimization_barrier(
        (wq, wk, wv, w_output, w_inner, w_outer)
    )
    wo, wi, wu = gather_second(w_output, w_inner, w_outer)
    attended, att_saved = attention_fwd(
        queries.reshape(groups, shard_rows, width), kv_local, pkv_local, kv_all, pkv_all, starts, mask
    )
    mixed_rows = tokens.astype(jnp.float32) + product(attended, wo)
    normed_first = layer_norm(mixed_rows, gain_full[0], bias_full[0])
    first_low = normed_first.astype(jnp.bfloat16)
    inner_act = product(first_low, wi)
    active = jax.nn.gelu(inner_act, approximate=False).astype(jnp.bfloat16)
    second = normed_first + product(active, wu)
    norm_value, second_back = jax.vjp(layer_norm, second, gain_full[1], bias_full[1])
    output = norm_value.astype(jnp.bfloat16)

    cotangent = grad_out.reshape(groups * shard_rows, width).astype(jnp.float32)
    grad_second, gain_second, bias_second = second_back(cotangent)
    grad_ffn_out = grad_second.astype(jnp.bfloat16)
    grad_outer = product_left(active, grad_ffn_out)
    grad_active = product_right(grad_ffn_out, wu)
    gelu_value, gelu_back = jax.vjp(partial(jax.nn.gelu, approximate=False), inner_act)
    grad_inner_act = gelu_back(grad_active)[0].astype(jnp.bfloat16)
    grad_inner = product_left(first_low, grad_inner_act)
    grad_first = grad_second + product_right(grad_inner_act, wi)
    first_value, first_back = jax.vjp(layer_norm, mixed_rows, gain_full[0], bias_full[0])
    grad_mixed, gain_first, bias_first = first_back(grad_first)
    grad_branch = grad_mixed.astype(jnp.bfloat16)
    grad_output = product_left(attended, grad_branch)
    grad_attended = product_right(grad_branch, wo).astype(jnp.bfloat16)
    early, grad_attended = reduce_seq_stage((grad_output, grad_inner, grad_outer.T), grad_attended)
    early_reduced, early_widths = early

    grad_rows = grad_attended.reshape(groups, shard_rows, width)
    key_phase = phase_weights(pool_full[0], group_len)
    value_phase = phase_weights(pool_full[1], group_len)
    pieces_back = []
    for g in range(groups):
        saved_g = tuple(item[g : g + 1] for item in att_saved)
        starts_g = tuple(item[g : g + 1] for item in starts)
        grad_g = grad_rows[g].reshape(shard_rows, width)
        grad_queries_g, full_g, pooled_g, unpooled_g = attention_bwd(grad_g, saved_g, starts_g, seq_index)
        if g == 1:
            full_g, pooled_g, unpooled_g, earlier_back, early_reduced = lax.optimization_barrier(
                (full_g, pooled_g, unpooled_g, pieces_back[0][4], early_reduced)
            )
            pieces_back[0] = pieces_back[0][:4] + (earlier_back,)
        key_partial_g = (
            full_g[0, :, :width] + unpooled_g[0, :, :width] * key_phase
        ).astype(jnp.bfloat16)
        value_partial_g = (
            full_g[0, :, width:] + unpooled_g[0, :, width:] * value_phase
        ).astype(jnp.bfloat16)
        back_g = product_right(key_partial_g, wk) + product_right(value_partial_g, wv)
        back_g = back_g.reshape(1, group_len, width).astype(jnp.bfloat16)
        if g == groups - 1:
            back_own_g = back_g
        else:
            back_own_g = lax.psum_scatter(back_g, "seq", scatter_dimension=1, tiled=True)
        pieces_back.append((grad_queries_g, pooled_g, key_partial_g, value_partial_g, back_own_g))
    grad_queries = jnp.concatenate([piece[0] for piece in pieces_back], axis=0)
    grad_pooled = jnp.concatenate([piece[1] for piece in pieces_back], axis=0)
    key_partial = jnp.concatenate([piece[2] for piece in pieces_back], axis=0)
    value_partial = jnp.concatenate([piece[3] for piece in pieces_back], axis=0)
    last_back = pieces_back[-1][4]
    early_dp = reduce_dp_stage(((early_reduced, early_widths),))
    grad_pooling = jnp.stack(
        [
            pool_grad_grouped(grad_pooled[..., :width], key_g),
            pool_grad_grouped(grad_pooled[..., width:], value_g),
        ]
    )
    grad_query_w = product_left(tokens, grad_queries)
    grad_key_w = product_left(all_tokens, key_partial)
    grad_value_w = product_left(all_tokens, value_partial)
    late_stacked, late_widths = stack_for_seq((grad_query_w, grad_key_w, grad_value_w))
    late_stacked, early_dp = lax.optimization_barrier((late_stacked, early_dp))
    seq_size = lax.psum(1, "seq")
    late_flat = late_stacked.reshape(seq_size, -1, width)
    back_flat = last_back.reshape(seq_size, -1, width)
    joined = jnp.concatenate([late_flat, back_flat], axis=1)
    chunk_rows = joined.shape[1]
    joined = joined.reshape(seq_size * chunk_rows, width)
    joined = lax.psum_scatter(joined, "seq", scatter_dimension=0, tiled=True)
    late_reduced = joined[: late_flat.shape[1]].reshape(
        late_stacked.shape[0] // seq_size, late_stacked.shape[1], late_stacked.shape[2]
    )
    back_last = joined[late_flat.shape[1] :].reshape(1, shard_rows, width)
    back_own = jnp.concatenate([piece[4] for piece in pieces_back[:-1]] + [back_last], axis=0)
    grad_tokens = (
        grad_mixed
        + product_right(grad_queries, wq)
        + back_own.reshape(groups * shard_rows, width).astype(jnp.float32)
    )
    late_dp = reduce_dp_stage(((late_reduced, late_widths),))
    accum = (late_dp[0], late_dp[1], late_dp[2], early_dp[0], early_dp[1], early_dp[2].T)
    small_sums = (
        lax.psum_scatter(grad_pooling, ("dp", "seq"), scatter_dimension=2, tiled=True),
        lax.psum_scatter(
            jnp.stack([gain_first, gain_second]), ("dp", "seq"), scatter_dimension=1, tiled=True
        ),
        lax.psum_scatter(
            jnp.stack([bias_first, bias_second]), ("dp", "seq"), scatter_dimension=1, tiled=True
        ),
    )
    return (
        output.reshape(groups, shard_rows, width),
        grad_tokens.astype(jnp.bfloat16).reshape(groups, shard_rows, width),
        accum[0],
        accum[1],
        accum[2],
        accum[3],
        accum[4],
        accum[5],
        small_sums[0],
        small_sums[1],
        small_sums[2],
    )


def solution(mesh):
    in_specs = (
        P("dp", "seq", None),
        P("seq", "dp"),
        P("seq", "dp"),
        P("seq", "dp"),
        P("seq", "dp"),
        P("seq", "dp"),
        P("dp", "seq"),
        P(None, None, ("dp", "seq")),
        P(None, ("dp", "seq")),
        P(None, ("dp", "seq")),
        P("dp", None),
        P("dp", "seq", None),
    )
    out_specs = (
        P("dp", "seq", None),
        P("dp", "seq", None),
        P("seq", "dp"),
        P("seq", "dp"),
        P("seq", "dp"),
        P("seq", "dp"),
        P("seq", "dp"),
        P("dp", "seq"),
        P(None, None, ("dp", "seq")),
        P(None, ("dp", "seq")),
        P(None, ("dp", "seq")),
    )
    return jax.shard_map(local, mesh=mesh, in_specs=in_specs, out_specs=out_specs, check_vma=False)
```

```python
from functools import partial

import jax
import jax.numpy as jnp
from jax import lax
from jax.sharding import PartitionSpec as P

HEADS = 12
HEAD_DIM = 64
PROMPT = 1024
CONT = 8
CLEN = 128
WINDOW = 128
POOL_SPAN = 512
STRIDE = 4


eps_norm = 1e-05


def token_layout(positions_in, offsets):
    in_prompt = positions_in < PROMPT
    segment = jnp.where(in_prompt, -1, (positions_in - PROMPT) // CLEN)
    within = positions_in - PROMPT - segment * CLEN
    choose = (segment[:, None] == jnp.arange(CONT, dtype=jnp.int32)[None, :]).astype(jnp.int32)
    cont_start = jnp.sum(choose * offsets[None, :], axis=1)
    position = jnp.where(in_prompt, positions_in, cont_start + within)
    prompt_limit = jnp.where(in_prompt, PROMPT, cont_start)
    return (segment, position, prompt_limit)


def visible_keys(query_rows, key_index, offsets, reach):
    query_seg, query_pos, query_limit = token_layout(query_rows, offsets)
    key_seg, key_pos, key_limit = token_layout(key_index, offsets)
    prompt_key = (key_seg[None, :] < 0) & (key_pos[None, :] < query_limit[:, None])
    own_key = (key_seg[None, :] == query_seg[:, None]) & (query_seg[:, None] >= 0)
    distance = key_pos[None, :] - query_pos[:, None]
    return (prompt_key | own_key) & (distance >= -(reach // 2)) & (distance < reach // 2)


def key_mask(query_rows, offsets):
    group_len = PROMPT + CONT * CLEN
    full_keys = jnp.arange(group_len, dtype=jnp.int32)
    pooled_keys = jnp.arange(group_len // STRIDE, dtype=jnp.int32) * STRIDE
    return jnp.concatenate(
        [
            visible_keys(query_rows, full_keys, offsets, WINDOW),
            visible_keys(query_rows, pooled_keys, offsets, POOL_SPAN),
        ],
        axis=1,
    )


def pool_rows(source, weight):
    return jnp.sum(
        source.reshape(source.shape[0] // STRIDE, STRIDE, source.shape[1]) * weight[None, :, :],
        axis=1,
    )


def unpool(pooled_grad, weight):
    return (pooled_grad[:, None, :] * weight[None, :, :]).reshape(-1, pooled_grad.shape[1])


def pool_grad(pooled_grad, source):
    blocks_view = source.astype(jnp.float32).reshape(-1, STRIDE, source.shape[1])
    return jnp.sum(pooled_grad[:, None, :] * blocks_view, axis=0)


def layer_norm(source, gain, bias):
    centre = jnp.mean(source, axis=-1, keepdims=True)
    centred = source - centre
    spread = jnp.mean(centred * centred, axis=-1, keepdims=True)
    return centred * lax.rsqrt(spread + eps_norm) * gain + bias


def product(left, right):
    return jnp.dot(left, right, preferred_element_type=jnp.float32)


def product_left(left, right):
    return lax.dot_general(
        left, right, (((0,), (0,)), ((), ())), preferred_element_type=jnp.float32
    )


def product_right(left, right):
    return lax.dot_general(
        left, right, (((1,), (1,)), ((), ())), preferred_element_type=jnp.float32
    )


def add_pair(left_term, right_term):
    return left_term + right_term


def gather_grouped(shards, tie=None):
    local_block = jnp.concatenate(shards, axis=1)
    across = lax.all_gather(local_block, "dp", axis=1, tiled=False)
    across, tie = lax.optimization_barrier((across, tie))
    return lax.all_gather(across, "seq", axis=0, tiled=True), tie


def split_grouped(gathered, widths):
    pieces, at = [], 0
    for width in widths:
        piece = gathered[:, :, at : at + width]
        pieces.append(piece.reshape(piece.shape[0], -1))
        at += width
    return pieces


def gather_first(w_query, w_key, w_value, tie):
    first, tie = gather_grouped((w_query, w_key, w_value), tie)
    return split_grouped(first, (w_query.shape[1], w_key.shape[1], w_value.shape[1])), tie


def gather_second(w_output, w_inner, w_outer):
    second, _ = gather_grouped((w_output, w_inner, w_outer.T))
    wo, wi, wu_t = split_grouped(second, (w_output.shape[1], w_inner.shape[1], w_outer.shape[0]))
    return (wo, wi, wu_t.T)


def reduce_seq_stage(grads, tie=None):
    dp_size = lax.psum(1, "dp")
    chunks = [grad.reshape(grad.shape[0], dp_size, grad.shape[1] // dp_size) for grad in grads]
    stacked = jnp.concatenate(chunks, axis=2).astype(jnp.bfloat16)
    stacked, tie = lax.optimization_barrier((stacked, tie))
    reduced = lax.psum_scatter(stacked, "seq", scatter_dimension=0, tiled=True)
    return (reduced, [c.shape[2] for c in chunks]), tie


def stack_for_seq(grads):
    dp_size = lax.psum(1, "dp")
    chunks = [grad.reshape(grad.shape[0], dp_size, grad.shape[1] // dp_size) for grad in grads]
    return jnp.concatenate(chunks, axis=2).astype(jnp.bfloat16), [c.shape[2] for c in chunks]


def reduce_dp_stage(stages):
    joined = jnp.concatenate([stage for stage, _ in stages], axis=2)
    over_dp = lax.psum_scatter(joined, "dp", scatter_dimension=1, tiled=True)[:, 0].astype(jnp.float32)
    pieces, at = [], 0
    for _, widths in stages:
        for width in widths:
            pieces.append(over_dp[:, at : at + width])
            at += width
    return pieces


HALF_FULL = WINDOW // 2
HALF_POOL = POOL_SPAN // 2 // STRIDE
BLOCK_POOL = CLEN // STRIDE


def layout_of(index, offsets):
    in_prompt = index < PROMPT
    segment = jnp.where(in_prompt, -1, (index - PROMPT) // CLEN)
    within = index - PROMPT - segment * CLEN
    choose = segment[..., None] == jnp.arange(CONT, dtype=jnp.int32)
    spread = offsets.reshape(offsets.shape[:1] + (1,) * (index.ndim - 1) + offsets.shape[1:])
    cont_start = jnp.sum(jnp.where(choose, spread, 0), axis=-1)
    position = jnp.where(in_prompt, index, cont_start + within)
    limit = jnp.where(in_prompt, PROMPT, cont_start)
    return segment, position, limit


def window_rows(source, starts, length):
    groups, blocks = starts.shape
    return jnp.stack(
        [
            jnp.stack(
                [lax.dynamic_slice_in_dim(source[g], starts[g, b], length, 0) for b in range(blocks)]
            )
            for g in range(groups)
        ]
    )


def window_add(target, updates, starts):
    groups, blocks = starts.shape
    length = updates.shape[2]
    rows = []
    for g in range(groups):
        row = target[g]
        for b in range(blocks):
            start = starts[g, b]
            current = lax.dynamic_slice_in_dim(row, start, length, 0)
            row = lax.dynamic_update_slice_in_dim(row, current + updates[g, b], start, 0)
        rows.append(row)
    return jnp.stack(rows)


def block_geometry(seq_index, groups, shard_rows, offsets):
    group_len = PROMPT + CONT * CLEN
    pooled_len = group_len // STRIDE
    blocks = shard_rows // CLEN
    block_start = (seq_index * blocks + jnp.arange(blocks, dtype=jnp.int32)) * CLEN
    prompt_block = block_start < PROMPT
    cont_index = jnp.clip((block_start - PROMPT) // CLEN, 0, CONT - 1)
    anchor = jnp.where(prompt_block[None, :], block_start[None, :], offsets[:, cont_index])
    pooled_start = block_start // STRIDE
    intended = (
        anchor - HALF_FULL,
        jnp.broadcast_to(block_start + CLEN, anchor.shape),
        anchor // STRIDE - HALF_POOL,
        jnp.broadcast_to(pooled_start + BLOCK_POOL, anchor.shape),
    )
    limits = (group_len, group_len, pooled_len, pooled_len)
    lengths = (HALF_FULL, HALF_FULL, HALF_POOL, HALF_POOL)
    clamped = tuple(
        jnp.clip(start, 0, limit - length) for start, limit, length in zip(intended, limits, lengths)
    )
    ramp = lambda n: jnp.arange(n, dtype=jnp.int32)

    def span(window):
        actual = clamped[window][:, :, None] + ramp(lengths[window])
        offset = actual - intended[window][:, :, None]
        return actual, (offset >= 0) & (offset < lengths[window])

    before_full, before_full_ok = span(0)
    after_full, after_full_ok = span(1)
    before_pool, before_pool_ok = span(2)
    after_pool, after_pool_ok = span(3)
    after_ok = prompt_block[None, :, None]
    own_full = jnp.broadcast_to(block_start[None, :, None] + ramp(CLEN), anchor.shape + (CLEN,))
    own_pool = jnp.broadcast_to(
        pooled_start[None, :, None] + ramp(BLOCK_POOL), anchor.shape + (BLOCK_POOL,)
    )
    full_index = jnp.concatenate([before_full, own_full, after_full], axis=2)
    pooled_index = jnp.concatenate([before_pool, own_pool, after_pool], axis=2)
    full_valid = jnp.concatenate(
        [before_full_ok, jnp.ones(own_full.shape, bool), after_ok & after_full_ok], axis=2
    )
    pooled_valid = jnp.concatenate(
        [before_pool_ok, jnp.ones(own_pool.shape, bool), after_ok & after_pool_ok], axis=2
    )
    query_index = block_start[None, :, None] + ramp(CLEN)
    query_index = jnp.broadcast_to(query_index, anchor.shape + (CLEN,))
    q_seg, q_pos, q_lim = layout_of(query_index, offsets)

    def visible(key_token, valid, reach):
        k_seg, k_pos, _ = layout_of(key_token, offsets)
        k_seg, k_pos, valid = k_seg[:, :, None, :], k_pos[:, :, None, :], valid[:, :, None, :]
        prompt_key = (k_seg < 0) & (k_pos < q_lim[..., None])
        own_key = (k_seg == q_seg[..., None]) & (q_seg[..., None] >= 0)
        distance = k_pos - q_pos[..., None]
        return valid & (prompt_key | own_key) & (distance >= -(reach // 2)) & (distance < reach // 2)

    mask = jnp.concatenate(
        [
            visible(full_index, full_valid, WINDOW),
            visible(pooled_index * STRIDE, pooled_valid, POOL_SPAN),
        ],
        axis=3,
    )
    return clamped, mask


def attention_fwd(queries, kv_local, pkv_local, kv_all, pkv_all, starts, mask):
    groups, shard_rows, width = queries.shape
    blocks = shard_rows // CLEN
    score_scale = 1.0 / HEAD_DIM**0.5
    keys_cat = jnp.concatenate(
        [
            window_rows(kv_all, starts[0], HALF_FULL),
            kv_local.reshape(groups, blocks, CLEN, 2 * width),
            window_rows(kv_all, starts[1], HALF_FULL),
            window_rows(pkv_all, starts[2], HALF_POOL),
            pkv_local.reshape(groups, blocks, BLOCK_POOL, 2 * width),
            window_rows(pkv_all, starts[3], HALF_POOL),
        ],
        axis=2,
    )
    span = keys_cat.shape[2]
    head_keys = keys_cat[..., :width].reshape(groups, blocks, span, HEADS, HEAD_DIM)
    head_values = keys_cat[..., width:].reshape(groups, blocks, span, HEADS, HEAD_DIM)
    head_query = queries.reshape(groups, blocks, CLEN, HEADS, HEAD_DIM)
    scores = jnp.einsum(
        "gbqhd,gbkhd->gbhqk", head_query, head_keys, preferred_element_type=jnp.float32
    )
    scores = jnp.where(mask[:, :, None], scores * score_scale, -1000000000.0)
    row_top = jnp.max(scores, axis=-1, keepdims=True)
    exponent = jnp.exp(scores - row_top)
    row_total = jnp.sum(exponent, axis=-1, keepdims=True)
    probs = exponent / row_total
    attended = jnp.einsum(
        "gbhqk,gbkhd->gbqhd",
        probs.astype(jnp.bfloat16),
        head_values,
        preferred_element_type=jnp.float32,
    )
    attended = attended.reshape(groups * shard_rows, width).astype(jnp.bfloat16)
    return attended, (head_query, head_keys, head_values, probs)


def attention_bwd(grad_attended, saved, starts, seq_index):
    head_query, head_keys, head_values, probs = saved
    groups, blocks = head_query.shape[:2]
    width = HEADS * HEAD_DIM
    score_scale = 1.0 / HEAD_DIM**0.5
    head_grad = grad_attended.reshape(groups, blocks, CLEN, HEADS, HEAD_DIM)
    grad_probs = jnp.einsum(
        "gbqhd,gbkhd->gbhqk", head_grad, head_values, preferred_element_type=jnp.float32
    )
    centre = jnp.sum(probs * grad_probs, axis=-1, keepdims=True)
    grad_scores = (probs * (grad_probs - centre)).astype(jnp.bfloat16)
    grad_queries = jnp.einsum(
        "gbhqk,gbkhd->gbqhd", grad_scores, head_keys, preferred_element_type=jnp.float32
    ) * score_scale
    grad_keys = jnp.einsum(
        "gbhqk,gbqhd->gbkhd", grad_scores, head_query, preferred_element_type=jnp.float32
    ) * score_scale
    grad_values = jnp.einsum(
        "gbhqk,gbqhd->gbkhd",
        probs.astype(jnp.bfloat16),
        head_grad,
        preferred_element_type=jnp.float32,
    )
    span = grad_keys.shape[2]
    grad_kv = jnp.concatenate(
        [grad_keys.reshape(groups, blocks, span, width), grad_values.reshape(groups, blocks, span, width)],
        axis=3,
    )
    shard_rows = blocks * CLEN
    group_len = PROMPT + CONT * CLEN
    pooled_len = group_len // STRIDE
    cut = (0, HALF_FULL, HALF_FULL + CLEN, 2 * HALF_FULL + CLEN)
    pcut = tuple(cut[-1] + c for c in (0, HALF_POOL, HALF_POOL + BLOCK_POOL, 2 * HALF_POOL + BLOCK_POOL))
    ramp = lambda n: jnp.arange(n, dtype=jnp.int32)
    own_full = grad_kv[:, :, cut[1] : cut[2]].reshape(groups, shard_rows, 2 * width)
    full = jnp.zeros((groups, group_len, 2 * width), jnp.float32)
    full = lax.dynamic_update_slice_in_dim(full, own_full, seq_index * shard_rows, 1)
    side_values = jnp.concatenate(
        [grad_kv[:, :, cut[0] : cut[1]], grad_kv[:, :, cut[2] : cut[3]]], axis=2
    ).reshape(groups, -1, 2 * width)
    side_rows = jnp.concatenate(
        [starts[0][:, :, None] + ramp(HALF_FULL), starts[1][:, :, None] + ramp(HALF_FULL)], axis=2
    ).reshape(groups, -1)
    own_pool_rows = (seq_index * (shard_rows // STRIDE) + ramp(blocks)[:, None] * BLOCK_POOL + ramp(BLOCK_POOL))
    pool_values = grad_kv[:, :, pcut[0] : pcut[3]].reshape(groups, -1, 2 * width)
    pool_rows_index = jnp.concatenate(
        [
            starts[2][:, :, None] + ramp(HALF_POOL),
            jnp.broadcast_to(own_pool_rows[None], (groups, blocks, BLOCK_POOL)),
            starts[3][:, :, None] + ramp(HALF_POOL),
        ],
        axis=2,
    ).reshape(groups, -1)
    fulls, pooleds, unpooleds = [], [], []
    for g in range(groups):
        fulls.append(full[g] + select_sum(side_values[g], side_rows[g] == ramp(group_len)[:, None]))
        pooleds.append(select_sum(pool_values[g], pool_rows_index[g] == ramp(pooled_len)[:, None]))
        unpooleds.append(
            select_sum(pool_values[g], pool_rows_index[g] == (ramp(group_len) // STRIDE)[:, None])
        )
    full = jnp.stack(fulls)
    pooled = jnp.stack(pooleds)
    unpooled = jnp.stack(unpooleds)
    grad_queries = grad_queries.reshape(groups * shard_rows, width).astype(jnp.bfloat16)
    return grad_queries, full, pooled, unpooled


def select_sum(values, chosen):
    onehot = chosen.astype(jnp.bfloat16)
    high = values.astype(jnp.bfloat16)
    low = (values - high.astype(jnp.float32)).astype(jnp.bfloat16)
    return product(onehot, high) + product(onehot, low)


def phase_weights(weight, rows):
    phase = (jnp.arange(rows, dtype=jnp.int32) % STRIDE)[:, None]
    total = jnp.zeros((rows, weight.shape[1]), jnp.float32)
    for r in range(STRIDE):
        total = total + jnp.where(phase == r, weight[r][None, :], 0.0)
    return total


def pool_grouped(source, weight):
    groups, rows, width = source.shape
    return jnp.sum(
        source.reshape(groups, rows // STRIDE, STRIDE, width) * weight[None, None], axis=2
    )


def unpool_grouped(pooled_grad, weight):
    groups, rows, width = pooled_grad.shape
    return (pooled_grad[:, :, None, :] * weight[None, None]).reshape(groups, rows * STRIDE, width)


def pool_grad_grouped(pooled_grad, source):
    groups, rows, width = source.shape
    blocks_view = source.astype(jnp.float32).reshape(groups, rows // STRIDE, STRIDE, width)
    return jnp.sum(pooled_grad[:, :, None, :] * blocks_view, axis=(0, 1))


def local(
    hidden_in,
    w_query,
    w_key,
    w_value,
    w_output,
    w_inner,
    w_outer,
    pool_weight,
    ln_gain,
    ln_bias,
    branch_blocks,
    grad_out,
):
    pool_rows_count = pool_weight.shape[0] * pool_weight.shape[1]
    small_local = jnp.concatenate(
        [pool_weight.reshape(pool_rows_count, -1), ln_gain, ln_bias], axis=0
    )
    hidden_all = lax.all_gather(hidden_in, "seq", axis=1, tiled=True)
    (wq, wk, wv), (hidden_all, small_local) = gather_first(
        w_query, w_key, w_value, (hidden_all, small_local)
    )
    small_full = lax.all_gather(small_local, ("dp", "seq"), axis=1, tiled=True)
    wq, wk, wv, small_full = lax.optimization_barrier((wq, wk, wv, small_full))
    pool_full = small_full[:pool_rows_count].reshape(pool_weight.shape[0], pool_weight.shape[1], -1)
    gain_full = small_full[pool_rows_count : pool_rows_count + ln_gain.shape[0]]
    bias_full = small_full[pool_rows_count + ln_gain.shape[0] :]
    groups, shard_rows, width = hidden_in.shape
    seq_index = lax.axis_index("seq")
    offsets = STRIDE * branch_blocks
    starts, mask = block_geometry(seq_index, groups, shard_rows, offsets)

    group_len = hidden_all.shape[1]
    tokens = hidden_in.reshape(groups * shard_rows, width)
    all_tokens = hidden_all.reshape(groups * group_len, width)
    queries = product(tokens, wq).astype(jnp.bfloat16)
    key_g = product(all_tokens, wk).astype(jnp.bfloat16).reshape(groups, group_len, width)
    value_g = product(all_tokens, wv).astype(jnp.bfloat16).reshape(groups, group_len, width)
    pooled_keys = pool_grouped(key_g.astype(jnp.float32), pool_full[0]).astype(jnp.bfloat16)
    pooled_values = pool_grouped(value_g.astype(jnp.float32), pool_full[1]).astype(jnp.bfloat16)
    kv_all = jnp.concatenate([key_g, value_g], axis=2)
    pkv_all = jnp.concatenate([pooled_keys, pooled_values], axis=2)
    kv_local = lax.dynamic_slice_in_dim(kv_all, seq_index * shard_rows, shard_rows, 1)
    pkv_local = lax.dynamic_slice_in_dim(
        pkv_all, seq_index * (shard_rows // STRIDE), shard_rows // STRIDE, 1
    )
    wq, wk, wv, w_output, w_inner, w_outer = lax.optimization_barrier(
        (wq, wk, wv, w_output, w_inner, w_outer)
    )
    wo, wi, wu = gather_second(w_output, w_inner, w_outer)
    attended, att_saved = attention_fwd(
        queries.reshape(groups, shard_rows, width), kv_local, pkv_local, kv_all, pkv_all, starts, mask
    )
    mixed_rows = tokens.astype(jnp.float32) + product(attended, wo)
    normed_first = layer_norm(mixed_rows, gain_full[0], bias_full[0])
    first_low = normed_first.astype(jnp.bfloat16)
    inner_act = product(first_low, wi)
    active = jax.nn.gelu(inner_act, approximate=False).astype(jnp.bfloat16)
    second = normed_first + product(active, wu)
    norm_value, second_back = jax.vjp(layer_norm, second, gain_full[1], bias_full[1])
    output = norm_value.astype(jnp.bfloat16)

    cotangent = grad_out.reshape(groups * shard_rows, width).astype(jnp.float32)
    grad_second, gain_second, bias_second = second_back(cotangent)
    grad_ffn_out = grad_second.astype(jnp.bfloat16)
    grad_outer = product_left(active, grad_ffn_out)
    grad_active = product_right(grad_ffn_out, wu)
    gelu_value, gelu_back = jax.vjp(partial(jax.nn.gelu, approximate=False), inner_act)
    grad_inner_act = gelu_back(grad_active)[0].astype(jnp.bfloat16)
    grad_inner = product_left(first_low, grad_inner_act)
    grad_first = grad_second + product_right(grad_inner_act, wi)
    first_value, first_back = jax.vjp(layer_norm, mixed_rows, gain_full[0], bias_full[0])
    grad_mixed, gain_first, bias_first = first_back(grad_first)
    grad_branch = grad_mixed.astype(jnp.bfloat16)
    grad_output = product_left(attended, grad_branch)
    grad_attended = product_right(grad_branch, wo).astype(jnp.bfloat16)
    early, grad_attended = reduce_seq_stage((grad_output, grad_inner, grad_outer.T), grad_attended)
    early_reduced, early_widths = early

    grad_rows = grad_attended.reshape(groups, shard_rows, width)
    key_phase = phase_weights(pool_full[0], group_len)
    value_phase = phase_weights(pool_full[1], group_len)
    pieces_back = []
    for g in range(groups):
        saved_g = tuple(item[g : g + 1] for item in att_saved)
        starts_g = tuple(item[g : g + 1] for item in starts)
        grad_g = grad_rows[g].reshape(shard_rows, width)
        grad_queries_g, full_g, pooled_g, unpooled_g = attention_bwd(grad_g, saved_g, starts_g, seq_index)
        if g == 1:
            full_g, pooled_g, unpooled_g, earlier_back, early_reduced = lax.optimization_barrier(
                (full_g, pooled_g, unpooled_g, pieces_back[0][4], early_reduced)
            )
            pieces_back[0] = pieces_back[0][:4] + (earlier_back,)
        key_partial_g = (
            full_g[0, :, :width] + unpooled_g[0, :, :width] * key_phase
        ).astype(jnp.bfloat16)
        value_partial_g = (
            full_g[0, :, width:] + unpooled_g[0, :, width:] * value_phase
        ).astype(jnp.bfloat16)
        back_g = product_right(key_partial_g, wk) + product_right(value_partial_g, wv)
        back_g = back_g.reshape(1, group_len, width).astype(jnp.bfloat16)
        if g == groups - 1:
            back_own_g = back_g
        else:
            back_own_g = lax.psum_scatter(back_g, "seq", scatter_dimension=1, tiled=True)
        pieces_back.append((grad_queries_g, pooled_g, key_partial_g, value_partial_g, back_own_g))
    grad_queries = jnp.concatenate([piece[0] for piece in pieces_back], axis=0)
    grad_pooled = jnp.concatenate([piece[1] for piece in pieces_back], axis=0)
    key_partial = jnp.concatenate([piece[2] for piece in pieces_back], axis=0)
    value_partial = jnp.concatenate([piece[3] for piece in pieces_back], axis=0)
    last_back = pieces_back[-1][4]
    early_dp = reduce_dp_stage(((early_reduced, early_widths),))
    grad_pooling = jnp.stack(
        [
            pool_grad_grouped(grad_pooled[..., :width], key_g),
            pool_grad_grouped(grad_pooled[..., width:], value_g),
        ]
    )
    grad_query_w = product_left(tokens, grad_queries)
    grad_key_w = product_left(all_tokens, key_partial)
    grad_value_w = product_left(all_tokens, value_partial)
    late_stacked, late_widths = stack_for_seq((grad_query_w, grad_key_w, grad_value_w))
    late_stacked, early_dp = lax.optimization_barrier((late_stacked, early_dp))
    seq_size = lax.psum(1, "seq")
    late_flat = late_stacked.reshape(seq_size, -1, width)
    back_flat = last_back.reshape(seq_size, -1, width)
    joined = jnp.concatenate([late_flat, back_flat], axis=1)
    chunk_rows = joined.shape[1]
    joined = joined.reshape(seq_size * chunk_rows, width)
    joined = lax.psum_scatter(joined, "seq", scatter_dimension=0, tiled=True)
    late_reduced = joined[: late_flat.shape[1]].reshape(
        late_stacked.shape[0] // seq_size, late_stacked.shape[1], late_stacked.shape[2]
    )
    back_last = joined[late_flat.shape[1] :].reshape(1, shard_rows, width)
    back_own = jnp.concatenate([piece[4] for piece in pieces_back[:-1]] + [back_last], axis=0)
    grad_tokens = (
        grad_mixed
        + product_right(grad_queries, wq)
        + back_own.reshape(groups * shard_rows, width).astype(jnp.float32)
    )
    late_dp = reduce_dp_stage(((late_reduced, late_widths),))
    accum = (late_dp[0], late_dp[1], late_dp[2], early_dp[0], early_dp[1], early_dp[2].T)
    small_sums = (
        lax.psum_scatter(grad_pooling, ("dp", "seq"), scatter_dimension=2, tiled=True),
        lax.psum_scatter(
            jnp.stack([gain_first, gain_second]), ("dp", "seq"), scatter_dimension=1, tiled=True
        ),
        lax.psum_scatter(
            jnp.stack([bias_first, bias_second]), ("dp", "seq"), scatter_dimension=1, tiled=True
        ),
    )
    return (
        output.reshape(groups, shard_rows, width),
        grad_tokens.astype(jnp.bfloat16).reshape(groups, shard_rows, width),
        accum[0],
        accum[1],
        accum[2],
        accum[3],
        accum[4],
        accum[5],
        small_sums[0],
        small_sums[1],
        small_sums[2],
    )


def solution(mesh):
    in_specs = (
        P("dp", "seq", None),
        P("seq", "dp"),
        P("seq", "dp"),
        P("seq", "dp"),
        P("seq", "dp"),
        P("seq", "dp"),
        P("dp", "seq"),
        P(None, None, ("dp", "seq")),
        P(None, ("dp", "seq")),
        P(None, ("dp", "seq")),
        P("dp", None),
        P("dp", "seq", None),
    )
    out_specs = (
        P("dp", "seq", None),
        P("dp", "seq", None),
        P("seq", "dp"),
        P("seq", "dp"),
        P("seq", "dp"),
        P("seq", "dp"),
        P("seq", "dp"),
        P("dp", "seq"),
        P(None, None, ("dp", "seq")),
        P(None, ("dp", "seq")),
        P(None, ("dp", "seq")),
    )
    return jax.shard_map(local, mesh=mesh, in_specs=in_specs, out_specs=out_specs, check_vma=False)
```

```python
from functools import partial

import jax
import jax.numpy as jnp
from jax import lax
from jax.sharding import PartitionSpec as P

HEADS = 12
HEAD_DIM = 64
PROMPT = 1024
CONT = 8
CLEN = 128
WINDOW = 128
POOL_SPAN = 512
STRIDE = 4


eps_norm = 1e-05


def token_layout(positions_in, offsets):
    in_prompt = positions_in < PROMPT
    segment = jnp.where(in_prompt, -1, (positions_in - PROMPT) // CLEN)
    within = positions_in - PROMPT - segment * CLEN
    choose = (segment[:, None] == jnp.arange(CONT, dtype=jnp.int32)[None, :]).astype(jnp.int32)
    cont_start = jnp.sum(choose * offsets[None, :], axis=1)
    position = jnp.where(in_prompt, positions_in, cont_start + within)
    prompt_limit = jnp.where(in_prompt, PROMPT, cont_start)
    return (segment, position, prompt_limit)


def visible_keys(query_rows, key_index, offsets, reach):
    query_seg, query_pos, query_limit = token_layout(query_rows, offsets)
    key_seg, key_pos, key_limit = token_layout(key_index, offsets)
    prompt_key = (key_seg[None, :] < 0) & (key_pos[None, :] < query_limit[:, None])
    own_key = (key_seg[None, :] == query_seg[:, None]) & (query_seg[:, None] >= 0)
    distance = key_pos[None, :] - query_pos[:, None]
    return (prompt_key | own_key) & (distance >= -(reach // 2)) & (distance < reach // 2)


def key_mask(query_rows, offsets):
    group_len = PROMPT + CONT * CLEN
    full_keys = jnp.arange(group_len, dtype=jnp.int32)
    pooled_keys = jnp.arange(group_len // STRIDE, dtype=jnp.int32) * STRIDE
    return jnp.concatenate(
        [
            visible_keys(query_rows, full_keys, offsets, WINDOW),
            visible_keys(query_rows, pooled_keys, offsets, POOL_SPAN),
        ],
        axis=1,
    )


def pool_rows(source, weight):
    return jnp.sum(
        source.reshape(source.shape[0] // STRIDE, STRIDE, source.shape[1]) * weight[None, :, :],
        axis=1,
    )


def unpool(pooled_grad, weight):
    return (pooled_grad[:, None, :] * weight[None, :, :]).reshape(-1, pooled_grad.shape[1])


def pool_grad(pooled_grad, source):
    blocks_view = source.astype(jnp.float32).reshape(-1, STRIDE, source.shape[1])
    return jnp.sum(pooled_grad[:, None, :] * blocks_view, axis=0)


def layer_norm(source, gain, bias):
    centre = jnp.mean(source, axis=-1, keepdims=True)
    centred = source - centre
    spread = jnp.mean(centred * centred, axis=-1, keepdims=True)
    return centred * lax.rsqrt(spread + eps_norm) * gain + bias


def product(left, right):
    return jnp.dot(left, right, preferred_element_type=jnp.float32)


def product_left(left, right):
    return lax.dot_general(
        left, right, (((0,), (0,)), ((), ())), preferred_element_type=jnp.float32
    )


def product_right(left, right):
    return lax.dot_general(
        left, right, (((1,), (1,)), ((), ())), preferred_element_type=jnp.float32
    )


def add_pair(left_term, right_term):
    return left_term + right_term


def gather_grouped(shards, tie=None):
    local_block = jnp.concatenate(shards, axis=1)
    across = lax.all_gather(local_block, "dp", axis=1, tiled=False)
    across, tie = lax.optimization_barrier((across, tie))
    return lax.all_gather(across, "seq", axis=0, tiled=True), tie


def split_grouped(gathered, widths):
    pieces, at = [], 0
    for width in widths:
        piece = gathered[:, :, at : at + width]
        pieces.append(piece.reshape(piece.shape[0], -1))
        at += width
    return pieces


def gather_first(w_query, w_key, w_value, tie):
    first, tie = gather_grouped((w_query, w_key, w_value), tie)
    return split_grouped(first, (w_query.shape[1], w_key.shape[1], w_value.shape[1])), tie


def gather_second(w_output, w_inner, w_outer):
    second, _ = gather_grouped((w_output, w_inner, w_outer.T))
    wo, wi, wu_t = split_grouped(second, (w_output.shape[1], w_inner.shape[1], w_outer.shape[0]))
    return (wo, wi, wu_t.T)


def reduce_seq_stage(grads, tie=None):
    dp_size = lax.psum(1, "dp")
    chunks = [grad.reshape(grad.shape[0], dp_size, grad.shape[1] // dp_size) for grad in grads]
    stacked = jnp.concatenate(chunks, axis=2).astype(jnp.bfloat16)
    stacked, tie = lax.optimization_barrier((stacked, tie))
    reduced = lax.psum_scatter(stacked, "seq", scatter_dimension=0, tiled=True)
    return (reduced, [c.shape[2] for c in chunks]), tie


def stack_for_seq(grads):
    dp_size = lax.psum(1, "dp")
    chunks = [grad.reshape(grad.shape[0], dp_size, grad.shape[1] // dp_size) for grad in grads]
    return jnp.concatenate(chunks, axis=2).astype(jnp.bfloat16), [c.shape[2] for c in chunks]


def reduce_dp_stage(stages):
    joined = jnp.concatenate([stage for stage, _ in stages], axis=2)
    over_dp = lax.psum_scatter(joined, "dp", scatter_dimension=1, tiled=True)[:, 0].astype(jnp.float32)
    pieces, at = [], 0
    for _, widths in stages:
        for width in widths:
            pieces.append(over_dp[:, at : at + width])
            at += width
    return pieces


HALF_FULL = WINDOW // 2
HALF_POOL = POOL_SPAN // 2 // STRIDE
BLOCK_POOL = CLEN // STRIDE


def layout_of(index, offsets):
    in_prompt = index < PROMPT
    segment = jnp.where(in_prompt, -1, (index - PROMPT) // CLEN)
    within = index - PROMPT - segment * CLEN
    choose = segment[..., None] == jnp.arange(CONT, dtype=jnp.int32)
    spread = offsets.reshape(offsets.shape[:1] + (1,) * (index.ndim - 1) + offsets.shape[1:])
    cont_start = jnp.sum(jnp.where(choose, spread, 0), axis=-1)
    position = jnp.where(in_prompt, index, cont_start + within)
    limit = jnp.where(in_prompt, PROMPT, cont_start)
    return segment, position, limit


def window_rows(source, starts, length):
    groups, blocks = starts.shape
    return jnp.stack(
        [
            jnp.stack(
                [lax.dynamic_slice_in_dim(source[g], starts[g, b], length, 0) for b in range(blocks)]
            )
            for g in range(groups)
        ]
    )


def window_add(target, updates, starts):
    groups, blocks = starts.shape
    length = updates.shape[2]
    rows = []
    for g in range(groups):
        row = target[g]
        for b in range(blocks):
            start = starts[g, b]
            current = lax.dynamic_slice_in_dim(row, start, length, 0)
            row = lax.dynamic_update_slice_in_dim(row, current + updates[g, b], start, 0)
        rows.append(row)
    return jnp.stack(rows)


def block_geometry(seq_index, groups, shard_rows, offsets):
    group_len = PROMPT + CONT * CLEN
    pooled_len = group_len // STRIDE
    blocks = shard_rows // CLEN
    block_start = (seq_index * blocks + jnp.arange(blocks, dtype=jnp.int32)) * CLEN
    prompt_block = block_start < PROMPT
    cont_index = jnp.clip((block_start - PROMPT) // CLEN, 0, CONT - 1)
    anchor = jnp.where(prompt_block[None, :], block_start[None, :], offsets[:, cont_index])
    pooled_start = block_start // STRIDE
    intended = (
        anchor - HALF_FULL,
        jnp.broadcast_to(block_start + CLEN, anchor.shape),
        anchor // STRIDE - HALF_POOL,
        jnp.broadcast_to(pooled_start + BLOCK_POOL, anchor.shape),
    )
    limits = (group_len, group_len, pooled_len, pooled_len)
    lengths = (HALF_FULL, HALF_FULL, HALF_POOL, HALF_POOL)
    clamped = tuple(
        jnp.clip(start, 0, limit - length) for start, limit, length in zip(intended, limits, lengths)
    )
    ramp = lambda n: jnp.arange(n, dtype=jnp.int32)

    def span(window):
        actual = clamped[window][:, :, None] + ramp(lengths[window])
        offset = actual - intended[window][:, :, None]
        return actual, (offset >= 0) & (offset < lengths[window])

    before_full, before_full_ok = span(0)
    after_full, after_full_ok = span(1)
    before_pool, before_pool_ok = span(2)
    after_pool, after_pool_ok = span(3)
    after_ok = prompt_block[None, :, None]
    own_full = jnp.broadcast_to(block_start[None, :, None] + ramp(CLEN), anchor.shape + (CLEN,))
    own_pool = jnp.broadcast_to(
        pooled_start[None, :, None] + ramp(BLOCK_POOL), anchor.shape + (BLOCK_POOL,)
    )
    full_index = jnp.concatenate([before_full, own_full, after_full], axis=2)
    pooled_index = jnp.concatenate([before_pool, own_pool, after_pool], axis=2)
    full_valid = jnp.concatenate(
        [before_full_ok, jnp.ones(own_full.shape, bool), after_ok & after_full_ok], axis=2
    )
    pooled_valid = jnp.concatenate(
        [before_pool_ok, jnp.ones(own_pool.shape, bool), after_ok & after_pool_ok], axis=2
    )
    query_index = block_start[None, :, None] + ramp(CLEN)
    query_index = jnp.broadcast_to(query_index, anchor.shape + (CLEN,))
    q_seg, q_pos, q_lim = layout_of(query_index, offsets)

    def visible(key_token, valid, reach):
        k_seg, k_pos, _ = layout_of(key_token, offsets)
        k_seg, k_pos, valid = k_seg[:, :, None, :], k_pos[:, :, None, :], valid[:, :, None, :]
        prompt_key = (k_seg < 0) & (k_pos < q_lim[..., None])
        own_key = (k_seg == q_seg[..., None]) & (q_seg[..., None] >= 0)
        distance = k_pos - q_pos[..., None]
        return valid & (prompt_key | own_key) & (distance >= -(reach // 2)) & (distance < reach // 2)

    mask = jnp.concatenate(
        [
            visible(full_index, full_valid, WINDOW),
            visible(pooled_index * STRIDE, pooled_valid, POOL_SPAN),
        ],
        axis=3,
    )
    return clamped, mask


def attention_fwd(queries, kv_local, pkv_local, kv_all, pkv_all, starts, mask):
    groups, shard_rows, width = queries.shape
    blocks = shard_rows // CLEN
    score_scale = 1.0 / HEAD_DIM**0.5
    keys_cat = jnp.concatenate(
        [
            window_rows(kv_all, starts[0], HALF_FULL),
            kv_local.reshape(groups, blocks, CLEN, 2 * width),
            window_rows(kv_all, starts[1], HALF_FULL),
            window_rows(pkv_all, starts[2], HALF_POOL),
            pkv_local.reshape(groups, blocks, BLOCK_POOL, 2 * width),
            window_rows(pkv_all, starts[3], HALF_POOL),
        ],
        axis=2,
    )
    span = keys_cat.shape[2]
    head_keys = keys_cat[..., :width].reshape(groups, blocks, span, HEADS, HEAD_DIM)
    head_values = keys_cat[..., width:].reshape(groups, blocks, span, HEADS, HEAD_DIM)
    head_query = queries.reshape(groups, blocks, CLEN, HEADS, HEAD_DIM)
    scores = jnp.einsum(
        "gbqhd,gbkhd->gbhqk", head_query, head_keys, preferred_element_type=jnp.float32
    )
    scores = jnp.where(mask[:, :, None], scores * score_scale, -1000000000.0)
    row_top = jnp.max(scores, axis=-1, keepdims=True)
    exponent = jnp.exp(scores - row_top)
    row_total = jnp.sum(exponent, axis=-1, keepdims=True)
    probs = exponent / row_total
    attended = jnp.einsum(
        "gbhqk,gbkhd->gbqhd",
        probs.astype(jnp.bfloat16),
        head_values,
        preferred_element_type=jnp.float32,
    )
    attended = attended.reshape(groups * shard_rows, width).astype(jnp.bfloat16)
    return attended, (head_query, head_keys, head_values, probs)


def attention_bwd(grad_attended, saved, starts, seq_index):
    head_query, head_keys, head_values, probs = saved
    groups, blocks = head_query.shape[:2]
    width = HEADS * HEAD_DIM
    score_scale = 1.0 / HEAD_DIM**0.5
    head_grad = grad_attended.reshape(groups, blocks, CLEN, HEADS, HEAD_DIM)
    grad_probs = jnp.einsum(
        "gbqhd,gbkhd->gbhqk", head_grad, head_values, preferred_element_type=jnp.float32
    )
    centre = jnp.sum(probs * grad_probs, axis=-1, keepdims=True)
    grad_scores = (probs * (grad_probs - centre)).astype(jnp.bfloat16)
    grad_queries = jnp.einsum(
        "gbhqk,gbkhd->gbqhd", grad_scores, head_keys, preferred_element_type=jnp.float32
    ) * score_scale
    grad_keys = jnp.einsum(
        "gbhqk,gbqhd->gbkhd", grad_scores, head_query, preferred_element_type=jnp.float32
    ) * score_scale
    grad_values = jnp.einsum(
        "gbhqk,gbqhd->gbkhd",
        probs.astype(jnp.bfloat16),
        head_grad,
        preferred_element_type=jnp.float32,
    )
    span = grad_keys.shape[2]
    grad_kv = jnp.concatenate(
        [grad_keys.reshape(groups, blocks, span, width), grad_values.reshape(groups, blocks, span, width)],
        axis=3,
    )
    shard_rows = blocks * CLEN
    group_len = PROMPT + CONT * CLEN
    pooled_len = group_len // STRIDE
    cut = (0, HALF_FULL, HALF_FULL + CLEN, 2 * HALF_FULL + CLEN)
    pcut = tuple(cut[-1] + c for c in (0, HALF_POOL, HALF_POOL + BLOCK_POOL, 2 * HALF_POOL + BLOCK_POOL))
    ramp = lambda n: jnp.arange(n, dtype=jnp.int32)
    own_full = grad_kv[:, :, cut[1] : cut[2]].reshape(groups, shard_rows, 2 * width)
    full = jnp.zeros((groups, group_len, 2 * width), jnp.float32)
    full = lax.dynamic_update_slice_in_dim(full, own_full, seq_index * shard_rows, 1)
    side_values = jnp.concatenate(
        [grad_kv[:, :, cut[0] : cut[1]], grad_kv[:, :, cut[2] : cut[3]]], axis=2
    ).reshape(groups, -1, 2 * width)
    side_rows = jnp.concatenate(
        [starts[0][:, :, None] + ramp(HALF_FULL), starts[1][:, :, None] + ramp(HALF_FULL)], axis=2
    ).reshape(groups, -1)
    own_pool_rows = (seq_index * (shard_rows // STRIDE) + ramp(blocks)[:, None] * BLOCK_POOL + ramp(BLOCK_POOL))
    pool_values = grad_kv[:, :, pcut[0] : pcut[3]].reshape(groups, -1, 2 * width)
    pool_rows_index = jnp.concatenate(
        [
            starts[2][:, :, None] + ramp(HALF_POOL),
            jnp.broadcast_to(own_pool_rows[None], (groups, blocks, BLOCK_POOL)),
            starts[3][:, :, None] + ramp(HALF_POOL),
        ],
        axis=2,
    ).reshape(groups, -1)
    fulls, pooleds, unpooleds = [], [], []
    for g in range(groups):
        fulls.append(full[g] + select_sum(side_values[g], side_rows[g] == ramp(group_len)[:, None]))
        pooleds.append(select_sum(pool_values[g], pool_rows_index[g] == ramp(pooled_len)[:, None]))
        unpooleds.append(
            select_sum(pool_values[g], pool_rows_index[g] == (ramp(group_len) // STRIDE)[:, None])
        )
    full = jnp.stack(fulls)
    pooled = jnp.stack(pooleds)
    unpooled = jnp.stack(unpooleds)
    grad_queries = grad_queries.reshape(groups * shard_rows, width).astype(jnp.bfloat16)
    return grad_queries, full, pooled, unpooled


def select_sum(values, chosen):
    onehot = chosen.astype(jnp.bfloat16)
    high = values.astype(jnp.bfloat16)
    low = (values - high.astype(jnp.float32)).astype(jnp.bfloat16)
    return product(onehot, high) + product(onehot, low)


def phase_weights(weight, rows):
    phase = (jnp.arange(rows, dtype=jnp.int32) % STRIDE)[:, None]
    total = jnp.zeros((rows, weight.shape[1]), jnp.float32)
    for r in range(STRIDE):
        total = total + jnp.where(phase == r, weight[r][None, :], 0.0)
    return total


def pool_grouped(source, weight):
    groups, rows, width = source.shape
    return jnp.sum(
        source.reshape(groups, rows // STRIDE, STRIDE, width) * weight[None, None], axis=2
    )


def unpool_grouped(pooled_grad, weight):
    groups, rows, width = pooled_grad.shape
    return (pooled_grad[:, :, None, :] * weight[None, None]).reshape(groups, rows * STRIDE, width)


def pool_grad_grouped(pooled_grad, source):
    groups, rows, width = source.shape
    blocks_view = source.astype(jnp.float32).reshape(groups, rows // STRIDE, STRIDE, width)
    return jnp.sum(pooled_grad[:, :, None, :] * blocks_view, axis=(0, 1))


def local(
    hidden_in,
    w_query,
    w_key,
    w_value,
    w_output,
    w_inner,
    w_outer,
    pool_weight,
    ln_gain,
    ln_bias,
    branch_blocks,
    grad_out,
):
    pool_rows_count = pool_weight.shape[0] * pool_weight.shape[1]
    small_local = jnp.concatenate(
        [pool_weight.reshape(pool_rows_count, -1), ln_gain, ln_bias], axis=0
    )
    small_full = lax.all_gather(small_local, ("dp", "seq"), axis=1, tiled=True)
    hidden_all = lax.all_gather(hidden_in, "seq", axis=1, tiled=True)
    (wq, wk, wv), (hidden_all, small_full) = gather_first(
        w_query, w_key, w_value, (hidden_all, small_full)
    )
    pool_full = small_full[:pool_rows_count].reshape(pool_weight.shape[0], pool_weight.shape[1], -1)
    gain_full = small_full[pool_rows_count : pool_rows_count + ln_gain.shape[0]]
    bias_full = small_full[pool_rows_count + ln_gain.shape[0] :]
    groups, shard_rows, width = hidden_in.shape
    seq_index = lax.axis_index("seq")
    offsets = STRIDE * branch_blocks
    starts, mask = block_geometry(seq_index, groups, shard_rows, offsets)

    group_len = hidden_all.shape[1]
    tokens = hidden_in.reshape(groups * shard_rows, width)
    all_tokens = hidden_all.reshape(groups * group_len, width)
    queries = product(tokens, wq).astype(jnp.bfloat16)
    key_g = product(all_tokens, wk).astype(jnp.bfloat16).reshape(groups, group_len, width)
    value_g = product(all_tokens, wv).astype(jnp.bfloat16).reshape(groups, group_len, width)
    pooled_keys = pool_grouped(key_g.astype(jnp.float32), pool_full[0]).astype(jnp.bfloat16)
    pooled_values = pool_grouped(value_g.astype(jnp.float32), pool_full[1]).astype(jnp.bfloat16)
    kv_all = jnp.concatenate([key_g, value_g], axis=2)
    pkv_all = jnp.concatenate([pooled_keys, pooled_values], axis=2)
    kv_local = lax.dynamic_slice_in_dim(kv_all, seq_index * shard_rows, shard_rows, 1)
    pkv_local = lax.dynamic_slice_in_dim(
        pkv_all, seq_index * (shard_rows // STRIDE), shard_rows // STRIDE, 1
    )
    wq, wk, wv, w_output, w_inner, w_outer = lax.optimization_barrier(
        (wq, wk, wv, w_output, w_inner, w_outer)
    )
    wo, wi, wu = gather_second(w_output, w_inner, w_outer)
    attended, att_saved = attention_fwd(
        queries.reshape(groups, shard_rows, width), kv_local, pkv_local, kv_all, pkv_all, starts, mask
    )
    mixed_rows = tokens.astype(jnp.float32) + product(attended, wo)
    normed_first = layer_norm(mixed_rows, gain_full[0], bias_full[0])
    first_low = normed_first.astype(jnp.bfloat16)
    inner_act = product(first_low, wi)
    active = jax.nn.gelu(inner_act, approximate=False).astype(jnp.bfloat16)
    second = normed_first + product(active, wu)
    norm_value, second_back = jax.vjp(layer_norm, second, gain_full[1], bias_full[1])
    output = norm_value.astype(jnp.bfloat16)

    cotangent = grad_out.reshape(groups * shard_rows, width).astype(jnp.float32)
    grad_second, gain_second, bias_second = second_back(cotangent)
    grad_ffn_out = grad_second.astype(jnp.bfloat16)
    grad_outer = product_left(active, grad_ffn_out)
    grad_active = product_right(grad_ffn_out, wu)
    gelu_value, gelu_back = jax.vjp(partial(jax.nn.gelu, approximate=False), inner_act)
    grad_inner_act = gelu_back(grad_active)[0].astype(jnp.bfloat16)
    grad_inner = product_left(first_low, grad_inner_act)
    grad_first = grad_second + product_right(grad_inner_act, wi)
    first_value, first_back = jax.vjp(layer_norm, mixed_rows, gain_full[0], bias_full[0])
    grad_mixed, gain_first, bias_first = first_back(grad_first)
    grad_branch = grad_mixed.astype(jnp.bfloat16)
    grad_output = product_left(attended, grad_branch)
    grad_attended = product_right(grad_branch, wo).astype(jnp.bfloat16)
    early, grad_attended = reduce_seq_stage((grad_output, grad_inner, grad_outer.T), grad_attended)
    early_reduced, early_widths = early

    grad_rows = grad_attended.reshape(groups, shard_rows, width)
    key_phase = phase_weights(pool_full[0], group_len)
    value_phase = phase_weights(pool_full[1], group_len)
    pieces_back = []
    for g in range(groups):
        saved_g = tuple(item[g : g + 1] for item in att_saved)
        starts_g = tuple(item[g : g + 1] for item in starts)
        grad_g = grad_rows[g].reshape(shard_rows, width)
        grad_queries_g, full_g, pooled_g, unpooled_g = attention_bwd(grad_g, saved_g, starts_g, seq_index)
        if g == 1:
            full_g, pooled_g, unpooled_g, earlier_back, early_reduced = lax.optimization_barrier(
                (full_g, pooled_g, unpooled_g, pieces_back[0][4], early_reduced)
            )
            pieces_back[0] = pieces_back[0][:4] + (earlier_back,)
        key_partial_g = (
            full_g[0, :, :width] + unpooled_g[0, :, :width] * key_phase
        ).astype(jnp.bfloat16)
        value_partial_g = (
            full_g[0, :, width:] + unpooled_g[0, :, width:] * value_phase
        ).astype(jnp.bfloat16)
        back_g = product_right(key_partial_g, wk) + product_right(value_partial_g, wv)
        back_g = back_g.reshape(1, group_len, width).astype(jnp.bfloat16)
        back_own_g = lax.psum_scatter(back_g, "seq", scatter_dimension=1, tiled=True)
        pieces_back.append((grad_queries_g, pooled_g, key_partial_g, value_partial_g, back_own_g))
    grad_queries = jnp.concatenate([piece[0] for piece in pieces_back], axis=0)
    grad_pooled = jnp.concatenate([piece[1] for piece in pieces_back], axis=0)
    key_partial = jnp.concatenate([piece[2] for piece in pieces_back], axis=0)
    value_partial = jnp.concatenate([piece[3] for piece in pieces_back], axis=0)
    last_back = pieces_back[-1][4]
    early_dp = reduce_dp_stage(((early_reduced, early_widths),))
    grad_pooling = jnp.stack(
        [
            pool_grad_grouped(grad_pooled[..., :width], key_g),
            pool_grad_grouped(grad_pooled[..., width:], value_g),
        ]
    )
    grad_query_w = product_left(tokens, grad_queries)
    grad_key_w = product_left(all_tokens, key_partial)
    grad_value_w = product_left(all_tokens, value_partial)
    late_stacked, late_widths = stack_for_seq((grad_query_w, grad_key_w, grad_value_w))
    late_stacked, early_dp = lax.optimization_barrier((late_stacked, early_dp))
    seq_size = lax.psum(1, "seq")
    dp_size = lax.psum(1, "dp")
    rows_each = late_stacked.shape[0] // seq_size
    late_blocks = late_stacked.reshape(seq_size, rows_each, dp_size, late_stacked.shape[2])
    late_blocks = jnp.transpose(late_blocks, (2, 0, 1, 3)).reshape(-1, late_stacked.shape[2])
    late_reduced = lax.psum_scatter(late_blocks, ("dp", "seq"), scatter_dimension=0, tiled=True)
    late_reduced = late_reduced.astype(jnp.float32)
    late_dp, at = [], 0
    for width_piece in late_widths:
        late_dp.append(late_reduced[:, at : at + width_piece])
        at += width_piece
    back_own = jnp.concatenate([piece[4] for piece in pieces_back], axis=0)
    grad_tokens = (
        grad_mixed
        + product_right(grad_queries, wq)
        + back_own.reshape(groups * shard_rows, width).astype(jnp.float32)
    )
    accum = (late_dp[0], late_dp[1], late_dp[2], early_dp[0], early_dp[1], early_dp[2].T)
    small_sums = (
        lax.psum_scatter(grad_pooling, ("dp", "seq"), scatter_dimension=2, tiled=True),
        lax.psum_scatter(
            jnp.stack([gain_first, gain_second]), ("dp", "seq"), scatter_dimension=1, tiled=True
        ),
        lax.psum_scatter(
            jnp.stack([bias_first, bias_second]), ("dp", "seq"), scatter_dimension=1, tiled=True
        ),
    )
    return (
        output.reshape(groups, shard_rows, width),
        grad_tokens.astype(jnp.bfloat16).reshape(groups, shard_rows, width),
        accum[0],
        accum[1],
        accum[2],
        accum[3],
        accum[4],
        accum[5],
        small_sums[0],
        small_sums[1],
        small_sums[2],
    )


def solution(mesh):
    in_specs = (
        P("dp", "seq", None),
        P("seq", "dp"),
        P("seq", "dp"),
        P("seq", "dp"),
        P("seq", "dp"),
        P("seq", "dp"),
        P("dp", "seq"),
        P(None, None, ("dp", "seq")),
        P(None, ("dp", "seq")),
        P(None, ("dp", "seq")),
        P("dp", None),
        P("dp", "seq", None),
    )
    out_specs = (
        P("dp", "seq", None),
        P("dp", "seq", None),
        P("seq", "dp"),
        P("seq", "dp"),
        P("seq", "dp"),
        P("seq", "dp"),
        P("seq", "dp"),
        P("dp", "seq"),
        P(None, None, ("dp", "seq")),
        P(None, ("dp", "seq")),
        P(None, ("dp", "seq")),
    )
    return jax.shard_map(local, mesh=mesh, in_specs=in_specs, out_specs=out_specs, check_vma=False)
```

```python
from functools import partial

import jax
import jax.numpy as jnp
from jax import lax
from jax.sharding import PartitionSpec as P

HEADS = 12
HEAD_DIM = 64
PROMPT = 1024
CONT = 8
CLEN = 128
WINDOW = 128
POOL_SPAN = 512
STRIDE = 4


eps_norm = 1e-05


def token_layout(positions_in, offsets):
    in_prompt = positions_in < PROMPT
    segment = jnp.where(in_prompt, -1, (positions_in - PROMPT) // CLEN)
    within = positions_in - PROMPT - segment * CLEN
    choose = (segment[:, None] == jnp.arange(CONT, dtype=jnp.int32)[None, :]).astype(jnp.int32)
    cont_start = jnp.sum(choose * offsets[None, :], axis=1)
    position = jnp.where(in_prompt, positions_in, cont_start + within)
    prompt_limit = jnp.where(in_prompt, PROMPT, cont_start)
    return (segment, position, prompt_limit)


def visible_keys(query_rows, key_index, offsets, reach):
    query_seg, query_pos, query_limit = token_layout(query_rows, offsets)
    key_seg, key_pos, key_limit = token_layout(key_index, offsets)
    prompt_key = (key_seg[None, :] < 0) & (key_pos[None, :] < query_limit[:, None])
    own_key = (key_seg[None, :] == query_seg[:, None]) & (query_seg[:, None] >= 0)
    distance = key_pos[None, :] - query_pos[:, None]
    return (prompt_key | own_key) & (distance >= -(reach // 2)) & (distance < reach // 2)


def key_mask(query_rows, offsets):
    group_len = PROMPT + CONT * CLEN
    full_keys = jnp.arange(group_len, dtype=jnp.int32)
    pooled_keys = jnp.arange(group_len // STRIDE, dtype=jnp.int32) * STRIDE
    return jnp.concatenate(
        [
            visible_keys(query_rows, full_keys, offsets, WINDOW),
            visible_keys(query_rows, pooled_keys, offsets, POOL_SPAN),
        ],
        axis=1,
    )


def pool_rows(source, weight):
    return jnp.sum(
        source.reshape(source.shape[0] // STRIDE, STRIDE, source.shape[1]) * weight[None, :, :],
        axis=1,
    )


def unpool(pooled_grad, weight):
    return (pooled_grad[:, None, :] * weight[None, :, :]).reshape(-1, pooled_grad.shape[1])


def pool_grad(pooled_grad, source):
    blocks_view = source.astype(jnp.float32).reshape(-1, STRIDE, source.shape[1])
    return jnp.sum(pooled_grad[:, None, :] * blocks_view, axis=0)


def layer_norm(source, gain, bias):
    centre = jnp.mean(source, axis=-1, keepdims=True)
    centred = source - centre
    spread = jnp.mean(centred * centred, axis=-1, keepdims=True)
    return centred * lax.rsqrt(spread + eps_norm) * gain + bias


def product(left, right):
    return jnp.dot(left, right, preferred_element_type=jnp.float32)


def product_left(left, right):
    return lax.dot_general(
        left, right, (((0,), (0,)), ((), ())), preferred_element_type=jnp.float32
    )


def product_right(left, right):
    return lax.dot_general(
        left, right, (((1,), (1,)), ((), ())), preferred_element_type=jnp.float32
    )


def add_pair(left_term, right_term):
    return left_term + right_term


def gather_grouped(shards, tie=None):
    local_block = jnp.concatenate(shards, axis=1)
    across = lax.all_gather(local_block, "dp", axis=1, tiled=False)
    across, tie = lax.optimization_barrier((across, tie))
    return lax.all_gather(across, "seq", axis=0, tiled=True), tie


def split_grouped(gathered, widths):
    pieces, at = [], 0
    for width in widths:
        piece = gathered[:, :, at : at + width]
        pieces.append(piece.reshape(piece.shape[0], -1))
        at += width
    return pieces


def code_exact(values, rows):
    parts, rest = [], values
    for _ in range(3):
        part = lax.optimization_barrier(rest.astype(jnp.bfloat16))
        parts.append(part)
        rest = rest - part.astype(jnp.float32)
    flat = jnp.concatenate([part.reshape(-1) for part in parts])
    columns = -(-flat.shape[0] // rows)
    flat = jnp.pad(flat, (0, rows * columns - flat.shape[0]))
    return flat.reshape(rows, columns)


def decode_exact(gathered, count, shape):
    seq_size = lax.psum(1, "seq")
    rows = gathered.shape[0] // seq_size
    blocks = gathered.reshape(seq_size, rows, gathered.shape[1], gathered.shape[2])
    blocks = jnp.transpose(blocks, (2, 0, 1, 3)).reshape(-1, rows * gathered.shape[2])
    parts = blocks[:, : 3 * count].reshape(blocks.shape[0], 3, shape[0], shape[1])
    parts = parts.astype(jnp.float32)
    joined = (parts[:, 0] + parts[:, 1]) + parts[:, 2]
    return jnp.transpose(joined, (1, 0, 2)).reshape(shape[0], -1)


def gather_first(w_query, w_key, w_value, small_local, tie):
    coded = code_exact(small_local, w_query.shape[0])
    first, tie = gather_grouped((w_query, w_key, w_value, coded), tie)
    widths = (w_query.shape[1], w_key.shape[1], w_value.shape[1])
    at = sum(widths)
    small_full = decode_exact(first[:, :, at:], small_local.size, small_local.shape)
    return split_grouped(first[:, :, :at], widths), small_full, tie


def gather_second(w_output, w_inner, w_outer):
    second, _ = gather_grouped((w_output, w_inner, w_outer.T))
    wo, wi, wu_t = split_grouped(second, (w_output.shape[1], w_inner.shape[1], w_outer.shape[0]))
    return (wo, wi, wu_t.T)


def reduce_seq_stage(grads, tie=None):
    dp_size = lax.psum(1, "dp")
    chunks = [grad.reshape(grad.shape[0], dp_size, grad.shape[1] // dp_size) for grad in grads]
    stacked = jnp.concatenate(chunks, axis=2).astype(jnp.bfloat16)
    stacked, tie = lax.optimization_barrier((stacked, tie))
    reduced = lax.psum_scatter(stacked, "seq", scatter_dimension=0, tiled=True)
    return (reduced, [c.shape[2] for c in chunks]), tie


def stack_for_seq(grads):
    dp_size = lax.psum(1, "dp")
    chunks = [grad.reshape(grad.shape[0], dp_size, grad.shape[1] // dp_size) for grad in grads]
    return jnp.concatenate(chunks, axis=2).astype(jnp.bfloat16), [c.shape[2] for c in chunks]


def reduce_dp_stage(stages):
    joined = jnp.concatenate([stage for stage, _ in stages], axis=2)
    over_dp = lax.psum_scatter(joined, "dp", scatter_dimension=1, tiled=True)[:, 0].astype(jnp.float32)
    pieces, at = [], 0
    for _, widths in stages:
        for width in widths:
            pieces.append(over_dp[:, at : at + width])
            at += width
    return pieces


HALF_FULL = WINDOW // 2
HALF_POOL = POOL_SPAN // 2 // STRIDE
BLOCK_POOL = CLEN // STRIDE


def layout_of(index, offsets):
    in_prompt = index < PROMPT
    segment = jnp.where(in_prompt, -1, (index - PROMPT) // CLEN)
    within = index - PROMPT - segment * CLEN
    choose = segment[..., None] == jnp.arange(CONT, dtype=jnp.int32)
    spread = offsets.reshape(offsets.shape[:1] + (1,) * (index.ndim - 1) + offsets.shape[1:])
    cont_start = jnp.sum(jnp.where(choose, spread, 0), axis=-1)
    position = jnp.where(in_prompt, index, cont_start + within)
    limit = jnp.where(in_prompt, PROMPT, cont_start)
    return segment, position, limit


def window_rows(source, starts, length):
    groups, blocks = starts.shape
    return jnp.stack(
        [
            jnp.stack(
                [lax.dynamic_slice_in_dim(source[g], starts[g, b], length, 0) for b in range(blocks)]
            )
            for g in range(groups)
        ]
    )


def window_add(target, updates, starts):
    groups, blocks = starts.shape
    length = updates.shape[2]
    rows = []
    for g in range(groups):
        row = target[g]
        for b in range(blocks):
            start = starts[g, b]
            current = lax.dynamic_slice_in_dim(row, start, length, 0)
            row = lax.dynamic_update_slice_in_dim(row, current + updates[g, b], start, 0)
        rows.append(row)
    return jnp.stack(rows)


def block_geometry(seq_index, groups, shard_rows, offsets):
    group_len = PROMPT + CONT * CLEN
    pooled_len = group_len // STRIDE
    blocks = shard_rows // CLEN
    block_start = (seq_index * blocks + jnp.arange(blocks, dtype=jnp.int32)) * CLEN
    prompt_block = block_start < PROMPT
    cont_index = jnp.clip((block_start - PROMPT) // CLEN, 0, CONT - 1)
    anchor = jnp.where(prompt_block[None, :], block_start[None, :], offsets[:, cont_index])
    pooled_start = block_start // STRIDE
    intended = (
        anchor - HALF_FULL,
        jnp.broadcast_to(block_start + CLEN, anchor.shape),
        anchor // STRIDE - HALF_POOL,
        jnp.broadcast_to(pooled_start + BLOCK_POOL, anchor.shape),
    )
    limits = (group_len, group_len, pooled_len, pooled_len)
    lengths = (HALF_FULL, HALF_FULL, HALF_POOL, HALF_POOL)
    clamped = tuple(
        jnp.clip(start, 0, limit - length) for start, limit, length in zip(intended, limits, lengths)
    )
    ramp = lambda n: jnp.arange(n, dtype=jnp.int32)

    def span(window):
        actual = clamped[window][:, :, None] + ramp(lengths[window])
        offset = actual - intended[window][:, :, None]
        return actual, (offset >= 0) & (offset < lengths[window])

    before_full, before_full_ok = span(0)
    after_full, after_full_ok = span(1)
    before_pool, before_pool_ok = span(2)
    after_pool, after_pool_ok = span(3)
    after_ok = prompt_block[None, :, None]
    own_full = jnp.broadcast_to(block_start[None, :, None] + ramp(CLEN), anchor.shape + (CLEN,))
    own_pool = jnp.broadcast_to(
        pooled_start[None, :, None] + ramp(BLOCK_POOL), anchor.shape + (BLOCK_POOL,)
    )
    full_index = jnp.concatenate([before_full, own_full, after_full], axis=2)
    pooled_index = jnp.concatenate([before_pool, own_pool, after_pool], axis=2)
    full_valid = jnp.concatenate(
        [before_full_ok, jnp.ones(own_full.shape, bool), after_ok & after_full_ok], axis=2
    )
    pooled_valid = jnp.concatenate(
        [before_pool_ok, jnp.ones(own_pool.shape, bool), after_ok & after_pool_ok], axis=2
    )
    query_index = block_start[None, :, None] + ramp(CLEN)
    query_index = jnp.broadcast_to(query_index, anchor.shape + (CLEN,))
    q_seg, q_pos, q_lim = layout_of(query_index, offsets)

    def visible(key_token, valid, reach):
        k_seg, k_pos, _ = layout_of(key_token, offsets)
        k_seg, k_pos, valid = k_seg[:, :, None, :], k_pos[:, :, None, :], valid[:, :, None, :]
        prompt_key = (k_seg < 0) & (k_pos < q_lim[..., None])
        own_key = (k_seg == q_seg[..., None]) & (q_seg[..., None] >= 0)
        distance = k_pos - q_pos[..., None]
        return valid & (prompt_key | own_key) & (distance >= -(reach // 2)) & (distance < reach // 2)

    mask = jnp.concatenate(
        [
            visible(full_index, full_valid, WINDOW),
            visible(pooled_index * STRIDE, pooled_valid, POOL_SPAN),
        ],
        axis=3,
    )
    return clamped, mask


def attention_fwd(queries, kv_local, pkv_local, kv_all, pkv_all, starts, mask):
    groups, shard_rows, width = queries.shape
    blocks = shard_rows // CLEN
    score_scale = 1.0 / HEAD_DIM**0.5
    keys_cat = jnp.concatenate(
        [
            window_rows(kv_all, starts[0], HALF_FULL),
            kv_local.reshape(groups, blocks, CLEN, 2 * width),
            window_rows(kv_all, starts[1], HALF_FULL),
            window_rows(pkv_all, starts[2], HALF_POOL),
            pkv_local.reshape(groups, blocks, BLOCK_POOL, 2 * width),
            window_rows(pkv_all, starts[3], HALF_POOL),
        ],
        axis=2,
    )
    span = keys_cat.shape[2]
    head_keys = keys_cat[..., :width].reshape(groups, blocks, span, HEADS, HEAD_DIM)
    head_values = keys_cat[..., width:].reshape(groups, blocks, span, HEADS, HEAD_DIM)
    head_query = queries.reshape(groups, blocks, CLEN, HEADS, HEAD_DIM)
    scores = jnp.einsum(
        "gbqhd,gbkhd->gbhqk", head_query, head_keys, preferred_element_type=jnp.float32
    )
    scores = jnp.where(mask[:, :, None], scores * score_scale, -1000000000.0)
    row_top = jnp.max(scores, axis=-1, keepdims=True)
    exponent = jnp.exp(scores - row_top)
    row_total = jnp.sum(exponent, axis=-1, keepdims=True)
    probs = exponent / row_total
    attended = jnp.einsum(
        "gbhqk,gbkhd->gbqhd",
        probs.astype(jnp.bfloat16),
        head_values,
        preferred_element_type=jnp.float32,
    )
    attended = attended.reshape(groups * shard_rows, width).astype(jnp.bfloat16)
    return attended, (head_query, head_keys, head_values, probs)


def attention_bwd(grad_attended, saved, starts, seq_index):
    head_query, head_keys, head_values, probs = saved
    groups, blocks = head_query.shape[:2]
    width = HEADS * HEAD_DIM
    score_scale = 1.0 / HEAD_DIM**0.5
    head_grad = grad_attended.reshape(groups, blocks, CLEN, HEADS, HEAD_DIM)
    grad_probs = jnp.einsum(
        "gbqhd,gbkhd->gbhqk", head_grad, head_values, preferred_element_type=jnp.float32
    )
    centre = jnp.sum(probs * grad_probs, axis=-1, keepdims=True)
    grad_scores = (probs * (grad_probs - centre)).astype(jnp.bfloat16)
    grad_queries = jnp.einsum(
        "gbhqk,gbkhd->gbqhd", grad_scores, head_keys, preferred_element_type=jnp.float32
    ) * score_scale
    grad_keys = jnp.einsum(
        "gbhqk,gbqhd->gbkhd", grad_scores, head_query, preferred_element_type=jnp.float32
    ) * score_scale
    grad_values = jnp.einsum(
        "gbhqk,gbqhd->gbkhd",
        probs.astype(jnp.bfloat16),
        head_grad,
        preferred_element_type=jnp.float32,
    )
    span = grad_keys.shape[2]
    grad_kv = jnp.concatenate(
        [grad_keys.reshape(groups, blocks, span, width), grad_values.reshape(groups, blocks, span, width)],
        axis=3,
    )
    shard_rows = blocks * CLEN
    group_len = PROMPT + CONT * CLEN
    pooled_len = group_len // STRIDE
    cut = (0, HALF_FULL, HALF_FULL + CLEN, 2 * HALF_FULL + CLEN)
    pcut = tuple(cut[-1] + c for c in (0, HALF_POOL, HALF_POOL + BLOCK_POOL, 2 * HALF_POOL + BLOCK_POOL))
    ramp = lambda n: jnp.arange(n, dtype=jnp.int32)
    own_full = grad_kv[:, :, cut[1] : cut[2]].reshape(groups, shard_rows, 2 * width)
    full = jnp.zeros((groups, group_len, 2 * width), jnp.float32)
    full = lax.dynamic_update_slice_in_dim(full, own_full, seq_index * shard_rows, 1)
    side_values = jnp.concatenate(
        [grad_kv[:, :, cut[0] : cut[1]], grad_kv[:, :, cut[2] : cut[3]]], axis=2
    ).reshape(groups, -1, 2 * width)
    side_rows = jnp.concatenate(
        [starts[0][:, :, None] + ramp(HALF_FULL), starts[1][:, :, None] + ramp(HALF_FULL)], axis=2
    ).reshape(groups, -1)
    own_pool_rows = (seq_index * (shard_rows // STRIDE) + ramp(blocks)[:, None] * BLOCK_POOL + ramp(BLOCK_POOL))
    pool_values = grad_kv[:, :, pcut[0] : pcut[3]].reshape(groups, -1, 2 * width)
    pool_rows_index = jnp.concatenate(
        [
            starts[2][:, :, None] + ramp(HALF_POOL),
            jnp.broadcast_to(own_pool_rows[None], (groups, blocks, BLOCK_POOL)),
            starts[3][:, :, None] + ramp(HALF_POOL),
        ],
        axis=2,
    ).reshape(groups, -1)
    fulls, pooleds, unpooleds = [], [], []
    for g in range(groups):
        fulls.append(full[g] + select_sum(side_values[g], side_rows[g] == ramp(group_len)[:, None]))
        pooleds.append(select_sum(pool_values[g], pool_rows_index[g] == ramp(pooled_len)[:, None]))
        unpooleds.append(
            select_sum(pool_values[g], pool_rows_index[g] == (ramp(group_len) // STRIDE)[:, None])
        )
    full = jnp.stack(fulls)
    pooled = jnp.stack(pooleds)
    unpooled = jnp.stack(unpooleds)
    grad_queries = grad_queries.reshape(groups * shard_rows, width).astype(jnp.bfloat16)
    return grad_queries, full, pooled, unpooled


def select_sum(values, chosen):
    onehot = chosen.astype(jnp.bfloat16)
    high = values.astype(jnp.bfloat16)
    low = (values - high.astype(jnp.float32)).astype(jnp.bfloat16)
    return product(onehot, high) + product(onehot, low)


def phase_weights(weight, rows):
    phase = (jnp.arange(rows, dtype=jnp.int32) % STRIDE)[:, None]
    total = jnp.zeros((rows, weight.shape[1]), jnp.float32)
    for r in range(STRIDE):
        total = total + jnp.where(phase == r, weight[r][None, :], 0.0)
    return total


def pool_grouped(source, weight):
    groups, rows, width = source.shape
    return jnp.sum(
        source.reshape(groups, rows // STRIDE, STRIDE, width) * weight[None, None], axis=2
    )


def unpool_grouped(pooled_grad, weight):
    groups, rows, width = pooled_grad.shape
    return (pooled_grad[:, :, None, :] * weight[None, None]).reshape(groups, rows * STRIDE, width)


def pool_grad_grouped(pooled_grad, source):
    groups, rows, width = source.shape
    blocks_view = source.astype(jnp.float32).reshape(groups, rows // STRIDE, STRIDE, width)
    return jnp.sum(pooled_grad[:, :, None, :] * blocks_view, axis=(0, 1))


def local(
    hidden_in,
    w_query,
    w_key,
    w_value,
    w_output,
    w_inner,
    w_outer,
    pool_weight,
    ln_gain,
    ln_bias,
    branch_blocks,
    grad_out,
):
    pool_rows_count = pool_weight.shape[0] * pool_weight.shape[1]
    small_local = jnp.concatenate(
        [pool_weight.reshape(pool_rows_count, -1), ln_gain, ln_bias], axis=0
    )
    hidden_all = lax.all_gather(hidden_in, "seq", axis=1, tiled=True)
    (wq, wk, wv), small_full, hidden_all = gather_first(
        w_query, w_key, w_value, small_local, hidden_all
    )
    pool_full = small_full[:pool_rows_count].reshape(pool_weight.shape[0], pool_weight.shape[1], -1)
    gain_full = small_full[pool_rows_count : pool_rows_count + ln_gain.shape[0]]
    bias_full = small_full[pool_rows_count + ln_gain.shape[0] :]
    groups, shard_rows, width = hidden_in.shape
    seq_index = lax.axis_index("seq")
    offsets = STRIDE * branch_blocks
    starts, mask = block_geometry(seq_index, groups, shard_rows, offsets)

    group_len = hidden_all.shape[1]
    tokens = hidden_in.reshape(groups * shard_rows, width)
    all_tokens = hidden_all.reshape(groups * group_len, width)
    queries = product(tokens, wq).astype(jnp.bfloat16)
    key_g = product(all_tokens, wk).astype(jnp.bfloat16).reshape(groups, group_len, width)
    value_g = product(all_tokens, wv).astype(jnp.bfloat16).reshape(groups, group_len, width)
    pooled_keys = pool_grouped(key_g.astype(jnp.float32), pool_full[0]).astype(jnp.bfloat16)
    pooled_values = pool_grouped(value_g.astype(jnp.float32), pool_full[1]).astype(jnp.bfloat16)
    kv_all = jnp.concatenate([key_g, value_g], axis=2)
    pkv_all = jnp.concatenate([pooled_keys, pooled_values], axis=2)
    kv_local = lax.dynamic_slice_in_dim(kv_all, seq_index * shard_rows, shard_rows, 1)
    pkv_local = lax.dynamic_slice_in_dim(
        pkv_all, seq_index * (shard_rows // STRIDE), shard_rows // STRIDE, 1
    )
    wq, wk, wv, w_output, w_inner, w_outer = lax.optimization_barrier(
        (wq, wk, wv, w_output, w_inner, w_outer)
    )
    wo, wi, wu = gather_second(w_output, w_inner, w_outer)
    attended, att_saved = attention_fwd(
        queries.reshape(groups, shard_rows, width), kv_local, pkv_local, kv_all, pkv_all, starts, mask
    )
    mixed_rows = tokens.astype(jnp.float32) + product(attended, wo)
    normed_first = layer_norm(mixed_rows, gain_full[0], bias_full[0])
    first_low = normed_first.astype(jnp.bfloat16)
    inner_act = product(first_low, wi)
    active = jax.nn.gelu(inner_act, approximate=False).astype(jnp.bfloat16)
    second = normed_first + product(active, wu)
    norm_value, second_back = jax.vjp(layer_norm, second, gain_full[1], bias_full[1])
    output = norm_value.astype(jnp.bfloat16)

    cotangent = grad_out.reshape(groups * shard_rows, width).astype(jnp.float32)
    grad_second, gain_second, bias_second = second_back(cotangent)
    grad_ffn_out = grad_second.astype(jnp.bfloat16)
    grad_outer = product_left(active, grad_ffn_out)
    grad_active = product_right(grad_ffn_out, wu)
    gelu_value, gelu_back = jax.vjp(partial(jax.nn.gelu, approximate=False), inner_act)
    grad_inner_act = gelu_back(grad_active)[0].astype(jnp.bfloat16)
    grad_inner = product_left(first_low, grad_inner_act)
    grad_first = grad_second + product_right(grad_inner_act, wi)
    first_value, first_back = jax.vjp(layer_norm, mixed_rows, gain_full[0], bias_full[0])
    grad_mixed, gain_first, bias_first = first_back(grad_first)
    grad_branch = grad_mixed.astype(jnp.bfloat16)
    grad_output = product_left(attended, grad_branch)
    grad_attended = product_right(grad_branch, wo).astype(jnp.bfloat16)
    early, grad_attended = reduce_seq_stage((grad_output, grad_inner, grad_outer.T), grad_attended)
    early_reduced, early_widths = early

    grad_rows = grad_attended.reshape(groups, shard_rows, width)
    key_phase = phase_weights(pool_full[0], group_len)
    value_phase = phase_weights(pool_full[1], group_len)
    pieces_back = []
    for g in range(groups):
        saved_g = tuple(item[g : g + 1] for item in att_saved)
        starts_g = tuple(item[g : g + 1] for item in starts)
        grad_g = grad_rows[g].reshape(shard_rows, width)
        grad_queries_g, full_g, pooled_g, unpooled_g = attention_bwd(grad_g, saved_g, starts_g, seq_index)
        if g == 1:
            full_g, pooled_g, unpooled_g, earlier_back, early_reduced = lax.optimization_barrier(
                (full_g, pooled_g, unpooled_g, pieces_back[0][4], early_reduced)
            )
            pieces_back[0] = pieces_back[0][:4] + (earlier_back,)
        key_partial_g = (
            full_g[0, :, :width] + unpooled_g[0, :, :width] * key_phase
        ).astype(jnp.bfloat16)
        value_partial_g = (
            full_g[0, :, width:] + unpooled_g[0, :, width:] * value_phase
        ).astype(jnp.bfloat16)
        back_g = product_right(key_partial_g, wk) + product_right(value_partial_g, wv)
        back_g = back_g.reshape(1, group_len, width).astype(jnp.bfloat16)
        back_own_g = lax.psum_scatter(back_g, "seq", scatter_dimension=1, tiled=True)
        pieces_back.append((grad_queries_g, pooled_g, key_partial_g, value_partial_g, back_own_g))
    grad_queries = jnp.concatenate([piece[0] for piece in pieces_back], axis=0)
    grad_pooled = jnp.concatenate([piece[1] for piece in pieces_back], axis=0)
    key_partial = jnp.concatenate([piece[2] for piece in pieces_back], axis=0)
    value_partial = jnp.concatenate([piece[3] for piece in pieces_back], axis=0)
    last_back = pieces_back[-1][4]
    early_dp = reduce_dp_stage(((early_reduced, early_widths),))
    grad_pooling = jnp.stack(
        [
            pool_grad_grouped(grad_pooled[..., :width], key_g),
            pool_grad_grouped(grad_pooled[..., width:], value_g),
        ]
    )
    grad_query_w = product_left(tokens, grad_queries)
    grad_key_w = product_left(all_tokens, key_partial)
    grad_value_w = product_left(all_tokens, value_partial)
    late_stacked, late_widths = stack_for_seq((grad_query_w, grad_key_w, grad_value_w))
    late_stacked, early_dp = lax.optimization_barrier((late_stacked, early_dp))
    seq_size = lax.psum(1, "seq")
    dp_size = lax.psum(1, "dp")
    rows_each = late_stacked.shape[0] // seq_size
    late_blocks = late_stacked.reshape(seq_size, rows_each, dp_size, late_stacked.shape[2])
    late_blocks = jnp.transpose(late_blocks, (2, 0, 1, 3)).reshape(-1, late_stacked.shape[2])
    late_reduced = lax.psum_scatter(late_blocks, ("dp", "seq"), scatter_dimension=0, tiled=True)
    late_reduced = late_reduced.astype(jnp.float32)
    late_dp, at = [], 0
    for width_piece in late_widths:
        late_dp.append(late_reduced[:, at : at + width_piece])
        at += width_piece
    back_own = jnp.concatenate([piece[4] for piece in pieces_back], axis=0)
    grad_tokens = (
        grad_mixed
        + product_right(grad_queries, wq)
        + back_own.reshape(groups * shard_rows, width).astype(jnp.float32)
    )
    accum = (late_dp[0], late_dp[1], late_dp[2], early_dp[0], early_dp[1], early_dp[2].T)
    small_sums = (
        lax.psum_scatter(grad_pooling, ("dp", "seq"), scatter_dimension=2, tiled=True),
        lax.psum_scatter(
            jnp.stack([gain_first, gain_second]), ("dp", "seq"), scatter_dimension=1, tiled=True
        ),
        lax.psum_scatter(
            jnp.stack([bias_first, bias_second]), ("dp", "seq"), scatter_dimension=1, tiled=True
        ),
    )
    return (
        output.reshape(groups, shard_rows, width),
        grad_tokens.astype(jnp.bfloat16).reshape(groups, shard_rows, width),
        accum[0],
        accum[1],
        accum[2],
        accum[3],
        accum[4],
        accum[5],
        small_sums[0],
        small_sums[1],
        small_sums[2],
    )


def solution(mesh):
    in_specs = (
        P("dp", "seq", None),
        P("seq", "dp"),
        P("seq", "dp"),
        P("seq", "dp"),
        P("seq", "dp"),
        P("seq", "dp"),
        P("dp", "seq"),
        P(None, None, ("dp", "seq")),
        P(None, ("dp", "seq")),
        P(None, ("dp", "seq")),
        P("dp", None),
        P("dp", "seq", None),
    )
    out_specs = (
        P("dp", "seq", None),
        P("dp", "seq", None),
        P("seq", "dp"),
        P("seq", "dp"),
        P("seq", "dp"),
        P("seq", "dp"),
        P("seq", "dp"),
        P("dp", "seq"),
        P(None, None, ("dp", "seq")),
        P(None, ("dp", "seq")),
        P(None, ("dp", "seq")),
    )
    return jax.shard_map(local, mesh=mesh, in_specs=in_specs, out_specs=out_specs, check_vma=False)
```

```python
from functools import partial

import jax
import jax.numpy as jnp
from jax import lax
from jax.sharding import PartitionSpec as P

HEADS = 12
HEAD_DIM = 64
PROMPT = 1024
CONT = 8
CLEN = 128
WINDOW = 128
POOL_SPAN = 512
STRIDE = 4


eps_norm = 1e-05


def token_layout(positions_in, offsets):
    in_prompt = positions_in < PROMPT
    segment = jnp.where(in_prompt, -1, (positions_in - PROMPT) // CLEN)
    within = positions_in - PROMPT - segment * CLEN
    choose = (segment[:, None] == jnp.arange(CONT, dtype=jnp.int32)[None, :]).astype(jnp.int32)
    cont_start = jnp.sum(choose * offsets[None, :], axis=1)
    position = jnp.where(in_prompt, positions_in, cont_start + within)
    prompt_limit = jnp.where(in_prompt, PROMPT, cont_start)
    return (segment, position, prompt_limit)


def visible_keys(query_rows, key_index, offsets, reach):
    query_seg, query_pos, query_limit = token_layout(query_rows, offsets)
    key_seg, key_pos, key_limit = token_layout(key_index, offsets)
    prompt_key = (key_seg[None, :] < 0) & (key_pos[None, :] < query_limit[:, None])
    own_key = (key_seg[None, :] == query_seg[:, None]) & (query_seg[:, None] >= 0)
    distance = key_pos[None, :] - query_pos[:, None]
    return (prompt_key | own_key) & (distance >= -(reach // 2)) & (distance < reach // 2)


def key_mask(query_rows, offsets):
    group_len = PROMPT + CONT * CLEN
    full_keys = jnp.arange(group_len, dtype=jnp.int32)
    pooled_keys = jnp.arange(group_len // STRIDE, dtype=jnp.int32) * STRIDE
    return jnp.concatenate(
        [
            visible_keys(query_rows, full_keys, offsets, WINDOW),
            visible_keys(query_rows, pooled_keys, offsets, POOL_SPAN),
        ],
        axis=1,
    )


def pool_rows(source, weight):
    return jnp.sum(
        source.reshape(source.shape[0] // STRIDE, STRIDE, source.shape[1]) * weight[None, :, :],
        axis=1,
    )


def unpool(pooled_grad, weight):
    return (pooled_grad[:, None, :] * weight[None, :, :]).reshape(-1, pooled_grad.shape[1])


def pool_grad(pooled_grad, source):
    blocks_view = source.astype(jnp.float32).reshape(-1, STRIDE, source.shape[1])
    return jnp.sum(pooled_grad[:, None, :] * blocks_view, axis=0)


def layer_norm(source, gain, bias):
    centre = jnp.mean(source, axis=-1, keepdims=True)
    centred = source - centre
    spread = jnp.mean(centred * centred, axis=-1, keepdims=True)
    return centred * lax.rsqrt(spread + eps_norm) * gain + bias


def product(left, right):
    return jnp.dot(left, right, preferred_element_type=jnp.float32)


def product_left(left, right):
    return lax.dot_general(
        left, right, (((0,), (0,)), ((), ())), preferred_element_type=jnp.float32
    )


def product_right(left, right):
    return lax.dot_general(
        left, right, (((1,), (1,)), ((), ())), preferred_element_type=jnp.float32
    )


def add_pair(left_term, right_term):
    return left_term + right_term


def gather_grouped(shards, tie=None):
    local_block = jnp.concatenate(shards, axis=1)
    across = lax.all_gather(local_block, "dp", axis=1, tiled=False)
    across, tie = lax.optimization_barrier((across, tie))
    return lax.all_gather(across, "seq", axis=0, tiled=True), tie


def split_grouped(gathered, widths):
    pieces, at = [], 0
    for width in widths:
        piece = gathered[:, :, at : at + width]
        pieces.append(piece.reshape(piece.shape[0], -1))
        at += width
    return pieces


def code_exact(values, rows):
    parts, rest = [], values
    for _ in range(3):
        part = lax.optimization_barrier(rest.astype(jnp.bfloat16))
        parts.append(part)
        rest = rest - part.astype(jnp.float32)
    flat = jnp.concatenate([part.reshape(-1) for part in parts])
    columns = -(-flat.shape[0] // rows)
    flat = jnp.pad(flat, (0, rows * columns - flat.shape[0]))
    return flat.reshape(rows, columns)


def decode_exact(gathered, count, shape):
    seq_size = lax.psum(1, "seq")
    rows = gathered.shape[0] // seq_size
    blocks = gathered.reshape(seq_size, rows, gathered.shape[1], gathered.shape[2])
    blocks = jnp.transpose(blocks, (2, 0, 1, 3)).reshape(-1, rows * gathered.shape[2])
    parts = blocks[:, : 3 * count].reshape(blocks.shape[0], 3, shape[0], shape[1])
    parts = parts.astype(jnp.float32)
    joined = (parts[:, 0] + parts[:, 1]) + parts[:, 2]
    return jnp.transpose(joined, (1, 0, 2)).reshape(shape[0], -1)


def gather_first(w_query, w_key, w_value, small_local, tie):
    coded = code_exact(small_local, w_query.shape[0])
    first, tie = gather_grouped((w_query, w_key, w_value, coded), tie)
    widths = (w_query.shape[1], w_key.shape[1], w_value.shape[1])
    at = sum(widths)
    small_full = decode_exact(first[:, :, at:], small_local.size, small_local.shape)
    return split_grouped(first[:, :, :at], widths), small_full, tie


def gather_second(w_output, w_inner, w_outer):
    second, _ = gather_grouped((w_output, w_inner, w_outer.T))
    wo, wi, wu_t = split_grouped(second, (w_output.shape[1], w_inner.shape[1], w_outer.shape[0]))
    return (wo, wi, wu_t.T)


def reduce_seq_stage(grads, tie=None):
    dp_size = lax.psum(1, "dp")
    chunks = [grad.reshape(grad.shape[0], dp_size, grad.shape[1] // dp_size) for grad in grads]
    stacked = jnp.concatenate(chunks, axis=2).astype(jnp.bfloat16)
    stacked, tie = lax.optimization_barrier((stacked, tie))
    reduced = lax.psum_scatter(stacked, "seq", scatter_dimension=0, tiled=True)
    return (reduced, [c.shape[2] for c in chunks]), tie


def stack_for_seq(grads):
    dp_size = lax.psum(1, "dp")
    chunks = [grad.reshape(grad.shape[0], dp_size, grad.shape[1] // dp_size) for grad in grads]
    return jnp.concatenate(chunks, axis=2).astype(jnp.bfloat16), [c.shape[2] for c in chunks]


def reduce_dp_stage(stages):
    joined = jnp.concatenate([stage for stage, _ in stages], axis=2)
    over_dp = lax.psum_scatter(joined, "dp", scatter_dimension=1, tiled=True)[:, 0].astype(jnp.float32)
    pieces, at = [], 0
    for _, widths in stages:
        for width in widths:
            pieces.append(over_dp[:, at : at + width])
            at += width
    return pieces


HALF_FULL = WINDOW // 2
HALF_POOL = POOL_SPAN // 2 // STRIDE
BLOCK_POOL = CLEN // STRIDE


def layout_of(index, offsets):
    in_prompt = index < PROMPT
    segment = jnp.where(in_prompt, -1, (index - PROMPT) // CLEN)
    within = index - PROMPT - segment * CLEN
    choose = segment[..., None] == jnp.arange(CONT, dtype=jnp.int32)
    spread = offsets.reshape(offsets.shape[:1] + (1,) * (index.ndim - 1) + offsets.shape[1:])
    cont_start = jnp.sum(jnp.where(choose, spread, 0), axis=-1)
    position = jnp.where(in_prompt, index, cont_start + within)
    limit = jnp.where(in_prompt, PROMPT, cont_start)
    return segment, position, limit


def window_rows(source, starts, length):
    groups, blocks = starts.shape
    return jnp.stack(
        [
            jnp.stack(
                [lax.dynamic_slice_in_dim(source[g], starts[g, b], length, 0) for b in range(blocks)]
            )
            for g in range(groups)
        ]
    )


def window_add(target, updates, starts):
    groups, blocks = starts.shape
    length = updates.shape[2]
    rows = []
    for g in range(groups):
        row = target[g]
        for b in range(blocks):
            start = starts[g, b]
            current = lax.dynamic_slice_in_dim(row, start, length, 0)
            row = lax.dynamic_update_slice_in_dim(row, current + updates[g, b], start, 0)
        rows.append(row)
    return jnp.stack(rows)


def block_geometry(seq_index, groups, shard_rows, offsets):
    group_len = PROMPT + CONT * CLEN
    pooled_len = group_len // STRIDE
    blocks = shard_rows // CLEN
    block_start = (seq_index * blocks + jnp.arange(blocks, dtype=jnp.int32)) * CLEN
    prompt_block = block_start < PROMPT
    cont_index = jnp.clip((block_start - PROMPT) // CLEN, 0, CONT - 1)
    anchor = jnp.where(prompt_block[None, :], block_start[None, :], offsets[:, cont_index])
    pooled_start = block_start // STRIDE
    intended = (
        anchor - HALF_FULL,
        jnp.broadcast_to(block_start + CLEN, anchor.shape),
        anchor // STRIDE - HALF_POOL,
        jnp.broadcast_to(pooled_start + BLOCK_POOL, anchor.shape),
    )
    limits = (group_len, group_len, pooled_len, pooled_len)
    lengths = (HALF_FULL, HALF_FULL, HALF_POOL, HALF_POOL)
    clamped = tuple(
        jnp.clip(start, 0, limit - length) for start, limit, length in zip(intended, limits, lengths)
    )
    ramp = lambda n: jnp.arange(n, dtype=jnp.int32)

    def span(window):
        actual = clamped[window][:, :, None] + ramp(lengths[window])
        offset = actual - intended[window][:, :, None]
        return actual, (offset >= 0) & (offset < lengths[window])

    before_full, before_full_ok = span(0)
    after_full, after_full_ok = span(1)
    before_pool, before_pool_ok = span(2)
    after_pool, after_pool_ok = span(3)
    after_ok = prompt_block[None, :, None]
    own_full = jnp.broadcast_to(block_start[None, :, None] + ramp(CLEN), anchor.shape + (CLEN,))
    own_pool = jnp.broadcast_to(
        pooled_start[None, :, None] + ramp(BLOCK_POOL), anchor.shape + (BLOCK_POOL,)
    )
    full_index = jnp.concatenate([before_full, own_full, after_full], axis=2)
    pooled_index = jnp.concatenate([before_pool, own_pool, after_pool], axis=2)
    full_valid = jnp.concatenate(
        [before_full_ok, jnp.ones(own_full.shape, bool), after_ok & after_full_ok], axis=2
    )
    pooled_valid = jnp.concatenate(
        [before_pool_ok, jnp.ones(own_pool.shape, bool), after_ok & after_pool_ok], axis=2
    )
    query_index = block_start[None, :, None] + ramp(CLEN)
    query_index = jnp.broadcast_to(query_index, anchor.shape + (CLEN,))
    q_seg, q_pos, q_lim = layout_of(query_index, offsets)

    def visible(key_token, valid, reach):
        k_seg, k_pos, _ = layout_of(key_token, offsets)
        k_seg, k_pos, valid = k_seg[:, :, None, :], k_pos[:, :, None, :], valid[:, :, None, :]
        prompt_key = (k_seg < 0) & (k_pos < q_lim[..., None])
        own_key = (k_seg == q_seg[..., None]) & (q_seg[..., None] >= 0)
        distance = k_pos - q_pos[..., None]
        return valid & (prompt_key | own_key) & (distance >= -(reach // 2)) & (distance < reach // 2)

    mask = jnp.concatenate(
        [
            visible(full_index, full_valid, WINDOW),
            visible(pooled_index * STRIDE, pooled_valid, POOL_SPAN),
        ],
        axis=3,
    )
    return clamped, mask


def attention_fwd(queries, kv_local, pkv_local, kv_all, pkv_all, starts, mask):
    groups, shard_rows, width = queries.shape
    blocks = shard_rows // CLEN
    score_scale = 1.0 / HEAD_DIM**0.5
    keys_cat = jnp.concatenate(
        [
            window_rows(kv_all, starts[0], HALF_FULL),
            kv_local.reshape(groups, blocks, CLEN, 2 * width),
            window_rows(kv_all, starts[1], HALF_FULL),
            window_rows(pkv_all, starts[2], HALF_POOL),
            pkv_local.reshape(groups, blocks, BLOCK_POOL, 2 * width),
            window_rows(pkv_all, starts[3], HALF_POOL),
        ],
        axis=2,
    )
    span = keys_cat.shape[2]
    head_keys = keys_cat[..., :width].reshape(groups, blocks, span, HEADS, HEAD_DIM)
    head_values = keys_cat[..., width:].reshape(groups, blocks, span, HEADS, HEAD_DIM)
    head_query = queries.reshape(groups, blocks, CLEN, HEADS, HEAD_DIM)
    scores = jnp.einsum(
        "gbqhd,gbkhd->gbhqk", head_query, head_keys, preferred_element_type=jnp.float32
    )
    scores = jnp.where(mask[:, :, None], scores * score_scale, -1000000000.0)
    row_top = jnp.max(scores, axis=-1, keepdims=True)
    exponent = jnp.exp(scores - row_top)
    row_total = jnp.sum(exponent, axis=-1, keepdims=True)
    probs = exponent / row_total
    attended = jnp.einsum(
        "gbhqk,gbkhd->gbqhd",
        probs.astype(jnp.bfloat16),
        head_values,
        preferred_element_type=jnp.float32,
    )
    attended = attended.reshape(groups * shard_rows, width).astype(jnp.bfloat16)
    return attended, (head_query, head_keys, head_values, probs)


def attention_bwd(grad_attended, saved, starts, seq_index):
    head_query, head_keys, head_values, probs = saved
    groups, blocks = head_query.shape[:2]
    width = HEADS * HEAD_DIM
    score_scale = 1.0 / HEAD_DIM**0.5
    head_grad = grad_attended.reshape(groups, blocks, CLEN, HEADS, HEAD_DIM)
    grad_probs = jnp.einsum(
        "gbqhd,gbkhd->gbhqk", head_grad, head_values, preferred_element_type=jnp.float32
    )
    centre = jnp.sum(probs * grad_probs, axis=-1, keepdims=True)
    grad_scores = (probs * (grad_probs - centre)).astype(jnp.bfloat16)
    grad_queries = jnp.einsum(
        "gbhqk,gbkhd->gbqhd", grad_scores, head_keys, preferred_element_type=jnp.float32
    ) * score_scale
    grad_keys = jnp.einsum(
        "gbhqk,gbqhd->gbkhd", grad_scores, head_query, preferred_element_type=jnp.float32
    ) * score_scale
    grad_values = jnp.einsum(
        "gbhqk,gbqhd->gbkhd",
        probs.astype(jnp.bfloat16),
        head_grad,
        preferred_element_type=jnp.float32,
    )
    span = grad_keys.shape[2]
    grad_kv = jnp.concatenate(
        [grad_keys.reshape(groups, blocks, span, width), grad_values.reshape(groups, blocks, span, width)],
        axis=3,
    )
    shard_rows = blocks * CLEN
    group_len = PROMPT + CONT * CLEN
    pooled_len = group_len // STRIDE
    cut = (0, HALF_FULL, HALF_FULL + CLEN, 2 * HALF_FULL + CLEN)
    pcut = tuple(cut[-1] + c for c in (0, HALF_POOL, HALF_POOL + BLOCK_POOL, 2 * HALF_POOL + BLOCK_POOL))
    ramp = lambda n: jnp.arange(n, dtype=jnp.int32)
    own_full = grad_kv[:, :, cut[1] : cut[2]].reshape(groups, shard_rows, 2 * width)
    full = jnp.zeros((groups, group_len, 2 * width), jnp.float32)
    full = lax.dynamic_update_slice_in_dim(full, own_full, seq_index * shard_rows, 1)
    side_values = jnp.concatenate(
        [grad_kv[:, :, cut[0] : cut[1]], grad_kv[:, :, cut[2] : cut[3]]], axis=2
    ).reshape(groups, -1, 2 * width)
    side_rows = jnp.concatenate(
        [starts[0][:, :, None] + ramp(HALF_FULL), starts[1][:, :, None] + ramp(HALF_FULL)], axis=2
    ).reshape(groups, -1)
    own_pool_rows = (seq_index * (shard_rows // STRIDE) + ramp(blocks)[:, None] * BLOCK_POOL + ramp(BLOCK_POOL))
    pool_values = grad_kv[:, :, pcut[0] : pcut[3]].reshape(groups, -1, 2 * width)
    pool_rows_index = jnp.concatenate(
        [
            starts[2][:, :, None] + ramp(HALF_POOL),
            jnp.broadcast_to(own_pool_rows[None], (groups, blocks, BLOCK_POOL)),
            starts[3][:, :, None] + ramp(HALF_POOL),
        ],
        axis=2,
    ).reshape(groups, -1)
    fulls, pooleds, unpooleds = [], [], []
    for g in range(groups):
        fulls.append(full[g] + select_sum(side_values[g], side_rows[g] == ramp(group_len)[:, None]))
        pooleds.append(select_sum(pool_values[g], pool_rows_index[g] == ramp(pooled_len)[:, None]))
        unpooleds.append(
            select_sum(pool_values[g], pool_rows_index[g] == (ramp(group_len) // STRIDE)[:, None])
        )
    full = jnp.stack(fulls)
    pooled = jnp.stack(pooleds)
    unpooled = jnp.stack(unpooleds)
    grad_queries = grad_queries.reshape(groups * shard_rows, width).astype(jnp.bfloat16)
    return grad_queries, full, pooled, unpooled


def select_sum(values, chosen):
    onehot = chosen.astype(jnp.bfloat16)
    high = values.astype(jnp.bfloat16)
    low = (values - high.astype(jnp.float32)).astype(jnp.bfloat16)
    return product(onehot, high) + product(onehot, low)


def phase_weights(weight, rows):
    phase = (jnp.arange(rows, dtype=jnp.int32) % STRIDE)[:, None]
    total = jnp.zeros((rows, weight.shape[1]), jnp.float32)
    for r in range(STRIDE):
        total = total + jnp.where(phase == r, weight[r][None, :], 0.0)
    return total


def pool_grouped(source, weight):
    groups, rows, width = source.shape
    return jnp.sum(
        source.reshape(groups, rows // STRIDE, STRIDE, width) * weight[None, None], axis=2
    )


def unpool_grouped(pooled_grad, weight):
    groups, rows, width = pooled_grad.shape
    return (pooled_grad[:, :, None, :] * weight[None, None]).reshape(groups, rows * STRIDE, width)


def pool_grad_grouped(pooled_grad, source):
    groups, rows, width = source.shape
    blocks_view = source.astype(jnp.float32).reshape(groups, rows // STRIDE, STRIDE, width)
    return jnp.sum(pooled_grad[:, :, None, :] * blocks_view, axis=(0, 1))


def local(
    hidden_in,
    w_query,
    w_key,
    w_value,
    w_output,
    w_inner,
    w_outer,
    pool_weight,
    ln_gain,
    ln_bias,
    branch_blocks,
    grad_out,
):
    pool_rows_count = pool_weight.shape[0] * pool_weight.shape[1]
    small_local = jnp.concatenate(
        [pool_weight.reshape(pool_rows_count, -1), ln_gain, ln_bias], axis=0
    )
    hidden_all = lax.all_gather(hidden_in, "seq", axis=1, tiled=True)
    groups, shard_rows, width = hidden_in.shape
    seq_index = lax.axis_index("seq")
    offsets = STRIDE * branch_blocks
    starts, mask = block_geometry(seq_index, groups, shard_rows, offsets)
    (wq, wk, wv), small_full, (hidden_all, starts, mask) = gather_first(
        w_query, w_key, w_value, small_local, (hidden_all, starts, mask)
    )
    pool_full = small_full[:pool_rows_count].reshape(pool_weight.shape[0], pool_weight.shape[1], -1)
    gain_full = small_full[pool_rows_count : pool_rows_count + ln_gain.shape[0]]
    bias_full = small_full[pool_rows_count + ln_gain.shape[0] :]
    groups, shard_rows, width = hidden_in.shape

    group_len = hidden_all.shape[1]
    tokens = hidden_in.reshape(groups * shard_rows, width)
    all_tokens = hidden_all.reshape(groups * group_len, width)
    queries = product(tokens, wq).astype(jnp.bfloat16)
    key_g = product(all_tokens, wk).astype(jnp.bfloat16).reshape(groups, group_len, width)
    value_g = product(all_tokens, wv).astype(jnp.bfloat16).reshape(groups, group_len, width)
    pooled_keys = pool_grouped(key_g.astype(jnp.float32), pool_full[0]).astype(jnp.bfloat16)
    pooled_values = pool_grouped(value_g.astype(jnp.float32), pool_full[1]).astype(jnp.bfloat16)
    kv_all = jnp.concatenate([key_g, value_g], axis=2)
    pkv_all = jnp.concatenate([pooled_keys, pooled_values], axis=2)
    kv_local = lax.dynamic_slice_in_dim(kv_all, seq_index * shard_rows, shard_rows, 1)
    pkv_local = lax.dynamic_slice_in_dim(
        pkv_all, seq_index * (shard_rows // STRIDE), shard_rows // STRIDE, 1
    )
    wq, wk, wv, w_output, w_inner, w_outer = lax.optimization_barrier(
        (wq, wk, wv, w_output, w_inner, w_outer)
    )
    wo, wi, wu = gather_second(w_output, w_inner, w_outer)
    attended, att_saved = attention_fwd(
        queries.reshape(groups, shard_rows, width), kv_local, pkv_local, kv_all, pkv_all, starts, mask
    )
    mixed_rows = tokens.astype(jnp.float32) + product(attended, wo)
    normed_first = layer_norm(mixed_rows, gain_full[0], bias_full[0])
    first_low = normed_first.astype(jnp.bfloat16)
    inner_act = product(first_low, wi)
    active = jax.nn.gelu(inner_act, approximate=False).astype(jnp.bfloat16)
    second = normed_first + product(active, wu)
    norm_value, second_back = jax.vjp(layer_norm, second, gain_full[1], bias_full[1])
    output = norm_value.astype(jnp.bfloat16)

    cotangent = grad_out.reshape(groups * shard_rows, width).astype(jnp.float32)
    grad_second, gain_second, bias_second = second_back(cotangent)
    grad_ffn_out = grad_second.astype(jnp.bfloat16)
    grad_outer = product_left(active, grad_ffn_out)
    grad_active = product_right(grad_ffn_out, wu)
    gelu_value, gelu_back = jax.vjp(partial(jax.nn.gelu, approximate=False), inner_act)
    grad_inner_act = gelu_back(grad_active)[0].astype(jnp.bfloat16)
    grad_inner = product_left(first_low, grad_inner_act)
    grad_first = grad_second + product_right(grad_inner_act, wi)
    first_value, first_back = jax.vjp(layer_norm, mixed_rows, gain_full[0], bias_full[0])
    grad_mixed, gain_first, bias_first = first_back(grad_first)
    grad_branch = grad_mixed.astype(jnp.bfloat16)
    grad_output = product_left(attended, grad_branch)
    grad_attended = product_right(grad_branch, wo).astype(jnp.bfloat16)
    early, grad_attended = reduce_seq_stage((grad_output, grad_inner, grad_outer.T), grad_attended)
    early_reduced, early_widths = early

    grad_rows = grad_attended.reshape(groups, shard_rows, width)
    key_phase = phase_weights(pool_full[0], group_len)
    value_phase = phase_weights(pool_full[1], group_len)
    pieces_back = []
    for g in range(groups):
        saved_g = tuple(item[g : g + 1] for item in att_saved)
        starts_g = tuple(item[g : g + 1] for item in starts)
        grad_g = grad_rows[g].reshape(shard_rows, width)
        grad_queries_g, full_g, pooled_g, unpooled_g = attention_bwd(grad_g, saved_g, starts_g, seq_index)
        if g == 1:
            full_g, pooled_g, unpooled_g, earlier_back, early_reduced = lax.optimization_barrier(
                (full_g, pooled_g, unpooled_g, pieces_back[0][4], early_reduced)
            )
            pieces_back[0] = pieces_back[0][:4] + (earlier_back,)
        key_partial_g = (
            full_g[0, :, :width] + unpooled_g[0, :, :width] * key_phase
        ).astype(jnp.bfloat16)
        value_partial_g = (
            full_g[0, :, width:] + unpooled_g[0, :, width:] * value_phase
        ).astype(jnp.bfloat16)
        back_g = product_right(key_partial_g, wk) + product_right(value_partial_g, wv)
        back_g = back_g.reshape(1, group_len, width).astype(jnp.bfloat16)
        back_own_g = lax.psum_scatter(back_g, "seq", scatter_dimension=1, tiled=True)
        pieces_back.append((grad_queries_g, pooled_g, key_partial_g, value_partial_g, back_own_g))
    grad_queries = jnp.concatenate([piece[0] for piece in pieces_back], axis=0)
    grad_pooled = jnp.concatenate([piece[1] for piece in pieces_back], axis=0)
    key_partial = jnp.concatenate([piece[2] for piece in pieces_back], axis=0)
    value_partial = jnp.concatenate([piece[3] for piece in pieces_back], axis=0)
    last_back = pieces_back[-1][4]
    early_dp = reduce_dp_stage(((early_reduced, early_widths),))
    grad_pooling = jnp.stack(
        [
            pool_grad_grouped(grad_pooled[..., :width], key_g),
            pool_grad_grouped(grad_pooled[..., width:], value_g),
        ]
    )
    grad_query_w = product_left(tokens, grad_queries)
    grad_key_w = product_left(all_tokens, key_partial)
    grad_value_w = product_left(all_tokens, value_partial)
    late_stacked, late_widths = stack_for_seq((grad_query_w, grad_key_w, grad_value_w))
    late_stacked, early_dp = lax.optimization_barrier((late_stacked, early_dp))
    seq_size = lax.psum(1, "seq")
    dp_size = lax.psum(1, "dp")
    rows_each = late_stacked.shape[0] // seq_size
    late_blocks = late_stacked.reshape(seq_size, rows_each, dp_size, late_stacked.shape[2])
    late_blocks = jnp.transpose(late_blocks, (2, 0, 1, 3)).reshape(-1, late_stacked.shape[2])
    late_reduced = lax.psum_scatter(late_blocks, ("dp", "seq"), scatter_dimension=0, tiled=True)
    late_reduced = late_reduced.astype(jnp.float32)
    late_dp, at = [], 0
    for width_piece in late_widths:
        late_dp.append(late_reduced[:, at : at + width_piece])
        at += width_piece
    back_own = jnp.concatenate([piece[4] for piece in pieces_back], axis=0)
    grad_tokens = (
        grad_mixed
        + product_right(grad_queries, wq)
        + back_own.reshape(groups * shard_rows, width).astype(jnp.float32)
    )
    accum = (late_dp[0], late_dp[1], late_dp[2], early_dp[0], early_dp[1], early_dp[2].T)
    small_sums = (
        lax.psum_scatter(grad_pooling, ("dp", "seq"), scatter_dimension=2, tiled=True),
        lax.psum_scatter(
            jnp.stack([gain_first, gain_second]), ("dp", "seq"), scatter_dimension=1, tiled=True
        ),
        lax.psum_scatter(
            jnp.stack([bias_first, bias_second]), ("dp", "seq"), scatter_dimension=1, tiled=True
        ),
    )
    return (
        output.reshape(groups, shard_rows, width),
        grad_tokens.astype(jnp.bfloat16).reshape(groups, shard_rows, width),
        accum[0],
        accum[1],
        accum[2],
        accum[3],
        accum[4],
        accum[5],
        small_sums[0],
        small_sums[1],
        small_sums[2],
    )


def solution(mesh):
    in_specs = (
        P("dp", "seq", None),
        P("seq", "dp"),
        P("seq", "dp"),
        P("seq", "dp"),
        P("seq", "dp"),
        P("seq", "dp"),
        P("dp", "seq"),
        P(None, None, ("dp", "seq")),
        P(None, ("dp", "seq")),
        P(None, ("dp", "seq")),
        P("dp", None),
        P("dp", "seq", None),
    )
    out_specs = (
        P("dp", "seq", None),
        P("dp", "seq", None),
        P("seq", "dp"),
        P("seq", "dp"),
        P("seq", "dp"),
        P("seq", "dp"),
        P("seq", "dp"),
        P("dp", "seq"),
        P(None, None, ("dp", "seq")),
        P(None, ("dp", "seq")),
        P(None, ("dp", "seq")),
    )
    return jax.shard_map(local, mesh=mesh, in_specs=in_specs, out_specs=out_specs, check_vma=False)
```

```python
from functools import partial

import jax
import jax.numpy as jnp
from jax import lax
from jax.sharding import PartitionSpec as P

HEADS = 12
HEAD_DIM = 64
PROMPT = 1024
CONT = 8
CLEN = 128
WINDOW = 128
POOL_SPAN = 512
STRIDE = 4


eps_norm = 1e-05


def token_layout(positions_in, offsets):
    in_prompt = positions_in < PROMPT
    segment = jnp.where(in_prompt, -1, (positions_in - PROMPT) // CLEN)
    within = positions_in - PROMPT - segment * CLEN
    choose = (segment[:, None] == jnp.arange(CONT, dtype=jnp.int32)[None, :]).astype(jnp.int32)
    cont_start = jnp.sum(choose * offsets[None, :], axis=1)
    position = jnp.where(in_prompt, positions_in, cont_start + within)
    prompt_limit = jnp.where(in_prompt, PROMPT, cont_start)
    return (segment, position, prompt_limit)


def visible_keys(query_rows, key_index, offsets, reach):
    query_seg, query_pos, query_limit = token_layout(query_rows, offsets)
    key_seg, key_pos, key_limit = token_layout(key_index, offsets)
    prompt_key = (key_seg[None, :] < 0) & (key_pos[None, :] < query_limit[:, None])
    own_key = (key_seg[None, :] == query_seg[:, None]) & (query_seg[:, None] >= 0)
    distance = key_pos[None, :] - query_pos[:, None]
    return (prompt_key | own_key) & (distance >= -(reach // 2)) & (distance < reach // 2)


def key_mask(query_rows, offsets):
    group_len = PROMPT + CONT * CLEN
    full_keys = jnp.arange(group_len, dtype=jnp.int32)
    pooled_keys = jnp.arange(group_len // STRIDE, dtype=jnp.int32) * STRIDE
    return jnp.concatenate(
        [
            visible_keys(query_rows, full_keys, offsets, WINDOW),
            visible_keys(query_rows, pooled_keys, offsets, POOL_SPAN),
        ],
        axis=1,
    )


def pool_rows(source, weight):
    return jnp.sum(
        source.reshape(source.shape[0] // STRIDE, STRIDE, source.shape[1]) * weight[None, :, :],
        axis=1,
    )


def unpool(pooled_grad, weight):
    return (pooled_grad[:, None, :] * weight[None, :, :]).reshape(-1, pooled_grad.shape[1])


def pool_grad(pooled_grad, source):
    blocks_view = source.astype(jnp.float32).reshape(-1, STRIDE, source.shape[1])
    return jnp.sum(pooled_grad[:, None, :] * blocks_view, axis=0)


def layer_norm(source, gain, bias):
    centre = jnp.mean(source, axis=-1, keepdims=True)
    centred = source - centre
    spread = jnp.mean(centred * centred, axis=-1, keepdims=True)
    return centred * lax.rsqrt(spread + eps_norm) * gain + bias


def product(left, right):
    return jnp.dot(left, right, preferred_element_type=jnp.float32)


def product_left(left, right):
    return lax.dot_general(
        left, right, (((0,), (0,)), ((), ())), preferred_element_type=jnp.float32
    )


def product_right(left, right):
    return lax.dot_general(
        left, right, (((1,), (1,)), ((), ())), preferred_element_type=jnp.float32
    )


def add_pair(left_term, right_term):
    return left_term + right_term


def gather_grouped(shards, tie=None):
    local_block = jnp.concatenate(shards, axis=1)
    across = lax.all_gather(local_block, "dp", axis=1, tiled=False)
    across, tie = lax.optimization_barrier((across, tie))
    return lax.all_gather(across, "seq", axis=0, tiled=True), tie


def split_grouped(gathered, widths):
    pieces, at = [], 0
    for width in widths:
        piece = gathered[:, :, at : at + width]
        pieces.append(piece.reshape(piece.shape[0], -1))
        at += width
    return pieces


def code_exact(values, rows):
    parts, rest = [], values
    for _ in range(3):
        part = lax.optimization_barrier(rest.astype(jnp.bfloat16))
        parts.append(part)
        rest = rest - part.astype(jnp.float32)
    flat = jnp.concatenate([part.reshape(-1) for part in parts])
    columns = -(-flat.shape[0] // rows)
    flat = jnp.pad(flat, (0, rows * columns - flat.shape[0]))
    return flat.reshape(rows, columns)


def decode_exact(gathered, count, shape):
    seq_size = lax.psum(1, "seq")
    rows = gathered.shape[0] // seq_size
    blocks = gathered.reshape(seq_size, rows, gathered.shape[1], gathered.shape[2])
    blocks = jnp.transpose(blocks, (2, 0, 1, 3)).reshape(-1, rows * gathered.shape[2])
    parts = blocks[:, : 3 * count].reshape(blocks.shape[0], 3, shape[0], shape[1])
    parts = parts.astype(jnp.float32)
    joined = (parts[:, 0] + parts[:, 1]) + parts[:, 2]
    return jnp.transpose(joined, (1, 0, 2)).reshape(shape[0], -1)


def gather_first(w_query, w_key, w_value, small_local, tie):
    coded = code_exact(small_local, w_query.shape[0])
    first, tie = gather_grouped((w_query, w_key, w_value, coded), tie)
    widths = (w_query.shape[1], w_key.shape[1], w_value.shape[1])
    at = sum(widths)
    small_full = decode_exact(first[:, :, at:], small_local.size, small_local.shape)
    return split_grouped(first[:, :, :at], widths), small_full, tie


def gather_second(w_output, w_inner, w_outer):
    second, _ = gather_grouped((w_output, w_inner, w_outer.T))
    wo, wi, wu_t = split_grouped(second, (w_output.shape[1], w_inner.shape[1], w_outer.shape[0]))
    return (wo, wi, wu_t.T)


def reduce_seq_stage(grads, tie=None):
    dp_size = lax.psum(1, "dp")
    chunks = [grad.reshape(grad.shape[0], dp_size, grad.shape[1] // dp_size) for grad in grads]
    stacked = jnp.concatenate(chunks, axis=2).astype(jnp.bfloat16)
    stacked, tie = lax.optimization_barrier((stacked, tie))
    reduced = lax.psum_scatter(stacked, "seq", scatter_dimension=0, tiled=True)
    return (reduced, [c.shape[2] for c in chunks]), tie


def stack_for_seq(grads):
    dp_size = lax.psum(1, "dp")
    chunks = [grad.reshape(grad.shape[0], dp_size, grad.shape[1] // dp_size) for grad in grads]
    return jnp.concatenate(chunks, axis=2).astype(jnp.bfloat16), [c.shape[2] for c in chunks]


def reduce_dp_stage(stages):
    joined = jnp.concatenate([stage for stage, _ in stages], axis=2)
    over_dp = lax.psum_scatter(joined, "dp", scatter_dimension=1, tiled=True)[:, 0].astype(jnp.float32)
    pieces, at = [], 0
    for _, widths in stages:
        for width in widths:
            pieces.append(over_dp[:, at : at + width])
            at += width
    return pieces


HALF_FULL = WINDOW // 2
HALF_POOL = POOL_SPAN // 2 // STRIDE
BLOCK_POOL = CLEN // STRIDE


def layout_of(index, offsets):
    in_prompt = index < PROMPT
    segment = jnp.where(in_prompt, -1, (index - PROMPT) // CLEN)
    within = index - PROMPT - segment * CLEN
    choose = segment[..., None] == jnp.arange(CONT, dtype=jnp.int32)
    spread = offsets.reshape(offsets.shape[:1] + (1,) * (index.ndim - 1) + offsets.shape[1:])
    cont_start = jnp.sum(jnp.where(choose, spread, 0), axis=-1)
    position = jnp.where(in_prompt, index, cont_start + within)
    limit = jnp.where(in_prompt, PROMPT, cont_start)
    return segment, position, limit


def window_rows(source, starts, length):
    groups, blocks = starts.shape
    return jnp.stack(
        [
            jnp.stack(
                [lax.dynamic_slice_in_dim(source[g], starts[g, b], length, 0) for b in range(blocks)]
            )
            for g in range(groups)
        ]
    )


def window_add(target, updates, starts):
    groups, blocks = starts.shape
    length = updates.shape[2]
    rows = []
    for g in range(groups):
        row = target[g]
        for b in range(blocks):
            start = starts[g, b]
            current = lax.dynamic_slice_in_dim(row, start, length, 0)
            row = lax.dynamic_update_slice_in_dim(row, current + updates[g, b], start, 0)
        rows.append(row)
    return jnp.stack(rows)


def block_geometry(seq_index, groups, shard_rows, offsets):
    group_len = PROMPT + CONT * CLEN
    pooled_len = group_len // STRIDE
    blocks = shard_rows // CLEN
    block_start = (seq_index * blocks + jnp.arange(blocks, dtype=jnp.int32)) * CLEN
    prompt_block = block_start < PROMPT
    cont_index = jnp.clip((block_start - PROMPT) // CLEN, 0, CONT - 1)
    anchor = jnp.where(prompt_block[None, :], block_start[None, :], offsets[:, cont_index])
    pooled_start = block_start // STRIDE
    intended = (
        anchor - HALF_FULL,
        jnp.broadcast_to(block_start + CLEN, anchor.shape),
        anchor // STRIDE - HALF_POOL,
        jnp.broadcast_to(pooled_start + BLOCK_POOL, anchor.shape),
    )
    limits = (group_len, group_len, pooled_len, pooled_len)
    lengths = (HALF_FULL, HALF_FULL, HALF_POOL, HALF_POOL)
    clamped = tuple(
        jnp.clip(start, 0, limit - length) for start, limit, length in zip(intended, limits, lengths)
    )
    ramp = lambda n: jnp.arange(n, dtype=jnp.int32)

    def span(window):
        actual = clamped[window][:, :, None] + ramp(lengths[window])
        offset = actual - intended[window][:, :, None]
        return actual, (offset >= 0) & (offset < lengths[window])

    before_full, before_full_ok = span(0)
    after_full, after_full_ok = span(1)
    before_pool, before_pool_ok = span(2)
    after_pool, after_pool_ok = span(3)
    after_ok = prompt_block[None, :, None]
    own_full = jnp.broadcast_to(block_start[None, :, None] + ramp(CLEN), anchor.shape + (CLEN,))
    own_pool = jnp.broadcast_to(
        pooled_start[None, :, None] + ramp(BLOCK_POOL), anchor.shape + (BLOCK_POOL,)
    )
    full_index = jnp.concatenate([before_full, own_full, after_full], axis=2)
    pooled_index = jnp.concatenate([before_pool, own_pool, after_pool], axis=2)
    full_valid = jnp.concatenate(
        [before_full_ok, jnp.ones(own_full.shape, bool), after_ok & after_full_ok], axis=2
    )
    pooled_valid = jnp.concatenate(
        [before_pool_ok, jnp.ones(own_pool.shape, bool), after_ok & after_pool_ok], axis=2
    )
    query_index = block_start[None, :, None] + ramp(CLEN)
    query_index = jnp.broadcast_to(query_index, anchor.shape + (CLEN,))
    q_seg, q_pos, q_lim = layout_of(query_index, offsets)

    def visible(key_token, valid, reach):
        k_seg, k_pos, _ = layout_of(key_token, offsets)
        k_seg, k_pos, valid = k_seg[:, :, None, :], k_pos[:, :, None, :], valid[:, :, None, :]
        prompt_key = (k_seg < 0) & (k_pos < q_lim[..., None])
        own_key = (k_seg == q_seg[..., None]) & (q_seg[..., None] >= 0)
        distance = k_pos - q_pos[..., None]
        return valid & (prompt_key | own_key) & (distance >= -(reach // 2)) & (distance < reach // 2)

    mask = jnp.concatenate(
        [
            visible(full_index, full_valid, WINDOW),
            visible(pooled_index * STRIDE, pooled_valid, POOL_SPAN),
        ],
        axis=3,
    )
    return clamped, mask


def attention_fwd(queries, kv_local, pkv_local, kv_all, pkv_all, starts, mask):
    groups, shard_rows, width = queries.shape
    blocks = shard_rows // CLEN
    score_scale = 1.0 / HEAD_DIM**0.5
    keys_cat = jnp.concatenate(
        [
            window_rows(kv_all, starts[0], HALF_FULL),
            kv_local.reshape(groups, blocks, CLEN, 2 * width),
            window_rows(kv_all, starts[1], HALF_FULL),
            window_rows(pkv_all, starts[2], HALF_POOL),
            pkv_local.reshape(groups, blocks, BLOCK_POOL, 2 * width),
            window_rows(pkv_all, starts[3], HALF_POOL),
        ],
        axis=2,
    )
    span = keys_cat.shape[2]
    head_keys = keys_cat[..., :width].reshape(groups, blocks, span, HEADS, HEAD_DIM)
    head_values = keys_cat[..., width:].reshape(groups, blocks, span, HEADS, HEAD_DIM)
    head_query = queries.reshape(groups, blocks, CLEN, HEADS, HEAD_DIM)
    scores = jnp.einsum(
        "gbqhd,gbkhd->gbhqk", head_query, head_keys, preferred_element_type=jnp.float32
    )
    scores = jnp.where(mask[:, :, None], scores * score_scale, -1000000000.0)
    row_top = jnp.max(scores, axis=-1, keepdims=True)
    exponent = jnp.exp(scores - row_top)
    row_total = jnp.sum(exponent, axis=-1, keepdims=True)
    probs = exponent / row_total
    attended = jnp.einsum(
        "gbhqk,gbkhd->gbqhd",
        probs.astype(jnp.bfloat16),
        head_values,
        preferred_element_type=jnp.float32,
    )
    attended = attended.reshape(groups * shard_rows, width).astype(jnp.bfloat16)
    return attended, (head_query, head_keys, head_values, probs)


def attention_bwd(grad_attended, saved, starts, seq_index):
    head_query, head_keys, head_values, probs = saved
    groups, blocks = head_query.shape[:2]
    width = HEADS * HEAD_DIM
    score_scale = 1.0 / HEAD_DIM**0.5
    head_grad = grad_attended.reshape(groups, blocks, CLEN, HEADS, HEAD_DIM)
    grad_probs = jnp.einsum(
        "gbqhd,gbkhd->gbhqk", head_grad, head_values, preferred_element_type=jnp.float32
    )
    centre = jnp.sum(probs * grad_probs, axis=-1, keepdims=True)
    grad_scores = (probs * (grad_probs - centre)).astype(jnp.bfloat16)
    grad_queries = jnp.einsum(
        "gbhqk,gbkhd->gbqhd", grad_scores, head_keys, preferred_element_type=jnp.float32
    ) * score_scale
    grad_keys = jnp.einsum(
        "gbhqk,gbqhd->gbkhd", grad_scores, head_query, preferred_element_type=jnp.float32
    ) * score_scale
    grad_values = jnp.einsum(
        "gbhqk,gbqhd->gbkhd",
        probs.astype(jnp.bfloat16),
        head_grad,
        preferred_element_type=jnp.float32,
    )
    span = grad_keys.shape[2]
    grad_kv = jnp.concatenate(
        [grad_keys.reshape(groups, blocks, span, width), grad_values.reshape(groups, blocks, span, width)],
        axis=3,
    )
    shard_rows = blocks * CLEN
    group_len = PROMPT + CONT * CLEN
    pooled_len = group_len // STRIDE
    cut = (0, HALF_FULL, HALF_FULL + CLEN, 2 * HALF_FULL + CLEN)
    pcut = tuple(cut[-1] + c for c in (0, HALF_POOL, HALF_POOL + BLOCK_POOL, 2 * HALF_POOL + BLOCK_POOL))
    ramp = lambda n: jnp.arange(n, dtype=jnp.int32)
    own_full = grad_kv[:, :, cut[1] : cut[2]].reshape(groups, shard_rows, 2 * width)
    full = jnp.zeros((groups, group_len, 2 * width), jnp.float32)
    full = lax.dynamic_update_slice_in_dim(full, own_full, seq_index * shard_rows, 1)
    side_values = jnp.concatenate(
        [grad_kv[:, :, cut[0] : cut[1]], grad_kv[:, :, cut[2] : cut[3]]], axis=2
    ).reshape(groups, -1, 2 * width)
    side_rows = jnp.concatenate(
        [starts[0][:, :, None] + ramp(HALF_FULL), starts[1][:, :, None] + ramp(HALF_FULL)], axis=2
    ).reshape(groups, -1)
    own_pool_rows = (seq_index * (shard_rows // STRIDE) + ramp(blocks)[:, None] * BLOCK_POOL + ramp(BLOCK_POOL))
    pool_values = grad_kv[:, :, pcut[0] : pcut[3]].reshape(groups, -1, 2 * width)
    pool_rows_index = jnp.concatenate(
        [
            starts[2][:, :, None] + ramp(HALF_POOL),
            jnp.broadcast_to(own_pool_rows[None], (groups, blocks, BLOCK_POOL)),
            starts[3][:, :, None] + ramp(HALF_POOL),
        ],
        axis=2,
    ).reshape(groups, -1)
    fulls, pooleds, unpooleds = [], [], []
    for g in range(groups):
        fulls.append(full[g] + select_sum(side_values[g], side_rows[g] == ramp(group_len)[:, None]))
        pooleds.append(select_sum(pool_values[g], pool_rows_index[g] == ramp(pooled_len)[:, None]))
        unpooleds.append(
            select_sum(pool_values[g], pool_rows_index[g] == (ramp(group_len) // STRIDE)[:, None])
        )
    full = jnp.stack(fulls)
    pooled = jnp.stack(pooleds)
    unpooled = jnp.stack(unpooleds)
    grad_queries = grad_queries.reshape(groups * shard_rows, width).astype(jnp.bfloat16)
    return grad_queries, full, pooled, unpooled


def select_sum(values, chosen):
    onehot = chosen.astype(jnp.bfloat16)
    high = values.astype(jnp.bfloat16)
    low = (values - high.astype(jnp.float32)).astype(jnp.bfloat16)
    return product(
        jnp.concatenate([onehot, onehot], axis=1), jnp.concatenate([high, low], axis=0)
    )


def phase_weights(weight, rows):
    phase = (jnp.arange(rows, dtype=jnp.int32) % STRIDE)[:, None]
    total = jnp.zeros((rows, weight.shape[1]), jnp.float32)
    for r in range(STRIDE):
        total = total + jnp.where(phase == r, weight[r][None, :], 0.0)
    return total


def pool_grouped(source, weight):
    groups, rows, width = source.shape
    return jnp.sum(
        source.reshape(groups, rows // STRIDE, STRIDE, width) * weight[None, None], axis=2
    )


def unpool_grouped(pooled_grad, weight):
    groups, rows, width = pooled_grad.shape
    return (pooled_grad[:, :, None, :] * weight[None, None]).reshape(groups, rows * STRIDE, width)


def pool_grad_grouped(pooled_grad, source):
    groups, rows, width = source.shape
    blocks_view = source.astype(jnp.float32).reshape(groups, rows // STRIDE, STRIDE, width)
    return jnp.sum(pooled_grad[:, :, None, :] * blocks_view, axis=(0, 1))


def local(
    hidden_in,
    w_query,
    w_key,
    w_value,
    w_output,
    w_inner,
    w_outer,
    pool_weight,
    ln_gain,
    ln_bias,
    branch_blocks,
    grad_out,
):
    pool_rows_count = pool_weight.shape[0] * pool_weight.shape[1]
    small_local = jnp.concatenate(
        [pool_weight.reshape(pool_rows_count, -1), ln_gain, ln_bias], axis=0
    )
    hidden_all = lax.all_gather(hidden_in, "seq", axis=1, tiled=True)
    groups, shard_rows, width = hidden_in.shape
    seq_index = lax.axis_index("seq")
    offsets = STRIDE * branch_blocks
    starts, mask = block_geometry(seq_index, groups, shard_rows, offsets)
    (wq, wk, wv), small_full, (hidden_all, starts, mask) = gather_first(
        w_query, w_key, w_value, small_local, (hidden_all, starts, mask)
    )
    pool_full = small_full[:pool_rows_count].reshape(pool_weight.shape[0], pool_weight.shape[1], -1)
    gain_full = small_full[pool_rows_count : pool_rows_count + ln_gain.shape[0]]
    bias_full = small_full[pool_rows_count + ln_gain.shape[0] :]
    groups, shard_rows, width = hidden_in.shape

    group_len = hidden_all.shape[1]
    tokens = hidden_in.reshape(groups * shard_rows, width)
    all_tokens = hidden_all.reshape(groups * group_len, width)
    queries = product(tokens, wq).astype(jnp.bfloat16)
    key_g = product(all_tokens, wk).astype(jnp.bfloat16).reshape(groups, group_len, width)
    value_g = product(all_tokens, wv).astype(jnp.bfloat16).reshape(groups, group_len, width)
    pooled_keys = pool_grouped(key_g.astype(jnp.float32), pool_full[0]).astype(jnp.bfloat16)
    pooled_values = pool_grouped(value_g.astype(jnp.float32), pool_full[1]).astype(jnp.bfloat16)
    kv_all = jnp.concatenate([key_g, value_g], axis=2)
    pkv_all = jnp.concatenate([pooled_keys, pooled_values], axis=2)
    kv_local = lax.dynamic_slice_in_dim(kv_all, seq_index * shard_rows, shard_rows, 1)
    pkv_local = lax.dynamic_slice_in_dim(
        pkv_all, seq_index * (shard_rows // STRIDE), shard_rows // STRIDE, 1
    )
    wq, wk, wv, w_output, w_inner, w_outer = lax.optimization_barrier(
        (wq, wk, wv, w_output, w_inner, w_outer)
    )
    wo, wi, wu = gather_second(w_output, w_inner, w_outer)
    attended, att_saved = attention_fwd(
        queries.reshape(groups, shard_rows, width), kv_local, pkv_local, kv_all, pkv_all, starts, mask
    )
    mixed_rows = tokens.astype(jnp.float32) + product(attended, wo)
    normed_first = layer_norm(mixed_rows, gain_full[0], bias_full[0])
    first_low = normed_first.astype(jnp.bfloat16)
    inner_act = product(first_low, wi)
    active = jax.nn.gelu(inner_act, approximate=False).astype(jnp.bfloat16)
    second = normed_first + product(active, wu)
    norm_value, second_back = jax.vjp(layer_norm, second, gain_full[1], bias_full[1])
    output = norm_value.astype(jnp.bfloat16)

    cotangent = grad_out.reshape(groups * shard_rows, width).astype(jnp.float32)
    grad_second, gain_second, bias_second = second_back(cotangent)
    grad_ffn_out = grad_second.astype(jnp.bfloat16)
    grad_outer = product_left(active, grad_ffn_out)
    grad_active = product_right(grad_ffn_out, wu)
    gelu_value, gelu_back = jax.vjp(partial(jax.nn.gelu, approximate=False), inner_act)
    grad_inner_act = gelu_back(grad_active)[0].astype(jnp.bfloat16)
    grad_inner = product_left(first_low, grad_inner_act)
    grad_first = grad_second + product_right(grad_inner_act, wi)
    first_value, first_back = jax.vjp(layer_norm, mixed_rows, gain_full[0], bias_full[0])
    grad_mixed, gain_first, bias_first = first_back(grad_first)
    grad_branch = grad_mixed.astype(jnp.bfloat16)
    grad_output = product_left(attended, grad_branch)
    grad_attended = product_right(grad_branch, wo).astype(jnp.bfloat16)
    early, grad_attended = reduce_seq_stage((grad_output, grad_inner, grad_outer.T), grad_attended)
    early_reduced, early_widths = early

    grad_rows = grad_attended.reshape(groups, shard_rows, width)
    key_phase = phase_weights(pool_full[0], group_len)
    value_phase = phase_weights(pool_full[1], group_len)
    pieces_back = []
    for g in range(groups):
        saved_g = tuple(item[g : g + 1] for item in att_saved)
        starts_g = tuple(item[g : g + 1] for item in starts)
        grad_g = grad_rows[g].reshape(shard_rows, width)
        grad_queries_g, full_g, pooled_g, unpooled_g = attention_bwd(grad_g, saved_g, starts_g, seq_index)
        if g == 1:
            full_g, pooled_g, unpooled_g, earlier_back, early_reduced = lax.optimization_barrier(
                (full_g, pooled_g, unpooled_g, pieces_back[0][4], early_reduced)
            )
            pieces_back[0] = pieces_back[0][:4] + (earlier_back,)
        key_partial_g = (
            full_g[0, :, :width] + unpooled_g[0, :, :width] * key_phase
        ).astype(jnp.bfloat16)
        value_partial_g = (
            full_g[0, :, width:] + unpooled_g[0, :, width:] * value_phase
        ).astype(jnp.bfloat16)
        back_g = product_right(key_partial_g, wk) + product_right(value_partial_g, wv)
        back_g = back_g.reshape(1, group_len, width).astype(jnp.bfloat16)
        back_own_g = lax.psum_scatter(back_g, "seq", scatter_dimension=1, tiled=True)
        pieces_back.append((grad_queries_g, pooled_g, key_partial_g, value_partial_g, back_own_g))
    grad_queries = jnp.concatenate([piece[0] for piece in pieces_back], axis=0)
    grad_pooled = jnp.concatenate([piece[1] for piece in pieces_back], axis=0)
    key_partial = jnp.concatenate([piece[2] for piece in pieces_back], axis=0)
    value_partial = jnp.concatenate([piece[3] for piece in pieces_back], axis=0)
    last_back = pieces_back[-1][4]
    early_dp = reduce_dp_stage(((early_reduced, early_widths),))
    grad_pooling = jnp.stack(
        [
            pool_grad_grouped(grad_pooled[..., :width], key_g),
            pool_grad_grouped(grad_pooled[..., width:], value_g),
        ]
    )
    grad_query_w = product_left(tokens, grad_queries)
    grad_key_w = product_left(all_tokens, key_partial)
    grad_value_w = product_left(all_tokens, value_partial)
    late_stacked, late_widths = stack_for_seq((grad_query_w, grad_key_w, grad_value_w))
    late_stacked, early_dp = lax.optimization_barrier((late_stacked, early_dp))
    seq_size = lax.psum(1, "seq")
    dp_size = lax.psum(1, "dp")
    rows_each = late_stacked.shape[0] // seq_size
    late_blocks = late_stacked.reshape(seq_size, rows_each, dp_size, late_stacked.shape[2])
    late_blocks = jnp.transpose(late_blocks, (2, 0, 1, 3)).reshape(-1, late_stacked.shape[2])
    late_reduced = lax.psum_scatter(late_blocks, ("dp", "seq"), scatter_dimension=0, tiled=True)
    late_reduced = late_reduced.astype(jnp.float32)
    late_dp, at = [], 0
    for width_piece in late_widths:
        late_dp.append(late_reduced[:, at : at + width_piece])
        at += width_piece
    back_own = jnp.concatenate([piece[4] for piece in pieces_back], axis=0)
    grad_tokens = (
        grad_mixed
        + product_right(grad_queries, wq)
        + back_own.reshape(groups * shard_rows, width).astype(jnp.float32)
    )
    accum = (late_dp[0], late_dp[1], late_dp[2], early_dp[0], early_dp[1], early_dp[2].T)
    small_sums = (
        lax.psum_scatter(grad_pooling, ("dp", "seq"), scatter_dimension=2, tiled=True),
        lax.psum_scatter(
            jnp.stack([gain_first, gain_second]), ("dp", "seq"), scatter_dimension=1, tiled=True
        ),
        lax.psum_scatter(
            jnp.stack([bias_first, bias_second]), ("dp", "seq"), scatter_dimension=1, tiled=True
        ),
    )
    return (
        output.reshape(groups, shard_rows, width),
        grad_tokens.astype(jnp.bfloat16).reshape(groups, shard_rows, width),
        accum[0],
        accum[1],
        accum[2],
        accum[3],
        accum[4],
        accum[5],
        small_sums[0],
        small_sums[1],
        small_sums[2],
    )


def solution(mesh):
    in_specs = (
        P("dp", "seq", None),
        P("seq", "dp"),
        P("seq", "dp"),
        P("seq", "dp"),
        P("seq", "dp"),
        P("seq", "dp"),
        P("dp", "seq"),
        P(None, None, ("dp", "seq")),
        P(None, ("dp", "seq")),
        P(None, ("dp", "seq")),
        P("dp", None),
        P("dp", "seq", None),
    )
    out_specs = (
        P("dp", "seq", None),
        P("dp", "seq", None),
        P("seq", "dp"),
        P("seq", "dp"),
        P("seq", "dp"),
        P("seq", "dp"),
        P("seq", "dp"),
        P("dp", "seq"),
        P(None, None, ("dp", "seq")),
        P(None, ("dp", "seq")),
        P(None, ("dp", "seq")),
    )
    return jax.shard_map(local, mesh=mesh, in_specs=in_specs, out_specs=out_specs, check_vma=False)
```

```python
from functools import partial

import jax
import jax.numpy as jnp
from jax import lax
from jax.sharding import PartitionSpec as P

HEADS = 12
HEAD_DIM = 64
PROMPT = 1024
CONT = 8
CLEN = 128
WINDOW = 128
POOL_SPAN = 512
STRIDE = 4


eps_norm = 1e-05


def token_layout(positions_in, offsets):
    in_prompt = positions_in < PROMPT
    segment = jnp.where(in_prompt, -1, (positions_in - PROMPT) // CLEN)
    within = positions_in - PROMPT - segment * CLEN
    choose = (segment[:, None] == jnp.arange(CONT, dtype=jnp.int32)[None, :]).astype(jnp.int32)
    cont_start = jnp.sum(choose * offsets[None, :], axis=1)
    position = jnp.where(in_prompt, positions_in, cont_start + within)
    prompt_limit = jnp.where(in_prompt, PROMPT, cont_start)
    return (segment, position, prompt_limit)


def visible_keys(query_rows, key_index, offsets, reach):
    query_seg, query_pos, query_limit = token_layout(query_rows, offsets)
    key_seg, key_pos, key_limit = token_layout(key_index, offsets)
    prompt_key = (key_seg[None, :] < 0) & (key_pos[None, :] < query_limit[:, None])
    own_key = (key_seg[None, :] == query_seg[:, None]) & (query_seg[:, None] >= 0)
    distance = key_pos[None, :] - query_pos[:, None]
    return (prompt_key | own_key) & (distance >= -(reach // 2)) & (distance < reach // 2)


def key_mask(query_rows, offsets):
    group_len = PROMPT + CONT * CLEN
    full_keys = jnp.arange(group_len, dtype=jnp.int32)
    pooled_keys = jnp.arange(group_len // STRIDE, dtype=jnp.int32) * STRIDE
    return jnp.concatenate(
        [
            visible_keys(query_rows, full_keys, offsets, WINDOW),
            visible_keys(query_rows, pooled_keys, offsets, POOL_SPAN),
        ],
        axis=1,
    )


def pool_rows(source, weight):
    return jnp.sum(
        source.reshape(source.shape[0] // STRIDE, STRIDE, source.shape[1]) * weight[None, :, :],
        axis=1,
    )


def unpool(pooled_grad, weight):
    return (pooled_grad[:, None, :] * weight[None, :, :]).reshape(-1, pooled_grad.shape[1])


def pool_grad(pooled_grad, source):
    blocks_view = source.astype(jnp.float32).reshape(-1, STRIDE, source.shape[1])
    return jnp.sum(pooled_grad[:, None, :] * blocks_view, axis=0)


def layer_norm(source, gain, bias):
    centre = jnp.mean(source, axis=-1, keepdims=True)
    centred = source - centre
    spread = jnp.mean(centred * centred, axis=-1, keepdims=True)
    return centred * lax.rsqrt(spread + eps_norm) * gain + bias


def product(left, right):
    return jnp.dot(left, right, preferred_element_type=jnp.float32)


def product_left(left, right):
    return lax.dot_general(
        left, right, (((0,), (0,)), ((), ())), preferred_element_type=jnp.float32
    )


def product_right(left, right):
    return lax.dot_general(
        left, right, (((1,), (1,)), ((), ())), preferred_element_type=jnp.float32
    )


def add_pair(left_term, right_term):
    return left_term + right_term


def gather_grouped(shards, tie=None):
    local_block = jnp.concatenate(shards, axis=1)
    across = lax.all_gather(local_block, "dp", axis=1, tiled=False)
    across, tie = lax.optimization_barrier((across, tie))
    return lax.all_gather(across, "seq", axis=0, tiled=True), tie


def split_grouped(gathered, widths):
    pieces, at = [], 0
    for width in widths:
        piece = gathered[:, :, at : at + width]
        pieces.append(piece.reshape(piece.shape[0], -1))
        at += width
    return pieces


def code_exact(values, rows):
    parts, rest = [], values
    for _ in range(3):
        part = lax.optimization_barrier(rest.astype(jnp.bfloat16))
        parts.append(part)
        rest = rest - part.astype(jnp.float32)
    flat = jnp.concatenate([part.reshape(-1) for part in parts])
    columns = -(-flat.shape[0] // rows)
    flat = jnp.pad(flat, (0, rows * columns - flat.shape[0]))
    return flat.reshape(rows, columns)


def decode_exact(gathered, count, shape):
    seq_size = lax.psum(1, "seq")
    rows = gathered.shape[0] // seq_size
    blocks = gathered.reshape(seq_size, rows, gathered.shape[1], gathered.shape[2])
    blocks = jnp.transpose(blocks, (2, 0, 1, 3)).reshape(-1, rows * gathered.shape[2])
    parts = blocks[:, : 3 * count].reshape(blocks.shape[0], 3, shape[0], shape[1])
    parts = parts.astype(jnp.float32)
    joined = (parts[:, 0] + parts[:, 1]) + parts[:, 2]
    return jnp.transpose(joined, (1, 0, 2)).reshape(shape[0], -1)


def gather_first(w_query, w_key, w_value, small_local, tie):
    coded = code_exact(small_local, w_query.shape[0])
    first, tie = gather_grouped((w_query, w_key, w_value, coded), tie)
    widths = (w_query.shape[1], w_key.shape[1], w_value.shape[1])
    at = sum(widths)
    small_full = decode_exact(first[:, :, at:], small_local.size, small_local.shape)
    return split_grouped(first[:, :, :at], widths), small_full, tie


def gather_second(w_output, w_inner, w_outer):
    second, _ = gather_grouped((w_output, w_inner, w_outer.T))
    wo, wi, wu_t = split_grouped(second, (w_output.shape[1], w_inner.shape[1], w_outer.shape[0]))
    return (wo, wi, wu_t.T)


def reduce_seq_stage(grads, tie=None):
    dp_size = lax.psum(1, "dp")
    chunks = [grad.reshape(grad.shape[0], dp_size, grad.shape[1] // dp_size) for grad in grads]
    stacked = jnp.concatenate(chunks, axis=2).astype(jnp.bfloat16)
    stacked, tie = lax.optimization_barrier((stacked, tie))
    reduced = lax.psum_scatter(stacked, "seq", scatter_dimension=0, tiled=True)
    return (reduced, [c.shape[2] for c in chunks]), tie


def stack_for_seq(grads):
    dp_size = lax.psum(1, "dp")
    chunks = [grad.reshape(grad.shape[0], dp_size, grad.shape[1] // dp_size) for grad in grads]
    return jnp.concatenate(chunks, axis=2).astype(jnp.bfloat16), [c.shape[2] for c in chunks]


def reduce_dp_stage(stages):
    joined = jnp.concatenate([stage for stage, _ in stages], axis=2)
    over_dp = lax.psum_scatter(joined, "dp", scatter_dimension=1, tiled=True)[:, 0].astype(jnp.float32)
    pieces, at = [], 0
    for _, widths in stages:
        for width in widths:
            pieces.append(over_dp[:, at : at + width])
            at += width
    return pieces


HALF_FULL = WINDOW // 2
HALF_POOL = POOL_SPAN // 2 // STRIDE
BLOCK_POOL = CLEN // STRIDE


def layout_of(index, offsets):
    in_prompt = index < PROMPT
    segment = jnp.where(in_prompt, -1, (index - PROMPT) // CLEN)
    within = index - PROMPT - segment * CLEN
    choose = segment[..., None] == jnp.arange(CONT, dtype=jnp.int32)
    spread = offsets.reshape(offsets.shape[:1] + (1,) * (index.ndim - 1) + offsets.shape[1:])
    cont_start = jnp.sum(jnp.where(choose, spread, 0), axis=-1)
    position = jnp.where(in_prompt, index, cont_start + within)
    limit = jnp.where(in_prompt, PROMPT, cont_start)
    return segment, position, limit


def window_rows(source, starts, length):
    groups, blocks = starts.shape
    return jnp.stack(
        [
            jnp.stack(
                [lax.dynamic_slice_in_dim(source[g], starts[g, b], length, 0) for b in range(blocks)]
            )
            for g in range(groups)
        ]
    )


def window_add(target, updates, starts):
    groups, blocks = starts.shape
    length = updates.shape[2]
    rows = []
    for g in range(groups):
        row = target[g]
        for b in range(blocks):
            start = starts[g, b]
            current = lax.dynamic_slice_in_dim(row, start, length, 0)
            row = lax.dynamic_update_slice_in_dim(row, current + updates[g, b], start, 0)
        rows.append(row)
    return jnp.stack(rows)


def block_geometry(seq_index, groups, shard_rows, offsets):
    group_len = PROMPT + CONT * CLEN
    pooled_len = group_len // STRIDE
    blocks = shard_rows // CLEN
    block_start = (seq_index * blocks + jnp.arange(blocks, dtype=jnp.int32)) * CLEN
    prompt_block = block_start < PROMPT
    cont_index = jnp.clip((block_start - PROMPT) // CLEN, 0, CONT - 1)
    anchor = jnp.where(prompt_block[None, :], block_start[None, :], offsets[:, cont_index])
    pooled_start = block_start // STRIDE
    intended = (
        anchor - HALF_FULL,
        jnp.broadcast_to(block_start + CLEN, anchor.shape),
        anchor // STRIDE - HALF_POOL,
        jnp.broadcast_to(pooled_start + BLOCK_POOL, anchor.shape),
    )
    limits = (group_len, group_len, pooled_len, pooled_len)
    lengths = (HALF_FULL, HALF_FULL, HALF_POOL, HALF_POOL)
    clamped = tuple(
        jnp.clip(start, 0, limit - length) for start, limit, length in zip(intended, limits, lengths)
    )
    ramp = lambda n: jnp.arange(n, dtype=jnp.int32)

    def span(window):
        actual = clamped[window][:, :, None] + ramp(lengths[window])
        offset = actual - intended[window][:, :, None]
        return actual, (offset >= 0) & (offset < lengths[window])

    before_full, before_full_ok = span(0)
    after_full, after_full_ok = span(1)
    before_pool, before_pool_ok = span(2)
    after_pool, after_pool_ok = span(3)
    after_ok = prompt_block[None, :, None]
    own_full = jnp.broadcast_to(block_start[None, :, None] + ramp(CLEN), anchor.shape + (CLEN,))
    own_pool = jnp.broadcast_to(
        pooled_start[None, :, None] + ramp(BLOCK_POOL), anchor.shape + (BLOCK_POOL,)
    )
    full_index = jnp.concatenate([before_full, own_full, after_full], axis=2)
    pooled_index = jnp.concatenate([before_pool, own_pool, after_pool], axis=2)
    full_valid = jnp.concatenate(
        [before_full_ok, jnp.ones(own_full.shape, bool), after_ok & after_full_ok], axis=2
    )
    pooled_valid = jnp.concatenate(
        [before_pool_ok, jnp.ones(own_pool.shape, bool), after_ok & after_pool_ok], axis=2
    )
    query_index = block_start[None, :, None] + ramp(CLEN)
    query_index = jnp.broadcast_to(query_index, anchor.shape + (CLEN,))
    q_seg, q_pos, q_lim = layout_of(query_index, offsets)

    def visible(key_token, valid, reach):
        k_seg, k_pos, _ = layout_of(key_token, offsets)
        k_seg, k_pos, valid = k_seg[:, :, None, :], k_pos[:, :, None, :], valid[:, :, None, :]
        prompt_key = (k_seg < 0) & (k_pos < q_lim[..., None])
        own_key = (k_seg == q_seg[..., None]) & (q_seg[..., None] >= 0)
        distance = k_pos - q_pos[..., None]
        return valid & (prompt_key | own_key) & (distance >= -(reach // 2)) & (distance < reach // 2)

    mask = jnp.concatenate(
        [
            visible(full_index, full_valid, WINDOW),
            visible(pooled_index * STRIDE, pooled_valid, POOL_SPAN),
        ],
        axis=3,
    )
    return clamped, mask


def attention_fwd(queries, kv_local, pkv_local, kv_all, pkv_all, starts, mask):
    groups, shard_rows, width = queries.shape
    blocks = shard_rows // CLEN
    score_scale = 1.0 / HEAD_DIM**0.5
    keys_cat = jnp.concatenate(
        [
            window_rows(kv_all, starts[0], HALF_FULL),
            kv_local.reshape(groups, blocks, CLEN, 2 * width),
            window_rows(kv_all, starts[1], HALF_FULL),
            window_rows(pkv_all, starts[2], HALF_POOL),
            pkv_local.reshape(groups, blocks, BLOCK_POOL, 2 * width),
            window_rows(pkv_all, starts[3], HALF_POOL),
        ],
        axis=2,
    )
    span = keys_cat.shape[2]
    head_keys = keys_cat[..., :width].reshape(groups, blocks, span, HEADS, HEAD_DIM)
    head_values = keys_cat[..., width:].reshape(groups, blocks, span, HEADS, HEAD_DIM)
    head_query = queries.reshape(groups, blocks, CLEN, HEADS, HEAD_DIM)
    scores = jnp.einsum(
        "gbqhd,gbkhd->gbhqk", head_query, head_keys, preferred_element_type=jnp.float32
    )
    scores = jnp.where(mask[:, :, None], scores * score_scale, -1000000000.0)
    row_top = jnp.max(scores, axis=-1, keepdims=True)
    exponent = jnp.exp(scores - row_top)
    row_total = jnp.sum(exponent, axis=-1, keepdims=True)
    probs = exponent / row_total
    attended = jnp.einsum(
        "gbhqk,gbkhd->gbqhd",
        probs.astype(jnp.bfloat16),
        head_values,
        preferred_element_type=jnp.float32,
    )
    attended = attended.reshape(groups * shard_rows, width).astype(jnp.bfloat16)
    return attended, (head_query, head_keys, head_values, probs)


def attention_bwd(grad_attended, saved, starts, seq_index):
    head_query, head_keys, head_values, probs = saved
    groups, blocks = head_query.shape[:2]
    width = HEADS * HEAD_DIM
    score_scale = 1.0 / HEAD_DIM**0.5
    head_grad = grad_attended.reshape(groups, blocks, CLEN, HEADS, HEAD_DIM)
    grad_probs = jnp.einsum(
        "gbqhd,gbkhd->gbhqk", head_grad, head_values, preferred_element_type=jnp.float32
    )
    centre = jnp.sum(probs * grad_probs, axis=-1, keepdims=True)
    grad_scores = (probs * (grad_probs - centre)).astype(jnp.bfloat16)
    grad_queries = jnp.einsum(
        "gbhqk,gbkhd->gbqhd", grad_scores, head_keys, preferred_element_type=jnp.float32
    ) * score_scale
    grad_keys = jnp.einsum(
        "gbhqk,gbqhd->gbkhd", grad_scores, head_query, preferred_element_type=jnp.float32
    ) * score_scale
    grad_values = jnp.einsum(
        "gbhqk,gbqhd->gbkhd",
        probs.astype(jnp.bfloat16),
        head_grad,
        preferred_element_type=jnp.float32,
    )
    span = grad_keys.shape[2]
    grad_kv = jnp.concatenate(
        [grad_keys.reshape(groups, blocks, span, width), grad_values.reshape(groups, blocks, span, width)],
        axis=3,
    )
    shard_rows = blocks * CLEN
    group_len = PROMPT + CONT * CLEN
    pooled_len = group_len // STRIDE
    cut = (0, HALF_FULL, HALF_FULL + CLEN, 2 * HALF_FULL + CLEN)
    pcut = tuple(cut[-1] + c for c in (0, HALF_POOL, HALF_POOL + BLOCK_POOL, 2 * HALF_POOL + BLOCK_POOL))
    ramp = lambda n: jnp.arange(n, dtype=jnp.int32)
    own_full = grad_kv[:, :, cut[1] : cut[2]].reshape(groups, shard_rows, 2 * width)
    full = jnp.zeros((groups, group_len, 2 * width), jnp.float32)
    full = lax.dynamic_update_slice_in_dim(full, own_full, seq_index * shard_rows, 1)
    side_values = jnp.concatenate(
        [grad_kv[:, :, cut[0] : cut[1]], grad_kv[:, :, cut[2] : cut[3]]], axis=2
    ).reshape(groups, -1, 2 * width)
    side_rows = jnp.concatenate(
        [starts[0][:, :, None] + ramp(HALF_FULL), starts[1][:, :, None] + ramp(HALF_FULL)], axis=2
    ).reshape(groups, -1)
    own_pool_rows = (seq_index * (shard_rows // STRIDE) + ramp(blocks)[:, None] * BLOCK_POOL + ramp(BLOCK_POOL))
    pool_values = grad_kv[:, :, pcut[0] : pcut[3]].reshape(groups, -1, 2 * width)
    pool_rows_index = jnp.concatenate(
        [
            starts[2][:, :, None] + ramp(HALF_POOL),
            jnp.broadcast_to(own_pool_rows[None], (groups, blocks, BLOCK_POOL)),
            starts[3][:, :, None] + ramp(HALF_POOL),
        ],
        axis=2,
    ).reshape(groups, -1)
    fulls, pooleds, unpooleds = [], [], []
    for g in range(groups):
        fulls.append(full[g] + select_sum(side_values[g], side_rows[g] == ramp(group_len)[:, None]))
        pooleds.append(select_sum(pool_values[g], pool_rows_index[g] == ramp(pooled_len)[:, None]))
        unpooleds.append(
            select_sum(pool_values[g], pool_rows_index[g] == (ramp(group_len) // STRIDE)[:, None])
        )
    full = jnp.stack(fulls)
    pooled = jnp.stack(pooleds)
    unpooled = jnp.stack(unpooleds)
    grad_queries = grad_queries.reshape(groups * shard_rows, width).astype(jnp.bfloat16)
    return grad_queries, full, pooled, unpooled


def select_sum(values, chosen):
    onehot = chosen.astype(jnp.bfloat16)
    high = values.astype(jnp.bfloat16)
    low = (values - high.astype(jnp.float32)).astype(jnp.bfloat16)
    return product(onehot, high) + product(onehot, low)


def phase_weights(weight, rows):
    phase = (jnp.arange(rows, dtype=jnp.int32) % STRIDE)[:, None]
    total = jnp.zeros((rows, weight.shape[1]), jnp.float32)
    for r in range(STRIDE):
        total = total + jnp.where(phase == r, weight[r][None, :], 0.0)
    return total


def pool_grouped(source, weight):
    groups, rows, width = source.shape
    return jnp.sum(
        source.reshape(groups, rows // STRIDE, STRIDE, width) * weight[None, None], axis=2
    )


def unpool_grouped(pooled_grad, weight):
    groups, rows, width = pooled_grad.shape
    return (pooled_grad[:, :, None, :] * weight[None, None]).reshape(groups, rows * STRIDE, width)


def pool_grad_grouped(pooled_grad, source):
    groups, rows, width = source.shape
    blocks_view = source.astype(jnp.float32).reshape(groups, rows // STRIDE, STRIDE, width)
    return jnp.sum(pooled_grad[:, :, None, :] * blocks_view, axis=(0, 1))


def local(
    hidden_in,
    w_query,
    w_key,
    w_value,
    w_output,
    w_inner,
    w_outer,
    pool_weight,
    ln_gain,
    ln_bias,
    branch_blocks,
    grad_out,
):
    pool_rows_count = pool_weight.shape[0] * pool_weight.shape[1]
    small_local = jnp.concatenate(
        [pool_weight.reshape(pool_rows_count, -1), ln_gain, ln_bias], axis=0
    )
    hidden_all = lax.all_gather(hidden_in, "seq", axis=1, tiled=True)
    groups, shard_rows, width = hidden_in.shape
    seq_index = lax.axis_index("seq")
    offsets = STRIDE * branch_blocks
    starts, mask = block_geometry(seq_index, groups, shard_rows, offsets)
    (wq, wk, wv), small_full, (hidden_all, starts, mask) = gather_first(
        w_query, w_key, w_value, small_local, (hidden_all, starts, mask)
    )
    pool_full = small_full[:pool_rows_count].reshape(pool_weight.shape[0], pool_weight.shape[1], -1)
    gain_full = small_full[pool_rows_count : pool_rows_count + ln_gain.shape[0]]
    bias_full = small_full[pool_rows_count + ln_gain.shape[0] :]
    groups, shard_rows, width = hidden_in.shape

    group_len = hidden_all.shape[1]
    tokens = hidden_in.reshape(groups * shard_rows, width)
    all_tokens = hidden_all.reshape(groups * group_len, width)
    queries = product(tokens, wq).astype(jnp.bfloat16)
    key_g = product(all_tokens, wk).astype(jnp.bfloat16).reshape(groups, group_len, width)
    value_g = product(all_tokens, wv).astype(jnp.bfloat16).reshape(groups, group_len, width)
    pooled_keys = pool_grouped(key_g.astype(jnp.float32), pool_full[0]).astype(jnp.bfloat16)
    pooled_values = pool_grouped(value_g.astype(jnp.float32), pool_full[1]).astype(jnp.bfloat16)
    kv_all = jnp.concatenate([key_g, value_g], axis=2)
    pkv_all = jnp.concatenate([pooled_keys, pooled_values], axis=2)
    kv_local = lax.dynamic_slice_in_dim(kv_all, seq_index * shard_rows, shard_rows, 1)
    pkv_local = lax.dynamic_slice_in_dim(
        pkv_all, seq_index * (shard_rows // STRIDE), shard_rows // STRIDE, 1
    )
    wq, wk, wv, w_output, w_inner, w_outer = lax.optimization_barrier(
        (wq, wk, wv, w_output, w_inner, w_outer)
    )
    wo, wi, wu = gather_second(w_output, w_inner, w_outer)
    attended, att_saved = attention_fwd(
        queries.reshape(groups, shard_rows, width), kv_local, pkv_local, kv_all, pkv_all, starts, mask
    )
    mixed_rows = tokens.astype(jnp.float32) + product(attended, wo)
    normed_first = layer_norm(mixed_rows, gain_full[0], bias_full[0])
    first_low = normed_first.astype(jnp.bfloat16)
    inner_act = product(first_low, wi)
    active = jax.nn.gelu(inner_act, approximate=False).astype(jnp.bfloat16)
    second = normed_first + product(active, wu)
    norm_value, second_back = jax.vjp(layer_norm, second, gain_full[1], bias_full[1])
    output = norm_value.astype(jnp.bfloat16)

    cotangent = grad_out.reshape(groups * shard_rows, width).astype(jnp.float32)
    grad_second, gain_second, bias_second = second_back(cotangent)
    grad_ffn_out = grad_second.astype(jnp.bfloat16)
    grad_outer = product_left(active, grad_ffn_out)
    grad_active = product_right(grad_ffn_out, wu)
    gelu_value, gelu_back = jax.vjp(partial(jax.nn.gelu, approximate=False), inner_act)
    grad_inner_act = gelu_back(grad_active)[0].astype(jnp.bfloat16)
    grad_inner = product_left(first_low, grad_inner_act)
    grad_first = grad_second + product_right(grad_inner_act, wi)
    first_value, first_back = jax.vjp(layer_norm, mixed_rows, gain_full[0], bias_full[0])
    grad_mixed, gain_first, bias_first = first_back(grad_first)
    grad_branch = grad_mixed.astype(jnp.bfloat16)
    grad_output = product_left(attended, grad_branch)
    grad_attended = product_right(grad_branch, wo).astype(jnp.bfloat16)
    early, grad_attended = reduce_seq_stage((grad_output, grad_inner, grad_outer.T), grad_attended)
    early_reduced, early_widths = early

    grad_rows = grad_attended.reshape(groups, shard_rows, width)
    key_phase = phase_weights(pool_full[0], group_len)
    value_phase = phase_weights(pool_full[1], group_len)
    pieces_back = []
    for g in range(groups):
        saved_g = tuple(item[g : g + 1] for item in att_saved)
        starts_g = tuple(item[g : g + 1] for item in starts)
        grad_g = grad_rows[g].reshape(shard_rows, width)
        grad_queries_g, full_g, pooled_g, unpooled_g = attention_bwd(grad_g, saved_g, starts_g, seq_index)
        if g == 1:
            full_g, pooled_g, unpooled_g, earlier_back, early_reduced = lax.optimization_barrier(
                (full_g, pooled_g, unpooled_g, pieces_back[0][4], early_reduced)
            )
            pieces_back[0] = pieces_back[0][:4] + (earlier_back,)
        key_partial_g = (
            full_g[0, :, :width] + unpooled_g[0, :, :width] * key_phase
        ).astype(jnp.bfloat16)
        value_partial_g = (
            full_g[0, :, width:] + unpooled_g[0, :, width:] * value_phase
        ).astype(jnp.bfloat16)
        back_g = product_right(key_partial_g, wk) + product_right(value_partial_g, wv)
        back_g = back_g.reshape(1, group_len, width).astype(jnp.bfloat16)
        if g == groups - 1:
            back_own_g = back_g
        else:
            back_own_g = lax.psum_scatter(back_g, "seq", scatter_dimension=1, tiled=True)
        pieces_back.append((grad_queries_g, pooled_g, key_partial_g, value_partial_g, back_own_g))
    grad_queries = jnp.concatenate([piece[0] for piece in pieces_back], axis=0)
    grad_pooled = jnp.concatenate([piece[1] for piece in pieces_back], axis=0)
    key_partial = jnp.concatenate([piece[2] for piece in pieces_back], axis=0)
    value_partial = jnp.concatenate([piece[3] for piece in pieces_back], axis=0)
    last_back = pieces_back[-1][4]
    grad_pooling = jnp.stack(
        [
            pool_grad_grouped(grad_pooled[..., :width], key_g),
            pool_grad_grouped(grad_pooled[..., width:], value_g),
        ]
    )
    grad_query_w = product_left(tokens, grad_queries)
    grad_key_w = product_left(all_tokens, key_partial)
    grad_value_w = product_left(all_tokens, value_partial)
    late_stacked, late_widths = stack_for_seq((grad_query_w, grad_key_w, grad_value_w))
    seq_size = lax.psum(1, "seq")
    late_flat = late_stacked.reshape(seq_size, -1, width)
    back_flat = last_back.reshape(seq_size, -1, width)
    joined = jnp.concatenate([late_flat, back_flat], axis=1)
    chunk_rows = joined.shape[1]
    joined = joined.reshape(seq_size * chunk_rows, width)
    joined = lax.psum_scatter(joined, "seq", scatter_dimension=0, tiled=True)
    late_reduced = joined[: late_flat.shape[1]].reshape(
        late_stacked.shape[0] // seq_size, late_stacked.shape[1], late_stacked.shape[2]
    )
    back_last = joined[late_flat.shape[1] :].reshape(1, shard_rows, width)
    back_own = jnp.concatenate([piece[4] for piece in pieces_back[:-1]] + [back_last], axis=0)
    grad_tokens = (
        grad_mixed
        + product_right(grad_queries, wq)
        + back_own.reshape(groups * shard_rows, width).astype(jnp.float32)
    )
    pieces = reduce_dp_stage(((early_reduced, early_widths), (late_reduced, late_widths)))
    accum = (pieces[3], pieces[4], pieces[5], pieces[0], pieces[1], pieces[2].T)
    small_sums = (
        lax.psum_scatter(grad_pooling, ("dp", "seq"), scatter_dimension=2, tiled=True),
        lax.psum_scatter(
            jnp.stack([gain_first, gain_second]), ("dp", "seq"), scatter_dimension=1, tiled=True
        ),
        lax.psum_scatter(
            jnp.stack([bias_first, bias_second]), ("dp", "seq"), scatter_dimension=1, tiled=True
        ),
    )
    return (
        output.reshape(groups, shard_rows, width),
        grad_tokens.astype(jnp.bfloat16).reshape(groups, shard_rows, width),
        accum[0],
        accum[1],
        accum[2],
        accum[3],
        accum[4],
        accum[5],
        small_sums[0],
        small_sums[1],
        small_sums[2],
    )


def solution(mesh):
    in_specs = (
        P("dp", "seq", None),
        P("seq", "dp"),
        P("seq", "dp"),
        P("seq", "dp"),
        P("seq", "dp"),
        P("seq", "dp"),
        P("dp", "seq"),
        P(None, None, ("dp", "seq")),
        P(None, ("dp", "seq")),
        P(None, ("dp", "seq")),
        P("dp", None),
        P("dp", "seq", None),
    )
    out_specs = (
        P("dp", "seq", None),
        P("dp", "seq", None),
        P("seq", "dp"),
        P("seq", "dp"),
        P("seq", "dp"),
        P("seq", "dp"),
        P("seq", "dp"),
        P("dp", "seq"),
        P(None, None, ("dp", "seq")),
        P(None, ("dp", "seq")),
        P(None, ("dp", "seq")),
    )
    return jax.shard_map(local, mesh=mesh, in_specs=in_specs, out_specs=out_specs, check_vma=False)
```

```python
from functools import partial

import jax
import jax.numpy as jnp
from jax import lax
from jax.sharding import PartitionSpec as P

HEADS = 12
HEAD_DIM = 64
PROMPT = 1024
CONT = 8
CLEN = 128
WINDOW = 128
POOL_SPAN = 512
STRIDE = 4


eps_norm = 1e-05


def token_layout(positions_in, offsets):
    in_prompt = positions_in < PROMPT
    segment = jnp.where(in_prompt, -1, (positions_in - PROMPT) // CLEN)
    within = positions_in - PROMPT - segment * CLEN
    choose = (segment[:, None] == jnp.arange(CONT, dtype=jnp.int32)[None, :]).astype(jnp.int32)
    cont_start = jnp.sum(choose * offsets[None, :], axis=1)
    position = jnp.where(in_prompt, positions_in, cont_start + within)
    prompt_limit = jnp.where(in_prompt, PROMPT, cont_start)
    return (segment, position, prompt_limit)


def visible_keys(query_rows, key_index, offsets, reach):
    query_seg, query_pos, query_limit = token_layout(query_rows, offsets)
    key_seg, key_pos, key_limit = token_layout(key_index, offsets)
    prompt_key = (key_seg[None, :] < 0) & (key_pos[None, :] < query_limit[:, None])
    own_key = (key_seg[None, :] == query_seg[:, None]) & (query_seg[:, None] >= 0)
    distance = key_pos[None, :] - query_pos[:, None]
    return (prompt_key | own_key) & (distance >= -(reach // 2)) & (distance < reach // 2)


def key_mask(query_rows, offsets):
    group_len = PROMPT + CONT * CLEN
    full_keys = jnp.arange(group_len, dtype=jnp.int32)
    pooled_keys = jnp.arange(group_len // STRIDE, dtype=jnp.int32) * STRIDE
    return jnp.concatenate(
        [
            visible_keys(query_rows, full_keys, offsets, WINDOW),
            visible_keys(query_rows, pooled_keys, offsets, POOL_SPAN),
        ],
        axis=1,
    )


def pool_rows(source, weight):
    return jnp.sum(
        source.reshape(source.shape[0] // STRIDE, STRIDE, source.shape[1]) * weight[None, :, :],
        axis=1,
    )


def unpool(pooled_grad, weight):
    return (pooled_grad[:, None, :] * weight[None, :, :]).reshape(-1, pooled_grad.shape[1])


def pool_grad(pooled_grad, source):
    blocks_view = source.astype(jnp.float32).reshape(-1, STRIDE, source.shape[1])
    return jnp.sum(pooled_grad[:, None, :] * blocks_view, axis=0)


def layer_norm(source, gain, bias):
    centre = jnp.mean(source, axis=-1, keepdims=True)
    centred = source - centre
    spread = jnp.mean(centred * centred, axis=-1, keepdims=True)
    return centred * lax.rsqrt(spread + eps_norm) * gain + bias


def product(left, right):
    return jnp.dot(left, right, preferred_element_type=jnp.float32)


def product_left(left, right):
    return lax.dot_general(
        left, right, (((0,), (0,)), ((), ())), preferred_element_type=jnp.float32
    )


def product_right(left, right):
    return lax.dot_general(
        left, right, (((1,), (1,)), ((), ())), preferred_element_type=jnp.float32
    )


def add_pair(left_term, right_term):
    return left_term + right_term


def gather_grouped(shards, tie=None):
    local_block = jnp.concatenate(shards, axis=1)
    across = lax.all_gather(local_block, "dp", axis=1, tiled=False)
    across, tie = lax.optimization_barrier((across, tie))
    return lax.all_gather(across, "seq", axis=0, tiled=True), tie


def split_grouped(gathered, widths):
    pieces, at = [], 0
    for width in widths:
        piece = gathered[:, :, at : at + width]
        pieces.append(piece.reshape(piece.shape[0], -1))
        at += width
    return pieces


def code_exact(values, rows):
    parts, rest = [], values
    for _ in range(3):
        part = lax.optimization_barrier(rest.astype(jnp.bfloat16))
        parts.append(part)
        rest = rest - part.astype(jnp.float32)
    flat = jnp.concatenate([part.reshape(-1) for part in parts])
    columns = -(-flat.shape[0] // rows)
    flat = jnp.pad(flat, (0, rows * columns - flat.shape[0]))
    return flat.reshape(rows, columns)


def decode_exact(gathered, count, shape):
    seq_size = lax.psum(1, "seq")
    rows = gathered.shape[0] // seq_size
    blocks = gathered.reshape(seq_size, rows, gathered.shape[1], gathered.shape[2])
    blocks = jnp.transpose(blocks, (2, 0, 1, 3)).reshape(-1, rows * gathered.shape[2])
    parts = blocks[:, : 3 * count].reshape(blocks.shape[0], 3, shape[0], shape[1])
    parts = parts.astype(jnp.float32)
    joined = (parts[:, 0] + parts[:, 1]) + parts[:, 2]
    return jnp.transpose(joined, (1, 0, 2)).reshape(shape[0], -1)


def gather_first(w_query, w_key, w_value, small_local, tie):
    coded = code_exact(small_local, w_query.shape[0])
    first, tie = gather_grouped((w_query, w_key, w_value, coded), tie)
    widths = (w_query.shape[1], w_key.shape[1], w_value.shape[1])
    at = sum(widths)
    small_full = decode_exact(first[:, :, at:], small_local.size, small_local.shape)
    return split_grouped(first[:, :, :at], widths), small_full, tie


def gather_second(w_output, w_inner, w_outer):
    second, _ = gather_grouped((w_output, w_inner, w_outer.T))
    wo, wi, wu_t = split_grouped(second, (w_output.shape[1], w_inner.shape[1], w_outer.shape[0]))
    return (wo, wi, wu_t.T)


def reduce_seq_stage(grads, tie=None):
    dp_size = lax.psum(1, "dp")
    chunks = [grad.reshape(grad.shape[0], dp_size, grad.shape[1] // dp_size) for grad in grads]
    stacked = jnp.concatenate(chunks, axis=2).astype(jnp.bfloat16)
    stacked, tie = lax.optimization_barrier((stacked, tie))
    reduced = lax.psum_scatter(stacked, "seq", scatter_dimension=0, tiled=True)
    return (reduced, [c.shape[2] for c in chunks]), tie


def stack_for_seq(grads):
    dp_size = lax.psum(1, "dp")
    chunks = [grad.reshape(grad.shape[0], dp_size, grad.shape[1] // dp_size) for grad in grads]
    return jnp.concatenate(chunks, axis=2).astype(jnp.bfloat16), [c.shape[2] for c in chunks]


def reduce_dp_stage(stages):
    joined = jnp.concatenate([stage for stage, _ in stages], axis=2)
    over_dp = lax.psum_scatter(joined, "dp", scatter_dimension=1, tiled=True)[:, 0].astype(jnp.float32)
    pieces, at = [], 0
    for _, widths in stages:
        for width in widths:
            pieces.append(over_dp[:, at : at + width])
            at += width
    return pieces


HALF_FULL = WINDOW // 2
HALF_POOL = POOL_SPAN // 2 // STRIDE
BLOCK_POOL = CLEN // STRIDE


def layout_of(index, offsets):
    in_prompt = index < PROMPT
    segment = jnp.where(in_prompt, -1, (index - PROMPT) // CLEN)
    within = index - PROMPT - segment * CLEN
    choose = segment[..., None] == jnp.arange(CONT, dtype=jnp.int32)
    spread = offsets.reshape(offsets.shape[:1] + (1,) * (index.ndim - 1) + offsets.shape[1:])
    cont_start = jnp.sum(jnp.where(choose, spread, 0), axis=-1)
    position = jnp.where(in_prompt, index, cont_start + within)
    limit = jnp.where(in_prompt, PROMPT, cont_start)
    return segment, position, limit


def window_rows(source, starts, length):
    groups, blocks = starts.shape
    return jnp.stack(
        [
            jnp.stack(
                [lax.dynamic_slice_in_dim(source[g], starts[g, b], length, 0) for b in range(blocks)]
            )
            for g in range(groups)
        ]
    )


def window_add(target, updates, starts):
    groups, blocks = starts.shape
    length = updates.shape[2]
    rows = []
    for g in range(groups):
        row = target[g]
        for b in range(blocks):
            start = starts[g, b]
            current = lax.dynamic_slice_in_dim(row, start, length, 0)
            row = lax.dynamic_update_slice_in_dim(row, current + updates[g, b], start, 0)
        rows.append(row)
    return jnp.stack(rows)


def block_geometry(seq_index, groups, shard_rows, offsets):
    group_len = PROMPT + CONT * CLEN
    pooled_len = group_len // STRIDE
    blocks = shard_rows // CLEN
    block_start = (seq_index * blocks + jnp.arange(blocks, dtype=jnp.int32)) * CLEN
    prompt_block = block_start < PROMPT
    cont_index = jnp.clip((block_start - PROMPT) // CLEN, 0, CONT - 1)
    anchor = jnp.where(prompt_block[None, :], block_start[None, :], offsets[:, cont_index])
    pooled_start = block_start // STRIDE
    intended = (
        anchor - HALF_FULL,
        jnp.broadcast_to(block_start + CLEN, anchor.shape),
        anchor // STRIDE - HALF_POOL,
        jnp.broadcast_to(pooled_start + BLOCK_POOL, anchor.shape),
    )
    limits = (group_len, group_len, pooled_len, pooled_len)
    lengths = (HALF_FULL, HALF_FULL, HALF_POOL, HALF_POOL)
    clamped = tuple(
        jnp.clip(start, 0, limit - length) for start, limit, length in zip(intended, limits, lengths)
    )
    ramp = lambda n: jnp.arange(n, dtype=jnp.int32)

    def span(window):
        actual = clamped[window][:, :, None] + ramp(lengths[window])
        offset = actual - intended[window][:, :, None]
        return actual, (offset >= 0) & (offset < lengths[window])

    before_full, before_full_ok = span(0)
    after_full, after_full_ok = span(1)
    before_pool, before_pool_ok = span(2)
    after_pool, after_pool_ok = span(3)
    after_ok = prompt_block[None, :, None]
    own_full = jnp.broadcast_to(block_start[None, :, None] + ramp(CLEN), anchor.shape + (CLEN,))
    own_pool = jnp.broadcast_to(
        pooled_start[None, :, None] + ramp(BLOCK_POOL), anchor.shape + (BLOCK_POOL,)
    )
    full_index = jnp.concatenate([before_full, own_full, after_full], axis=2)
    pooled_index = jnp.concatenate([before_pool, own_pool, after_pool], axis=2)
    full_valid = jnp.concatenate(
        [before_full_ok, jnp.ones(own_full.shape, bool), after_ok & after_full_ok], axis=2
    )
    pooled_valid = jnp.concatenate(
        [before_pool_ok, jnp.ones(own_pool.shape, bool), after_ok & after_pool_ok], axis=2
    )
    query_index = block_start[None, :, None] + ramp(CLEN)
    query_index = jnp.broadcast_to(query_index, anchor.shape + (CLEN,))
    q_seg, q_pos, q_lim = layout_of(query_index, offsets)

    def visible(key_token, valid, reach):
        k_seg, k_pos, _ = layout_of(key_token, offsets)
        k_seg, k_pos, valid = k_seg[:, :, None, :], k_pos[:, :, None, :], valid[:, :, None, :]
        prompt_key = (k_seg < 0) & (k_pos < q_lim[..., None])
        own_key = (k_seg == q_seg[..., None]) & (q_seg[..., None] >= 0)
        distance = k_pos - q_pos[..., None]
        return valid & (prompt_key | own_key) & (distance >= -(reach // 2)) & (distance < reach // 2)

    mask = jnp.concatenate(
        [
            visible(full_index, full_valid, WINDOW),
            visible(pooled_index * STRIDE, pooled_valid, POOL_SPAN),
        ],
        axis=3,
    )
    return clamped, mask


def attention_fwd(queries, kv_local, pkv_local, kv_all, pkv_all, starts, mask):
    groups, shard_rows, width = queries.shape
    blocks = shard_rows // CLEN
    score_scale = 1.0 / HEAD_DIM**0.5
    keys_cat = jnp.concatenate(
        [
            window_rows(kv_all, starts[0], HALF_FULL),
            kv_local.reshape(groups, blocks, CLEN, 2 * width),
            window_rows(kv_all, starts[1], HALF_FULL),
            window_rows(pkv_all, starts[2], HALF_POOL),
            pkv_local.reshape(groups, blocks, BLOCK_POOL, 2 * width),
            window_rows(pkv_all, starts[3], HALF_POOL),
        ],
        axis=2,
    )
    span = keys_cat.shape[2]
    head_keys = keys_cat[..., :width].reshape(groups, blocks, span, HEADS, HEAD_DIM)
    head_values = keys_cat[..., width:].reshape(groups, blocks, span, HEADS, HEAD_DIM)
    head_query = queries.reshape(groups, blocks, CLEN, HEADS, HEAD_DIM)
    scores = jnp.einsum(
        "gbqhd,gbkhd->gbhqk", head_query, head_keys, preferred_element_type=jnp.float32
    )
    scores = jnp.where(mask[:, :, None], scores * score_scale, -1000000000.0)
    row_top = jnp.max(scores, axis=-1, keepdims=True)
    exponent = jnp.exp(scores - row_top)
    row_total = jnp.sum(exponent, axis=-1, keepdims=True)
    probs = exponent / row_total
    attended = jnp.einsum(
        "gbhqk,gbkhd->gbqhd",
        probs.astype(jnp.bfloat16),
        head_values,
        preferred_element_type=jnp.float32,
    )
    attended = attended.reshape(groups * shard_rows, width).astype(jnp.bfloat16)
    return attended, (head_query, head_keys, head_values, probs)


def attention_bwd(grad_attended, saved, starts, seq_index):
    head_query, head_keys, head_values, probs = saved
    groups, blocks = head_query.shape[:2]
    width = HEADS * HEAD_DIM
    score_scale = 1.0 / HEAD_DIM**0.5
    head_grad = grad_attended.reshape(groups, blocks, CLEN, HEADS, HEAD_DIM)
    grad_probs = jnp.einsum(
        "gbqhd,gbkhd->gbhqk", head_grad, head_values, preferred_element_type=jnp.float32
    )
    centre = jnp.sum(probs * grad_probs, axis=-1, keepdims=True)
    grad_scores = (probs * (grad_probs - centre)).astype(jnp.bfloat16)
    grad_queries = jnp.einsum(
        "gbhqk,gbkhd->gbqhd", grad_scores, head_keys, preferred_element_type=jnp.float32
    ) * score_scale
    grad_keys = jnp.einsum(
        "gbhqk,gbqhd->gbkhd", grad_scores, head_query, preferred_element_type=jnp.float32
    ) * score_scale
    grad_values = jnp.einsum(
        "gbhqk,gbqhd->gbkhd",
        probs.astype(jnp.bfloat16),
        head_grad,
        preferred_element_type=jnp.float32,
    )
    span = grad_keys.shape[2]
    grad_kv = jnp.concatenate(
        [grad_keys.reshape(groups, blocks, span, width), grad_values.reshape(groups, blocks, span, width)],
        axis=3,
    )
    shard_rows = blocks * CLEN
    group_len = PROMPT + CONT * CLEN
    pooled_len = group_len // STRIDE
    cut = (0, HALF_FULL, HALF_FULL + CLEN, 2 * HALF_FULL + CLEN)
    pcut = tuple(cut[-1] + c for c in (0, HALF_POOL, HALF_POOL + BLOCK_POOL, 2 * HALF_POOL + BLOCK_POOL))
    ramp = lambda n: jnp.arange(n, dtype=jnp.int32)
    own_full = grad_kv[:, :, cut[1] : cut[2]].reshape(groups, shard_rows, 2 * width)
    full = jnp.zeros((groups, group_len, 2 * width), jnp.float32)
    full = lax.dynamic_update_slice_in_dim(full, own_full, seq_index * shard_rows, 1)
    side_values = jnp.concatenate(
        [grad_kv[:, :, cut[0] : cut[1]], grad_kv[:, :, cut[2] : cut[3]]], axis=2
    ).reshape(groups, -1, 2 * width)
    side_rows = jnp.concatenate(
        [starts[0][:, :, None] + ramp(HALF_FULL), starts[1][:, :, None] + ramp(HALF_FULL)], axis=2
    ).reshape(groups, -1)
    own_pool_rows = (seq_index * (shard_rows // STRIDE) + ramp(blocks)[:, None] * BLOCK_POOL + ramp(BLOCK_POOL))
    pool_values = grad_kv[:, :, pcut[0] : pcut[3]].reshape(groups, -1, 2 * width)
    pool_rows_index = jnp.concatenate(
        [
            starts[2][:, :, None] + ramp(HALF_POOL),
            jnp.broadcast_to(own_pool_rows[None], (groups, blocks, BLOCK_POOL)),
            starts[3][:, :, None] + ramp(HALF_POOL),
        ],
        axis=2,
    ).reshape(groups, -1)
    fulls, pooleds, unpooleds = [], [], []
    for g in range(groups):
        fulls.append(full[g] + select_sum(side_values[g], side_rows[g] == ramp(group_len)[:, None]))
        pooleds.append(select_sum(pool_values[g], pool_rows_index[g] == ramp(pooled_len)[:, None]))
        unpooleds.append(
            select_sum(pool_values[g], pool_rows_index[g] == (ramp(group_len) // STRIDE)[:, None])
        )
    full = jnp.stack(fulls)
    pooled = jnp.stack(pooleds)
    unpooled = jnp.stack(unpooleds)
    grad_queries = grad_queries.reshape(groups * shard_rows, width).astype(jnp.bfloat16)
    return grad_queries, full, pooled, unpooled


def back_projection(key_partial, value_partial, wk, wv):
    rows, width = key_partial.shape
    back = product_right(key_partial, wk) + product_right(value_partial, wv)
    back = back.reshape(1, rows, width).astype(jnp.bfloat16)
    return lax.psum_scatter(back, "seq", scatter_dimension=1, tiled=True)


def select_sum(values, chosen):
    onehot = chosen.astype(jnp.bfloat16)
    high = values.astype(jnp.bfloat16)
    low = (values - high.astype(jnp.float32)).astype(jnp.bfloat16)
    return product(onehot, high) + product(onehot, low)


def phase_weights(weight, rows):
    phase = (jnp.arange(rows, dtype=jnp.int32) % STRIDE)[:, None]
    total = jnp.zeros((rows, weight.shape[1]), jnp.float32)
    for r in range(STRIDE):
        total = total + jnp.where(phase == r, weight[r][None, :], 0.0)
    return total


def pool_grouped(source, weight):
    groups, rows, width = source.shape
    return jnp.sum(
        source.reshape(groups, rows // STRIDE, STRIDE, width) * weight[None, None], axis=2
    )


def unpool_grouped(pooled_grad, weight):
    groups, rows, width = pooled_grad.shape
    return (pooled_grad[:, :, None, :] * weight[None, None]).reshape(groups, rows * STRIDE, width)


def pool_grad_grouped(pooled_grad, source):
    groups, rows, width = source.shape
    blocks_view = source.astype(jnp.float32).reshape(groups, rows // STRIDE, STRIDE, width)
    return jnp.sum(pooled_grad[:, :, None, :] * blocks_view, axis=(0, 1))


def local(
    hidden_in,
    w_query,
    w_key,
    w_value,
    w_output,
    w_inner,
    w_outer,
    pool_weight,
    ln_gain,
    ln_bias,
    branch_blocks,
    grad_out,
):
    pool_rows_count = pool_weight.shape[0] * pool_weight.shape[1]
    small_local = jnp.concatenate(
        [pool_weight.reshape(pool_rows_count, -1), ln_gain, ln_bias], axis=0
    )
    hidden_all = lax.all_gather(hidden_in, "seq", axis=1, tiled=True)
    groups, shard_rows, width = hidden_in.shape
    seq_index = lax.axis_index("seq")
    offsets = STRIDE * branch_blocks
    starts, mask = block_geometry(seq_index, groups, shard_rows, offsets)
    (wq, wk, wv), small_full, (hidden_all, starts, mask) = gather_first(
        w_query, w_key, w_value, small_local, (hidden_all, starts, mask)
    )
    pool_full = small_full[:pool_rows_count].reshape(pool_weight.shape[0], pool_weight.shape[1], -1)
    gain_full = small_full[pool_rows_count : pool_rows_count + ln_gain.shape[0]]
    bias_full = small_full[pool_rows_count + ln_gain.shape[0] :]
    groups, shard_rows, width = hidden_in.shape

    group_len = hidden_all.shape[1]
    tokens = hidden_in.reshape(groups * shard_rows, width)
    all_tokens = hidden_all.reshape(groups * group_len, width)
    queries = product(tokens, wq).astype(jnp.bfloat16)
    key_g = product(all_tokens, wk).astype(jnp.bfloat16).reshape(groups, group_len, width)
    value_g = product(all_tokens, wv).astype(jnp.bfloat16).reshape(groups, group_len, width)
    pooled_keys = pool_grouped(key_g.astype(jnp.float32), pool_full[0]).astype(jnp.bfloat16)
    pooled_values = pool_grouped(value_g.astype(jnp.float32), pool_full[1]).astype(jnp.bfloat16)
    kv_all = jnp.concatenate([key_g, value_g], axis=2)
    pkv_all = jnp.concatenate([pooled_keys, pooled_values], axis=2)
    kv_local = lax.dynamic_slice_in_dim(kv_all, seq_index * shard_rows, shard_rows, 1)
    pkv_local = lax.dynamic_slice_in_dim(
        pkv_all, seq_index * (shard_rows // STRIDE), shard_rows // STRIDE, 1
    )
    wq, wk, wv, w_output, w_inner, w_outer = lax.optimization_barrier(
        (wq, wk, wv, w_output, w_inner, w_outer)
    )
    wo, wi, wu = gather_second(w_output, w_inner, w_outer)
    attended, att_saved = attention_fwd(
        queries.reshape(groups, shard_rows, width), kv_local, pkv_local, kv_all, pkv_all, starts, mask
    )
    mixed_rows = tokens.astype(jnp.float32) + product(attended, wo)
    normed_first = layer_norm(mixed_rows, gain_full[0], bias_full[0])
    first_low = normed_first.astype(jnp.bfloat16)
    inner_act = product(first_low, wi)
    active = jax.nn.gelu(inner_act, approximate=False).astype(jnp.bfloat16)
    second = normed_first + product(active, wu)
    norm_value, second_back = jax.vjp(layer_norm, second, gain_full[1], bias_full[1])
    output = norm_value.astype(jnp.bfloat16)

    cotangent = grad_out.reshape(groups * shard_rows, width).astype(jnp.float32)
    grad_second, gain_second, bias_second = second_back(cotangent)
    grad_ffn_out = grad_second.astype(jnp.bfloat16)
    grad_outer = product_left(active, grad_ffn_out)
    grad_active = product_right(grad_ffn_out, wu)
    gelu_value, gelu_back = jax.vjp(partial(jax.nn.gelu, approximate=False), inner_act)
    grad_inner_act = gelu_back(grad_active)[0].astype(jnp.bfloat16)
    grad_inner = product_left(first_low, grad_inner_act)
    grad_first = grad_second + product_right(grad_inner_act, wi)
    first_value, first_back = jax.vjp(layer_norm, mixed_rows, gain_full[0], bias_full[0])
    grad_mixed, gain_first, bias_first = first_back(grad_first)
    grad_branch = grad_mixed.astype(jnp.bfloat16)
    grad_output = product_left(attended, grad_branch)
    grad_attended = product_right(grad_branch, wo).astype(jnp.bfloat16)
    early, grad_attended = reduce_seq_stage((grad_output, grad_inner, grad_outer.T), grad_attended)
    early_reduced, early_widths = early

    grad_rows = grad_attended.reshape(groups, shard_rows, width)
    key_phase = phase_weights(pool_full[0], group_len)
    value_phase = phase_weights(pool_full[1], group_len)
    pieces_back = []
    for g in range(groups):
        saved_g = tuple(item[g : g + 1] for item in att_saved)
        starts_g = tuple(item[g : g + 1] for item in starts)
        grad_g = grad_rows[g].reshape(shard_rows, width)
        grad_queries_g, full_g, pooled_g, unpooled_g = attention_bwd(grad_g, saved_g, starts_g, seq_index)
        if g == 1:
            full_g, pooled_g, unpooled_g, earlier_back, early_reduced = lax.optimization_barrier(
                (full_g, pooled_g, unpooled_g, pieces_back[0][4], early_reduced)
            )
            pieces_back[0] = pieces_back[0][:4] + (earlier_back,)
        key_partial_g = (
            full_g[0, :, :width] + unpooled_g[0, :, :width] * key_phase
        ).astype(jnp.bfloat16)
        value_partial_g = (
            full_g[0, :, width:] + unpooled_g[0, :, width:] * value_phase
        ).astype(jnp.bfloat16)
        if g == groups - 1:
            back_own_g = None
        else:
            back_own_g = back_projection(key_partial_g, value_partial_g, wk, wv)
        pieces_back.append((grad_queries_g, pooled_g, key_partial_g, value_partial_g, back_own_g))
    grad_queries = jnp.concatenate([piece[0] for piece in pieces_back], axis=0)
    grad_pooled = jnp.concatenate([piece[1] for piece in pieces_back], axis=0)
    key_partial = jnp.concatenate([piece[2] for piece in pieces_back], axis=0)
    value_partial = jnp.concatenate([piece[3] for piece in pieces_back], axis=0)
    early_dp = reduce_dp_stage(((early_reduced, early_widths),))
    grad_pooling = jnp.stack(
        [
            pool_grad_grouped(grad_pooled[..., :width], key_g),
            pool_grad_grouped(grad_pooled[..., width:], value_g),
        ]
    )
    grad_query_w = product_left(tokens, grad_queries)
    grad_key_w = product_left(all_tokens, key_partial)
    grad_value_w = product_left(all_tokens, value_partial)
    late_stacked, late_widths = stack_for_seq((grad_query_w, grad_key_w, grad_value_w))
    late_stacked, early_dp, last_keys, last_values = lax.optimization_barrier(
        (late_stacked, early_dp, pieces_back[-1][2], pieces_back[-1][3])
    )
    seq_size = lax.psum(1, "seq")
    dp_size = lax.psum(1, "dp")
    rows_each = late_stacked.shape[0] // seq_size
    late_blocks = late_stacked.reshape(seq_size, rows_each, dp_size, late_stacked.shape[2])
    late_blocks = jnp.transpose(late_blocks, (2, 0, 1, 3)).reshape(-1, late_stacked.shape[2])
    late_reduced = lax.psum_scatter(late_blocks, ("dp", "seq"), scatter_dimension=0, tiled=True)
    late_reduced = late_reduced.astype(jnp.float32)
    late_dp, at = [], 0
    for width_piece in late_widths:
        late_dp.append(late_reduced[:, at : at + width_piece])
        at += width_piece
    last_own = back_projection(last_keys, last_values, wk, wv)
    back_own = jnp.concatenate([piece[4] for piece in pieces_back[:-1]] + [last_own], axis=0)
    grad_tokens = (
        grad_mixed
        + product_right(grad_queries, wq)
        + back_own.reshape(groups * shard_rows, width).astype(jnp.float32)
    )
    accum = (late_dp[0], late_dp[1], late_dp[2], early_dp[0], early_dp[1], early_dp[2].T)
    small_sums = (
        lax.psum_scatter(grad_pooling, ("dp", "seq"), scatter_dimension=2, tiled=True),
        lax.psum_scatter(
            jnp.stack([gain_first, gain_second]), ("dp", "seq"), scatter_dimension=1, tiled=True
        ),
        lax.psum_scatter(
            jnp.stack([bias_first, bias_second]), ("dp", "seq"), scatter_dimension=1, tiled=True
        ),
    )
    return (
        output.reshape(groups, shard_rows, width),
        grad_tokens.astype(jnp.bfloat16).reshape(groups, shard_rows, width),
        accum[0],
        accum[1],
        accum[2],
        accum[3],
        accum[4],
        accum[5],
        small_sums[0],
        small_sums[1],
        small_sums[2],
    )


def solution(mesh):
    in_specs = (
        P("dp", "seq", None),
        P("seq", "dp"),
        P("seq", "dp"),
        P("seq", "dp"),
        P("seq", "dp"),
        P("seq", "dp"),
        P("dp", "seq"),
        P(None, None, ("dp", "seq")),
        P(None, ("dp", "seq")),
        P(None, ("dp", "seq")),
        P("dp", None),
        P("dp", "seq", None),
    )
    out_specs = (
        P("dp", "seq", None),
        P("dp", "seq", None),
        P("seq", "dp"),
        P("seq", "dp"),
        P("seq", "dp"),
        P("seq", "dp"),
        P("seq", "dp"),
        P("dp", "seq"),
        P(None, None, ("dp", "seq")),
        P(None, ("dp", "seq")),
        P(None, ("dp", "seq")),
    )
    return jax.shard_map(local, mesh=mesh, in_specs=in_specs, out_specs=out_specs, check_vma=False)
```

```python
from functools import partial

import jax
import jax.numpy as jnp
from jax import lax
from jax.sharding import PartitionSpec as P

HEADS = 12
HEAD_DIM = 64
PROMPT = 1024
CONT = 8
CLEN = 128
WINDOW = 128
POOL_SPAN = 512
STRIDE = 4


eps_norm = 1e-05


def token_layout(positions_in, offsets):
    in_prompt = positions_in < PROMPT
    segment = jnp.where(in_prompt, -1, (positions_in - PROMPT) // CLEN)
    within = positions_in - PROMPT - segment * CLEN
    choose = (segment[:, None] == jnp.arange(CONT, dtype=jnp.int32)[None, :]).astype(jnp.int32)
    cont_start = jnp.sum(choose * offsets[None, :], axis=1)
    position = jnp.where(in_prompt, positions_in, cont_start + within)
    prompt_limit = jnp.where(in_prompt, PROMPT, cont_start)
    return (segment, position, prompt_limit)


def visible_keys(query_rows, key_index, offsets, reach):
    query_seg, query_pos, query_limit = token_layout(query_rows, offsets)
    key_seg, key_pos, key_limit = token_layout(key_index, offsets)
    prompt_key = (key_seg[None, :] < 0) & (key_pos[None, :] < query_limit[:, None])
    own_key = (key_seg[None, :] == query_seg[:, None]) & (query_seg[:, None] >= 0)
    distance = key_pos[None, :] - query_pos[:, None]
    return (prompt_key | own_key) & (distance >= -(reach // 2)) & (distance < reach // 2)


def key_mask(query_rows, offsets):
    group_len = PROMPT + CONT * CLEN
    full_keys = jnp.arange(group_len, dtype=jnp.int32)
    pooled_keys = jnp.arange(group_len // STRIDE, dtype=jnp.int32) * STRIDE
    return jnp.concatenate(
        [
            visible_keys(query_rows, full_keys, offsets, WINDOW),
            visible_keys(query_rows, pooled_keys, offsets, POOL_SPAN),
        ],
        axis=1,
    )


def pool_rows(source, weight):
    return jnp.sum(
        source.reshape(source.shape[0] // STRIDE, STRIDE, source.shape[1]) * weight[None, :, :],
        axis=1,
    )


def unpool(pooled_grad, weight):
    return (pooled_grad[:, None, :] * weight[None, :, :]).reshape(-1, pooled_grad.shape[1])


def pool_grad(pooled_grad, source):
    blocks_view = source.astype(jnp.float32).reshape(-1, STRIDE, source.shape[1])
    return jnp.sum(pooled_grad[:, None, :] * blocks_view, axis=0)


def layer_norm(source, gain, bias):
    centre = jnp.mean(source, axis=-1, keepdims=True)
    centred = source - centre
    spread = jnp.mean(centred * centred, axis=-1, keepdims=True)
    return centred * lax.rsqrt(spread + eps_norm) * gain + bias


def product(left, right):
    return jnp.dot(left, right, preferred_element_type=jnp.float32)


def product_left(left, right):
    return lax.dot_general(
        left, right, (((0,), (0,)), ((), ())), preferred_element_type=jnp.float32
    )


def product_right(left, right):
    return lax.dot_general(
        left, right, (((1,), (1,)), ((), ())), preferred_element_type=jnp.float32
    )


def add_pair(left_term, right_term):
    return left_term + right_term


def gather_grouped(shards, tie=None):
    local_block = jnp.concatenate(shards, axis=1)
    across = lax.all_gather(local_block, "dp", axis=1, tiled=False)
    across, tie = lax.optimization_barrier((across, tie))
    return lax.all_gather(across, "seq", axis=0, tiled=True), tie


def split_grouped(gathered, widths):
    pieces, at = [], 0
    for width in widths:
        piece = gathered[:, :, at : at + width]
        pieces.append(piece.reshape(piece.shape[0], -1))
        at += width
    return pieces


def code_exact(values, rows):
    parts, rest = [], values
    for _ in range(3):
        part = lax.optimization_barrier(rest.astype(jnp.bfloat16))
        parts.append(part)
        rest = rest - part.astype(jnp.float32)
    flat = jnp.concatenate([part.reshape(-1) for part in parts])
    columns = -(-flat.shape[0] // rows)
    flat = jnp.pad(flat, (0, rows * columns - flat.shape[0]))
    return flat.reshape(rows, columns)


def decode_exact(gathered, count, shape):
    seq_size = lax.psum(1, "seq")
    rows = gathered.shape[0] // seq_size
    blocks = gathered.reshape(seq_size, rows, gathered.shape[1], gathered.shape[2])
    blocks = jnp.transpose(blocks, (2, 0, 1, 3)).reshape(-1, rows * gathered.shape[2])
    parts = blocks[:, : 3 * count].reshape(blocks.shape[0], 3, shape[0], shape[1])
    parts = parts.astype(jnp.float32)
    joined = (parts[:, 0] + parts[:, 1]) + parts[:, 2]
    return jnp.transpose(joined, (1, 0, 2)).reshape(shape[0], -1)


def gather_first(w_query, w_key, w_value, small_local, tie):
    coded = code_exact(small_local, w_query.shape[0])
    first, tie = gather_grouped((w_query, w_key, w_value, coded), tie)
    widths = (w_query.shape[1], w_key.shape[1], w_value.shape[1])
    at = sum(widths)
    small_full = decode_exact(first[:, :, at:], small_local.size, small_local.shape)
    return split_grouped(first[:, :, :at], widths), small_full, tie


def gather_second(w_output, w_inner, w_outer):
    second, _ = gather_grouped((w_output, w_inner, w_outer.T))
    wo, wi, wu_t = split_grouped(second, (w_output.shape[1], w_inner.shape[1], w_outer.shape[0]))
    return (wo, wi, wu_t.T)


def reduce_seq_stage(grads, tie=None):
    dp_size = lax.psum(1, "dp")
    chunks = [grad.reshape(grad.shape[0], dp_size, grad.shape[1] // dp_size) for grad in grads]
    stacked = jnp.concatenate(chunks, axis=2).astype(jnp.bfloat16)
    stacked, tie = lax.optimization_barrier((stacked, tie))
    reduced = lax.psum_scatter(stacked, "seq", scatter_dimension=0, tiled=True)
    return (reduced, [c.shape[2] for c in chunks]), tie


def stack_for_seq(grads):
    dp_size = lax.psum(1, "dp")
    chunks = [grad.reshape(grad.shape[0], dp_size, grad.shape[1] // dp_size) for grad in grads]
    return jnp.concatenate(chunks, axis=2).astype(jnp.bfloat16), [c.shape[2] for c in chunks]


def reduce_dp_stage(stages):
    joined = jnp.concatenate([stage for stage, _ in stages], axis=2)
    over_dp = lax.psum_scatter(joined, "dp", scatter_dimension=1, tiled=True)[:, 0].astype(jnp.float32)
    pieces, at = [], 0
    for _, widths in stages:
        for width in widths:
            pieces.append(over_dp[:, at : at + width])
            at += width
    return pieces


HALF_FULL = WINDOW // 2
HALF_POOL = POOL_SPAN // 2 // STRIDE
BLOCK_POOL = CLEN // STRIDE


def layout_of(index, offsets):
    in_prompt = index < PROMPT
    segment = jnp.where(in_prompt, -1, (index - PROMPT) // CLEN)
    within = index - PROMPT - segment * CLEN
    choose = segment[..., None] == jnp.arange(CONT, dtype=jnp.int32)
    spread = offsets.reshape(offsets.shape[:1] + (1,) * (index.ndim - 1) + offsets.shape[1:])
    cont_start = jnp.sum(jnp.where(choose, spread, 0), axis=-1)
    position = jnp.where(in_prompt, index, cont_start + within)
    limit = jnp.where(in_prompt, PROMPT, cont_start)
    return segment, position, limit


def window_rows(source, starts, length):
    groups, blocks = starts.shape
    return jnp.stack(
        [
            jnp.stack(
                [lax.dynamic_slice_in_dim(source[g], starts[g, b], length, 0) for b in range(blocks)]
            )
            for g in range(groups)
        ]
    )


def window_add(target, updates, starts):
    groups, blocks = starts.shape
    length = updates.shape[2]
    rows = []
    for g in range(groups):
        row = target[g]
        for b in range(blocks):
            start = starts[g, b]
            current = lax.dynamic_slice_in_dim(row, start, length, 0)
            row = lax.dynamic_update_slice_in_dim(row, current + updates[g, b], start, 0)
        rows.append(row)
    return jnp.stack(rows)


def block_geometry(seq_index, groups, shard_rows, offsets):
    group_len = PROMPT + CONT * CLEN
    pooled_len = group_len // STRIDE
    blocks = shard_rows // CLEN
    block_start = (seq_index * blocks + jnp.arange(blocks, dtype=jnp.int32)) * CLEN
    prompt_block = block_start < PROMPT
    cont_index = jnp.clip((block_start - PROMPT) // CLEN, 0, CONT - 1)
    anchor = jnp.where(prompt_block[None, :], block_start[None, :], offsets[:, cont_index])
    pooled_start = block_start // STRIDE
    intended = (
        anchor - HALF_FULL,
        jnp.broadcast_to(block_start + CLEN, anchor.shape),
        anchor // STRIDE - HALF_POOL,
        jnp.broadcast_to(pooled_start + BLOCK_POOL, anchor.shape),
    )
    limits = (group_len, group_len, pooled_len, pooled_len)
    lengths = (HALF_FULL, HALF_FULL, HALF_POOL, HALF_POOL)
    clamped = tuple(
        jnp.clip(start, 0, limit - length) for start, limit, length in zip(intended, limits, lengths)
    )
    ramp = lambda n: jnp.arange(n, dtype=jnp.int32)

    def span(window):
        actual = clamped[window][:, :, None] + ramp(lengths[window])
        offset = actual - intended[window][:, :, None]
        return actual, (offset >= 0) & (offset < lengths[window])

    before_full, before_full_ok = span(0)
    after_full, after_full_ok = span(1)
    before_pool, before_pool_ok = span(2)
    after_pool, after_pool_ok = span(3)
    after_ok = prompt_block[None, :, None]
    own_full = jnp.broadcast_to(block_start[None, :, None] + ramp(CLEN), anchor.shape + (CLEN,))
    own_pool = jnp.broadcast_to(
        pooled_start[None, :, None] + ramp(BLOCK_POOL), anchor.shape + (BLOCK_POOL,)
    )
    full_index = jnp.concatenate([before_full, own_full, after_full], axis=2)
    pooled_index = jnp.concatenate([before_pool, own_pool, after_pool], axis=2)
    full_valid = jnp.concatenate(
        [before_full_ok, jnp.ones(own_full.shape, bool), after_ok & after_full_ok], axis=2
    )
    pooled_valid = jnp.concatenate(
        [before_pool_ok, jnp.ones(own_pool.shape, bool), after_ok & after_pool_ok], axis=2
    )
    query_index = block_start[None, :, None] + ramp(CLEN)
    query_index = jnp.broadcast_to(query_index, anchor.shape + (CLEN,))
    q_seg, q_pos, q_lim = layout_of(query_index, offsets)

    def visible(key_token, valid, reach):
        k_seg, k_pos, _ = layout_of(key_token, offsets)
        k_seg, k_pos, valid = k_seg[:, :, None, :], k_pos[:, :, None, :], valid[:, :, None, :]
        prompt_key = (k_seg < 0) & (k_pos < q_lim[..., None])
        own_key = (k_seg == q_seg[..., None]) & (q_seg[..., None] >= 0)
        distance = k_pos - q_pos[..., None]
        return valid & (prompt_key | own_key) & (distance >= -(reach // 2)) & (distance < reach // 2)

    mask = jnp.concatenate(
        [
            visible(full_index, full_valid, WINDOW),
            visible(pooled_index * STRIDE, pooled_valid, POOL_SPAN),
        ],
        axis=3,
    )
    return clamped, mask


def attention_fwd(queries, kv_local, pkv_local, kv_all, pkv_all, starts, mask):
    groups, shard_rows, width = queries.shape
    blocks = shard_rows // CLEN
    score_scale = 1.0 / HEAD_DIM**0.5
    keys_cat = jnp.concatenate(
        [
            window_rows(kv_all, starts[0], HALF_FULL),
            kv_local.reshape(groups, blocks, CLEN, 2 * width),
            window_rows(kv_all, starts[1], HALF_FULL),
            window_rows(pkv_all, starts[2], HALF_POOL),
            pkv_local.reshape(groups, blocks, BLOCK_POOL, 2 * width),
            window_rows(pkv_all, starts[3], HALF_POOL),
        ],
        axis=2,
    )
    span = keys_cat.shape[2]
    head_keys = keys_cat[..., :width].reshape(groups, blocks, span, HEADS, HEAD_DIM)
    head_values = keys_cat[..., width:].reshape(groups, blocks, span, HEADS, HEAD_DIM)
    head_query = queries.reshape(groups, blocks, CLEN, HEADS, HEAD_DIM)
    scores = jnp.einsum(
        "gbqhd,gbkhd->gbhqk", head_query, head_keys, preferred_element_type=jnp.float32
    )
    scores = jnp.where(mask[:, :, None], scores * score_scale, -1000000000.0)
    row_top = jnp.max(scores, axis=-1, keepdims=True)
    exponent = jnp.exp(scores - row_top)
    row_total = jnp.sum(exponent, axis=-1, keepdims=True)
    probs = exponent / row_total
    attended = jnp.einsum(
        "gbhqk,gbkhd->gbqhd",
        probs.astype(jnp.bfloat16),
        head_values,
        preferred_element_type=jnp.float32,
    )
    attended = attended.reshape(groups * shard_rows, width).astype(jnp.bfloat16)
    return attended, (head_query, head_keys, head_values, probs)


def attention_bwd(grad_attended, saved, starts, seq_index):
    head_query, head_keys, head_values, probs = saved
    groups, blocks = head_query.shape[:2]
    width = HEADS * HEAD_DIM
    score_scale = 1.0 / HEAD_DIM**0.5
    head_grad = grad_attended.reshape(groups, blocks, CLEN, HEADS, HEAD_DIM)
    grad_probs = jnp.einsum(
        "gbqhd,gbkhd->gbhqk", head_grad, head_values, preferred_element_type=jnp.float32
    )
    centre = jnp.sum(probs * grad_probs, axis=-1, keepdims=True)
    grad_scores = (probs * (grad_probs - centre)).astype(jnp.bfloat16)
    grad_queries = jnp.einsum(
        "gbhqk,gbkhd->gbqhd", grad_scores, head_keys, preferred_element_type=jnp.float32
    ) * score_scale
    grad_keys = jnp.einsum(
        "gbhqk,gbqhd->gbkhd", grad_scores, head_query, preferred_element_type=jnp.float32
    ) * score_scale
    grad_values = jnp.einsum(
        "gbhqk,gbqhd->gbkhd",
        probs.astype(jnp.bfloat16),
        head_grad,
        preferred_element_type=jnp.float32,
    )
    span = grad_keys.shape[2]
    grad_kv = jnp.concatenate(
        [grad_keys.reshape(groups, blocks, span, width), grad_values.reshape(groups, blocks, span, width)],
        axis=3,
    )
    shard_rows = blocks * CLEN
    group_len = PROMPT + CONT * CLEN
    pooled_len = group_len // STRIDE
    cut = (0, HALF_FULL, HALF_FULL + CLEN, 2 * HALF_FULL + CLEN)
    pcut = tuple(cut[-1] + c for c in (0, HALF_POOL, HALF_POOL + BLOCK_POOL, 2 * HALF_POOL + BLOCK_POOL))
    ramp = lambda n: jnp.arange(n, dtype=jnp.int32)
    own_full = grad_kv[:, :, cut[1] : cut[2]].reshape(groups, shard_rows, 2 * width)
    full = jnp.zeros((groups, group_len, 2 * width), jnp.float32)
    full = lax.dynamic_update_slice_in_dim(full, own_full, seq_index * shard_rows, 1)
    side_values = jnp.concatenate(
        [grad_kv[:, :, cut[0] : cut[1]], grad_kv[:, :, cut[2] : cut[3]]], axis=2
    ).reshape(groups, -1, 2 * width)
    side_rows = jnp.concatenate(
        [starts[0][:, :, None] + ramp(HALF_FULL), starts[1][:, :, None] + ramp(HALF_FULL)], axis=2
    ).reshape(groups, -1)
    own_pool_rows = (seq_index * (shard_rows // STRIDE) + ramp(blocks)[:, None] * BLOCK_POOL + ramp(BLOCK_POOL))
    pool_values = grad_kv[:, :, pcut[0] : pcut[3]].reshape(groups, -1, 2 * width)
    pool_rows_index = jnp.concatenate(
        [
            starts[2][:, :, None] + ramp(HALF_POOL),
            jnp.broadcast_to(own_pool_rows[None], (groups, blocks, BLOCK_POOL)),
            starts[3][:, :, None] + ramp(HALF_POOL),
        ],
        axis=2,
    ).reshape(groups, -1)
    fulls, pooleds, unpooleds = [], [], []
    for g in range(groups):
        fulls.append(full[g] + select_sum(side_values[g], side_rows[g] == ramp(group_len)[:, None]))
        pooleds.append(select_sum(pool_values[g], pool_rows_index[g] == ramp(pooled_len)[:, None]))
        unpooleds.append(
            product(
                (pool_rows_index[g] == (ramp(group_len) // STRIDE)[:, None]).astype(jnp.bfloat16),
                pool_values[g].astype(jnp.bfloat16),
            )
        )
    full = jnp.stack(fulls)
    pooled = jnp.stack(pooleds)
    unpooled = jnp.stack(unpooleds)
    grad_queries = grad_queries.reshape(groups * shard_rows, width).astype(jnp.bfloat16)
    return grad_queries, full, pooled, unpooled


def select_sum(values, chosen):
    onehot = chosen.astype(jnp.bfloat16)
    high = values.astype(jnp.bfloat16)
    low = (values - high.astype(jnp.float32)).astype(jnp.bfloat16)
    return product(onehot, high) + product(onehot, low)


def phase_weights(weight, rows):
    phase = (jnp.arange(rows, dtype=jnp.int32) % STRIDE)[:, None]
    total = jnp.zeros((rows, weight.shape[1]), jnp.float32)
    for r in range(STRIDE):
        total = total + jnp.where(phase == r, weight[r][None, :], 0.0)
    return total


def pool_grouped(source, weight):
    groups, rows, width = source.shape
    return jnp.sum(
        source.reshape(groups, rows // STRIDE, STRIDE, width) * weight[None, None], axis=2
    )


def unpool_grouped(pooled_grad, weight):
    groups, rows, width = pooled_grad.shape
    return (pooled_grad[:, :, None, :] * weight[None, None]).reshape(groups, rows * STRIDE, width)


def pool_grad_grouped(pooled_grad, source):
    groups, rows, width = source.shape
    blocks_view = source.astype(jnp.float32).reshape(groups, rows // STRIDE, STRIDE, width)
    return jnp.sum(pooled_grad[:, :, None, :] * blocks_view, axis=(0, 1))


def local(
    hidden_in,
    w_query,
    w_key,
    w_value,
    w_output,
    w_inner,
    w_outer,
    pool_weight,
    ln_gain,
    ln_bias,
    branch_blocks,
    grad_out,
):
    pool_rows_count = pool_weight.shape[0] * pool_weight.shape[1]
    small_local = jnp.concatenate(
        [pool_weight.reshape(pool_rows_count, -1), ln_gain, ln_bias], axis=0
    )
    hidden_all = lax.all_gather(hidden_in, "seq", axis=1, tiled=True)
    groups, shard_rows, width = hidden_in.shape
    seq_index = lax.axis_index("seq")
    offsets = STRIDE * branch_blocks
    starts, mask = block_geometry(seq_index, groups, shard_rows, offsets)
    (wq, wk, wv), small_full, (hidden_all, starts, mask) = gather_first(
        w_query, w_key, w_value, small_local, (hidden_all, starts, mask)
    )
    pool_full = small_full[:pool_rows_count].reshape(pool_weight.shape[0], pool_weight.shape[1], -1)
    gain_full = small_full[pool_rows_count : pool_rows_count + ln_gain.shape[0]]
    bias_full = small_full[pool_rows_count + ln_gain.shape[0] :]
    groups, shard_rows, width = hidden_in.shape

    group_len = hidden_all.shape[1]
    tokens = hidden_in.reshape(groups * shard_rows, width)
    all_tokens = hidden_all.reshape(groups * group_len, width)
    queries = product(tokens, wq).astype(jnp.bfloat16)
    key_g = product(all_tokens, wk).astype(jnp.bfloat16).reshape(groups, group_len, width)
    value_g = product(all_tokens, wv).astype(jnp.bfloat16).reshape(groups, group_len, width)
    pooled_keys = pool_grouped(key_g.astype(jnp.float32), pool_full[0]).astype(jnp.bfloat16)
    pooled_values = pool_grouped(value_g.astype(jnp.float32), pool_full[1]).astype(jnp.bfloat16)
    kv_all = jnp.concatenate([key_g, value_g], axis=2)
    pkv_all = jnp.concatenate([pooled_keys, pooled_values], axis=2)
    kv_local = lax.dynamic_slice_in_dim(kv_all, seq_index * shard_rows, shard_rows, 1)
    pkv_local = lax.dynamic_slice_in_dim(
        pkv_all, seq_index * (shard_rows // STRIDE), shard_rows // STRIDE, 1
    )
    wq, wk, wv, w_output, w_inner, w_outer = lax.optimization_barrier(
        (wq, wk, wv, w_output, w_inner, w_outer)
    )
    wo, wi, wu = gather_second(w_output, w_inner, w_outer)
    attended, att_saved = attention_fwd(
        queries.reshape(groups, shard_rows, width), kv_local, pkv_local, kv_all, pkv_all, starts, mask
    )
    mixed_rows = tokens.astype(jnp.float32) + product(attended, wo)
    normed_first = layer_norm(mixed_rows, gain_full[0], bias_full[0])
    first_low = normed_first.astype(jnp.bfloat16)
    inner_act = product(first_low, wi)
    active = jax.nn.gelu(inner_act, approximate=False).astype(jnp.bfloat16)
    second = normed_first + product(active, wu)
    norm_value, second_back = jax.vjp(layer_norm, second, gain_full[1], bias_full[1])
    output = norm_value.astype(jnp.bfloat16)

    cotangent = grad_out.reshape(groups * shard_rows, width).astype(jnp.float32)
    grad_second, gain_second, bias_second = second_back(cotangent)
    grad_ffn_out = grad_second.astype(jnp.bfloat16)
    grad_outer = product_left(active, grad_ffn_out)
    grad_active = product_right(grad_ffn_out, wu)
    gelu_value, gelu_back = jax.vjp(partial(jax.nn.gelu, approximate=False), inner_act)
    grad_inner_act = gelu_back(grad_active)[0].astype(jnp.bfloat16)
    grad_inner = product_left(first_low, grad_inner_act)
    grad_first = grad_second + product_right(grad_inner_act, wi)
    first_value, first_back = jax.vjp(layer_norm, mixed_rows, gain_full[0], bias_full[0])
    grad_mixed, gain_first, bias_first = first_back(grad_first)
    grad_branch = grad_mixed.astype(jnp.bfloat16)
    grad_output = product_left(attended, grad_branch)
    grad_attended = product_right(grad_branch, wo).astype(jnp.bfloat16)
    early, grad_attended = reduce_seq_stage((grad_output, grad_inner, grad_outer.T), grad_attended)
    early_reduced, early_widths = early

    grad_rows = grad_attended.reshape(groups, shard_rows, width)
    key_phase = phase_weights(pool_full[0], group_len)
    value_phase = phase_weights(pool_full[1], group_len)
    pieces_back = []
    for g in range(groups):
        saved_g = tuple(item[g : g + 1] for item in att_saved)
        starts_g = tuple(item[g : g + 1] for item in starts)
        grad_g = grad_rows[g].reshape(shard_rows, width)
        grad_queries_g, full_g, pooled_g, unpooled_g = attention_bwd(grad_g, saved_g, starts_g, seq_index)
        if g == 1:
            full_g, pooled_g, unpooled_g, earlier_back, early_reduced = lax.optimization_barrier(
                (full_g, pooled_g, unpooled_g, pieces_back[0][4], early_reduced)
            )
            pieces_back[0] = pieces_back[0][:4] + (earlier_back,)
        key_partial_g = (
            full_g[0, :, :width] + unpooled_g[0, :, :width] * key_phase
        ).astype(jnp.bfloat16)
        value_partial_g = (
            full_g[0, :, width:] + unpooled_g[0, :, width:] * value_phase
        ).astype(jnp.bfloat16)
        back_g = product_right(key_partial_g, wk) + product_right(value_partial_g, wv)
        back_g = back_g.reshape(1, group_len, width).astype(jnp.bfloat16)
        back_own_g = lax.psum_scatter(back_g, "seq", scatter_dimension=1, tiled=True)
        pieces_back.append((grad_queries_g, pooled_g, key_partial_g, value_partial_g, back_own_g))
    grad_queries = jnp.concatenate([piece[0] for piece in pieces_back], axis=0)
    grad_pooled = jnp.concatenate([piece[1] for piece in pieces_back], axis=0)
    key_partial = jnp.concatenate([piece[2] for piece in pieces_back], axis=0)
    value_partial = jnp.concatenate([piece[3] for piece in pieces_back], axis=0)
    last_back = pieces_back[-1][4]
    early_dp = reduce_dp_stage(((early_reduced, early_widths),))
    grad_pooling = jnp.stack(
        [
            pool_grad_grouped(grad_pooled[..., :width], key_g),
            pool_grad_grouped(grad_pooled[..., width:], value_g),
        ]
    )
    grad_query_w = product_left(tokens, grad_queries)
    grad_key_w = product_left(all_tokens, key_partial)
    grad_value_w = product_left(all_tokens, value_partial)
    late_stacked, late_widths = stack_for_seq((grad_query_w, grad_key_w, grad_value_w))
    late_stacked, early_dp = lax.optimization_barrier((late_stacked, early_dp))
    seq_size = lax.psum(1, "seq")
    dp_size = lax.psum(1, "dp")
    rows_each = late_stacked.shape[0] // seq_size
    late_blocks = late_stacked.reshape(seq_size, rows_each, dp_size, late_stacked.shape[2])
    late_blocks = jnp.transpose(late_blocks, (2, 0, 1, 3)).reshape(-1, late_stacked.shape[2])
    late_reduced = lax.psum_scatter(late_blocks, ("dp", "seq"), scatter_dimension=0, tiled=True)
    late_reduced = late_reduced.astype(jnp.float32)
    late_dp, at = [], 0
    for width_piece in late_widths:
        late_dp.append(late_reduced[:, at : at + width_piece])
        at += width_piece
    back_own = jnp.concatenate([piece[4] for piece in pieces_back], axis=0)
    grad_tokens = (
        grad_mixed
        + product_right(grad_queries, wq)
        + back_own.reshape(groups * shard_rows, width).astype(jnp.float32)
    )
    accum = (late_dp[0], late_dp[1], late_dp[2], early_dp[0], early_dp[1], early_dp[2].T)
    small_sums = (
        lax.psum_scatter(grad_pooling, ("dp", "seq"), scatter_dimension=2, tiled=True),
        lax.psum_scatter(
            jnp.stack([gain_first, gain_second]), ("dp", "seq"), scatter_dimension=1, tiled=True
        ),
        lax.psum_scatter(
            jnp.stack([bias_first, bias_second]), ("dp", "seq"), scatter_dimension=1, tiled=True
        ),
    )
    return (
        output.reshape(groups, shard_rows, width),
        grad_tokens.astype(jnp.bfloat16).reshape(groups, shard_rows, width),
        accum[0],
        accum[1],
        accum[2],
        accum[3],
        accum[4],
        accum[5],
        small_sums[0],
        small_sums[1],
        small_sums[2],
    )


def solution(mesh):
    in_specs = (
        P("dp", "seq", None),
        P("seq", "dp"),
        P("seq", "dp"),
        P("seq", "dp"),
        P("seq", "dp"),
        P("seq", "dp"),
        P("dp", "seq"),
        P(None, None, ("dp", "seq")),
        P(None, ("dp", "seq")),
        P(None, ("dp", "seq")),
        P("dp", None),
        P("dp", "seq", None),
    )
    out_specs = (
        P("dp", "seq", None),
        P("dp", "seq", None),
        P("seq", "dp"),
        P("seq", "dp"),
        P("seq", "dp"),
        P("seq", "dp"),
        P("seq", "dp"),
        P("dp", "seq"),
        P(None, None, ("dp", "seq")),
        P(None, ("dp", "seq")),
        P(None, ("dp", "seq")),
    )
    return jax.shard_map(local, mesh=mesh, in_specs=in_specs, out_specs=out_specs, check_vma=False)
```

```python
from functools import partial

import jax
import jax.numpy as jnp
from jax import lax
from jax.sharding import PartitionSpec as P

HEADS = 12
HEAD_DIM = 64
PROMPT = 1024
CONT = 8
CLEN = 128
WINDOW = 128
POOL_SPAN = 512
STRIDE = 4


eps_norm = 1e-05


def token_layout(positions_in, offsets):
    in_prompt = positions_in < PROMPT
    segment = jnp.where(in_prompt, -1, (positions_in - PROMPT) // CLEN)
    within = positions_in - PROMPT - segment * CLEN
    choose = (segment[:, None] == jnp.arange(CONT, dtype=jnp.int32)[None, :]).astype(jnp.int32)
    cont_start = jnp.sum(choose * offsets[None, :], axis=1)
    position = jnp.where(in_prompt, positions_in, cont_start + within)
    prompt_limit = jnp.where(in_prompt, PROMPT, cont_start)
    return (segment, position, prompt_limit)


def visible_keys(query_rows, key_index, offsets, reach):
    query_seg, query_pos, query_limit = token_layout(query_rows, offsets)
    key_seg, key_pos, key_limit = token_layout(key_index, offsets)
    prompt_key = (key_seg[None, :] < 0) & (key_pos[None, :] < query_limit[:, None])
    own_key = (key_seg[None, :] == query_seg[:, None]) & (query_seg[:, None] >= 0)
    distance = key_pos[None, :] - query_pos[:, None]
    return (prompt_key | own_key) & (distance >= -(reach // 2)) & (distance < reach // 2)


def key_mask(query_rows, offsets):
    group_len = PROMPT + CONT * CLEN
    full_keys = jnp.arange(group_len, dtype=jnp.int32)
    pooled_keys = jnp.arange(group_len // STRIDE, dtype=jnp.int32) * STRIDE
    return jnp.concatenate(
        [
            visible_keys(query_rows, full_keys, offsets, WINDOW),
            visible_keys(query_rows, pooled_keys, offsets, POOL_SPAN),
        ],
        axis=1,
    )


def pool_rows(source, weight):
    return jnp.sum(
        source.reshape(source.shape[0] // STRIDE, STRIDE, source.shape[1]) * weight[None, :, :],
        axis=1,
    )


def unpool(pooled_grad, weight):
    return (pooled_grad[:, None, :] * weight[None, :, :]).reshape(-1, pooled_grad.shape[1])


def pool_grad(pooled_grad, source):
    blocks_view = source.astype(jnp.float32).reshape(-1, STRIDE, source.shape[1])
    return jnp.sum(pooled_grad[:, None, :] * blocks_view, axis=0)


def layer_norm(source, gain, bias):
    centre = jnp.mean(source, axis=-1, keepdims=True)
    centred = source - centre
    spread = jnp.mean(centred * centred, axis=-1, keepdims=True)
    return centred * lax.rsqrt(spread + eps_norm) * gain + bias


def product(left, right):
    return jnp.dot(left, right, preferred_element_type=jnp.float32)


def product_left(left, right):
    return lax.dot_general(
        left, right, (((0,), (0,)), ((), ())), preferred_element_type=jnp.float32
    )


def product_right(left, right):
    return lax.dot_general(
        left, right, (((1,), (1,)), ((), ())), preferred_element_type=jnp.float32
    )


def add_pair(left_term, right_term):
    return left_term + right_term


def gather_grouped(shards, tie=None):
    local_block = jnp.concatenate(shards, axis=1)
    across = lax.all_gather(local_block, "dp", axis=1, tiled=False)
    across, tie = lax.optimization_barrier((across, tie))
    return lax.all_gather(across, "seq", axis=0, tiled=True), tie


def split_grouped(gathered, widths):
    pieces, at = [], 0
    for width in widths:
        piece = gathered[:, :, at : at + width]
        pieces.append(piece.reshape(piece.shape[0], -1))
        at += width
    return pieces


def code_exact(values, rows):
    parts, rest = [], values
    for _ in range(3):
        part = lax.optimization_barrier(rest.astype(jnp.bfloat16))
        parts.append(part)
        rest = rest - part.astype(jnp.float32)
    flat = jnp.concatenate([part.reshape(-1) for part in parts])
    columns = -(-flat.shape[0] // rows)
    flat = jnp.pad(flat, (0, rows * columns - flat.shape[0]))
    return flat.reshape(rows, columns)


def decode_exact(gathered, count, shape):
    seq_size = lax.psum(1, "seq")
    rows = gathered.shape[0] // seq_size
    blocks = gathered.reshape(seq_size, rows, gathered.shape[1], gathered.shape[2])
    blocks = jnp.transpose(blocks, (2, 0, 1, 3)).reshape(-1, rows * gathered.shape[2])
    parts = blocks[:, : 3 * count].reshape(blocks.shape[0], 3, shape[0], shape[1])
    parts = parts.astype(jnp.float32)
    joined = (parts[:, 0] + parts[:, 1]) + parts[:, 2]
    return jnp.transpose(joined, (1, 0, 2)).reshape(shape[0], -1)


def gather_first(w_query, w_key, w_value, small_local, tie):
    coded = code_exact(small_local, w_query.shape[0])
    first, tie = gather_grouped((w_query, w_key, w_value, coded), tie)
    widths = (w_query.shape[1], w_key.shape[1], w_value.shape[1])
    at = sum(widths)
    small_full = decode_exact(first[:, :, at:], small_local.size, small_local.shape)
    return split_grouped(first[:, :, :at], widths), small_full, tie


def gather_second(w_output, w_inner, w_outer):
    second, _ = gather_grouped((w_output, w_inner, w_outer.T))
    wo, wi, wu_t = split_grouped(second, (w_output.shape[1], w_inner.shape[1], w_outer.shape[0]))
    return (wo, wi, wu_t.T)


def reduce_seq_stage(grads, tie=None):
    dp_size = lax.psum(1, "dp")
    chunks = [grad.reshape(grad.shape[0], dp_size, grad.shape[1] // dp_size) for grad in grads]
    stacked = jnp.concatenate(chunks, axis=2).astype(jnp.bfloat16)
    stacked, tie = lax.optimization_barrier((stacked, tie))
    reduced = lax.psum_scatter(stacked, "seq", scatter_dimension=0, tiled=True)
    return (reduced, [c.shape[2] for c in chunks]), tie


def stack_for_seq(grads):
    dp_size = lax.psum(1, "dp")
    chunks = [grad.reshape(grad.shape[0], dp_size, grad.shape[1] // dp_size) for grad in grads]
    return jnp.concatenate(chunks, axis=2).astype(jnp.bfloat16), [c.shape[2] for c in chunks]


def reduce_dp_stage(stages):
    joined = jnp.concatenate([stage for stage, _ in stages], axis=2)
    over_dp = lax.psum_scatter(joined, "dp", scatter_dimension=1, tiled=True)[:, 0].astype(jnp.float32)
    pieces, at = [], 0
    for _, widths in stages:
        for width in widths:
            pieces.append(over_dp[:, at : at + width])
            at += width
    return pieces


HALF_FULL = WINDOW // 2
HALF_POOL = POOL_SPAN // 2 // STRIDE
BLOCK_POOL = CLEN // STRIDE


def layout_of(index, offsets):
    in_prompt = index < PROMPT
    segment = jnp.where(in_prompt, -1, (index - PROMPT) // CLEN)
    within = index - PROMPT - segment * CLEN
    choose = segment[..., None] == jnp.arange(CONT, dtype=jnp.int32)
    spread = offsets.reshape(offsets.shape[:1] + (1,) * (index.ndim - 1) + offsets.shape[1:])
    cont_start = jnp.sum(jnp.where(choose, spread, 0), axis=-1)
    position = jnp.where(in_prompt, index, cont_start + within)
    limit = jnp.where(in_prompt, PROMPT, cont_start)
    return segment, position, limit


def window_rows(source, starts, length):
    groups, blocks = starts.shape
    return jnp.stack(
        [
            jnp.stack(
                [lax.dynamic_slice_in_dim(source[g], starts[g, b], length, 0) for b in range(blocks)]
            )
            for g in range(groups)
        ]
    )


def window_add(target, updates, starts):
    groups, blocks = starts.shape
    length = updates.shape[2]
    rows = []
    for g in range(groups):
        row = target[g]
        for b in range(blocks):
            start = starts[g, b]
            current = lax.dynamic_slice_in_dim(row, start, length, 0)
            row = lax.dynamic_update_slice_in_dim(row, current + updates[g, b], start, 0)
        rows.append(row)
    return jnp.stack(rows)


def block_geometry(seq_index, groups, shard_rows, offsets):
    group_len = PROMPT + CONT * CLEN
    pooled_len = group_len // STRIDE
    blocks = shard_rows // CLEN
    block_start = (seq_index * blocks + jnp.arange(blocks, dtype=jnp.int32)) * CLEN
    prompt_block = block_start < PROMPT
    cont_index = jnp.clip((block_start - PROMPT) // CLEN, 0, CONT - 1)
    anchor = jnp.where(prompt_block[None, :], block_start[None, :], offsets[:, cont_index])
    pooled_start = block_start // STRIDE
    intended = (
        anchor - HALF_FULL,
        jnp.broadcast_to(block_start + CLEN, anchor.shape),
        anchor // STRIDE - HALF_POOL,
        jnp.broadcast_to(pooled_start + BLOCK_POOL, anchor.shape),
    )
    limits = (group_len, group_len, pooled_len, pooled_len)
    lengths = (HALF_FULL, HALF_FULL, HALF_POOL, HALF_POOL)
    clamped = tuple(
        jnp.clip(start, 0, limit - length) for start, limit, length in zip(intended, limits, lengths)
    )
    ramp = lambda n: jnp.arange(n, dtype=jnp.int32)

    def span(window):
        actual = clamped[window][:, :, None] + ramp(lengths[window])
        offset = actual - intended[window][:, :, None]
        return actual, (offset >= 0) & (offset < lengths[window])

    before_full, before_full_ok = span(0)
    after_full, after_full_ok = span(1)
    before_pool, before_pool_ok = span(2)
    after_pool, after_pool_ok = span(3)
    after_ok = prompt_block[None, :, None]
    own_full = jnp.broadcast_to(block_start[None, :, None] + ramp(CLEN), anchor.shape + (CLEN,))
    own_pool = jnp.broadcast_to(
        pooled_start[None, :, None] + ramp(BLOCK_POOL), anchor.shape + (BLOCK_POOL,)
    )
    full_index = jnp.concatenate([before_full, own_full, after_full], axis=2)
    pooled_index = jnp.concatenate([before_pool, own_pool, after_pool], axis=2)
    full_valid = jnp.concatenate(
        [before_full_ok, jnp.ones(own_full.shape, bool), after_ok & after_full_ok], axis=2
    )
    pooled_valid = jnp.concatenate(
        [before_pool_ok, jnp.ones(own_pool.shape, bool), after_ok & after_pool_ok], axis=2
    )
    query_index = block_start[None, :, None] + ramp(CLEN)
    query_index = jnp.broadcast_to(query_index, anchor.shape + (CLEN,))
    q_seg, q_pos, q_lim = layout_of(query_index, offsets)

    def visible(key_token, valid, reach):
        k_seg, k_pos, _ = layout_of(key_token, offsets)
        k_seg, k_pos, valid = k_seg[:, :, None, :], k_pos[:, :, None, :], valid[:, :, None, :]
        prompt_key = (k_seg < 0) & (k_pos < q_lim[..., None])
        own_key = (k_seg == q_seg[..., None]) & (q_seg[..., None] >= 0)
        distance = k_pos - q_pos[..., None]
        return valid & (prompt_key | own_key) & (distance >= -(reach // 2)) & (distance < reach // 2)

    mask = jnp.concatenate(
        [
            visible(full_index, full_valid, WINDOW),
            visible(pooled_index * STRIDE, pooled_valid, POOL_SPAN),
        ],
        axis=3,
    )
    return clamped, mask


def attention_fwd(queries, kv_local, pkv_local, kv_all, pkv_all, starts, mask):
    groups, shard_rows, width = queries.shape
    blocks = shard_rows // CLEN
    score_scale = 1.0 / HEAD_DIM**0.5
    keys_cat = jnp.concatenate(
        [
            window_rows(kv_all, starts[0], HALF_FULL),
            kv_local.reshape(groups, blocks, CLEN, 2 * width),
            window_rows(kv_all, starts[1], HALF_FULL),
            window_rows(pkv_all, starts[2], HALF_POOL),
            pkv_local.reshape(groups, blocks, BLOCK_POOL, 2 * width),
            window_rows(pkv_all, starts[3], HALF_POOL),
        ],
        axis=2,
    )
    span = keys_cat.shape[2]
    head_keys = keys_cat[..., :width].reshape(groups, blocks, span, HEADS, HEAD_DIM)
    head_values = keys_cat[..., width:].reshape(groups, blocks, span, HEADS, HEAD_DIM)
    head_query = queries.reshape(groups, blocks, CLEN, HEADS, HEAD_DIM)
    scores = jnp.einsum(
        "gbqhd,gbkhd->gbhqk", head_query, head_keys, preferred_element_type=jnp.float32
    )
    scores = jnp.where(mask[:, :, None], scores * score_scale, -1000000000.0)
    row_top = jnp.max(scores, axis=-1, keepdims=True)
    exponent = jnp.exp(scores - row_top)
    row_total = jnp.sum(exponent, axis=-1, keepdims=True)
    probs = exponent / row_total
    attended = jnp.einsum(
        "gbhqk,gbkhd->gbqhd",
        probs.astype(jnp.bfloat16),
        head_values,
        preferred_element_type=jnp.float32,
    )
    attended = attended.reshape(groups * shard_rows, width).astype(jnp.bfloat16)
    return attended, (head_query, head_keys, head_values, probs)


def attention_bwd(grad_attended, saved, starts, seq_index):
    head_query, head_keys, head_values, probs = saved
    groups, blocks = head_query.shape[:2]
    width = HEADS * HEAD_DIM
    score_scale = 1.0 / HEAD_DIM**0.5
    head_grad = grad_attended.reshape(groups, blocks, CLEN, HEADS, HEAD_DIM)
    grad_probs = jnp.einsum(
        "gbqhd,gbkhd->gbhqk", head_grad, head_values, preferred_element_type=jnp.float32
    )
    centre = jnp.sum(probs * grad_probs, axis=-1, keepdims=True)
    grad_scores = (probs * (grad_probs - centre)).astype(jnp.bfloat16)
    grad_queries = jnp.einsum(
        "gbhqk,gbkhd->gbqhd", grad_scores, head_keys, preferred_element_type=jnp.float32
    ) * score_scale
    grad_keys = jnp.einsum(
        "gbhqk,gbqhd->gbkhd", grad_scores, head_query, preferred_element_type=jnp.float32
    ) * score_scale
    grad_values = jnp.einsum(
        "gbhqk,gbqhd->gbkhd",
        probs.astype(jnp.bfloat16),
        head_grad,
        preferred_element_type=jnp.float32,
    )
    span = grad_keys.shape[2]
    grad_kv = jnp.concatenate(
        [grad_keys.reshape(groups, blocks, span, width), grad_values.reshape(groups, blocks, span, width)],
        axis=3,
    )
    shard_rows = blocks * CLEN
    group_len = PROMPT + CONT * CLEN
    pooled_len = group_len // STRIDE
    cut = (0, HALF_FULL, HALF_FULL + CLEN, 2 * HALF_FULL + CLEN)
    pcut = tuple(cut[-1] + c for c in (0, HALF_POOL, HALF_POOL + BLOCK_POOL, 2 * HALF_POOL + BLOCK_POOL))
    ramp = lambda n: jnp.arange(n, dtype=jnp.int32)
    own_full = grad_kv[:, :, cut[1] : cut[2]].reshape(groups, shard_rows, 2 * width)
    full = jnp.zeros((groups, group_len, 2 * width), jnp.float32)
    full = lax.dynamic_update_slice_in_dim(full, own_full, seq_index * shard_rows, 1)
    side_values = jnp.concatenate(
        [grad_kv[:, :, cut[0] : cut[1]], grad_kv[:, :, cut[2] : cut[3]]], axis=2
    ).reshape(groups, -1, 2 * width)
    side_rows = jnp.concatenate(
        [starts[0][:, :, None] + ramp(HALF_FULL), starts[1][:, :, None] + ramp(HALF_FULL)], axis=2
    ).reshape(groups, -1)
    own_pool_rows = (seq_index * (shard_rows // STRIDE) + ramp(blocks)[:, None] * BLOCK_POOL + ramp(BLOCK_POOL))
    pool_values = grad_kv[:, :, pcut[0] : pcut[3]].reshape(groups, -1, 2 * width)
    pool_rows_index = jnp.concatenate(
        [
            starts[2][:, :, None] + ramp(HALF_POOL),
            jnp.broadcast_to(own_pool_rows[None], (groups, blocks, BLOCK_POOL)),
            starts[3][:, :, None] + ramp(HALF_POOL),
        ],
        axis=2,
    ).reshape(groups, -1)
    fulls, pooleds, unpooleds = [], [], []
    for g in range(groups):
        fulls.append(
            full[g]
            + product(
                (side_rows[g] == ramp(group_len)[:, None]).astype(jnp.bfloat16),
                side_values[g].astype(jnp.bfloat16),
            )
        )
        pooleds.append(select_sum(pool_values[g], pool_rows_index[g] == ramp(pooled_len)[:, None]))
        unpooleds.append(
            product(
                (pool_rows_index[g] == (ramp(group_len) // STRIDE)[:, None]).astype(jnp.bfloat16),
                pool_values[g].astype(jnp.bfloat16),
            )
        )
    full = jnp.stack(fulls)
    pooled = jnp.stack(pooleds)
    unpooled = jnp.stack(unpooleds)
    grad_queries = grad_queries.reshape(groups * shard_rows, width).astype(jnp.bfloat16)
    return grad_queries, full, pooled, unpooled


def select_sum(values, chosen):
    onehot = chosen.astype(jnp.bfloat16)
    high = values.astype(jnp.bfloat16)
    low = (values - high.astype(jnp.float32)).astype(jnp.bfloat16)
    return product(onehot, high) + product(onehot, low)


def phase_weights(weight, rows):
    phase = (jnp.arange(rows, dtype=jnp.int32) % STRIDE)[:, None]
    total = jnp.zeros((rows, weight.shape[1]), jnp.float32)
    for r in range(STRIDE):
        total = total + jnp.where(phase == r, weight[r][None, :], 0.0)
    return total


def pool_grouped(source, weight):
    groups, rows, width = source.shape
    return jnp.sum(
        source.reshape(groups, rows // STRIDE, STRIDE, width) * weight[None, None], axis=2
    )


def unpool_grouped(pooled_grad, weight):
    groups, rows, width = pooled_grad.shape
    return (pooled_grad[:, :, None, :] * weight[None, None]).reshape(groups, rows * STRIDE, width)


def pool_grad_grouped(pooled_grad, source):
    groups, rows, width = source.shape
    blocks_view = source.astype(jnp.float32).reshape(groups, rows // STRIDE, STRIDE, width)
    return jnp.sum(pooled_grad[:, :, None, :] * blocks_view, axis=(0, 1))


def local(
    hidden_in,
    w_query,
    w_key,
    w_value,
    w_output,
    w_inner,
    w_outer,
    pool_weight,
    ln_gain,
    ln_bias,
    branch_blocks,
    grad_out,
):
    pool_rows_count = pool_weight.shape[0] * pool_weight.shape[1]
    small_local = jnp.concatenate(
        [pool_weight.reshape(pool_rows_count, -1), ln_gain, ln_bias], axis=0
    )
    hidden_all = lax.all_gather(hidden_in, "seq", axis=1, tiled=True)
    groups, shard_rows, width = hidden_in.shape
    seq_index = lax.axis_index("seq")
    offsets = STRIDE * branch_blocks
    starts, mask = block_geometry(seq_index, groups, shard_rows, offsets)
    (wq, wk, wv), small_full, (hidden_all, starts, mask) = gather_first(
        w_query, w_key, w_value, small_local, (hidden_all, starts, mask)
    )
    pool_full = small_full[:pool_rows_count].reshape(pool_weight.shape[0], pool_weight.shape[1], -1)
    gain_full = small_full[pool_rows_count : pool_rows_count + ln_gain.shape[0]]
    bias_full = small_full[pool_rows_count + ln_gain.shape[0] :]
    groups, shard_rows, width = hidden_in.shape

    group_len = hidden_all.shape[1]
    tokens = hidden_in.reshape(groups * shard_rows, width)
    all_tokens = hidden_all.reshape(groups * group_len, width)
    queries = product(tokens, wq).astype(jnp.bfloat16)
    key_g = product(all_tokens, wk).astype(jnp.bfloat16).reshape(groups, group_len, width)
    value_g = product(all_tokens, wv).astype(jnp.bfloat16).reshape(groups, group_len, width)
    pooled_keys = pool_grouped(key_g.astype(jnp.float32), pool_full[0]).astype(jnp.bfloat16)
    pooled_values = pool_grouped(value_g.astype(jnp.float32), pool_full[1]).astype(jnp.bfloat16)
    kv_all = jnp.concatenate([key_g, value_g], axis=2)
    pkv_all = jnp.concatenate([pooled_keys, pooled_values], axis=2)
    kv_local = lax.dynamic_slice_in_dim(kv_all, seq_index * shard_rows, shard_rows, 1)
    pkv_local = lax.dynamic_slice_in_dim(
        pkv_all, seq_index * (shard_rows // STRIDE), shard_rows // STRIDE, 1
    )
    wq, wk, wv, w_output, w_inner, w_outer = lax.optimization_barrier(
        (wq, wk, wv, w_output, w_inner, w_outer)
    )
    wo, wi, wu = gather_second(w_output, w_inner, w_outer)
    attended, att_saved = attention_fwd(
        queries.reshape(groups, shard_rows, width), kv_local, pkv_local, kv_all, pkv_all, starts, mask
    )
    mixed_rows = tokens.astype(jnp.float32) + product(attended, wo)
    normed_first = layer_norm(mixed_rows, gain_full[0], bias_full[0])
    first_low = normed_first.astype(jnp.bfloat16)
    inner_act = product(first_low, wi)
    active = jax.nn.gelu(inner_act, approximate=False).astype(jnp.bfloat16)
    second = normed_first + product(active, wu)
    norm_value, second_back = jax.vjp(layer_norm, second, gain_full[1], bias_full[1])
    output = norm_value.astype(jnp.bfloat16)

    cotangent = grad_out.reshape(groups * shard_rows, width).astype(jnp.float32)
    grad_second, gain_second, bias_second = second_back(cotangent)
    grad_ffn_out = grad_second.astype(jnp.bfloat16)
    grad_outer = product_left(active, grad_ffn_out)
    grad_active = product_right(grad_ffn_out, wu)
    gelu_value, gelu_back = jax.vjp(partial(jax.nn.gelu, approximate=False), inner_act)
    grad_inner_act = gelu_back(grad_active)[0].astype(jnp.bfloat16)
    grad_inner = product_left(first_low, grad_inner_act)
    grad_first = grad_second + product_right(grad_inner_act, wi)
    first_value, first_back = jax.vjp(layer_norm, mixed_rows, gain_full[0], bias_full[0])
    grad_mixed, gain_first, bias_first = first_back(grad_first)
    grad_branch = grad_mixed.astype(jnp.bfloat16)
    grad_output = product_left(attended, grad_branch)
    grad_attended = product_right(grad_branch, wo).astype(jnp.bfloat16)
    early, grad_attended = reduce_seq_stage((grad_output, grad_inner, grad_outer.T), grad_attended)
    early_reduced, early_widths = early

    grad_rows = grad_attended.reshape(groups, shard_rows, width)
    key_phase = phase_weights(pool_full[0], group_len)
    value_phase = phase_weights(pool_full[1], group_len)
    pieces_back = []
    for g in range(groups):
        saved_g = tuple(item[g : g + 1] for item in att_saved)
        starts_g = tuple(item[g : g + 1] for item in starts)
        grad_g = grad_rows[g].reshape(shard_rows, width)
        grad_queries_g, full_g, pooled_g, unpooled_g = attention_bwd(grad_g, saved_g, starts_g, seq_index)
        if g == 1:
            full_g, pooled_g, unpooled_g, earlier_back, early_reduced = lax.optimization_barrier(
                (full_g, pooled_g, unpooled_g, pieces_back[0][4], early_reduced)
            )
            pieces_back[0] = pieces_back[0][:4] + (earlier_back,)
        key_partial_g = (
            full_g[0, :, :width] + unpooled_g[0, :, :width] * key_phase
        ).astype(jnp.bfloat16)
        value_partial_g = (
            full_g[0, :, width:] + unpooled_g[0, :, width:] * value_phase
        ).astype(jnp.bfloat16)
        back_g = product_right(key_partial_g, wk) + product_right(value_partial_g, wv)
        back_g = back_g.reshape(1, group_len, width).astype(jnp.bfloat16)
        back_own_g = lax.psum_scatter(back_g, "seq", scatter_dimension=1, tiled=True)
        pieces_back.append((grad_queries_g, pooled_g, key_partial_g, value_partial_g, back_own_g))
    grad_queries = jnp.concatenate([piece[0] for piece in pieces_back], axis=0)
    grad_pooled = jnp.concatenate([piece[1] for piece in pieces_back], axis=0)
    key_partial = jnp.concatenate([piece[2] for piece in pieces_back], axis=0)
    value_partial = jnp.concatenate([piece[3] for piece in pieces_back], axis=0)
    last_back = pieces_back[-1][4]
    early_dp = reduce_dp_stage(((early_reduced, early_widths),))
    grad_pooling = jnp.stack(
        [
            pool_grad_grouped(grad_pooled[..., :width], key_g),
            pool_grad_grouped(grad_pooled[..., width:], value_g),
        ]
    )
    grad_query_w = product_left(tokens, grad_queries)
    grad_key_w = product_left(all_tokens, key_partial)
    grad_value_w = product_left(all_tokens, value_partial)
    late_stacked, late_widths = stack_for_seq((grad_query_w, grad_key_w, grad_value_w))
    late_stacked, early_dp = lax.optimization_barrier((late_stacked, early_dp))
    seq_size = lax.psum(1, "seq")
    dp_size = lax.psum(1, "dp")
    rows_each = late_stacked.shape[0] // seq_size
    late_blocks = late_stacked.reshape(seq_size, rows_each, dp_size, late_stacked.shape[2])
    late_blocks = jnp.transpose(late_blocks, (2, 0, 1, 3)).reshape(-1, late_stacked.shape[2])
    late_reduced = lax.psum_scatter(late_blocks, ("dp", "seq"), scatter_dimension=0, tiled=True)
    late_reduced = late_reduced.astype(jnp.float32)
    late_dp, at = [], 0
    for width_piece in late_widths:
        late_dp.append(late_reduced[:, at : at + width_piece])
        at += width_piece
    back_own = jnp.concatenate([piece[4] for piece in pieces_back], axis=0)
    grad_tokens = (
        grad_mixed
        + product_right(grad_queries, wq)
        + back_own.reshape(groups * shard_rows, width).astype(jnp.float32)
    )
    accum = (late_dp[0], late_dp[1], late_dp[2], early_dp[0], early_dp[1], early_dp[2].T)
    small_sums = (
        lax.psum_scatter(grad_pooling, ("dp", "seq"), scatter_dimension=2, tiled=True),
        lax.psum_scatter(
            jnp.stack([gain_first, gain_second]), ("dp", "seq"), scatter_dimension=1, tiled=True
        ),
        lax.psum_scatter(
            jnp.stack([bias_first, bias_second]), ("dp", "seq"), scatter_dimension=1, tiled=True
        ),
    )
    return (
        output.reshape(groups, shard_rows, width),
        grad_tokens.astype(jnp.bfloat16).reshape(groups, shard_rows, width),
        accum[0],
        accum[1],
        accum[2],
        accum[3],
        accum[4],
        accum[5],
        small_sums[0],
        small_sums[1],
        small_sums[2],
    )


def solution(mesh):
    in_specs = (
        P("dp", "seq", None),
        P("seq", "dp"),
        P("seq", "dp"),
        P("seq", "dp"),
        P("seq", "dp"),
        P("seq", "dp"),
        P("dp", "seq"),
        P(None, None, ("dp", "seq")),
        P(None, ("dp", "seq")),
        P(None, ("dp", "seq")),
        P("dp", None),
        P("dp", "seq", None),
    )
    out_specs = (
        P("dp", "seq", None),
        P("dp", "seq", None),
        P("seq", "dp"),
        P("seq", "dp"),
        P("seq", "dp"),
        P("seq", "dp"),
        P("seq", "dp"),
        P("dp", "seq"),
        P(None, None, ("dp", "seq")),
        P(None, ("dp", "seq")),
        P(None, ("dp", "seq")),
    )
    return jax.shard_map(local, mesh=mesh, in_specs=in_specs, out_specs=out_specs, check_vma=False)
```
